32 devices in a mesh: dp: 16 (over z, y, core), tensor: 2 (over x).
Axes of the slice: x: 2, y: 2, z: 4, core: 2. Of those that a mesh axis runs over, the one named last changes fastest.
Arguments:
- tokens: bfloat16 [8192, 2048], P(('dp', 'tensor')), may hold values from -6 to 6
- seg_ids: int32 [16, 512], P('dp'), may hold values from 0 to 1, as said below
- w_query: bfloat16 [2048, 2048], P('dp', 'tensor'), may hold values from -0.125 to 0.125
- w_key: bfloat16 [2048, 1024], P('dp', 'tensor'), may hold values from -0.125 to 0.125
- w_value: bfloat16 [2048, 1024], P('dp', 'tensor'), may hold values from -0.125 to 0.125
- w_output: bfloat16 [2048, 2048], P('tensor', 'dp'), may hold values from -0.5 to 0.5
- w_gate: bfloat16 [2048, 6144], P('dp', 'tensor'), may hold values from -0.125 to 0.125
- w_up: bfloat16 [2048, 6144], P('dp', 'tensor'), may hold values from -0.125 to 0.125
- w_down: bfloat16 [6144, 2048], P('tensor', 'dp'), may hold values from -0.078125 to 0.078125
- gain_attn: bfloat16 [2048], P('dp'), may hold values from 0.5 to 1.5
- gain_mlp: bfloat16 [2048], P('dp'), may hold values from 0.5 to 1.5
- gain_qk: bfloat16 [256], P('dp'), may hold values from 0.5 to 1.5
- cotangent: bfloat16 [8192, 2048], P(('dp', 'tensor')), may hold values from -6 to 6
Outputs:
- result: bfloat16 [8192, 2048], P(('dp', 'tensor'))
- input_grad: bfloat16 [8192, 2048], P(('dp', 'tensor'))
- grad_query: float32 [2048, 2048], P('dp', 'tensor')
- grad_key: float32 [2048, 1024], P('dp', 'tensor')
- grad_value: float32 [2048, 1024], P('dp', 'tensor')
- grad_output: float32 [2048, 2048], P('tensor', 'dp')
- grad_gate: float32 [2048, 6144], P('dp', 'tensor')
- grad_up: float32 [2048, 6144], P('dp', 'tensor')
- grad_down: float32 [6144, 2048], P('tensor', 'dp')
- grad_gain_attn: float32 [2048], P('dp')
- grad_gain_mlp: float32 [2048], P('dp')
- grad_gain_qk: float32 [256], P('dp')
The draws below stay inside these ranges and needn't reach their ends.
Inputs may be any that keep to these rules, and one draw needn't show every extreme that they name: `seg_ids`: within each sequence the ids never fall and cover all 2 documents, each of 200 tokens or more.
All inputs are finite; a program needn't handle non-finite values.
Results may differ from the reference program's by a relative error of at most 0.017.
Values may be sent and summed in bfloat16 or wider, within the bound.
A program may use at most 256 MiB of HBM per device.

```python
import jax
import jax.numpy as jnp
from jax import lax

D = 2048
QH = 16
KVH = 8
HD = 128
FF = 6144
DOCS = 2
MIN_DOC = 200
SEQ = 512
SEQS = 16
TOKENS = 8192


def draw_seg_ids(key, part):
    spare = SEQ - DOCS * MIN_DOC
    cuts = jax.random.randint(key, (SEQS, DOCS - 1), 0, spare + 1).astype(jnp.int32)
    cuts = jnp.sort(cuts, axis=1)
    offsets = (jnp.arange(1, DOCS, dtype=jnp.int32) * MIN_DOC)[None, :]
    starts = cuts + offsets
    places = jnp.arange(SEQ, dtype=jnp.int32)
    return jnp.sum((places[None, None, :] >= starts[:, :, None]).astype(jnp.int32), axis=1)


def with_spikes(values, own_key, source, target, shards_of, factor):
    def block_of(dim):
        return (jnp.arange(values.shape[dim]) // (values.shape[dim] // shards_of)).reshape((-1,) + (1,) * (values.ndim - 1 - dim))

    one_side = jax.random.permutation(own_key, shards_of)[block_of(target)]
    second = (block_of(target) + shards_of // 2) % shards_of
    return jnp.where((block_of(source) == one_side) | (block_of(source) == second), factor * values, values)


def levels(stream_key, dims, cuts, low, largest):
    def one(axis_at, shards_of):
        heights = jax.random.uniform(jax.random.fold_in(jax.random.fold_in(stream_key, 6), axis_at), (shards_of,), jnp.float32, low / len(cuts), largest / len(cuts))
        return jnp.repeat(jnp.exp(heights), dims[axis_at] // shards_of).reshape((-1,) + (1,) * (len(dims) - axis_at - 1))

    level = one(*cuts[0])
    for cut in cuts[1:]:
        level = level * one(*cut)
    return level


def gaussian(stream_key, dims, width, reach, split=(), kind=jnp.bfloat16):
    factor_of = levels(stream_key, dims, split, -0.22, 0.18) if split else 1.0
    array = jax.random.normal(stream_key, dims, jnp.float32) * width * factor_of
    return jnp.minimum(jnp.maximum(array, -reach), reach).astype(kind)


def gaussian_with(key, dims, spread, limit, pieces, heavy, kind=jnp.bfloat16):
    values = spread * jax.random.normal(key, dims, jnp.float32)
    if pieces:
        values = values * levels(key, dims, pieces, -0.22, 0.18)
    return jnp.clip(with_spikes(values, jax.random.fold_in(key, 3), *heavy), -limit, limit).astype(kind)


def setup_inputs(seed: int = 0) -> dict:
    streams_of = jax.random.split(jax.random.key(seed), 14)
    tokens = gaussian_with(streams_of[0], (TOKENS, D), 1.0, 6.0, ((0, 32),), (0, 1, 32, 2.75))
    seg_ids = draw_seg_ids(jax.random.fold_in(streams_of[13], 71), 0)
    w_query = gaussian(streams_of[2], (D, QH * HD), D ** -0.5, 0.125, ((0, 16), (1, 2)))
    w_key = gaussian(streams_of[3], (D, KVH * HD), D ** -0.5, 0.125, ((0, 16), (1, 2)))
    w_value = gaussian(streams_of[4], (D, KVH * HD), D ** -0.5, 0.125, ((0, 16), (1, 2)))
    w_output = gaussian(streams_of[5], (QH * HD, D), (QH * HD // 16) ** -0.5, 0.5, ((0, 2), (1, 16)))
    w_gate = gaussian(streams_of[6], (D, FF), D ** -0.5, 0.125, ((0, 16), (1, 2)))
    w_up = gaussian(streams_of[7], (D, FF), D ** -0.5, 0.125, ((0, 16), (1, 2)))
    w_down = gaussian(streams_of[8], (FF, D), FF ** -0.5, 0.078125, ((0, 2), (1, 16)))
    gain_attn = jnp.clip(1.0 + 0.1 * jax.random.normal(streams_of[9], (D,), jnp.float32), 0.5, 1.5).astype(jnp.bfloat16)
    gain_mlp = jnp.clip(1.0 + 0.1 * jax.random.normal(streams_of[10], (D,), jnp.float32), 0.5, 1.5).astype(jnp.bfloat16)
    gain_qk = jnp.clip(1.0 + 0.1 * jax.random.normal(streams_of[11], (2 * HD,), jnp.float32), 0.5, 1.5).astype(jnp.bfloat16)
    cotangent = gaussian_with(streams_of[12], (TOKENS, D), 1.0, 6.0, ((0, 32),), (0, 1, 32, 2.75))
    return dict(tokens=tokens, seg_ids=seg_ids, w_query=w_query, w_key=w_key, w_value=w_value, w_output=w_output, w_gate=w_gate, w_up=w_up, w_down=w_down, gain_attn=gain_attn, gain_mlp=gain_mlp, gain_qk=gain_qk, cotangent=cotangent)


epsilon = 1e-06
rope_base = 1000000.0
highest = lax.Precision.HIGHEST

@jax.custom_vjp
def low(v):
    return lax.optimization_barrier(v.astype(jnp.bfloat16)).astype(jnp.float32)

@jax.custom_vjp
def low_back(v):
    return v

def low_keep(v):
    return (low(v), None)

def low_pass(kept, grad):
    return (grad,)

def back_keep(v):
    return (v, None)

def back_low(kept, grad):
    return (low(grad),)
low.defvjp(low_keep, low_pass)
low_back.defvjp(back_keep, back_low)

def product(left, right):
    return jnp.dot(left, right, precision=highest, preferred_element_type=jnp.float32)

def rms_scaled(values, norm_gain):
    return values * lax.rsqrt(lax.optimization_barrier(jnp.mean(values * values, axis=-1, keepdims=True)) + epsilon) * norm_gain

def rotate(values, cosine_table, sine_table):
    half_width = values.shape[-1] // 2
    turned = jnp.concatenate([-values[..., half_width:], values[..., :half_width]], axis=-1)
    return values * cosine_table + turned * sine_table

def tables(segments):
    seq_len = segments.shape[0]
    token_index = jnp.arange(seq_len, dtype=jnp.int32)
    doc_start = lax.optimization_barrier(jnp.sum((segments[None, :] < segments[:, None]).astype(jnp.int32), axis=1))
    doc_pos = (token_index - doc_start).astype(jnp.float32)
    frequency = rope_base ** (-jnp.arange(0, HD, 2).astype(jnp.float32) / HD)
    angles = doc_pos[:, None] * frequency[None, :]
    cosine_table = jnp.concatenate([jnp.cos(angles), jnp.cos(angles)], axis=1)
    sine_table = jnp.concatenate([jnp.sin(angles), jnp.sin(angles)], axis=1)
    allowed = (segments[:, None] == segments[None, :]) & (token_index[None, :] <= token_index[:, None])
    return (cosine_table, sine_table, allowed)

def layer(input_rows, params, cosine_table, sine_table, allowed):
    q_weight, k_weight, v_weight, o_weight, gate_weight, up_weight, down_weight, attn_gain, mlp_gain, qk_gain = params
    seq_len = input_rows.shape[0]
    per_group = QH // KVH
    cosine_heads = cosine_table[:, None, :]
    sine_heads = sine_table[:, None, :]
    normed_one = low(rms_scaled(input_rows, attn_gain))
    query_raw = low_back(product(normed_one, q_weight)).reshape(seq_len, QH, HD)
    key_raw = low_back(product(normed_one, k_weight)).reshape(seq_len, KVH, HD)
    value_heads = low(low_back(product(normed_one, v_weight))).reshape(seq_len, KVH, HD)
    query_rot = low(rotate(rms_scaled(query_raw, qk_gain[:HD]), cosine_heads, sine_heads)).reshape(seq_len, KVH, per_group, HD)
    key_rot = low(rotate(rms_scaled(key_raw, qk_gain[HD:]), cosine_heads, sine_heads))
    scores = low_back(jnp.einsum('sgrd,tgd->grst', query_rot, key_rot, precision=highest) * HD ** (-0.5))
    exp_scores = jnp.where(allowed, jnp.exp(scores), 0.0)
    probs = low(exp_scores / lax.optimization_barrier(jnp.sum(exp_scores, axis=-1, keepdims=True)))
    attn_heads = jnp.einsum('grst,tgd->sgrd', probs, value_heads, precision=highest)
    attn_rows = low(low_back(attn_heads)).reshape(seq_len, QH * HD)
    resid = input_rows + low_back(product(attn_rows, o_weight))
    normed_two = low(rms_scaled(resid, mlp_gain))
    gate_rows = low_back(product(normed_two, gate_weight))
    up_rows = low_back(product(normed_two, up_weight))
    act_rows = low(jax.nn.silu(gate_rows) * up_rows)
    return resid + low_back(product(act_rows, down_weight))

def reference(tokens, seg_ids, w_query, w_key, w_value, w_output, w_gate, w_up, w_down, gain_attn, gain_mlp, gain_qk, cotangent):
    params = tuple((weight.astype(jnp.float32) for weight in (w_query, w_key, w_value, w_output, w_gate, w_up, w_down, gain_attn, gain_mlp, gain_qk)))
    input_seqs = tokens.astype(jnp.float32).reshape(SEQS, SEQ, D)
    cot_seqs = cotangent.astype(jnp.float32).reshape(SEQS, SEQ, D)
    zeros_init = tuple((jnp.zeros_like(weight) for weight in params))

    def one_seq(running, item):
        input_rows, cot_rows, segments = item
        cosine_table, sine_table, allowed = tables(segments)

        def forward(rows_in, weights_in):
            return layer(rows_in, weights_in, cosine_table, sine_table, allowed)
        output_rows, backward = jax.vjp(forward, input_rows, params)
        grad_rows, grad_params = backward(cot_rows)
        running = tuple((first + second for first, second in zip(running, grad_params)))
        return (running, (output_rows.astype(jnp.bfloat16), grad_rows.astype(jnp.bfloat16)))
    totals, outputs = lax.scan(one_seq, zeros_init, (input_seqs, cot_seqs, seg_ids))
    result_rows = outputs[0].reshape(TOKENS, D)
    input_grad = outputs[1].reshape(TOKENS, D)
    return (result_rows, input_grad, totals[0], totals[1], totals[2], totals[3], totals[4], totals[5], totals[6], totals[7], totals[8], totals[9])
```

```python
import functools
import jax
import jax.numpy as jnp
from jax import lax
from jax.experimental import pallas as pl
from jax.experimental.pallas import tpu as pltpu

from jax.sharding import PartitionSpec as P

MESH = pl.DeviceIdType.MESH
HD = 128
epsilon = 1e-06
rope_base = 1000000.0


def ring_place(n):
    me = lax.axis_index("dp")
    chip = me // 2
    core = me % 2
    odd = chip % 2
    pos = (1 - odd) * (chip // 2) + odd * (n - 1 - chip // 2)
    return pos, core


def chip_at(pos, n):
    high = pos // (n // 2)
    return (1 - high) * (2 * pos) + high * (2 * (n - 1 - pos) + 1)


def at(pos, core, n):
    return (chip_at(pos, n) * 2 + core, lax.axis_index("tensor"))


def meet(peers):
    barrier = pltpu.get_barrier_semaphore()
    for peer in peers:
        pl.semaphore_signal(barrier, inc=1, device_id=peer, device_id_type=MESH)
    pl.semaphore_wait(barrier, len(peers))


def remote(src, dst, send, recv, peer):
    return pltpu.make_async_remote_copy(
        src_ref=src, dst_ref=dst, send_sem=send, recv_sem=recv, device_id=peer, device_id_type=MESH
    )


def gather_kernel(n, parts, count, swaps, *refs):
    shards = refs[:count]
    halves = refs[count : count + swaps]
    fulls = refs[count + swaps : 2 * count + swaps]
    wholes = refs[2 * count + swaps : 2 * (count + swaps)]
    own_sem, send_sem, recv_sem, give_sem, take_sem, swap_sem = refs[2 * (count + swaps) :]
    pos, core = ring_place(n)
    lane = lax.axis_index("tensor")
    nexts = (at((pos + 1) % n, core, n), at((pos + n - 1) % n, core, n))
    mate = at(pos, 1 - core, n)
    twin = (lax.axis_index("dp"), 1 - lane)
    meet((*nexts, mate, twin))
    messages = [(w, part) for w in range(count) for part in range(parts[w])]

    def sizes(w):
        rows = shards[w].shape[0]
        return rows, rows // 2, rows // 2 // parts[w]

    def spot(w, owner, who, side, part):
        rows, half, piece = sizes(w)
        start = (chip_at(owner, n) * 2 + who) * rows + (side * half + part * piece)
        return fulls[w].at[pl.ds(pl.multiple_of(start, piece), piece)]

    def shard_of(w, who):
        rows = shards[w].shape[0]
        return fulls[w].at[pl.ds(pl.multiple_of((chip_at(pos, n) * 2 + who) * rows, rows), rows)]

    def swap_spot(s, which):
        rows = halves[s].shape[0]
        return wholes[s].at[pl.ds(pl.multiple_of(which * rows, rows), rows)]

    for k, (w, part) in enumerate(messages):
        rows, half, piece = sizes(w)
        for side in range(2):
            src = shards[w].at[pl.ds(side * half + part * piece, piece)]
            remote(
                src, spot(w, pos, core, side, part), send_sem.at[k, side, 0], recv_sem.at[k, side, 0], nexts[side]
            ).start()
    for s in range(swaps):
        remote(halves[s], swap_spot(s, lane), swap_sem.at[s, 0], swap_sem.at[s, 1], twin).start()
        pltpu.make_async_copy(halves[s], swap_spot(s, lane), own_sem.at[count + s]).start()
    for w in range(count):
        remote(shards[w], shard_of(w, core), give_sem.at[w, 0, n - 1], take_sem.at[w, 0, n - 1], mate).start()
        pltpu.make_async_copy(shards[w], shard_of(w, core), own_sem.at[w]).start()

    def owner_of(side, step):
        if side == 0:
            return (pos - 1 - step + 2 * n) % n
        return (pos + 1 + step) % n

    def step_body(step, carry):
        for k, (w, part) in enumerate(messages):
            for side in range(2):
                block = spot(w, owner_of(side, step), core, side, part)
                remote(block, block, send_sem.at[k, side, step], recv_sem.at[k, side, step], nexts[side]).wait_recv()

                @pl.when(step < n - 2)
                def _():
                    remote(
                        block, block, send_sem.at[k, side, step + 1], recv_sem.at[k, side, step + 1], nexts[side]
                    ).start()

                remote(block, block, give_sem.at[k, side, step], take_sem.at[k, side, step], mate).start()
        return carry

    lax.fori_loop(0, n - 1, step_body, 0)

    def drain(step, carry):
        for k, (w, part) in enumerate(messages):
            for side in range(2):
                owner = owner_of(side, step)
                block = spot(w, owner, core, side, part)
                theirs = spot(w, owner, 1 - core, side, part)
                remote(block, block, send_sem.at[k, side, step], recv_sem.at[k, side, step], nexts[side]).wait_send()
                given = remote(block, theirs, give_sem.at[k, side, step], take_sem.at[k, side, step], mate)
                given.wait_send()
                given.wait_recv()
        return carry

    lax.fori_loop(0, n - 1, drain, 0)
    for w in range(count):
        pltpu.make_async_copy(shards[w], shard_of(w, core), own_sem.at[w]).wait()
        given = remote(shards[w], shard_of(w, 1 - core), give_sem.at[w, 0, n - 1], take_sem.at[w, 0, n - 1], mate)
        given.wait_send()
        given.wait_recv()
    for s in range(swaps):
        pltpu.make_async_copy(halves[s], swap_spot(s, lane), own_sem.at[count + s]).wait()
        other = remote(halves[s], swap_spot(s, 1 - lane), swap_sem.at[s, 0], swap_sem.at[s, 1], twin)
        other.wait_send()
        other.wait_recv()


def gather_weights(shards, swaps, parts, dp, collective_id):
    n = dp // 2
    count = len(shards)
    msgs = sum(parts)
    dma = pltpu.SemaphoreType.DMA
    outs = pl.pallas_call(
        functools.partial(gather_kernel, n, tuple(parts), count, len(swaps)),
        out_shape=[
            *[jax.ShapeDtypeStruct((s.shape[0] * dp, s.shape[1]), s.dtype) for s in shards],
            *[jax.ShapeDtypeStruct((s.shape[0] * 2, s.shape[1]), s.dtype) for s in swaps],
        ],
        in_specs=[pl.BlockSpec(memory_space=pltpu.VMEM)] * (count + len(swaps)),
        out_specs=[pl.BlockSpec(memory_space=pltpu.HBM)] * (count + len(swaps)),
        scratch_shapes=[
            dma((count + len(swaps),)),
            dma((msgs, 2, n - 1)),
            dma((msgs, 2, n - 1)),
            dma((msgs, 2, n)),
            dma((msgs, 2, n)),
            dma((max(1, len(swaps)), 2)),
        ],
        compiler_params=pltpu.CompilerParams(collective_id=collective_id, has_side_effects=True),
    )(*shards, *swaps)
    return outs[:count], outs[count:]


def reduce_kernel(n, pairs, *refs):
    n_left = 1 + max(p[0] for p in pairs)
    n_right = 1 + max(p[1] for p in pairs)
    count = len(pairs)
    lefts = refs[:n_left]
    rights = refs[n_left : n_left + n_right]
    outs = refs[n_left + n_right : n_left + n_right + count]
    rest = refs[n_left + n_right + count :]
    mine, give, take, ship, land = (rest[i * count : (i + 1) * count] for i in range(5))
    term, give_sem, take_sem, ship_sem, land_sem = rest[5 * count :]
    pos, core = ring_place(n)
    nexts = (at((pos + 1) % n, core, n), at((pos + n - 1) % n, core, n))
    mate = at(pos, 1 - core, n)
    meet((*nexts, mate))
    rows = outs[0].shape[0]

    def owner_of(side, step):
        if side == 0:
            return (pos - 1 - step + 2 * n) % n
        return (pos + 1 + step) % n

    def early(m, side, step):
        left, right = pairs[m]
        wide = outs[m].shape[1] // 2
        slot = step % 2
        start = pl.multiple_of(chip_at(owner_of(side, step), n) * 2 * rows, 2 * rows)
        part = term.at[:, pl.ds(0, wide)]
        part[...] = jnp.dot(
            lefts[left][pl.ds(start, 2 * rows), :],
            rights[right][:, pl.ds(side * wide, wide)],
            preferred_element_type=jnp.float32,
        )
        other = pl.ds(pl.multiple_of((1 - core) * rows, rows), rows)
        same = pl.ds(pl.multiple_of(core * rows, rows), rows)
        given = remote(
            give[m].at[side, slot], take[m].at[side, slot],
            give_sem.at[m, side, slot], take_sem.at[m, side, slot], mate,
        )

        @pl.when(step >= 2)
        def _():
            given.wait_send()

        give[m][side, slot] = part[other, :].astype(jnp.bfloat16)
        given.start()
        mine[m][side] = part[same, :]

    def shipped(m, side, step):
        return remote(
            ship[m].at[side, step % 2], land[m].at[side, step],
            ship_sem.at[m, side, step % 2], land_sem.at[m, side, step], nexts[side],
        )

    def local_sum(m, side, step):
        slot = step % 2
        remote(
            give[m].at[side, slot], take[m].at[side, slot],
            give_sem.at[m, side, slot], take_sem.at[m, side, slot], mate,
        ).wait_recv()
        return mine[m][side] + take[m][side, slot].astype(jnp.float32)

    for m in range(count):
        for side in range(2):
            early(m, side, 0)
    for m in range(count):
        for side in range(2):
            total = local_sum(m, side, 0)
            ship[m][side, 0] = total.astype(jnp.bfloat16)
            shipped(m, side, 0).start()
            early(m, side, 1)

    def step_body(step, carry):
        for m in range(count):
            for side in range(2):
                total = local_sum(m, side, step)
                shipped(m, side, step - 1).wait_recv()
                total = total + land[m][side, step - 1].astype(jnp.float32)

                @pl.when(step >= 2)
                def _():
                    shipped(m, side, step - 2).wait_send()

                ship[m][side, step % 2] = total.astype(jnp.bfloat16)
                shipped(m, side, step).start()
                early(m, side, step + 1)
        return carry

    lax.fori_loop(1, n - 1, step_body, 0)
    last = n - 1
    for m in range(count):
        wide = outs[m].shape[1] // 2
        for side in range(2):
            total = local_sum(m, side, last)
            shipped(m, side, last - 1).wait_recv()
            outs[m][:, pl.ds(side * wide, wide)] = total + land[m][side, last - 1].astype(jnp.float32)
    for m in range(count):
        for side in range(2):
            shipped(m, side, last - 1).wait_send()
            if last >= 2:
                shipped(m, side, last - 2).wait_send()
            for slot in range(2):
                remote(
                    give[m].at[side, slot], take[m].at[side, slot],
                    give_sem.at[m, side, slot], take_sem.at[m, side, slot], mate,
                ).wait_send()


def reduce_grads(lefts, rights, pairs, dp, collective_id):
    n = dp // 2
    count = len(pairs)
    rows = lefts[0].shape[0] // dp
    wides = [rights[r].shape[1] // 2 for _, r in pairs]
    low = jnp.bfloat16
    return pl.pallas_call(
        functools.partial(reduce_kernel, n, tuple(pairs)),
        out_shape=[jax.ShapeDtypeStruct((rows, 2 * w), jnp.float32) for w in wides],
        in_specs=[pl.BlockSpec(memory_space=pltpu.VMEM)] * (len(lefts) + len(rights)),
        out_specs=[pl.BlockSpec(memory_space=pltpu.VMEM)] * count,
        scratch_shapes=[
            *[pltpu.VMEM((2, rows, w), jnp.float32) for w in wides],
            *[pltpu.VMEM((2, 2, rows, w), low) for w in wides],
            *[pltpu.VMEM((2, 2, rows, w), low) for w in wides],
            *[pltpu.VMEM((2, 2, rows, w), low) for w in wides],
            *[pltpu.VMEM((2, n - 1, rows, w), low) for w in wides],
            pltpu.VMEM((2 * rows, max(wides)), jnp.float32),
            pltpu.SemaphoreType.DMA((count, 2, 2)),
            pltpu.SemaphoreType.DMA((count, 2, 2)),
            pltpu.SemaphoreType.DMA((count, 2, 2)),
            pltpu.SemaphoreType.DMA((count, 2, n - 1)),
        ],
        compiler_params=pltpu.CompilerParams(
            collective_id=collective_id, has_side_effects=True, vmem_limit_bytes=67043328
        ),
    )(*lefts, *rights)


def product(left, right):
    return jnp.dot(left, right, preferred_element_type=jnp.float32)


def lead_product(left, right):
    return lax.dot_general(
        left, right, (((0,), (0,)), ((), ())), preferred_element_type=jnp.float32
    )


def tail_product(left, right):
    return lax.dot_general(
        left, right, (((1,), (1,)), ((), ())), preferred_element_type=jnp.float32
    )


def norm_rows(values):
    return lax.rsqrt(jnp.mean(values * values, axis=-1, keepdims=True) + epsilon)


def norm_back(incoming, normed, inverse):
    return inverse * (incoming - normed * jnp.mean(incoming * normed, axis=-1, keepdims=True))


def rotate(values, cosine_table, sine_table):
    half_width = values.shape[-1] // 2
    turned = jnp.concatenate([-values[..., half_width:], values[..., :half_width]], axis=-1)
    return values * cosine_table + turned * sine_table


def rotate_back(incoming, cosine_table, sine_table):
    half_width = incoming.shape[-1] // 2
    scaled = incoming * sine_table
    return incoming * cosine_table + jnp.concatenate(
        [scaled[..., half_width:], -scaled[..., :half_width]], axis=-1
    )


def tables(segments):
    seq_len = segments.shape[0]
    token_index = jnp.arange(seq_len, dtype=jnp.int32)
    doc_start = jnp.sum((segments[None, :] < segments[:, None]).astype(jnp.int32), axis=1)
    doc_pos = (token_index - doc_start).astype(jnp.float32)
    frequency = rope_base ** (-jnp.arange(0, HD, 2).astype(jnp.float32) / HD)
    angles = doc_pos[:, None] * frequency[None, :]
    cosine_table = jnp.concatenate([jnp.cos(angles), jnp.cos(angles)], axis=1)
    sine_table = jnp.concatenate([jnp.sin(angles), jnp.sin(angles)], axis=1)
    allowed = (segments[:, None] == segments[None, :]) & (
        token_index[None, :] <= token_index[:, None]
    )
    return (cosine_table, sine_table, allowed)


def on_device(
    tokens,
    seg_ids,
    w_query,
    w_key,
    w_value,
    w_output,
    w_gate,
    w_up,
    w_down,
    gain_attn,
    gain_mlp,
    gain_qk,
    cotangent,
):
    dp = lax.axis_size("dp")
    input_rows = tokens.astype(jnp.float32)
    model = input_rows.shape[1]
    inverse_one = norm_rows(input_rows)
    normed_one = input_rows * inverse_one
    gain_row = jnp.concatenate(
        [
            jnp.pad(g.astype(jnp.float32), (0, 128 - g.shape[0]))
            for g in (gain_attn, gain_mlp, gain_qk)
        ]
    )
    gain_shard = jnp.broadcast_to(gain_row[None, :], (16, gain_row.shape[0]))
    shard_qkv = jnp.concatenate([w_query, w_key, w_value], axis=1)
    (qkv_weight, out_weight, gain_all), (full_rows, full_cot) = gather_weights(
        [shard_qkv, w_output.T, gain_shard], [tokens, cotangent], [2, 1, 1], dp, 0
    )
    gain_all = gain_all.reshape(dp, 16, 3, 128)[:, 0]
    attn_gain = gain_all[:, 0, : gain_attn.shape[0]].reshape(-1)
    full_rows = full_rows.astype(jnp.float32)
    full_one = (full_rows * norm_rows(full_rows) * attn_gain).astype(jnp.bfloat16)
    mlp_gain = gain_all[:, 1, : gain_mlp.shape[0]].reshape(-1)
    qk_gain = gain_all[:, 2, : gain_qk.shape[0]].reshape(-1)
    query_gain = qk_gain[:HD]
    key_gain = qk_gain[HD:]
    score_scale = HD ** (-0.5)
    cosine_table, sine_table, allowed = tables(seg_ids[0])
    cosine_heads = cosine_table[:, None, :]
    sine_heads = sine_table[:, None, :]
    seq_len = full_one.shape[0]
    q_width = w_query.shape[1]
    kv_width = w_key.shape[1]
    q_heads = q_width // HD
    kv_heads = kv_width // HD
    per_group = q_heads // kv_heads
    projected = product(full_one, qkv_weight)
    query_raw = projected[:, :q_width].reshape(seq_len, q_heads, HD)
    key_raw = projected[:, q_width : q_width + kv_width].reshape(seq_len, kv_heads, HD)
    value_all = (
        projected[:, q_width + kv_width :].astype(jnp.bfloat16).reshape(seq_len, kv_heads, HD)
    )
    query_inverse = norm_rows(query_raw)
    query_hat = query_raw * query_inverse
    query_rot = (
        rotate(query_hat * query_gain, cosine_heads, sine_heads)
        .astype(jnp.bfloat16)
        .reshape(seq_len, kv_heads, per_group, HD)
    )
    key_inverse = norm_rows(key_raw)
    key_hat = key_raw * key_inverse
    key_all = rotate(key_hat * key_gain, cosine_heads, sine_heads).astype(jnp.bfloat16)
    scores = (
        jnp.einsum("sgrd,tgd->grst", query_rot, key_all, preferred_element_type=jnp.float32)
        * score_scale
    )
    exp_scores = jnp.where(allowed, jnp.exp(scores), 0.0)
    row_totals = jnp.sum(exp_scores, axis=-1, keepdims=True)
    log_totals = jnp.log(row_totals)
    probs_low = (exp_scores / row_totals).astype(jnp.bfloat16)
    attn_heads = jnp.einsum(
        "grst,tgd->sgrd", probs_low, value_all, preferred_element_type=jnp.float32
    )
    attn_rows = attn_heads.astype(jnp.bfloat16).reshape(seq_len, q_heads * HD)
    attn_branch = lax.psum_scatter(
        tail_product(attn_rows, out_weight).astype(jnp.bfloat16),
        "tensor",
        scatter_dimension=0,
        tiled=True,
    ).astype(jnp.float32)
    resid = input_rows + attn_branch
    inverse_two = norm_rows(resid)
    normed_two = resid * inverse_two
    full_two = lax.all_gather(
        (normed_two * mlp_gain).astype(jnp.bfloat16), "tensor", axis=0, tiled=True
    )
    (gate_weight, up_weight, down_weight), _ = gather_weights(
        [w_gate, w_up, w_down.T], [], [1, 1, 1], dp, 1
    )
    gate_rows = product(full_two, gate_weight)
    up_rows = product(full_two, up_weight)
    gate_sig = jax.nn.sigmoid(gate_rows)
    act_rows = (gate_rows * gate_sig * up_rows).astype(jnp.bfloat16)
    mlp_branch = lax.psum_scatter(
        tail_product(act_rows, down_weight).astype(jnp.bfloat16),
        "tensor",
        scatter_dimension=0,
        tiled=True,
    ).astype(jnp.float32)
    result_rows = (resid + mlp_branch).astype(jnp.bfloat16)
    cot_rows = cotangent.astype(jnp.float32)
    d_act = product(full_cot, down_weight)
    d_gate = (d_act * up_rows * gate_sig * (1.0 + gate_rows * (1.0 - gate_sig))).astype(
        jnp.bfloat16
    )
    d_up = (d_act * gate_rows * gate_sig).astype(jnp.bfloat16)
    grad_gate, grad_up, grad_down = reduce_grads(
        [full_two.T, full_cot.T], [d_gate, d_up, act_rows], [(0, 0), (0, 1), (1, 2)], dp, 2
    )
    d_normed_two = lax.psum_scatter(
        (tail_product(d_gate, gate_weight) + tail_product(d_up, up_weight)).astype(jnp.bfloat16),
        "tensor",
        scatter_dimension=0,
        tiled=True,
    ).astype(jnp.float32)
    mlp_gain_part = jnp.sum(d_normed_two * normed_two, axis=0)
    d_resid = cot_rows + norm_back(d_normed_two * mlp_gain, normed_two, inverse_two)
    full_resid = lax.all_gather(d_resid.astype(jnp.bfloat16), "tensor", axis=0, tiled=True)
    d_attn = (
        product(full_resid, out_weight)
        .astype(jnp.bfloat16)
        .reshape(seq_len, kv_heads, per_group, HD)
    )
    scores_again = (
        jnp.einsum("sgrd,tgd->grst", query_rot, key_all, preferred_element_type=jnp.float32)
        * score_scale
    )
    probs_again = jnp.where(allowed, jnp.exp(scores_again - log_totals), 0.0)
    d_value_all = jnp.einsum(
        "grst,sgrd->tgd",
        probs_again.astype(jnp.bfloat16),
        d_attn,
        preferred_element_type=jnp.float32,
    )
    d_probs = jnp.einsum("sgrd,tgd->grst", d_attn, value_all, preferred_element_type=jnp.float32)
    row_delta = jnp.sum(probs_again * d_probs, axis=-1, keepdims=True)
    d_scores = (probs_again * (d_probs - row_delta)).astype(jnp.bfloat16)
    d_query = (
        jnp.einsum("grst,tgd->sgrd", d_scores, key_all, preferred_element_type=jnp.float32)
        * score_scale
    )
    d_key = (
        jnp.einsum("grst,sgrd->tgd", d_scores, query_rot, preferred_element_type=jnp.float32)
        * score_scale
    )
    d_value = d_value_all.astype(jnp.bfloat16).reshape(seq_len, kv_heads * HD)
    d_query_norm = rotate_back(d_query.reshape(seq_len, q_heads, HD), cosine_heads, sine_heads)
    d_key_norm = rotate_back(d_key, cosine_heads, sine_heads)
    query_gain_part = jnp.sum(d_query_norm * query_hat, axis=(0, 1))
    key_gain_part = jnp.sum(d_key_norm * key_hat, axis=(0, 1))
    d_query_raw = (
        norm_back(d_query_norm * query_gain, query_hat, query_inverse)
        .astype(jnp.bfloat16)
        .reshape(seq_len, q_heads * HD)
    )
    d_key_raw = (
        norm_back(d_key_norm * key_gain, key_hat, key_inverse)
        .astype(jnp.bfloat16)
        .reshape(seq_len, kv_heads * HD)
    )
    d_projected = jnp.concatenate([d_query_raw, d_key_raw, d_value], axis=1)
    grad_qkv, grad_out = reduce_grads(
        [full_one.T, full_resid.T], [d_projected, attn_rows], [(0, 0), (1, 1)], dp, 3
    )
    d_normed_one = lax.psum_scatter(
        tail_product(d_projected, qkv_weight).astype(jnp.bfloat16),
        "tensor",
        scatter_dimension=0,
        tiled=True,
    ).astype(jnp.float32)
    attn_gain_part = jnp.sum(d_normed_one * normed_one, axis=0)
    input_grad = (d_resid + norm_back(d_normed_one * attn_gain, normed_one, inverse_one)).astype(
        jnp.bfloat16
    )
    gain_sums = lax.psum(
        jnp.concatenate([attn_gain_part, mlp_gain_part, query_gain_part, key_gain_part]),
        ("dp", "tensor"),
    )
    me = lax.axis_index("dp")
    share = model // dp
    qk_share = 2 * HD // dp
    return (
        result_rows,
        input_grad,
        grad_qkv[:, :q_width],
        grad_qkv[:, q_width : q_width + kv_width],
        grad_qkv[:, q_width + kv_width :],
        grad_out.T,
        grad_gate,
        grad_up,
        grad_down.T,
        lax.dynamic_slice(gain_sums, (me * share,), (share,)),
        lax.dynamic_slice(gain_sums, (model + me * share,), (share,)),
        lax.dynamic_slice(gain_sums, (2 * model + me * qk_share,), (qk_share,)),
    )


def solution(mesh):
    return jax.shard_map(
        on_device,
        mesh=mesh,
        in_specs=(
            P(("dp", "tensor"), None),
            P("dp", None),
            P("dp", "tensor"),
            P("dp", "tensor"),
            P("dp", "tensor"),
            P("tensor", "dp"),
            P("dp", "tensor"),
            P("dp", "tensor"),
            P("tensor", "dp"),
            P("dp"),
            P("dp"),
            P("dp"),
            P(("dp", "tensor"), None),
        ),
        out_specs=(
            P(("dp", "tensor"), None),
            P(("dp", "tensor"), None),
            P("dp", "tensor"),
            P("dp", "tensor"),
            P("dp", "tensor"),
            P("tensor", "dp"),
            P("dp", "tensor"),
            P("dp", "tensor"),
            P("tensor", "dp"),
            P("dp"),
            P("dp"),
            P("dp"),
        ),
        check_vma=False,
    )
```

```python
import functools
import jax
import jax.numpy as jnp
from jax import lax
from jax.experimental import pallas as pl
from jax.experimental.pallas import tpu as pltpu

from jax.sharding import PartitionSpec as P

MESH = pl.DeviceIdType.MESH
HD = 128
epsilon = 1e-06
rope_base = 1000000.0


def ring_place(n):
    me = lax.axis_index("dp")
    chip = me // 2
    core = me % 2
    odd = chip % 2
    pos = (1 - odd) * (chip // 2) + odd * (n - 1 - chip // 2)
    return pos, core


def chip_at(pos, n):
    high = pos // (n // 2)
    return (1 - high) * (2 * pos) + high * (2 * (n - 1 - pos) + 1)


def at(pos, core, n):
    return (chip_at(pos, n) * 2 + core, lax.axis_index("tensor"))


def meet(peers):
    barrier = pltpu.get_barrier_semaphore()
    for peer in peers:
        pl.semaphore_signal(barrier, inc=1, device_id=peer, device_id_type=MESH)
    pl.semaphore_wait(barrier, len(peers))


def remote(src, dst, send, recv, peer):
    return pltpu.make_async_remote_copy(
        src_ref=src, dst_ref=dst, send_sem=send, recv_sem=recv, device_id=peer, device_id_type=MESH
    )


def gather_kernel(n, parts, count, swaps, *refs):
    shards = refs[:count]
    halves = refs[count : count + swaps]
    fulls = refs[count + swaps : 2 * count + swaps]
    wholes = refs[2 * count + swaps : 2 * (count + swaps)]
    own_sem, send_sem, recv_sem, give_sem, take_sem, swap_sem = refs[2 * (count + swaps) :]
    pos, core = ring_place(n)
    lane = lax.axis_index("tensor")
    nexts = (at((pos + 1) % n, core, n), at((pos + n - 1) % n, core, n))
    mate = at(pos, 1 - core, n)
    twin = (lax.axis_index("dp"), 1 - lane)
    meet((*nexts, mate, twin))
    messages = [(w, part) for w in range(count) for part in range(parts[w])]

    def sizes(w):
        rows = shards[w].shape[0]
        return rows, rows // 2, rows // 2 // parts[w]

    def spot(w, owner, who, side, part):
        rows, half, piece = sizes(w)
        start = (chip_at(owner, n) * 2 + who) * rows + (side * half + part * piece)
        return fulls[w].at[pl.ds(pl.multiple_of(start, piece), piece)]

    def shard_of(w, who):
        rows = shards[w].shape[0]
        return fulls[w].at[pl.ds(pl.multiple_of((chip_at(pos, n) * 2 + who) * rows, rows), rows)]

    def swap_spot(s, which):
        rows = halves[s].shape[0]
        return wholes[s].at[pl.ds(pl.multiple_of(which * rows, rows), rows)]

    for k, (w, part) in enumerate(messages):
        rows, half, piece = sizes(w)
        for side in range(2):
            src = shards[w].at[pl.ds(side * half + part * piece, piece)]
            remote(
                src, spot(w, pos, core, side, part), send_sem.at[k, side, 0], recv_sem.at[k, side, 0], nexts[side]
            ).start()
    for s in range(swaps):
        remote(halves[s], swap_spot(s, lane), swap_sem.at[s, 0], swap_sem.at[s, 1], twin).start()
        pltpu.make_async_copy(halves[s], swap_spot(s, lane), own_sem.at[count + s]).start()
    for w in range(count):
        remote(shards[w], shard_of(w, core), give_sem.at[w, 0, n - 1], take_sem.at[w, 0, n - 1], mate).start()
        pltpu.make_async_copy(shards[w], shard_of(w, core), own_sem.at[w]).start()

    def owner_of(side, step):
        if side == 0:
            return (pos - 1 - step + 2 * n) % n
        return (pos + 1 + step) % n

    def step_body(step, carry):
        for k, (w, part) in enumerate(messages):
            for side in range(2):
                block = spot(w, owner_of(side, step), core, side, part)
                remote(block, block, send_sem.at[k, side, step], recv_sem.at[k, side, step], nexts[side]).wait_recv()

                @pl.when(step < n - 2)
                def _():
                    remote(
                        block, block, send_sem.at[k, side, step + 1], recv_sem.at[k, side, step + 1], nexts[side]
                    ).start()

                remote(block, block, give_sem.at[k, side, step], take_sem.at[k, side, step], mate).start()
        return carry

    lax.fori_loop(0, n - 1, step_body, 0)

    def drain(step, carry):
        for k, (w, part) in enumerate(messages):
            for side in range(2):
                owner = owner_of(side, step)
                block = spot(w, owner, core, side, part)
                theirs = spot(w, owner, 1 - core, side, part)
                remote(block, block, send_sem.at[k, side, step], recv_sem.at[k, side, step], nexts[side]).wait_send()
                given = remote(block, theirs, give_sem.at[k, side, step], take_sem.at[k, side, step], mate)
                given.wait_send()
                given.wait_recv()
        return carry

    lax.fori_loop(0, n - 1, drain, 0)
    for w in range(count):
        pltpu.make_async_copy(shards[w], shard_of(w, core), own_sem.at[w]).wait()
        given = remote(shards[w], shard_of(w, 1 - core), give_sem.at[w, 0, n - 1], take_sem.at[w, 0, n - 1], mate)
        given.wait_send()
        given.wait_recv()
    for s in range(swaps):
        pltpu.make_async_copy(halves[s], swap_spot(s, lane), own_sem.at[count + s]).wait()
        other = remote(halves[s], swap_spot(s, 1 - lane), swap_sem.at[s, 0], swap_sem.at[s, 1], twin)
        other.wait_send()
        other.wait_recv()


def gather_weights(shards, swaps, parts, dp, collective_id):
    n = dp // 2
    count = len(shards)
    msgs = sum(parts)
    dma = pltpu.SemaphoreType.DMA
    outs = pl.pallas_call(
        functools.partial(gather_kernel, n, tuple(parts), count, len(swaps)),
        out_shape=[
            *[jax.ShapeDtypeStruct((s.shape[0] * dp, s.shape[1]), s.dtype) for s in shards],
            *[jax.ShapeDtypeStruct((s.shape[0] * 2, s.shape[1]), s.dtype) for s in swaps],
        ],
        in_specs=[pl.BlockSpec(memory_space=pltpu.VMEM)] * (count + len(swaps)),
        out_specs=[pl.BlockSpec(memory_space=pltpu.HBM)] * (count + len(swaps)),
        scratch_shapes=[
            dma((count + len(swaps),)),
            dma((msgs, 2, n - 1)),
            dma((msgs, 2, n - 1)),
            dma((msgs, 2, n)),
            dma((msgs, 2, n)),
            dma((max(1, len(swaps)), 2)),
        ],
        compiler_params=pltpu.CompilerParams(collective_id=collective_id, has_side_effects=True),
    )(*shards, *swaps)
    return outs[:count], outs[count:]


def reduce_kernel(n, pairs, *refs):
    n_left = 1 + max(p[0] for p in pairs)
    n_right = 1 + max(p[1] for p in pairs)
    count = len(pairs)
    lefts = refs[:n_left]
    rights = refs[n_left : n_left + n_right]
    outs = refs[n_left + n_right : n_left + n_right + count]
    rest = refs[n_left + n_right + count :]
    mine, give, take, ship, land = (rest[i * count : (i + 1) * count] for i in range(5))
    term, give_sem, take_sem, ship_sem, land_sem = rest[5 * count :]
    pos, core = ring_place(n)
    nexts = (at((pos + 1) % n, core, n), at((pos + n - 1) % n, core, n))
    mate = at(pos, 1 - core, n)
    meet((*nexts, mate))
    rows = outs[0].shape[0]

    def owner_of(side, step):
        if side == 0:
            return (pos - 1 - step + 2 * n) % n
        return (pos + 1 + step) % n

    def early(m, side, step):
        left, right = pairs[m]
        wide = outs[m].shape[1] // 2
        slot = step % 2
        start = pl.multiple_of(chip_at(owner_of(side, step), n) * 2 * rows, 2 * rows)
        part = term.at[:, pl.ds(0, wide)]
        part[...] = jnp.dot(
            lefts[left][pl.ds(start, 2 * rows), :],
            rights[right][:, pl.ds(side * wide, wide)],
            preferred_element_type=jnp.float32,
        )
        other = pl.ds(pl.multiple_of((1 - core) * rows, rows), rows)
        same = pl.ds(pl.multiple_of(core * rows, rows), rows)
        given = remote(
            give[m].at[side, slot], take[m].at[side, slot],
            give_sem.at[m, side, slot], take_sem.at[m, side, slot], mate,
        )

        @pl.when(step >= 2)
        def _():
            given.wait_send()

        give[m][side, slot] = part[other, :].astype(jnp.bfloat16)
        given.start()
        mine[m][side] = part[same, :]

    def shipped(m, side, step):
        return remote(
            ship[m].at[side, step % 2], land[m].at[side, step],
            ship_sem.at[m, side, step % 2], land_sem.at[m, side, step], nexts[side],
        )

    def local_sum(m, side, step):
        slot = step % 2
        remote(
            give[m].at[side, slot], take[m].at[side, slot],
            give_sem.at[m, side, slot], take_sem.at[m, side, slot], mate,
        ).wait_recv()
        return mine[m][side] + take[m][side, slot].astype(jnp.float32)

    for m in range(count):
        for side in range(2):
            early(m, side, 0)
    for m in range(count):
        for side in range(2):
            total = local_sum(m, side, 0)
            ship[m][side, 0] = total.astype(jnp.bfloat16)
            shipped(m, side, 0).start()
            early(m, side, 1)

    def step_body(step, carry):
        for m in range(count):
            for side in range(2):
                total = local_sum(m, side, step)
                shipped(m, side, step - 1).wait_recv()
                total = total + land[m][side, step - 1].astype(jnp.float32)

                @pl.when(step >= 2)
                def _():
                    shipped(m, side, step - 2).wait_send()

                ship[m][side, step % 2] = total.astype(jnp.bfloat16)
                shipped(m, side, step).start()
                early(m, side, step + 1)
        return carry

    lax.fori_loop(1, n - 1, step_body, 0)
    last = n - 1
    for m in range(count):
        wide = outs[m].shape[1] // 2
        for side in range(2):
            total = local_sum(m, side, last)
            shipped(m, side, last - 1).wait_recv()
            outs[m][:, pl.ds(side * wide, wide)] = total + land[m][side, last - 1].astype(jnp.float32)
    for m in range(count):
        for side in range(2):
            shipped(m, side, last - 1).wait_send()
            if last >= 2:
                shipped(m, side, last - 2).wait_send()
            for slot in range(2):
                remote(
                    give[m].at[side, slot], take[m].at[side, slot],
                    give_sem.at[m, side, slot], take_sem.at[m, side, slot], mate,
                ).wait_send()


def reduce_grads(lefts, rights, pairs, dp, collective_id):
    n = dp // 2
    count = len(pairs)
    rows = lefts[0].shape[0] // dp
    wides = [rights[r].shape[1] // 2 for _, r in pairs]
    low = jnp.bfloat16
    return pl.pallas_call(
        functools.partial(reduce_kernel, n, tuple(pairs)),
        out_shape=[jax.ShapeDtypeStruct((rows, 2 * w), jnp.float32) for w in wides],
        in_specs=[pl.BlockSpec(memory_space=pltpu.VMEM)] * (len(lefts) + len(rights)),
        out_specs=[pl.BlockSpec(memory_space=pltpu.VMEM)] * count,
        scratch_shapes=[
            *[pltpu.VMEM((2, rows, w), jnp.float32) for w in wides],
            *[pltpu.VMEM((2, 2, rows, w), low) for w in wides],
            *[pltpu.VMEM((2, 2, rows, w), low) for w in wides],
            *[pltpu.VMEM((2, 2, rows, w), low) for w in wides],
            *[pltpu.VMEM((2, n - 1, rows, w), low) for w in wides],
            pltpu.VMEM((2 * rows, max(wides)), jnp.float32),
            pltpu.SemaphoreType.DMA((count, 2, 2)),
            pltpu.SemaphoreType.DMA((count, 2, 2)),
            pltpu.SemaphoreType.DMA((count, 2, 2)),
            pltpu.SemaphoreType.DMA((count, 2, n - 1)),
        ],
        compiler_params=pltpu.CompilerParams(
            collective_id=collective_id, has_side_effects=True, vmem_limit_bytes=67043328
        ),
    )(*lefts, *rights)


def product(left, right):
    return jnp.dot(left, right, preferred_element_type=jnp.float32)


def lead_product(left, right):
    return lax.dot_general(
        left, right, (((0,), (0,)), ((), ())), preferred_element_type=jnp.float32
    )


def tail_product(left, right):
    return lax.dot_general(
        left, right, (((1,), (1,)), ((), ())), preferred_element_type=jnp.float32
    )


def norm_rows(values):
    return lax.rsqrt(jnp.mean(values * values, axis=-1, keepdims=True) + epsilon)


def norm_back(incoming, normed, inverse):
    return inverse * (incoming - normed * jnp.mean(incoming * normed, axis=-1, keepdims=True))


def rotate(values, cosine_table, sine_table):
    half_width = values.shape[-1] // 2
    turned = jnp.concatenate([-values[..., half_width:], values[..., :half_width]], axis=-1)
    return values * cosine_table + turned * sine_table


def rotate_back(incoming, cosine_table, sine_table):
    half_width = incoming.shape[-1] // 2
    scaled = incoming * sine_table
    return incoming * cosine_table + jnp.concatenate(
        [scaled[..., half_width:], -scaled[..., :half_width]], axis=-1
    )


def tables(segments):
    seq_len = segments.shape[0]
    token_index = jnp.arange(seq_len, dtype=jnp.int32)
    doc_start = jnp.sum((segments[None, :] < segments[:, None]).astype(jnp.int32), axis=1)
    doc_pos = (token_index - doc_start).astype(jnp.float32)
    frequency = rope_base ** (-jnp.arange(0, HD, 2).astype(jnp.float32) / HD)
    angles = doc_pos[:, None] * frequency[None, :]
    cosine_table = jnp.concatenate([jnp.cos(angles), jnp.cos(angles)], axis=1)
    sine_table = jnp.concatenate([jnp.sin(angles), jnp.sin(angles)], axis=1)
    allowed = (segments[:, None] == segments[None, :]) & (
        token_index[None, :] <= token_index[:, None]
    )
    return (cosine_table, sine_table, allowed)


def turn(values):
    return pltpu.roll(values, values.shape[-1] // 2, 1)


def row_scale(values):
    return lax.rsqrt(jnp.mean(values * values, axis=-1, keepdims=True) + epsilon)


def head_at(index):
    return pl.ds(pl.multiple_of(index * HD, HD), HD)


def prepared(raw, gain, cosine, sine):
    inverse = row_scale(raw)
    hat = raw * inverse
    scaled = hat * gain
    return inverse, hat, (scaled * cosine + turn(scaled) * sine).astype(jnp.bfloat16)


def exp_block(query, keys, seg_col, seg_row, first):
    width = keys.shape[0]
    scores = tail_product(query, keys) * HD ** (-0.5)
    rows = lax.broadcasted_iota(jnp.int32, scores.shape, 0) + first
    columns = lax.broadcasted_iota(jnp.int32, scores.shape, 1)
    allowed = (seg_col[first : first + scores.shape[0], :] == seg_row[:, :width]) & (
        columns <= rows
    )
    return jnp.where(allowed, jnp.exp(scores), 0.0)


def attend_group(group, dims, qkv, tab, seg_col, seg_row, gains, attn, kept):
    q_heads, kv_heads, seq, block = dims
    per_group = q_heads // kv_heads
    cosine, sine = tab[0], tab[1]
    raw = qkv[:, head_at(q_heads + group)]
    kept[0] = prepared(raw, gains[1:2, :], cosine, sine)[2]
    kept[1] = qkv[:, head_at(q_heads + kv_heads + group)].astype(jnp.bfloat16)
    for r in range(per_group):
        head = group * per_group + r
        raw = qkv[:, head_at(head)]
        query = prepared(raw, gains[0:1, :], cosine, sine)[2]
        for first in range(0, seq, block):
            width = first + block
            exps = exp_block(query[first:width], kept[0, :width, :], seg_col, seg_row, first)
            probs = (exps / jnp.sum(exps, axis=-1, keepdims=True)).astype(jnp.bfloat16)
            attn[first:width, head_at(head)] = product(probs, kept[1, :width, :]).astype(jnp.bfloat16)


def block_columns(ref, index, width):
    if width % 128 == 0:
        return ref[:, pl.ds(pl.multiple_of(index * width, width), width)]
    fold = 128 // width
    tile = ref[:, pl.ds(pl.multiple_of((index // fold) * 128, 128), 128)]
    picked = tile[:, :width]
    for i in range(1, fold):
        picked = jnp.where(index % fold == i, tile[:, i * width : (i + 1) * width], picked)
    return picked


def forward_kernel(n, dims, *refs):
    (
        shards, qkv, out_weight, tokens, cot_full, tab, seg_col, seg_row, gains, mlp_gain,
        weights, attn, resid, full_two, act,
        kept, part, peer, acc, blocks,
        own_sem, send_sem, recv_sem, give_sem, take_sem, swap_sem, load_sem,
    ) = refs
    q_heads, kv_heads, seq, block = dims
    pos, core = ring_place(n)
    lane = lax.axis_index("tensor")
    nexts = (at((pos + 1) % n, core, n), at((pos + n - 1) % n, core, n))
    mate = at(pos, 1 - core, n)
    twin = (lax.axis_index("dp"), 1 - lane)
    count, rows, width = shards.shape
    wide = width // 2
    model = 2 * n * rows
    half = seq // 2
    meet((*nexts, mate, twin))

    def owner_of(side, step):
        if side == 0:
            return (pos - step + 2 * n) % n
        return (pos + step) % n

    def spot(w, chip, who, side):
        start = w * model + (chip * 2 + who) * rows
        return weights.at[pl.ds(pl.multiple_of(start, rows), rows), pl.ds(side * wide, wide)]

    def hop(w, side, step):
        here = spot(w, chip_at(owner_of(side, step), n), core, side)
        return remote(here, here, send_sem.at[w, side, step], recv_sem.at[w, side, step], nexts[side])

    def first_hop(w, side):
        return remote(
            shards.at[w, :, pl.ds(side * wide, wide)],
            spot(w, chip_at(pos, n), core, side),
            send_sem.at[w, side, 1], recv_sem.at[w, side, 1], nexts[side],
        )

    def onward(w, side, step):
        here = spot(w, chip_at(owner_of(side, step), n), core, side)
        return remote(here, here, send_sem.at[w, side, step + 1], recv_sem.at[w, side, step + 1], nexts[side])

    def hand(w, side, step, who):
        here = spot(w, chip_at(owner_of(side, step), n), who, side)
        return remote(here, here, give_sem.at[w, side, step], take_sem.at[w, side, step], mate)

    def hand_own(w, side, who):
        return remote(
            shards.at[w, :, pl.ds(side * wide, wide)],
            spot(w, chip_at(pos, n), who, side),
            give_sem.at[w, side, 0], take_sem.at[w, side, 0], mate,
        )

    def keep_own(w, side):
        return pltpu.make_async_copy(
            shards.at[w, :, pl.ds(side * wide, wide)], spot(w, chip_at(pos, n), core, side), own_sem.at[w, side]
        )

    for w in range(count):
        for side in range(2):
            first_hop(w, side).start()
    for w in range(count):
        for side in range(2):
            hand_own(w, side, core).start()
            keep_own(w, side).start()

    def service(event):
        step, w = event // count + 1, event % count
        for side in range(2):
            hop(w, side, step).wait_recv()

            @pl.when(step < n - 1)
            def _():
                onward(w, side, step).start()

            hand(w, side, step, core).start()

    def load(job, side):
        step, w = job // count, job % count
        start = w * model + chip_at(owner_of(side, step), n) * 2 * rows
        return pltpu.make_async_copy(
            weights.at[pl.ds(pl.multiple_of(start, 2 * rows), 2 * rows), pl.ds(side * wide, wide)],
            blocks.at[side], load_sem.at[side],
        )

    def work(job):
        step, w = job // count, job % count
        for side in range(2):
            @pl.when(step > 0)
            def _():
                hand(w, side, step, 1 - core).wait_recv()

            @pl.when(step == 0)
            def _():
                hand_own(w, side, 1 - core).wait_recv()
                keep_own(w, side).wait()

            load(job, side).start()
        for side in range(2):
            load(job, side).wait()
            chip = chip_at(owner_of(side, step), n)

            def with_left(left):
                tile = wide // 3

                def one(i, carry):
                    there = pl.ds(pl.multiple_of(side * wide + i * tile, tile), tile)
                    gained = product(left, blocks[side, :, pl.ds(pl.multiple_of(i * tile, tile), tile)])

                    @pl.when(step == 0)
                    def _():
                        acc[w, :, there] = gained

                    @pl.when(step > 0)
                    def _():
                        acc[w, :, there] += gained

                    return carry

                lax.fori_loop(0, 3, one, 0)

            @pl.when(w < 2)
            def _():
                with_left(block_columns(full_two, chip, 2 * rows))

            @pl.when(w == 2)
            def _():
                with_left(block_columns(cot_full, chip, 2 * rows))

    groups = (qkv, tab, seg_col, seg_row, gains, attn, kept)

    def attend(first, last):
        def one(group, carry):
            attend_group(group, dims, *groups)
            return carry

        lax.fori_loop(first, last, one, 0)

    attend(0, kv_heads // 2)
    service(0)
    attend(kv_heads // 2, kv_heads)
    service(1)
    theirs = pl.ds(pl.multiple_of((1 - lane) * half, half), half)
    ours = pl.ds(pl.multiple_of(lane * half, half), half)
    part[...] = tail_product(attn[theirs, :], out_weight[...]).astype(jnp.bfloat16)
    send_part = remote(part, peer, swap_sem.at[0, 0], swap_sem.at[0, 1], twin)
    send_part.start()
    resid[...] = tokens[...].astype(jnp.float32) + tail_product(attn[ours, :], out_weight[...])
    for event in range(2, 6):
        service(event)
    send_part.wait_recv()
    summed = resid[...] + peer[...].astype(jnp.float32)
    resid[...] = summed
    send_part.wait_send()
    part[...] = (summed * row_scale(summed) * mlp_gain[...]).astype(jnp.bfloat16)
    send_two = remote(part, full_two.at[ours], swap_sem.at[1, 0], swap_sem.at[1, 1], twin)
    send_two.start()
    full_two[ours, :] = part[...]
    ready = 9
    for event in range(6, ready):
        service(event)
    remote(part, full_two.at[theirs], swap_sem.at[1, 0], swap_sem.at[1, 1], twin).wait_recv()

    def both(i, carry):
        service(ready + i)

        @pl.when(i < ready + 3)
        def _():
            def one(q, carry):
                work(2 * i + q)
                return carry

            lax.fori_loop(0, 2, one, 0)

        @pl.when(i >= ready + 3)
        def _():
            work(ready + 3 + i)

        return carry

    lax.fori_loop(0, count * (n - 1) - ready, both, 0)
    send_two.wait_send()

    strip = 32

    def finish(i, carry):
        there = pl.ds(pl.multiple_of(i * strip, strip), strip)
        gate = acc[0, there, :]
        up = acc[1, there, :]
        d_act = acc[2, there, :]
        sig = 1.0 / (1.0 + jnp.exp(-gate))
        silu = gate * sig
        act[0, there, :] = (d_act * up * sig * (1.0 + gate * (1.0 - sig))).astype(jnp.bfloat16)
        act[1, there, :] = (d_act * silu).astype(jnp.bfloat16)
        act[2, there, :] = (silu * up).astype(jnp.bfloat16)
        return carry

    lax.fori_loop(0, seq // strip, finish, 0)

    def drain(step, carry):
        for w in range(count):
            for side in range(2):
                hop(w, side, step).wait_send()
                hand(w, side, step, core).wait_send()
        return carry

    lax.fori_loop(1, n, drain, 0)
    for w in range(count):
        for side in range(2):
            hand_own(w, side, core).wait_send()


def forward_block(shards, qkv, out_weight, tokens, cot_full, tab, segments, gains, mlp_gain, q_heads, kv_heads, dp):
    n = dp // 2
    count, rows, width = shards.shape
    seq, model = cot_full.shape
    half = seq // 2
    low, dma, vmem = jnp.bfloat16, pltpu.SemaphoreType.DMA, pltpu.VMEM
    shape = jax.ShapeDtypeStruct
    place = lambda kind: pl.BlockSpec(memory_space=kind)
    return pl.pallas_call(
        functools.partial(forward_kernel, n, (q_heads, kv_heads, seq, seq // 2)),
        out_shape=[
            shape((count * model, width), low),
            shape((seq, q_heads * HD), low),
            shape((half, model), jnp.float32),
            shape((seq, model), low),
            shape((count, seq, width), low),
        ],
        in_specs=[place(vmem)] * 10,
        out_specs=[place(pltpu.HBM)] + [place(vmem)] * 4,
        scratch_shapes=[
            vmem((2, seq, HD), low),
            vmem((half, model), low),
            vmem((half, model), low),
            vmem((count, seq, width), jnp.float32),
            vmem((2, 2 * rows, width // 2), low),
            dma((count, 2)),
            dma((count, 2, n)),
            dma((count, 2, n)),
            dma((count, 2, n)),
            dma((count, 2, n)),
            dma((2, 2)),
            dma((2,)),
        ],
        compiler_params=pltpu.CompilerParams(
            collective_id=1, has_side_effects=True, vmem_limit_bytes=67043328
        ),
    )(
        shards, qkv, out_weight, tokens, cot_full, tab,
        segments.reshape(seq, 1), segments.reshape(1, seq), gains, mlp_gain,
    )


SLOTS = 3


def undo(incoming, hat, inverse, gain, cosine, sine):
    turned = incoming * cosine - turn(incoming) * sine
    total = jnp.sum(turned * hat, axis=0, keepdims=True)
    scaled = turned * gain
    raw = inverse * (scaled - hat * jnp.mean(scaled * hat, axis=-1, keepdims=True))
    return total, raw.astype(jnp.bfloat16)


def attend_back(group, dims, heads, tab, seg_col, seg_row, gains, d_attn, d_proj, sums, kept):
    q_heads, kv_heads, seq, block = dims
    per_group = q_heads // kv_heads
    low = jnp.bfloat16
    scale = HD ** (-0.5)
    cosine, sine = tab[0], tab[1]
    keys = prepared(heads[per_group], gains[1:2, :], cosine, sine)[2]
    values = heads[per_group + 1].astype(low)
    for r in range(per_group):
        head = group * per_group + r
        q_inverse, q_hat, query = prepared(heads[r], gains[0:1, :], cosine, sine)
        for first in range(0, seq, block):
            width = first + block
            exps = exp_block(query[first:width], keys[:width], seg_col, seg_row, first)
            probs = exps / jnp.sum(exps, axis=-1, keepdims=True)
            incoming = d_attn[first:width, head_at(head)]
            d_probs = tail_product(incoming, values[:width])
            delta = jnp.sum(probs * d_probs, axis=-1, keepdims=True)
            d_scores = (probs * (d_probs - delta)).astype(low)
            kept[0, first:width, :] = product(d_scores, keys[:width]) * scale
            d_keys = lead_product(d_scores, query[first:width])
            d_values = lead_product(probs.astype(low), incoming)
            if r == 0 and first == 0:
                kept[1] = jnp.zeros_like(kept[1])
                kept[2] = jnp.zeros_like(kept[2])
            kept[1, :width, :] += d_keys
            kept[2, :width, :] += d_values
        total, raw = undo(kept[0], q_hat, q_inverse, gains[0:1, :], cosine, sine)
        sums[0:1, :] += total
        d_proj[:, head_at(head)] = raw
    k_inverse, k_hat, _ = prepared(heads[per_group], gains[1:2, :], cosine, sine)
    total, raw = undo(kept[1] * scale, k_hat, k_inverse, gains[1:2, :], cosine, sine)
    sums[1:2, :] += total
    d_proj[:, head_at(q_heads + group)] = raw
    d_proj[:, head_at(q_heads + kv_heads + group)] = kept[2].astype(low)


def reducer(n, pos, core, nexts, mate, refs, left_of):
    lefts, rights, out, mine, term, give, take, ship, land, give_sem, take_sem, ship_sem, land_sem, free_sem, out_sem = refs
    count = rights.shape[0]
    wide = rights.shape[2] // 2
    rows = out.shape[1]

    def owner_of(side, step):
        if side == 0:
            return (pos - 1 - step + 2 * n) % n
        return (pos + 1 + step) % n

    def given(m, side, step):
        return remote(
            give.at[m, side], take.at[m, side, step % 2],
            give_sem.at[m, side], take_sem.at[m, side, step % 2], mate,
        )

    def shipped(m, side, step):
        return remote(
            ship.at[m, side], land.at[m, side, step % SLOTS],
            ship_sem.at[m, side], land_sem.at[m, side, step % SLOTS], nexts[side],
        )

    def early(m, step):
        for side in range(2):
            start = pl.multiple_of(chip_at(owner_of(side, step), n) * 2 * rows, 2 * rows)
            left = lefts[left_of(m), pl.ds(start, 2 * rows), :]
            tile = wide // 3

            def one(i, carry):
                there = pl.multiple_of(i * tile, tile)
                term[:, pl.ds(there, tile)] = product(
                    left, rights[m, :, pl.ds(pl.multiple_of(side * wide + there, tile), tile)]
                )
                return carry

            lax.fori_loop(0, 3, one, 0)

            @pl.when(step >= 1)
            def _():
                given(m, side, step - 1).wait_send()

            give[m, side] = term[pl.ds(pl.multiple_of((1 - core) * rows, rows), rows), :].astype(jnp.bfloat16)
            given(m, side, step).start()
            mine[m, side] = term[pl.ds(pl.multiple_of(core * rows, rows), rows), :]

    def event(e):
        step, m = e // count, e % count
        for side in range(2):
            given(m, side, step).wait_recv()

            @pl.when(step == 0)
            def _():
                mine[m, side] += take[m, side, 0].astype(jnp.float32)

            @pl.when(step > 0)
            def _():
                shipped(m, side, step - 1).wait_recv()
                mine[m, side] += take[m, side, step % 2].astype(jnp.float32) + land[
                    m, side, (step - 1) % SLOTS
                ].astype(jnp.float32)

                @pl.when(step - 1 + SLOTS <= n - 2)
                def _():
                    pl.semaphore_signal(
                        free_sem.at[m, side], inc=1, device_id=nexts[1 - side], device_id_type=MESH
                    )

                shipped(m, side, step - 1).wait_send()

            @pl.when(step < n - 1)
            def _():
                @pl.when(step >= SLOTS)
                def _():
                    pl.semaphore_wait(free_sem.at[m, side], 1)

                ship[m, side] = mine[m, side].astype(jnp.bfloat16)
                shipped(m, side, step).start()

            @pl.when(step == n - 1)
            def _():
                written(m, side).start()

        @pl.when(step < n - 1)
        def _():
            early(m, step + 1)

    def written(m, side):
        return pltpu.make_async_copy(mine.at[m, side], out.at[m, :, pl.ds(side * wide, wide)], out_sem.at[m, side])

    def finish():
        for m in range(count):
            for side in range(2):
                given(m, side, n - 1).wait_send()
                written(m, side).wait()

    return early, event, finish


def reduce_scratch(n, count, rows, wide):
    low, dma, vmem = jnp.bfloat16, pltpu.SemaphoreType.DMA, pltpu.VMEM
    return [
        vmem((count, 2, rows, wide), jnp.float32),
        vmem((2 * rows, wide), jnp.float32),
        vmem((count, 2, rows, wide), low),
        vmem((count, 2, 2, rows, wide), low),
        vmem((count, 2, rows, wide), low),
        vmem((count, 2, SLOTS, rows, wide), low),
        dma((count, 2)),
        dma((count, 2, 2)),
        dma((count, 2)),
        dma((count, 2, SLOTS)),
        pltpu.SemaphoreType.REGULAR((count, 2)),
        dma((count, 2)),
    ]


def backward_kernel(n, dims, *refs):
    (
        lefts, act, weights, qkv, out_weight, cot, resid, tab, seg_col, seg_row, gains, mlp_gain,
        grads, d_proj, d_full, d_resid, mlp_sum, qk_sum,
        gate_block, up_block, own, part, peer, d_attn, heads, kept,
        swap_sem, load_sem, head_sem,
    ) = refs[:29]
    q_heads, kv_heads, seq, block = dims
    pos, core = ring_place(n)
    lane = lax.axis_index("tensor")
    nexts = (at((pos + 1) % n, core, n), at((pos + n - 1) % n, core, n))
    mate = at(pos, 1 - core, n)
    twin = (lax.axis_index("dp"), 1 - lane)
    meet((*nexts, mate, twin))
    count = act.shape[0]
    model = resid.shape[1]
    half = seq // 2
    early, event, finish = reducer(
        n, pos, core, nexts, mate, (lefts, act, grads, *refs[29:]), lambda m: m // 2
    )
    for m in range(count):
        early(m, 0)
    for m in range(count):
        event(m)

    theirs = pl.ds(pl.multiple_of((1 - lane) * half, half), half)
    ours = pl.ds(pl.multiple_of(lane * half, half), half)
    deep = gate_block.shape[0]
    turns = model // deep

    def fetch(i, which):
        target = (gate_block, up_block)[which]
        start = which * model + i * deep
        return pltpu.make_async_copy(
            weights.at[pl.ds(pl.multiple_of(start, deep), deep), :], target, load_sem.at[which]
        )

    fetch(0, 0).start()
    fetch(0, 1).start()

    def narrow(i, carry):
        there = pl.ds(pl.multiple_of(i * deep, deep), deep)
        for which, target in enumerate((gate_block, up_block)):
            fetch(i, which).wait()
            other = tail_product(act[which, theirs, :], target[...])
            same = tail_product(act[which, ours, :], target[...])
            if which == 0:
                own[:, there] = same
                d_resid[:, there] = other
            else:
                own[:, there] += same
                part[:, there] = (d_resid[:, there] + other).astype(jnp.bfloat16)

            @pl.when(i < turns - 1)
            def _():
                fetch(i + 1, which).start()

        @pl.when(i % 3 == 2)
        def _():
            event(count + i // 3)

        return carry

    lax.fori_loop(0, turns, narrow, 0)
    done = count + turns // 3
    send = remote(part, peer, swap_sem.at[0, 0], swap_sem.at[0, 1], twin)
    send.start()
    for e in range(done, done + 3):
        event(e)
    done = done + 3
    send.wait_recv()
    send.wait_send()
    strip = 32

    def norm_strip(i, carry):
        there = pl.ds(pl.multiple_of(i * strip, strip), strip)
        incoming = own[there, :] + peer[there, :].astype(jnp.float32)
        hidden = resid[there, :]
        inverse = row_scale(hidden)
        normed = hidden * inverse
        scaled = incoming * mlp_gain[...]
        change = cot[there, :].astype(jnp.float32) + inverse * (
            scaled - normed * jnp.mean(scaled * normed, axis=-1, keepdims=True)
        )
        d_resid[there, :] = change
        part[there, :] = change.astype(jnp.bfloat16)
        total = jnp.sum(incoming * normed, axis=0, keepdims=True)

        @pl.when(i == 0)
        def _():
            mlp_sum[...] = total

        @pl.when(i > 0)
        def _():
            mlp_sum[...] += total

        return carry

    lax.fori_loop(0, half // strip, norm_strip, 0)
    send = remote(part, d_full.at[ours], swap_sem.at[1, 0], swap_sem.at[1, 1], twin)
    send.start()
    d_full[ours, :] = part[...]
    columns = out_weight.shape[1]
    quarter = columns // 4

    for e in range(done, done + 3):
        event(e)
    done = done + 3
    remote(part, d_full.at[theirs], swap_sem.at[1, 0], swap_sem.at[1, 1], twin).wait_recv()
    send.wait_send()
    for i in range(4):
        there = pl.ds(i * quarter, quarter)
        d_attn[:, there] = product(d_full[...], out_weight[:, there]).astype(jnp.bfloat16)
    event(done)
    done = done + 1
    per_group = q_heads // kv_heads
    qk_sum[...] = jnp.zeros_like(qk_sum)

    def group_step(group, carry):
        places = [group * per_group + r for r in range(per_group)]
        places += [q_heads + group, q_heads + kv_heads + group]
        copies = [
            pltpu.make_async_copy(qkv.at[:, head_at(place)], heads.at[i], head_sem.at[i])
            for i, place in enumerate(places)
        ]
        for copy in copies:
            copy.start()
        for copy in copies:
            copy.wait()
        attend_back(group, dims, heads, tab, seg_col, seg_row, gains, d_attn, d_proj, qk_sum, kept)
        event(done + group)
        return carry

    lax.fori_loop(0, kv_heads, group_step, 0)
    done = done + kv_heads

    def rest(e, carry):
        event(e)
        return carry

    lax.fori_loop(done, count * n, rest, 0)
    finish()


def backward_block(
    lefts, act, weights, qkv, out_weight, cot, resid, tab, segments, gains, mlp_gain, q_heads, kv_heads, dp
):
    n = dp // 2
    count, seq, width = act.shape
    half, model = resid.shape
    rows = model // dp
    low, dma, vmem = jnp.bfloat16, pltpu.SemaphoreType.DMA, pltpu.VMEM
    shape = jax.ShapeDtypeStruct
    place = lambda kind: pl.BlockSpec(memory_space=kind)
    deep = 256
    return pl.pallas_call(
        functools.partial(backward_kernel, n, (q_heads, kv_heads, seq, seq // 2)),
        out_shape=[
            shape((count, rows, width), jnp.float32),
            shape((seq, (q_heads + 2 * kv_heads) * HD), low),
            shape((seq, model), low),
            shape((half, model), jnp.float32),
            shape((1, model), jnp.float32),
            shape((8, HD), jnp.float32),
        ],
        in_specs=[place(vmem)] * 2 + [place(pltpu.HBM)] * 2 + [place(vmem)] * 8,
        out_specs=[place(pltpu.HBM)] + [place(vmem)] * 5,
        scratch_shapes=[
            vmem((deep, width), low),
            vmem((deep, width), low),
            vmem((half, model), jnp.float32),
            vmem((half, model), low),
            vmem((half, model), low),
            vmem((seq, q_heads * HD), low),
            vmem((q_heads // kv_heads + 2, seq, HD), jnp.float32),
            vmem((3, seq, HD), jnp.float32),
            dma((2, 2)),
            dma((2,)),
            dma((q_heads // kv_heads + 2,)),
            *reduce_scratch(n, count, rows, width // 2),
        ],
        compiler_params=pltpu.CompilerParams(
            collective_id=2, has_side_effects=True, vmem_limit_bytes=67043328
        ),
    )(
        lefts, act, weights, qkv, out_weight, cot, resid, tab,
        segments.reshape(seq, 1), segments.reshape(1, seq), gains, mlp_gain,
    )


def on_device(
    tokens,
    seg_ids,
    w_query,
    w_key,
    w_value,
    w_output,
    w_gate,
    w_up,
    w_down,
    gain_attn,
    gain_mlp,
    gain_qk,
    cotangent,
):
    dp = lax.axis_size("dp")
    input_rows = tokens.astype(jnp.float32)
    model = input_rows.shape[1]
    inverse_one = norm_rows(input_rows)
    normed_one = input_rows * inverse_one
    gain_row = jnp.concatenate(
        [
            jnp.pad(g.astype(jnp.float32), (0, 128 - g.shape[0]))
            for g in (gain_attn, gain_mlp, gain_qk)
        ]
    )
    gain_shard = jnp.broadcast_to(gain_row[None, :], (16, gain_row.shape[0]))
    shard_qkv = jnp.concatenate([w_query, w_key, w_value], axis=1)
    (qkv_weight, out_weight, gain_all), (full_rows, full_cot) = gather_weights(
        [shard_qkv, w_output.T, gain_shard], [tokens, cotangent], [2, 1, 1], dp, 0
    )
    gain_all = gain_all.reshape(dp, 16, 3, 128)[:, 0]
    attn_gain = gain_all[:, 0, : gain_attn.shape[0]].reshape(-1)
    full_rows = full_rows.astype(jnp.float32)
    full_one = (full_rows * norm_rows(full_rows) * attn_gain).astype(jnp.bfloat16)
    mlp_gain = gain_all[:, 1, : gain_mlp.shape[0]].reshape(-1)
    qk_gain = gain_all[:, 2, : gain_qk.shape[0]].reshape(-1)
    query_gain = qk_gain[:HD]
    key_gain = qk_gain[HD:]
    cosine_table, sine_table, _ = tables(seg_ids[0])
    seq_len = full_one.shape[0]
    q_width = w_query.shape[1]
    kv_width = w_key.shape[1]
    q_heads = q_width // HD
    kv_heads = kv_width // HD
    projected = product(full_one, qkv_weight)
    pair = jnp.stack([query_gain, key_gain])
    signed = jnp.concatenate([-sine_table[:, : HD // 2], sine_table[:, HD // 2 :]], axis=1)
    rope_tab = jnp.stack([cosine_table, signed])
    weights, attn_rows, resid, full_two, act = forward_block(
        jnp.stack([w_gate, w_up, w_down.T]),
        projected,
        out_weight,
        tokens,
        full_cot,
        rope_tab,
        seg_ids[0],
        pair,
        mlp_gain[None, :],
        q_heads,
        kv_heads,
        dp,
    )
    mlp_branch = lax.psum_scatter(
        tail_product(act[2], weights[2 * model :]).astype(jnp.bfloat16),
        "tensor",
        scatter_dimension=0,
        tiled=True,
    ).astype(jnp.float32)
    result_rows = (resid + mlp_branch).astype(jnp.bfloat16)
    grads, d_projected, full_resid, d_resid, mlp_gain_part, qk_part = backward_block(
        jnp.stack([full_two.T, full_cot.T]),
        act,
        weights,
        projected,
        out_weight,
        cotangent,
        resid,
        rope_tab,
        seg_ids[0],
        pair,
        mlp_gain[None, :],
        q_heads,
        kv_heads,
        dp,
    )
    grad_gate, grad_up, grad_down = grads[0], grads[1], grads[2]
    mlp_gain_part = mlp_gain_part[0]
    query_gain_part, key_gain_part = qk_part[0], qk_part[1]
    grad_qkv, grad_out = reduce_grads(
        [full_one.T, full_resid.T], [d_projected, attn_rows], [(0, 0), (1, 1)], dp, 3
    )
    d_normed_one = lax.psum_scatter(
        tail_product(d_projected, qkv_weight).astype(jnp.bfloat16),
        "tensor",
        scatter_dimension=0,
        tiled=True,
    ).astype(jnp.float32)
    attn_gain_part = jnp.sum(d_normed_one * normed_one, axis=0)
    input_grad = (d_resid + norm_back(d_normed_one * attn_gain, normed_one, inverse_one)).astype(
        jnp.bfloat16
    )
    gain_sums = lax.psum(
        jnp.concatenate([attn_gain_part, mlp_gain_part, query_gain_part, key_gain_part]),
        ("dp", "tensor"),
    )
    me = lax.axis_index("dp")
    share = model // dp
    qk_share = 2 * HD // dp
    return (
        result_rows,
        input_grad,
        grad_qkv[:, :q_width],
        grad_qkv[:, q_width : q_width + kv_width],
        grad_qkv[:, q_width + kv_width :],
        grad_out.T,
        grad_gate,
        grad_up,
        grad_down.T,
        lax.dynamic_slice(gain_sums, (me * share,), (share,)),
        lax.dynamic_slice(gain_sums, (model + me * share,), (share,)),
        lax.dynamic_slice(gain_sums, (2 * model + me * qk_share,), (qk_share,)),
    )


def solution(mesh):
    return jax.shard_map(
        on_device,
        mesh=mesh,
        in_specs=(
            P(("dp", "tensor"), None),
            P("dp", None),
            P("dp", "tensor"),
            P("dp", "tensor"),
            P("dp", "tensor"),
            P("tensor", "dp"),
            P("dp", "tensor"),
            P("dp", "tensor"),
            P("tensor", "dp"),
            P("dp"),
            P("dp"),
            P("dp"),
            P(("dp", "tensor"), None),
        ),
        out_specs=(
            P(("dp", "tensor"), None),
            P(("dp", "tensor"), None),
            P("dp", "tensor"),
            P("dp", "tensor"),
            P("dp", "tensor"),
            P("tensor", "dp"),
            P("dp", "tensor"),
            P("dp", "tensor"),
            P("tensor", "dp"),
            P("dp"),
            P("dp"),
            P("dp"),
        ),
        check_vma=False,
    )
```

```python
import functools
import jax
import jax.numpy as jnp
from jax import lax
from jax.experimental import pallas as pl
from jax.experimental.pallas import tpu as pltpu

from jax.sharding import PartitionSpec as P

MESH = pl.DeviceIdType.MESH
HD = 128
epsilon = 1e-06
rope_base = 1000000.0


def ring_place(n):
    me = lax.axis_index("dp")
    chip = me // 2
    core = me % 2
    odd = chip % 2
    pos = (1 - odd) * (chip // 2) + odd * (n - 1 - chip // 2)
    return pos, core


def chip_at(pos, n):
    high = pos // (n // 2)
    return (1 - high) * (2 * pos) + high * (2 * (n - 1 - pos) + 1)


def at(pos, core, n):
    return (chip_at(pos, n) * 2 + core, lax.axis_index("tensor"))


def meet(peers):
    barrier = pltpu.get_barrier_semaphore()
    for peer in peers:
        pl.semaphore_signal(barrier, inc=1, device_id=peer, device_id_type=MESH)
    pl.semaphore_wait(barrier, len(peers))


def remote(src, dst, send, recv, peer):
    return pltpu.make_async_remote_copy(
        src_ref=src, dst_ref=dst, send_sem=send, recv_sem=recv, device_id=peer, device_id_type=MESH
    )


def gather_kernel(n, parts, count, swaps, *refs):
    shards = refs[:count]
    halves = refs[count : count + swaps]
    fulls = refs[count + swaps : 2 * count + swaps]
    wholes = refs[2 * count + swaps : 2 * (count + swaps)]
    own_sem, send_sem, recv_sem, give_sem, take_sem, swap_sem = refs[2 * (count + swaps) :]
    pos, core = ring_place(n)
    lane = lax.axis_index("tensor")
    nexts = (at((pos + 1) % n, core, n), at((pos + n - 1) % n, core, n))
    mate = at(pos, 1 - core, n)
    twin = (lax.axis_index("dp"), 1 - lane)
    meet((*nexts, mate, twin))
    messages = [(w, part) for w in range(count) for part in range(parts[w])]

    def sizes(w):
        rows = shards[w].shape[0]
        return rows, rows // 2, rows // 2 // parts[w]

    def spot(w, owner, who, side, part):
        rows, half, piece = sizes(w)
        start = (chip_at(owner, n) * 2 + who) * rows + (side * half + part * piece)
        return fulls[w].at[pl.ds(pl.multiple_of(start, piece), piece)]

    def shard_of(w, who):
        rows = shards[w].shape[0]
        return fulls[w].at[pl.ds(pl.multiple_of((chip_at(pos, n) * 2 + who) * rows, rows), rows)]

    def swap_spot(s, which):
        rows = halves[s].shape[0]
        return wholes[s].at[pl.ds(pl.multiple_of(which * rows, rows), rows)]

    for k, (w, part) in enumerate(messages):
        rows, half, piece = sizes(w)
        for side in range(2):
            src = shards[w].at[pl.ds(side * half + part * piece, piece)]
            remote(
                src, spot(w, pos, core, side, part), send_sem.at[k, side, 0], recv_sem.at[k, side, 0], nexts[side]
            ).start()
    for s in range(swaps):
        remote(halves[s], swap_spot(s, lane), swap_sem.at[s, 0], swap_sem.at[s, 1], twin).start()
        pltpu.make_async_copy(halves[s], swap_spot(s, lane), own_sem.at[count + s]).start()
    for w in range(count):
        remote(shards[w], shard_of(w, core), give_sem.at[w, 0, n - 1], take_sem.at[w, 0, n - 1], mate).start()
        pltpu.make_async_copy(shards[w], shard_of(w, core), own_sem.at[w]).start()

    def owner_of(side, step):
        if side == 0:
            return (pos - 1 - step + 2 * n) % n
        return (pos + 1 + step) % n

    def step_body(step, carry):
        for k, (w, part) in enumerate(messages):
            for side in range(2):
                block = spot(w, owner_of(side, step), core, side, part)
                remote(block, block, send_sem.at[k, side, step], recv_sem.at[k, side, step], nexts[side]).wait_recv()

                @pl.when(step < n - 2)
                def _():
                    remote(
                        block, block, send_sem.at[k, side, step + 1], recv_sem.at[k, side, step + 1], nexts[side]
                    ).start()

                remote(block, block, give_sem.at[k, side, step], take_sem.at[k, side, step], mate).start()
        return carry

    lax.fori_loop(0, n - 1, step_body, 0)

    def drain(step, carry):
        for k, (w, part) in enumerate(messages):
            for side in range(2):
                owner = owner_of(side, step)
                block = spot(w, owner, core, side, part)
                theirs = spot(w, owner, 1 - core, side, part)
                remote(block, block, send_sem.at[k, side, step], recv_sem.at[k, side, step], nexts[side]).wait_send()
                given = remote(block, theirs, give_sem.at[k, side, step], take_sem.at[k, side, step], mate)
                given.wait_send()
                given.wait_recv()
        return carry

    lax.fori_loop(0, n - 1, drain, 0)
    for w in range(count):
        pltpu.make_async_copy(shards[w], shard_of(w, core), own_sem.at[w]).wait()
        given = remote(shards[w], shard_of(w, 1 - core), give_sem.at[w, 0, n - 1], take_sem.at[w, 0, n - 1], mate)
        given.wait_send()
        given.wait_recv()
    for s in range(swaps):
        pltpu.make_async_copy(halves[s], swap_spot(s, lane), own_sem.at[count + s]).wait()
        other = remote(halves[s], swap_spot(s, 1 - lane), swap_sem.at[s, 0], swap_sem.at[s, 1], twin)
        other.wait_send()
        other.wait_recv()


def gather_weights(shards, swaps, parts, dp, collective_id):
    n = dp // 2
    count = len(shards)
    msgs = sum(parts)
    dma = pltpu.SemaphoreType.DMA
    outs = pl.pallas_call(
        functools.partial(gather_kernel, n, tuple(parts), count, len(swaps)),
        out_shape=[
            *[jax.ShapeDtypeStruct((s.shape[0] * dp, s.shape[1]), s.dtype) for s in shards],
            *[jax.ShapeDtypeStruct((s.shape[0] * 2, s.shape[1]), s.dtype) for s in swaps],
        ],
        in_specs=[pl.BlockSpec(memory_space=pltpu.VMEM)] * (count + len(swaps)),
        out_specs=[pl.BlockSpec(memory_space=pltpu.HBM)] * (count + len(swaps)),
        scratch_shapes=[
            dma((count + len(swaps),)),
            dma((msgs, 2, n - 1)),
            dma((msgs, 2, n - 1)),
            dma((msgs, 2, n)),
            dma((msgs, 2, n)),
            dma((max(1, len(swaps)), 2)),
        ],
        compiler_params=pltpu.CompilerParams(collective_id=collective_id, has_side_effects=True),
    )(*shards, *swaps)
    return outs[:count], outs[count:]


def reduce_kernel(n, pairs, *refs):
    n_left = 1 + max(p[0] for p in pairs)
    n_right = 1 + max(p[1] for p in pairs)
    count = len(pairs)
    lefts = refs[:n_left]
    rights = refs[n_left : n_left + n_right]
    outs = refs[n_left + n_right : n_left + n_right + count]
    rest = refs[n_left + n_right + count :]
    mine, give, take, ship, land = (rest[i * count : (i + 1) * count] for i in range(5))
    term, give_sem, take_sem, ship_sem, land_sem = rest[5 * count :]
    pos, core = ring_place(n)
    nexts = (at((pos + 1) % n, core, n), at((pos + n - 1) % n, core, n))
    mate = at(pos, 1 - core, n)
    meet((*nexts, mate))
    rows = outs[0].shape[0]

    def owner_of(side, step):
        if side == 0:
            return (pos - 1 - step + 2 * n) % n
        return (pos + 1 + step) % n

    def early(m, side, step):
        left, right = pairs[m]
        wide = outs[m].shape[1] // 2
        slot = step % 2
        start = pl.multiple_of(chip_at(owner_of(side, step), n) * 2 * rows, 2 * rows)
        part = term.at[:, pl.ds(0, wide)]
        part[...] = jnp.dot(
            lefts[left][pl.ds(start, 2 * rows), :],
            rights[right][:, pl.ds(side * wide, wide)],
            preferred_element_type=jnp.float32,
        )
        other = pl.ds(pl.multiple_of((1 - core) * rows, rows), rows)
        same = pl.ds(pl.multiple_of(core * rows, rows), rows)
        given = remote(
            give[m].at[side, slot], take[m].at[side, slot],
            give_sem.at[m, side, slot], take_sem.at[m, side, slot], mate,
        )

        @pl.when(step >= 2)
        def _():
            given.wait_send()

        give[m][side, slot] = part[other, :].astype(jnp.bfloat16)
        given.start()
        mine[m][side] = part[same, :]

    def shipped(m, side, step):
        return remote(
            ship[m].at[side, step % 2], land[m].at[side, step],
            ship_sem.at[m, side, step % 2], land_sem.at[m, side, step], nexts[side],
        )

    def local_sum(m, side, step):
        slot = step % 2
        remote(
            give[m].at[side, slot], take[m].at[side, slot],
            give_sem.at[m, side, slot], take_sem.at[m, side, slot], mate,
        ).wait_recv()
        return mine[m][side] + take[m][side, slot].astype(jnp.float32)

    for m in range(count):
        for side in range(2):
            early(m, side, 0)
    for m in range(count):
        for side in range(2):
            total = local_sum(m, side, 0)
            ship[m][side, 0] = total.astype(jnp.bfloat16)
            shipped(m, side, 0).start()
            early(m, side, 1)

    def step_body(step, carry):
        for m in range(count):
            for side in range(2):
                total = local_sum(m, side, step)
                shipped(m, side, step - 1).wait_recv()
                total = total + land[m][side, step - 1].astype(jnp.float32)

                @pl.when(step >= 2)
                def _():
                    shipped(m, side, step - 2).wait_send()

                ship[m][side, step % 2] = total.astype(jnp.bfloat16)
                shipped(m, side, step).start()
                early(m, side, step + 1)
        return carry

    lax.fori_loop(1, n - 1, step_body, 0)
    last = n - 1
    for m in range(count):
        wide = outs[m].shape[1] // 2
        for side in range(2):
            total = local_sum(m, side, last)
            shipped(m, side, last - 1).wait_recv()
            outs[m][:, pl.ds(side * wide, wide)] = total + land[m][side, last - 1].astype(jnp.float32)
    for m in range(count):
        for side in range(2):
            shipped(m, side, last - 1).wait_send()
            if last >= 2:
                shipped(m, side, last - 2).wait_send()
            for slot in range(2):
                remote(
                    give[m].at[side, slot], take[m].at[side, slot],
                    give_sem.at[m, side, slot], take_sem.at[m, side, slot], mate,
                ).wait_send()


def reduce_grads(lefts, rights, pairs, dp, collective_id):
    n = dp // 2
    count = len(pairs)
    rows = lefts[0].shape[0] // dp
    wides = [rights[r].shape[1] // 2 for _, r in pairs]
    low = jnp.bfloat16
    return pl.pallas_call(
        functools.partial(reduce_kernel, n, tuple(pairs)),
        out_shape=[jax.ShapeDtypeStruct((rows, 2 * w), jnp.float32) for w in wides],
        in_specs=[pl.BlockSpec(memory_space=pltpu.VMEM)] * (len(lefts) + len(rights)),
        out_specs=[pl.BlockSpec(memory_space=pltpu.VMEM)] * count,
        scratch_shapes=[
            *[pltpu.VMEM((2, rows, w), jnp.float32) for w in wides],
            *[pltpu.VMEM((2, 2, rows, w), low) for w in wides],
            *[pltpu.VMEM((2, 2, rows, w), low) for w in wides],
            *[pltpu.VMEM((2, 2, rows, w), low) for w in wides],
            *[pltpu.VMEM((2, n - 1, rows, w), low) for w in wides],
            pltpu.VMEM((2 * rows, max(wides)), jnp.float32),
            pltpu.SemaphoreType.DMA((count, 2, 2)),
            pltpu.SemaphoreType.DMA((count, 2, 2)),
            pltpu.SemaphoreType.DMA((count, 2, 2)),
            pltpu.SemaphoreType.DMA((count, 2, n - 1)),
        ],
        compiler_params=pltpu.CompilerParams(
            collective_id=collective_id, has_side_effects=True, vmem_limit_bytes=67043328
        ),
    )(*lefts, *rights)


def product(left, right):
    return jnp.dot(left, right, preferred_element_type=jnp.float32)


def lead_product(left, right):
    return lax.dot_general(
        left, right, (((0,), (0,)), ((), ())), preferred_element_type=jnp.float32
    )


def tail_product(left, right):
    return lax.dot_general(
        left, right, (((1,), (1,)), ((), ())), preferred_element_type=jnp.float32
    )


def norm_rows(values):
    return lax.rsqrt(jnp.mean(values * values, axis=-1, keepdims=True) + epsilon)


def norm_back(incoming, normed, inverse):
    return inverse * (incoming - normed * jnp.mean(incoming * normed, axis=-1, keepdims=True))


def rotate(values, cosine_table, sine_table):
    half_width = values.shape[-1] // 2
    turned = jnp.concatenate([-values[..., half_width:], values[..., :half_width]], axis=-1)
    return values * cosine_table + turned * sine_table


def rotate_back(incoming, cosine_table, sine_table):
    half_width = incoming.shape[-1] // 2
    scaled = incoming * sine_table
    return incoming * cosine_table + jnp.concatenate(
        [scaled[..., half_width:], -scaled[..., :half_width]], axis=-1
    )


def tables(segments):
    seq_len = segments.shape[0]
    token_index = jnp.arange(seq_len, dtype=jnp.int32)
    doc_start = jnp.sum((segments[None, :] < segments[:, None]).astype(jnp.int32), axis=1)
    doc_pos = (token_index - doc_start).astype(jnp.float32)
    frequency = rope_base ** (-jnp.arange(0, HD, 2).astype(jnp.float32) / HD)
    angles = doc_pos[:, None] * frequency[None, :]
    cosine_table = jnp.concatenate([jnp.cos(angles), jnp.cos(angles)], axis=1)
    sine_table = jnp.concatenate([jnp.sin(angles), jnp.sin(angles)], axis=1)
    allowed = (segments[:, None] == segments[None, :]) & (
        token_index[None, :] <= token_index[:, None]
    )
    return (cosine_table, sine_table, allowed)


def turn(values):
    return pltpu.roll(values, values.shape[-1] // 2, 1)


def row_scale(values):
    return lax.rsqrt(jnp.mean(values * values, axis=-1, keepdims=True) + epsilon)


def head_at(index):
    return pl.ds(pl.multiple_of(index * HD, HD), HD)


def prepared(raw, gain, cosine, sine):
    inverse = row_scale(raw)
    hat = raw * inverse
    scaled = hat * gain
    return inverse, hat, (scaled * cosine + turn(scaled) * sine).astype(jnp.bfloat16)


def exp_block(query, keys, seg_col, seg_row, first):
    width = keys.shape[0]
    scores = tail_product(query, keys) * HD ** (-0.5)
    rows = lax.broadcasted_iota(jnp.int32, scores.shape, 0) + first
    columns = lax.broadcasted_iota(jnp.int32, scores.shape, 1)
    allowed = (seg_col[first : first + scores.shape[0], :] == seg_row[:, :width]) & (
        columns <= rows
    )
    return jnp.where(allowed, jnp.exp(scores), 0.0)


def attend_group(group, dims, qkv, tab, seg_col, seg_row, gains, attn, kept):
    q_heads, kv_heads, seq, block = dims
    per_group = q_heads // kv_heads
    cosine, sine = tab[0], tab[1]
    raw = qkv[:, head_at(q_heads + group)]
    kept[0] = prepared(raw, gains[1:2, :], cosine, sine)[2]
    kept[1] = qkv[:, head_at(q_heads + kv_heads + group)].astype(jnp.bfloat16)
    for r in range(per_group):
        head = group * per_group + r
        raw = qkv[:, head_at(head)]
        query = prepared(raw, gains[0:1, :], cosine, sine)[2]
        for first in range(0, seq, block):
            width = first + block
            exps = exp_block(query[first:width], kept[0, :width, :], seg_col, seg_row, first)
            probs = (exps / jnp.sum(exps, axis=-1, keepdims=True)).astype(jnp.bfloat16)
            attn[first:width, head_at(head)] = product(probs, kept[1, :width, :]).astype(jnp.bfloat16)


def block_columns(ref, index, width):
    if width % 128 == 0:
        return ref[:, pl.ds(pl.multiple_of(index * width, width), width)]
    fold = 128 // width
    tile = ref[:, pl.ds(pl.multiple_of((index // fold) * 128, 128), 128)]
    picked = tile[:, :width]
    for i in range(1, fold):
        picked = jnp.where(index % fold == i, tile[:, i * width : (i + 1) * width], picked)
    return picked


def flip_into(source, target, stage, stage_sem):
    deep = stage.shape[1]
    turns = source.shape[1] // deep

    def put(i):
        return pltpu.make_async_copy(
            stage.at[i % 2], target.at[pl.ds(pl.multiple_of(i * deep, deep), deep)], stage_sem.at[i % 2]
        )

    def one(i, carry):
        @pl.when(i >= 2)
        def _():
            put(i - 2).wait()

        stage[i % 2] = source[:, pl.ds(pl.multiple_of(i * deep, deep), deep)].T
        put(i).start()
        return carry

    lax.fori_loop(0, turns, one, 0)
    put(turns - 2).wait()
    put(turns - 1).wait()


def forward_kernel(n, dims, *refs):
    (
        shards, qkv, out_weight, tokens, full_one, cot_full, tab, seg_col, seg_row, gains, mlp_gain,
        weights, attn, resid, flipped, act,
        full_two, kept, part, peer, acc, blocks, stage,
        own_sem, send_sem, recv_sem, give_sem, take_sem, swap_sem, load_sem, stage_sem,
    ) = refs
    q_heads, kv_heads, seq, block = dims
    pos, core = ring_place(n)
    lane = lax.axis_index("tensor")
    nexts = (at((pos + 1) % n, core, n), at((pos + n - 1) % n, core, n))
    mate = at(pos, 1 - core, n)
    twin = (lax.axis_index("dp"), 1 - lane)
    count, rows, width = shards.shape
    wide = width // 2
    model = 2 * n * rows
    half = seq // 2
    meet((*nexts, mate, twin))

    def owner_of(side, step):
        if side == 0:
            return (pos - step + 2 * n) % n
        return (pos + step) % n

    def spot(w, chip, who, side):
        start = w * model + (chip * 2 + who) * rows
        return weights.at[pl.ds(pl.multiple_of(start, rows), rows), pl.ds(side * wide, wide)]

    def hop(w, side, step):
        here = spot(w, chip_at(owner_of(side, step), n), core, side)
        return remote(here, here, send_sem.at[w, side, step], recv_sem.at[w, side, step], nexts[side])

    def first_hop(w, side):
        return remote(
            shards.at[w, :, pl.ds(side * wide, wide)],
            spot(w, chip_at(pos, n), core, side),
            send_sem.at[w, side, 1], recv_sem.at[w, side, 1], nexts[side],
        )

    def onward(w, side, step):
        here = spot(w, chip_at(owner_of(side, step), n), core, side)
        return remote(here, here, send_sem.at[w, side, step + 1], recv_sem.at[w, side, step + 1], nexts[side])

    def hand(w, side, step, who):
        here = spot(w, chip_at(owner_of(side, step), n), who, side)
        return remote(here, here, give_sem.at[w, side, step], take_sem.at[w, side, step], mate)

    def hand_own(w, side, who):
        return remote(
            shards.at[w, :, pl.ds(side * wide, wide)],
            spot(w, chip_at(pos, n), who, side),
            give_sem.at[w, side, 0], take_sem.at[w, side, 0], mate,
        )

    def keep_own(w, side):
        return pltpu.make_async_copy(
            shards.at[w, :, pl.ds(side * wide, wide)], spot(w, chip_at(pos, n), core, side), own_sem.at[w, side]
        )

    for w in range(count):
        for side in range(2):
            first_hop(w, side).start()
    for w in range(count):
        for side in range(2):
            hand_own(w, side, core).start()
            keep_own(w, side).start()

    def service(event):
        step, w = event // count + 1, event % count
        for side in range(2):
            hop(w, side, step).wait_recv()

            @pl.when(step < n - 1)
            def _():
                onward(w, side, step).start()

            hand(w, side, step, core).start()

    def load(job, side):
        step, w = job // count, job % count
        start = w * model + chip_at(owner_of(side, step), n) * 2 * rows
        return pltpu.make_async_copy(
            weights.at[pl.ds(pl.multiple_of(start, 2 * rows), 2 * rows), pl.ds(side * wide, wide)],
            blocks.at[side], load_sem.at[side],
        )

    def work(job):
        step, w = job // count, job % count
        for side in range(2):
            @pl.when(step > 0)
            def _():
                hand(w, side, step, 1 - core).wait_recv()

            @pl.when(step == 0)
            def _():
                hand_own(w, side, 1 - core).wait_recv()
                keep_own(w, side).wait()

            load(job, side).start()
        for side in range(2):
            load(job, side).wait()
            chip = chip_at(owner_of(side, step), n)

            def with_left(left):
                tile = wide // 3

                def one(i, carry):
                    there = pl.ds(pl.multiple_of(side * wide + i * tile, tile), tile)
                    gained = product(left, blocks[side, :, pl.ds(pl.multiple_of(i * tile, tile), tile)])

                    @pl.when(step == 0)
                    def _():
                        acc[w, :, there] = gained

                    @pl.when(step > 0)
                    def _():
                        acc[w, :, there] += gained

                    return carry

                lax.fori_loop(0, 3, one, 0)

            @pl.when(w < 2)
            def _():
                with_left(block_columns(full_two, chip, 2 * rows))

            @pl.when(w == 2)
            def _():
                with_left(block_columns(cot_full, chip, 2 * rows))

    def flip(source, target):
        flip_into(source, flipped.at[target], stage, stage_sem)

    groups = (qkv, tab, seg_col, seg_row, gains, attn, kept)

    def attend(first, last):
        def one(group, carry):
            attend_group(group, dims, *groups)
            return carry

        lax.fori_loop(first, last, one, 0)

    attend(0, kv_heads // 2)
    service(0)
    attend(kv_heads // 2, kv_heads)
    service(1)
    theirs = pl.ds(pl.multiple_of((1 - lane) * half, half), half)
    ours = pl.ds(pl.multiple_of(lane * half, half), half)
    part[...] = tail_product(attn[theirs, :], out_weight[...]).astype(jnp.bfloat16)
    send_part = remote(part, peer, swap_sem.at[0, 0], swap_sem.at[0, 1], twin)
    send_part.start()
    resid[...] = tokens[...].astype(jnp.float32) + tail_product(attn[ours, :], out_weight[...])
    service(2)
    flip(full_one, 2)
    service(3)
    flip(cot_full, 1)
    for event in range(4, 6):
        service(event)
    send_part.wait_recv()
    summed = resid[...] + peer[...].astype(jnp.float32)
    resid[...] = summed
    send_part.wait_send()
    part[...] = (summed * row_scale(summed) * mlp_gain[...]).astype(jnp.bfloat16)
    send_two = remote(part, full_two.at[ours], swap_sem.at[1, 0], swap_sem.at[1, 1], twin)
    send_two.start()
    full_two[ours, :] = part[...]
    ready = 9
    for event in range(6, ready):
        service(event)
    remote(part, full_two.at[theirs], swap_sem.at[1, 0], swap_sem.at[1, 1], twin).wait_recv()
    flip(full_two, 0)

    def both(i, carry):
        service(ready + i)

        @pl.when(i < ready + 3)
        def _():
            def one(q, carry):
                work(2 * i + q)
                return carry

            lax.fori_loop(0, 2, one, 0)

        @pl.when(i >= ready + 3)
        def _():
            work(ready + 3 + i)

        return carry

    lax.fori_loop(0, count * (n - 1) - ready, both, 0)
    send_two.wait_send()

    strip = 32

    def finish(i, carry):
        there = pl.ds(pl.multiple_of(i * strip, strip), strip)
        gate = acc[0, there, :]
        up = acc[1, there, :]
        d_act = acc[2, there, :]
        sig = 1.0 / (1.0 + jnp.exp(-gate))
        silu = gate * sig
        act[0, there, :] = (d_act * up * sig * (1.0 + gate * (1.0 - sig))).astype(jnp.bfloat16)
        act[1, there, :] = (d_act * silu).astype(jnp.bfloat16)
        act[2, there, :] = (silu * up).astype(jnp.bfloat16)
        return carry

    lax.fori_loop(0, seq // strip, finish, 0)

    def drain(step, carry):
        for w in range(count):
            for side in range(2):
                hop(w, side, step).wait_send()
                hand(w, side, step, core).wait_send()
        return carry

    lax.fori_loop(1, n, drain, 0)
    for w in range(count):
        for side in range(2):
            hand_own(w, side, core).wait_send()


def forward_block(shards, qkv, out_weight, tokens, full_one, cot_full, tab, segments, gains, mlp_gain, q_heads, kv_heads, dp):
    n = dp // 2
    count, rows, width = shards.shape
    seq, model = cot_full.shape
    half = seq // 2
    low, dma, vmem = jnp.bfloat16, pltpu.SemaphoreType.DMA, pltpu.VMEM
    shape = jax.ShapeDtypeStruct
    place = lambda kind: pl.BlockSpec(memory_space=kind)
    return pl.pallas_call(
        functools.partial(forward_kernel, n, (q_heads, kv_heads, seq, seq // 2)),
        out_shape=[
            shape((count * model, width), low),
            shape((seq, q_heads * HD), low),
            shape((half, model), jnp.float32),
            shape((3, model, seq), low),
            shape((count, seq, width), low),
        ],
        in_specs=[place(vmem)] * 11,
        out_specs=[place(pltpu.HBM), place(vmem), place(vmem), place(pltpu.HBM), place(vmem)],
        scratch_shapes=[
            vmem((seq, model), low),
            vmem((2, seq, HD), low),
            vmem((half, model), low),
            vmem((half, model), low),
            vmem((count, seq, width), jnp.float32),
            vmem((2, 2 * rows, width // 2), low),
            vmem((2, 256, seq), low),
            dma((count, 2)),
            dma((count, 2, n)),
            dma((count, 2, n)),
            dma((count, 2, n)),
            dma((count, 2, n)),
            dma((2, 2)),
            dma((2,)),
            dma((2,)),
        ],
        compiler_params=pltpu.CompilerParams(
            collective_id=1, has_side_effects=True, vmem_limit_bytes=67043328
        ),
    )(
        shards, qkv, out_weight, tokens, full_one, cot_full, tab,
        segments.reshape(seq, 1), segments.reshape(1, seq), gains, mlp_gain,
    )


SLOTS = 3


def undo(incoming, hat, inverse, gain, cosine, sine):
    turned = incoming * cosine - turn(incoming) * sine
    total = jnp.sum(turned * hat, axis=0, keepdims=True)
    scaled = turned * gain
    raw = inverse * (scaled - hat * jnp.mean(scaled * hat, axis=-1, keepdims=True))
    return total, raw.astype(jnp.bfloat16)


def attend_back(group, dims, heads, tab, seg_col, seg_row, gains, d_attn, d_proj, sums, kept):
    q_heads, kv_heads, seq, block = dims
    per_group = q_heads // kv_heads
    low = jnp.bfloat16
    scale = HD ** (-0.5)
    cosine, sine = tab[0], tab[1]
    keys = prepared(heads[per_group], gains[1:2, :], cosine, sine)[2]
    values = heads[per_group + 1].astype(low)
    for r in range(per_group):
        head = group * per_group + r
        q_inverse, q_hat, query = prepared(heads[r], gains[0:1, :], cosine, sine)
        for first in range(0, seq, block):
            width = first + block
            exps = exp_block(query[first:width], keys[:width], seg_col, seg_row, first)
            probs = exps / jnp.sum(exps, axis=-1, keepdims=True)
            incoming = d_attn[first:width, head_at(head)]
            d_probs = tail_product(incoming, values[:width])
            delta = jnp.sum(probs * d_probs, axis=-1, keepdims=True)
            d_scores = (probs * (d_probs - delta)).astype(low)
            kept[0, first:width, :] = product(d_scores, keys[:width]) * scale
            d_keys = lead_product(d_scores, query[first:width])
            d_values = lead_product(probs.astype(low), incoming)
            if r == 0 and first == 0:
                kept[1] = jnp.zeros_like(kept[1])
                kept[2] = jnp.zeros_like(kept[2])
            kept[1, :width, :] += d_keys
            kept[2, :width, :] += d_values
        total, raw = undo(kept[0], q_hat, q_inverse, gains[0:1, :], cosine, sine)
        sums[0:1, :] += total
        d_proj[0, :, head_at(head)] = raw
    k_inverse, k_hat, _ = prepared(heads[per_group], gains[1:2, :], cosine, sine)
    total, raw = undo(kept[1] * scale, k_hat, k_inverse, gains[1:2, :], cosine, sine)
    sums[1:2, :] += total
    d_proj[1, :, head_at(group)] = raw
    d_proj[1, :, head_at(kv_heads + group)] = kept[2].astype(low)


def reducer(n, pos, core, nexts, mate, refs, left_of):
    lefts, rights, out, mine, term, give, take, ship, land, give_sem, take_sem, ship_sem, land_sem, free_sem, out_sem = refs
    count = rights.shape[0]
    wide = rights.shape[2] // 2
    rows = out.shape[1]

    def owner_of(side, step):
        if side == 0:
            return (pos - 1 - step + 2 * n) % n
        return (pos + 1 + step) % n

    def given(m, side, step):
        return remote(
            give.at[m, side], take.at[m, side, step % 2],
            give_sem.at[m, side], take_sem.at[m, side, step % 2], mate,
        )

    def shipped(m, side, step):
        return remote(
            ship.at[m, side], land.at[m, side, step % SLOTS],
            ship_sem.at[m, side], land_sem.at[m, side, step % SLOTS], nexts[side],
        )

    def early(m, step):
        for side in range(2):
            start = pl.multiple_of(chip_at(owner_of(side, step), n) * 2 * rows, 2 * rows)
            left = lefts[left_of(m), pl.ds(start, 2 * rows), :]
            tile = min(512, wide)

            def one(i, carry):
                there = pl.multiple_of(i * tile, tile)
                term[:, pl.ds(there, tile)] = product(
                    left, rights[m, :, pl.ds(pl.multiple_of(side * wide + there, tile), tile)]
                )
                return carry

            lax.fori_loop(0, wide // tile, one, 0)

            @pl.when(step >= 1)
            def _():
                given(m, side, step - 1).wait_send()

            give[m, side] = term[pl.ds(pl.multiple_of((1 - core) * rows, rows), rows), :].astype(jnp.bfloat16)
            given(m, side, step).start()
            mine[m, side] = term[pl.ds(pl.multiple_of(core * rows, rows), rows), :]

    def event(e):
        step, m = e // count, e % count
        for side in range(2):
            given(m, side, step).wait_recv()

            @pl.when(step == 0)
            def _():
                mine[m, side] += take[m, side, 0].astype(jnp.float32)

            @pl.when(step > 0)
            def _():
                shipped(m, side, step - 1).wait_recv()
                mine[m, side] += take[m, side, step % 2].astype(jnp.float32) + land[
                    m, side, (step - 1) % SLOTS
                ].astype(jnp.float32)

                @pl.when(step - 1 + SLOTS <= n - 2)
                def _():
                    pl.semaphore_signal(
                        free_sem.at[m, side], inc=1, device_id=nexts[1 - side], device_id_type=MESH
                    )

                shipped(m, side, step - 1).wait_send()

            @pl.when(step < n - 1)
            def _():
                @pl.when(step >= SLOTS)
                def _():
                    pl.semaphore_wait(free_sem.at[m, side], 1)

                ship[m, side] = mine[m, side].astype(jnp.bfloat16)
                shipped(m, side, step).start()

            @pl.when(step == n - 1)
            def _():
                written(m, side).start()

        @pl.when(step < n - 1)
        def _():
            early(m, step + 1)

    def written(m, side):
        return pltpu.make_async_copy(mine.at[m, side], out.at[m, :, pl.ds(side * wide, wide)], out_sem.at[m, side])

    def finish():
        for m in range(count):
            for side in range(2):
                given(m, side, n - 1).wait_send()
                written(m, side).wait()

    return early, event, finish


def reduce_scratch(n, count, rows, wide):
    low, dma, vmem = jnp.bfloat16, pltpu.SemaphoreType.DMA, pltpu.VMEM
    return [
        vmem((count, 2, rows, wide), jnp.float32),
        vmem((2 * rows, wide), jnp.float32),
        vmem((count, 2, rows, wide), low),
        vmem((count, 2, 2, rows, wide), low),
        vmem((count, 2, rows, wide), low),
        vmem((count, 2, SLOTS, rows, wide), low),
        dma((count, 2)),
        dma((count, 2, 2)),
        dma((count, 2)),
        dma((count, 2, SLOTS)),
        pltpu.SemaphoreType.REGULAR((count, 2)),
        dma((count, 2)),
    ]


def backward_kernel(n, dims, *refs):
    (
        flipped, act, weights, qkv, attn, out_weight, cot, resid, tab, seg_col, seg_row, gains, mlp_gain,
        grads, d_proj, d_flip, d_resid, mlp_sum, qk_sum,
        lefts, d_full, gate_block, up_block, own, part, peer, d_attn, heads, kept, stage,
        swap_sem, load_sem, head_sem, left_sem, stage_sem,
    ) = refs[:35]
    q_heads, kv_heads, seq, block = dims
    pos, core = ring_place(n)
    lane = lax.axis_index("tensor")
    nexts = (at((pos + 1) % n, core, n), at((pos + n - 1) % n, core, n))
    mate = at(pos, 1 - core, n)
    twin = (lax.axis_index("dp"), 1 - lane)
    fetch_lefts = pltpu.make_async_copy(flipped.at[pl.ds(0, 2)], lefts, left_sem.at[0])
    fetch_lefts.start()
    fetch_attn = pltpu.make_async_copy(attn, d_proj.at[2], left_sem.at[1])
    fetch_attn.start()
    meet((*nexts, mate, twin))
    fetch_lefts.wait()
    fetch_attn.wait()
    count = act.shape[0]
    model = resid.shape[1]
    half = seq // 2
    early, event, finish = reducer(
        n, pos, core, nexts, mate, (lefts, act, grads, *refs[35:]), lambda m: m // 2
    )
    for m in range(count):
        early(m, 0)
    for m in range(count):
        event(m)

    theirs = pl.ds(pl.multiple_of((1 - lane) * half, half), half)
    ours = pl.ds(pl.multiple_of(lane * half, half), half)
    deep = gate_block.shape[0]
    turns = model // deep

    def fetch(i, which):
        target = (gate_block, up_block)[which]
        start = which * model + i * deep
        return pltpu.make_async_copy(
            weights.at[pl.ds(pl.multiple_of(start, deep), deep), :], target, load_sem.at[which]
        )

    fetch(0, 0).start()
    fetch(0, 1).start()

    def narrow(i, carry):
        there = pl.ds(pl.multiple_of(i * deep, deep), deep)
        for which, target in enumerate((gate_block, up_block)):
            fetch(i, which).wait()
            other = tail_product(act[which, theirs, :], target[...])
            same = tail_product(act[which, ours, :], target[...])
            if which == 0:
                own[:, there] = same
                d_resid[:, there] = other
            else:
                own[:, there] += same
                part[:, there] = (d_resid[:, there] + other).astype(jnp.bfloat16)

            @pl.when(i < turns - 1)
            def _():
                fetch(i + 1, which).start()

        @pl.when(i % 3 == 2)
        def _():
            event(count + i // 3)

        return carry

    lax.fori_loop(0, turns, narrow, 0)
    done = count + turns // 3
    send = remote(part, peer, swap_sem.at[0, 0], swap_sem.at[0, 1], twin)
    send.start()
    for e in range(done, done + 3):
        event(e)
    done = done + 3
    send.wait_recv()
    send.wait_send()
    strip = 32

    def norm_strip(i, carry):
        there = pl.ds(pl.multiple_of(i * strip, strip), strip)
        incoming = own[there, :] + peer[there, :].astype(jnp.float32)
        hidden = resid[there, :]
        inverse = row_scale(hidden)
        normed = hidden * inverse
        scaled = incoming * mlp_gain[...]
        change = cot[there, :].astype(jnp.float32) + inverse * (
            scaled - normed * jnp.mean(scaled * normed, axis=-1, keepdims=True)
        )
        d_resid[there, :] = change
        part[there, :] = change.astype(jnp.bfloat16)
        total = jnp.sum(incoming * normed, axis=0, keepdims=True)

        @pl.when(i == 0)
        def _():
            mlp_sum[...] = total

        @pl.when(i > 0)
        def _():
            mlp_sum[...] += total

        return carry

    lax.fori_loop(0, half // strip, norm_strip, 0)
    send = remote(part, d_full.at[ours], swap_sem.at[1, 0], swap_sem.at[1, 1], twin)
    send.start()
    d_full[ours, :] = part[...]
    columns = out_weight.shape[1]
    quarter = columns // 4

    for e in range(done, done + 3):
        event(e)
    done = done + 3
    remote(part, d_full.at[theirs], swap_sem.at[1, 0], swap_sem.at[1, 1], twin).wait_recv()
    send.wait_send()
    for i in range(4):
        there = pl.ds(i * quarter, quarter)
        d_attn[:, there] = product(d_full[...], out_weight[:, there]).astype(jnp.bfloat16)
    event(done)
    done = done + 1
    flip_into(d_full, d_flip, stage, stage_sem)
    per_group = q_heads // kv_heads
    qk_sum[...] = jnp.zeros_like(qk_sum)

    def group_step(group, carry):
        places = [group * per_group + r for r in range(per_group)]
        places += [q_heads + group, q_heads + kv_heads + group]
        copies = [
            pltpu.make_async_copy(qkv.at[:, head_at(place)], heads.at[i], head_sem.at[i])
            for i, place in enumerate(places)
        ]
        for copy in copies:
            copy.start()
        for copy in copies:
            copy.wait()
        attend_back(group, dims, heads, tab, seg_col, seg_row, gains, d_attn, d_proj, qk_sum, kept)
        event(done + group)
        return carry

    lax.fori_loop(0, kv_heads, group_step, 0)
    done = done + kv_heads

    def rest(e, carry):
        event(e)
        return carry

    lax.fori_loop(done, count * n, rest, 0)
    finish()


def backward_block(
    flipped, act, weights, qkv, attn, out_weight, cot, resid, tab, segments, gains, mlp_gain, q_heads, kv_heads, dp
):
    n = dp // 2
    count, seq, width = act.shape
    half, model = resid.shape
    rows = model // dp
    low, dma, vmem = jnp.bfloat16, pltpu.SemaphoreType.DMA, pltpu.VMEM
    shape = jax.ShapeDtypeStruct
    place = lambda kind: pl.BlockSpec(memory_space=kind)
    deep = 256
    return pl.pallas_call(
        functools.partial(backward_kernel, n, (q_heads, kv_heads, seq, seq // 2)),
        out_shape=[
            shape((count, rows, width), jnp.float32),
            shape((3, seq, q_heads * HD), low),
            shape((model, seq), low),
            shape((half, model), jnp.float32),
            shape((1, model), jnp.float32),
            shape((8, HD), jnp.float32),
        ],
        in_specs=[place(pltpu.HBM), place(vmem)] + [place(pltpu.HBM)] * 3 + [place(vmem)] * 8,
        out_specs=[place(pltpu.HBM), place(vmem), place(pltpu.HBM)] + [place(vmem)] * 3,
        scratch_shapes=[
            vmem((2, model, seq), low),
            vmem((seq, model), low),
            vmem((deep, width), low),
            vmem((deep, width), low),
            vmem((half, model), jnp.float32),
            vmem((half, model), low),
            vmem((half, model), low),
            vmem((seq, q_heads * HD), low),
            vmem((q_heads // kv_heads + 2, seq, HD), jnp.float32),
            vmem((3, seq, HD), jnp.float32),
            vmem((2, 256, seq), low),
            dma((2, 2)),
            dma((2,)),
            dma((q_heads // kv_heads + 2,)),
            dma((2,)),
            dma((2,)),
            *reduce_scratch(n, count, rows, width // 2),
        ],
        compiler_params=pltpu.CompilerParams(
            collective_id=2, has_side_effects=True, vmem_limit_bytes=67043328
        ),
    )(
        flipped, act, weights, qkv, attn, out_weight, cot, resid, tab,
        segments.reshape(seq, 1), segments.reshape(1, seq), gains, mlp_gain,
    )


def closing_kernel(n, *refs):
    (
        flipped, d_flip, d_proj, qkv_weight, weights, act, tokens, resid, d_resid, attn_gain, mlp_sum, qk_sum,
        grads, result, input_grad, gain_out,
        lefts, acts, first_block, second_block, own, part, peer, attn_sum, table, others, inbox,
        swap_sem, load_sem, first_sem, second_sem, trade_sem, post_sem, mail_sem,
    ) = refs[:34]
    pos, core = ring_place(n)
    me = lax.axis_index("dp")
    lane = lax.axis_index("tensor")
    nexts = (at((pos + 1) % n, core, n), at((pos + n - 1) % n, core, n))
    mate = at(pos, 1 - core, n)
    twin = (me, 1 - lane)
    fetches = [
        pltpu.make_async_copy(flipped.at[2], lefts.at[0], load_sem.at[0]),
        pltpu.make_async_copy(d_flip, lefts.at[1], load_sem.at[1]),
        pltpu.make_async_copy(act.at[2], acts, load_sem.at[2]),
    ]
    for fetch in fetches:
        fetch.start()
    barrier = pltpu.get_barrier_semaphore()

    def greet(o, carry):
        pl.semaphore_signal(barrier, inc=1, device_id=at((pos + o) % n, core, n), device_id_type=MESH)
        return carry

    lax.fori_loop(1, n, greet, 0)
    for other in (mate, twin):
        pl.semaphore_signal(barrier, inc=1, device_id=other, device_id_type=MESH)
    pl.semaphore_wait(barrier, n + 1)
    for fetch in fetches:
        fetch.wait()
    count, seq, width = d_proj.shape
    half, model = resid.shape
    early, event, finish = reducer(
        n, pos, core, nexts, mate, (lefts, d_proj, grads, *refs[34:]), lambda m: m // 2
    )
    for m in range(count):
        early(m, 0)
    for m in range(count):
        event(m)
    theirs = pl.ds(pl.multiple_of((1 - lane) * half, half), half)
    ours = pl.ds(pl.multiple_of(lane * half, half), half)
    deep = first_block.shape[1]
    turns = model // deep

    def stream(source, offset, block, sem):
        def fetch(i):
            return pltpu.make_async_copy(
                source.at[pl.ds(pl.multiple_of(offset + i * deep, deep), deep)], block.at[i % 2], sem.at[i % 2]
            )

        return fetch

    first_fetch = stream(qkv_weight, 0, first_block, first_sem)
    second_fetch = stream(weights, 2 * model, second_block, second_sem)
    first_fetch(0).start()

    def narrow(which, fetch, block, rows_of, every, base):
        def one(i, carry):
            @pl.when(i < turns - 1)
            def _():
                fetch(i + 1).start()

            fetch(i).wait()
            there = pl.ds(pl.multiple_of(i * deep, deep), deep)
            for rows, target in ((theirs, part), (ours, own)):
                total = None
                for left, start in rows_of(rows):
                    gained = tail_product(left, block[i % 2, :, pl.ds(start, left.shape[1])])
                    total = gained if total is None else total + gained
                target[which, :, there] = total.astype(target.dtype)

            @pl.when(i % every == every - 1)
            def _():
                event(base + i // every)

            return carry

        lax.fori_loop(0, turns, one, 0)

    narrow(
        0, first_fetch, first_block,
        lambda rows: [(d_proj[0, rows, :], 0), (d_proj[1, rows, :], width)], 4, count,
    )
    sends = [remote(part.at[i], peer.at[i], swap_sem.at[i, 0], swap_sem.at[i, 1], twin) for i in range(2)]
    sends[0].start()
    second_fetch(0).start()
    done = count + turns // 4
    narrow(1, second_fetch, second_block, lambda rows: [(acts[rows, :], 0)], 2, done)
    sends[1].start()
    done = done + turns // 2

    def events(number):
        nonlocal done
        for e in range(done, done + number):
            event(e)
        done = done + number

    events(4)
    sends[0].wait_recv()
    strip = 32

    def norm_strip(i, carry):
        there = pl.ds(pl.multiple_of(i * strip, strip), strip)
        incoming = own[0, there, :] + peer[0, there, :].astype(jnp.float32)
        values = tokens[there, :].astype(jnp.float32)
        inverse = row_scale(values)
        normed = values * inverse
        scaled = incoming * attn_gain[...]
        change = d_resid[there, :] + inverse * (
            scaled - normed * jnp.mean(scaled * normed, axis=-1, keepdims=True)
        )
        input_grad[there, :] = change.astype(jnp.bfloat16)
        total = jnp.sum(incoming * normed, axis=0, keepdims=True)

        @pl.when(i == 0)
        def _():
            attn_sum[...] = total

        @pl.when(i > 0)
        def _():
            attn_sum[...] += total

        return carry

    lax.fori_loop(0, half // strip, norm_strip, 0)
    events(1)
    dp = 2 * n
    share, head_share = model // dp, 2 * HD // dp
    table[...] = jnp.zeros_like(table)
    for d in range(dp):
        start = d * share // 128 * 128
        row = d * head_share // HD
        table[d, 0:1, :] = attn_sum[:, start : start + 128]
        table[d, 1:2, :] = mlp_sum[:, start : start + 128]
        table[d, 2:3, :] = qk_sum[row : row + 1, :]
    for i, partner in enumerate((twin, mate)):
        trade = remote(table, others.at[i], trade_sem.at[i, 0], trade_sem.at[i, 1], partner)
        trade.start()
        events(1)
        trade.wait()
        table[...] += others[i]

    def mail(o, target):
        return remote(table.at[target], inbox.at[o], post_sem.at[o], mail_sem.at[o], at((pos + o) % n, core, n))

    def post(o, carry):
        mail(o, chip_at((pos + o) % n, n) * 2 + core).start()
        return carry

    lax.fori_loop(1, n, post, 0)
    events(3)
    sends[1].wait_recv()

    def last_strip(i, carry):
        there = pl.ds(pl.multiple_of(i * strip, strip), strip)
        result[there, :] = (
            resid[there, :] + (own[1, there, :] + peer[1, there, :].astype(jnp.float32))
        ).astype(jnp.bfloat16)
        return carry

    lax.fori_loop(0, half // strip, last_strip, 0)
    gain_out[...] = table[me]

    def collect(o, carry):
        mail(o, 0).wait_recv()
        gain_out[...] += inbox[o]
        return carry

    lax.fori_loop(1, n, collect, 0)

    def rest(e, carry):
        event(e)
        return carry

    lax.fori_loop(done, count * n, rest, 0)
    finish()
    for send in sends:
        send.wait_send()

    def sent(o, carry):
        mail(o, 0).wait_send()
        return carry

    lax.fori_loop(1, n, sent, 0)


def closing_block(
    flipped, d_flip, d_proj, qkv_weight, weights, act, tokens, resid, d_resid, attn_gain, mlp_sum, qk_sum, dp
):
    n = dp // 2
    count, seq, width = d_proj.shape
    half, model = resid.shape
    hidden = act.shape[2]
    rows = model // dp
    deep = 256
    low, dma, vmem = jnp.bfloat16, pltpu.SemaphoreType.DMA, pltpu.VMEM
    shape = jax.ShapeDtypeStruct
    place = lambda kind: pl.BlockSpec(memory_space=kind)
    hbm = pltpu.HBM
    return pl.pallas_call(
        functools.partial(closing_kernel, n),
        out_shape=[
            shape((count, rows, width), jnp.float32),
            shape((half, model), low),
            shape((half, model), low),
            shape((8, 128), jnp.float32),
        ],
        in_specs=[place(k) for k in (hbm, hbm, vmem, hbm, hbm, hbm, *[vmem] * 6)],
        out_specs=[place(hbm), place(vmem), place(vmem), place(vmem)],
        scratch_shapes=[
            vmem((2, model, seq), low),
            vmem((seq, hidden), low),
            vmem((2, deep, qkv_weight.shape[1]), low),
            vmem((2, deep, hidden), low),
            vmem((2, half, model), jnp.float32),
            vmem((2, half, model), low),
            vmem((2, half, model), low),
            vmem((1, model), jnp.float32),
            vmem((dp, 8, 128), jnp.float32),
            vmem((2, dp, 8, 128), jnp.float32),
            vmem((n, 8, 128), jnp.float32),
            dma((2, 2)),
            dma((3,)),
            dma((2,)),
            dma((2,)),
            dma((2, 2)),
            dma((n,)),
            dma((n,)),
            *reduce_scratch(n, count, rows, width // 2),
        ],
        compiler_params=pltpu.CompilerParams(
            collective_id=3, has_side_effects=True, vmem_limit_bytes=67043328
        ),
    )(flipped, d_flip, d_proj, qkv_weight, weights, act, tokens, resid, d_resid, attn_gain, mlp_sum, qk_sum)


def on_device(
    tokens,
    seg_ids,
    w_query,
    w_key,
    w_value,
    w_output,
    w_gate,
    w_up,
    w_down,
    gain_attn,
    gain_mlp,
    gain_qk,
    cotangent,
):
    dp = lax.axis_size("dp")
    model = tokens.shape[1]
    gain_row = jnp.concatenate(
        [
            jnp.pad(g.astype(jnp.float32), (0, 128 - g.shape[0]))
            for g in (gain_attn, gain_mlp, gain_qk)
        ]
    )
    gain_shard = jnp.broadcast_to(gain_row[None, :], (16, gain_row.shape[0]))
    shard_qkv = jnp.concatenate([w_query, w_key, w_value], axis=1)
    (qkv_weight, out_weight, gain_all), (full_rows, full_cot) = gather_weights(
        [shard_qkv, w_output.T, gain_shard], [tokens, cotangent], [2, 1, 1], dp, 0
    )
    gain_all = gain_all.reshape(dp, 16, 3, 128)[:, 0]
    attn_gain = gain_all[:, 0, : gain_attn.shape[0]].reshape(-1)
    full_rows = full_rows.astype(jnp.float32)
    full_one = (full_rows * norm_rows(full_rows) * attn_gain).astype(jnp.bfloat16)
    mlp_gain = gain_all[:, 1, : gain_mlp.shape[0]].reshape(-1)
    qk_gain = gain_all[:, 2, : gain_qk.shape[0]].reshape(-1)
    query_gain = qk_gain[:HD]
    key_gain = qk_gain[HD:]
    cosine_table, sine_table, _ = tables(seg_ids[0])
    seq_len = full_one.shape[0]
    q_width = w_query.shape[1]
    kv_width = w_key.shape[1]
    q_heads = q_width // HD
    kv_heads = kv_width // HD
    projected = product(full_one, qkv_weight)
    pair = jnp.stack([query_gain, key_gain])
    signed = jnp.concatenate([-sine_table[:, : HD // 2], sine_table[:, HD // 2 :]], axis=1)
    rope_tab = jnp.stack([cosine_table, signed])
    weights, attn_rows, resid, flipped, act = forward_block(
        jnp.stack([w_gate, w_up, w_down.T]),
        projected,
        out_weight,
        tokens,
        full_one,
        full_cot,
        rope_tab,
        seg_ids[0],
        pair,
        mlp_gain[None, :],
        q_heads,
        kv_heads,
        dp,
    )
    grads, d_projected, d_flip, d_resid, mlp_sum, qk_sum = backward_block(
        flipped,
        act,
        weights,
        projected,
        attn_rows,
        out_weight,
        cotangent,
        resid,
        rope_tab,
        seg_ids[0],
        pair,
        mlp_gain[None, :],
        q_heads,
        kv_heads,
        dp,
    )
    grad_gate, grad_up, grad_down = grads[0], grads[1], grads[2]
    late_grads, result_rows, input_grad, gain_sums = closing_block(
        flipped,
        d_flip,
        d_projected,
        qkv_weight,
        weights,
        act,
        tokens,
        resid,
        d_resid,
        attn_gain[None, :],
        mlp_sum,
        qk_sum,
        dp,
    )
    me = lax.axis_index("dp")
    share = model // dp
    qk_share = 2 * HD // dp
    return (
        result_rows,
        input_grad,
        late_grads[0],
        late_grads[1, :, :kv_width],
        late_grads[1, :, kv_width:],
        late_grads[2].T,
        grad_gate,
        grad_up,
        grad_down.T,
        lax.dynamic_slice(gain_sums, (0, me * share % 128), (1, share))[0],
        lax.dynamic_slice(gain_sums, (1, me * share % 128), (1, share))[0],
        lax.dynamic_slice(gain_sums, (2, me * qk_share % HD), (1, qk_share))[0],
    )


def solution(mesh):
    return jax.shard_map(
        on_device,
        mesh=mesh,
        in_specs=(
            P(("dp", "tensor"), None),
            P("dp", None),
            P("dp", "tensor"),
            P("dp", "tensor"),
            P("dp", "tensor"),
            P("tensor", "dp"),
            P("dp", "tensor"),
            P("dp", "tensor"),
            P("tensor", "dp"),
            P("dp"),
            P("dp"),
            P("dp"),
            P(("dp", "tensor"), None),
        ),
        out_specs=(
            P(("dp", "tensor"), None),
            P(("dp", "tensor"), None),
            P("dp", "tensor"),
            P("dp", "tensor"),
            P("dp", "tensor"),
            P("tensor", "dp"),
            P("dp", "tensor"),
            P("dp", "tensor"),
            P("tensor", "dp"),
            P("dp"),
            P("dp"),
            P("dp"),
        ),
        check_vma=False,
    )
```

```python
import functools
import jax
import jax.numpy as jnp
from jax import lax
from jax.experimental import pallas as pl
from jax.experimental.pallas import tpu as pltpu

from jax.sharding import PartitionSpec as P

MESH = pl.DeviceIdType.MESH
HD = 128
epsilon = 1e-06
rope_base = 1000000.0


def ring_place(n):
    me = lax.axis_index("dp")
    chip = me // 2
    core = me % 2
    odd = chip % 2
    pos = (1 - odd) * (chip // 2) + odd * (n - 1 - chip // 2)
    return pos, core


def chip_at(pos, n):
    high = pos // (n // 2)
    return (1 - high) * (2 * pos) + high * (2 * (n - 1 - pos) + 1)


def at(pos, core, n):
    return (chip_at(pos, n) * 2 + core, lax.axis_index("tensor"))


def meet(peers):
    barrier = pltpu.get_barrier_semaphore()
    for peer in peers:
        pl.semaphore_signal(barrier, inc=1, device_id=peer, device_id_type=MESH)
    pl.semaphore_wait(barrier, len(peers))


def remote(src, dst, send, recv, peer):
    return pltpu.make_async_remote_copy(
        src_ref=src, dst_ref=dst, send_sem=send, recv_sem=recv, device_id=peer, device_id_type=MESH
    )


def product(left, right):
    return jnp.dot(left, right, preferred_element_type=jnp.float32)


def lead_product(left, right):
    return lax.dot_general(
        left, right, (((0,), (0,)), ((), ())), preferred_element_type=jnp.float32
    )


def tail_product(left, right):
    return lax.dot_general(
        left, right, (((1,), (1,)), ((), ())), preferred_element_type=jnp.float32
    )


def norm_rows(values):
    return lax.rsqrt(jnp.mean(values * values, axis=-1, keepdims=True) + epsilon)


def norm_back(incoming, normed, inverse):
    return inverse * (incoming - normed * jnp.mean(incoming * normed, axis=-1, keepdims=True))


def rotate(values, cosine_table, sine_table):
    half_width = values.shape[-1] // 2
    turned = jnp.concatenate([-values[..., half_width:], values[..., :half_width]], axis=-1)
    return values * cosine_table + turned * sine_table


def rotate_back(incoming, cosine_table, sine_table):
    half_width = incoming.shape[-1] // 2
    scaled = incoming * sine_table
    return incoming * cosine_table + jnp.concatenate(
        [scaled[..., half_width:], -scaled[..., :half_width]], axis=-1
    )


def tables(segments):
    seq_len = segments.shape[0]
    token_index = jnp.arange(seq_len, dtype=jnp.int32)
    doc_start = jnp.sum((segments[None, :] < segments[:, None]).astype(jnp.int32), axis=1)
    doc_pos = (token_index - doc_start).astype(jnp.float32)
    frequency = rope_base ** (-jnp.arange(0, HD, 2).astype(jnp.float32) / HD)
    angles = doc_pos[:, None] * frequency[None, :]
    cosine_table = jnp.concatenate([jnp.cos(angles), jnp.cos(angles)], axis=1)
    sine_table = jnp.concatenate([jnp.sin(angles), jnp.sin(angles)], axis=1)
    allowed = (segments[:, None] == segments[None, :]) & (
        token_index[None, :] <= token_index[:, None]
    )
    return (cosine_table, sine_table, allowed)


def turn(values):
    return pltpu.roll(values, values.shape[-1] // 2, 1)


def row_scale(values):
    return lax.rsqrt(jnp.mean(values * values, axis=-1, keepdims=True) + epsilon)


def head_at(index):
    return pl.ds(pl.multiple_of(index * HD, HD), HD)


def prepared(raw, gain, cosine, sine):
    inverse = row_scale(raw)
    hat = raw * inverse
    scaled = hat * gain
    return inverse, hat, (scaled * cosine + turn(scaled) * sine).astype(jnp.bfloat16)


def exp_block(query, keys, seg_col, seg_row, first):
    width = keys.shape[0]
    scores = tail_product(query, keys) * HD ** (-0.5)
    rows = lax.broadcasted_iota(jnp.int32, scores.shape, 0) + first
    columns = lax.broadcasted_iota(jnp.int32, scores.shape, 1)
    allowed = (seg_col[first : first + scores.shape[0], :] == seg_row[:, :width]) & (
        columns <= rows
    )
    return jnp.where(allowed, jnp.exp(scores), 0.0)


def attend_group(group, dims, qkv, tab, seg_col, seg_row, gains, attn, kept):
    q_heads, kv_heads, seq, block = dims
    per_group = q_heads // kv_heads
    cosine, sine = tab[0], tab[1]
    raw = qkv[:, head_at(q_heads + group)]
    kept[0] = prepared(raw, gains[1:2, :], cosine, sine)[2]
    kept[1] = qkv[:, head_at(q_heads + kv_heads + group)].astype(jnp.bfloat16)
    for r in range(per_group):
        head = group * per_group + r
        raw = qkv[:, head_at(head)]
        query = prepared(raw, gains[0:1, :], cosine, sine)[2]
        for first in range(0, seq, block):
            width = first + block
            exps = exp_block(query[first:width], kept[0, :width, :], seg_col, seg_row, first)
            probs = (exps / jnp.sum(exps, axis=-1, keepdims=True)).astype(jnp.bfloat16)
            attn[first:width, head_at(head)] = product(probs, kept[1, :width, :]).astype(jnp.bfloat16)


def block_columns(ref, index, width):
    if width % 128 == 0:
        return ref[:, pl.ds(pl.multiple_of(index * width, width), width)]
    fold = 128 // width
    tile = ref[:, pl.ds(pl.multiple_of((index // fold) * 128, 128), 128)]
    picked = tile[:, :width]
    for i in range(1, fold):
        picked = jnp.where(index % fold == i, tile[:, i * width : (i + 1) * width], picked)
    return picked


def flip_into(source, target, stage, stage_sem):
    deep = stage.shape[1]
    turns = source.shape[1] // deep

    def put(i):
        return pltpu.make_async_copy(
            stage.at[i % 2], target.at[pl.ds(pl.multiple_of(i * deep, deep), deep)], stage_sem.at[i % 2]
        )

    def one(i, carry):
        @pl.when(i >= 2)
        def _():
            put(i - 2).wait()

        stage[i % 2] = source[:, pl.ds(pl.multiple_of(i * deep, deep), deep)].T
        put(i).start()
        return carry

    lax.fori_loop(0, turns, one, 0)
    put(turns - 2).wait()
    put(turns - 1).wait()


def forward_kernel(n, dims, *refs):
    (
        mixed, ffn_shards, tile, tokens, cot, tab, seg_col, seg_row,
        weights, qkv_out, attn, resid, flipped, act, attn_gain, mlp_gain, gains,
        full_rows, cot_full, full_two, out_weight, columns, box, kept, part, peer, acc, blocks, stage,
        own_sem, send_sem, recv_sem, give_sem, take_sem, swap_sem, load_sem, stage_sem, column_sem, tile_sem,
    ) = refs
    q_heads, kv_heads, seq, block = dims
    pos, core = ring_place(n)
    me = lax.axis_index("dp")
    lane = lax.axis_index("tensor")
    nexts = (at((pos + 1) % n, core, n), at((pos + n - 1) % n, core, n))
    mate = at(pos, 1 - core, n)
    twin = (me, 1 - lane)
    count, rows, width = ffn_shards.shape
    wide = width // 2
    narrow = wide // 2
    model = 2 * n * rows
    half = seq // 2
    theirs = pl.ds(pl.multiple_of((1 - lane) * half, half), half)
    ours = pl.ds(pl.multiple_of(lane * half, half), half)
    meet((*nexts, mate, twin))

    def owner_of(side, step):
        if side == 0:
            return (pos - step + 2 * n) % n
        return (pos + step) % n

    def small(sub, side):
        return (sub, 0, pl.ds(side * wide + sub * narrow, narrow), mixed)

    def large(w, side):
        return (w + 2, (w + 1) * model, pl.ds(side * wide, wide), None if not isinstance(w, int) else ffn_shards.at[w])

    def spot(message, chip, who):
        start = message[1] + (chip * 2 + who) * rows
        return weights.at[pl.ds(pl.multiple_of(start, rows), rows), message[2]]

    def hop(message, side, step):
        k = message[0]
        here = spot(message, chip_at(owner_of(side, step - 1), n), core)
        return remote(here, here, send_sem.at[k, side, step], recv_sem.at[k, side, step], nexts[side])

    def arrived(message, side, step):
        k = message[0]
        here = spot(message, chip_at(owner_of(side, step), n), core)
        return remote(here, here, send_sem.at[k, side, step], recv_sem.at[k, side, step], nexts[side])

    def hand(message, side, step, who):
        k = message[0]
        here = spot(message, chip_at(owner_of(side, step), n), who)
        return remote(here, here, give_sem.at[k, side, step], take_sem.at[k, side, step], mate)

    def begin(message, side):
        k = message[0]
        source = message[3].at[:, message[2]]
        here = spot(message, chip_at(pos, n), core)
        remote(source, here, send_sem.at[k, side, 1], recv_sem.at[k, side, 1], nexts[side]).start()
        remote(source, here, give_sem.at[k, side, 0], take_sem.at[k, side, 0], mate).start()
        pltpu.make_async_copy(source, here, own_sem.at[k, side]).start()

    def keep_own(message, side):
        here = spot(message, chip_at(pos, n), core)
        return pltpu.make_async_copy(here, here, own_sem.at[message[0], side])

    def tile_hop(step, owner):
        place = chip_at(owner, n) * 2 + core
        return remote(box.at[place], box.at[place], tile_sem.at[0, step], tile_sem.at[1, step], nexts[0])

    def tile_hand(step, who):
        place = chip_at(owner_of(0, step), n) * 2 + who
        return remote(box.at[place], box.at[place], tile_sem.at[2, step], tile_sem.at[3, step], mate)

    box[me] = tile[...]
    swaps = [
        remote(source, target.at[ours], swap_sem.at[i, 0], swap_sem.at[i, 1], twin)
        for i, (source, target) in enumerate(((tokens, full_rows), (cot, cot_full)))
    ]
    remote(tile, box.at[me], tile_sem.at[0, 1], tile_sem.at[1, 1], nexts[0]).start()
    remote(tile, box.at[me], tile_sem.at[2, 0], tile_sem.at[3, 0], mate).start()
    for sub in range(2):
        for side in range(2):
            begin(small(sub, side), side)
    for swap in swaps:
        swap.start()
    full_rows[ours, :] = tokens[...]
    cot_full[ours, :] = cot[...]

    def pass_on(message, side, step):
        arrived(message, side, step).wait_recv()

        @pl.when(step < n - 1)
        def _():
            hop(message, side, step + 1).start()

        hand(message, side, step, core).start()

    def pass_tile(step):
        tile_hop(step, owner_of(0, step)).wait_recv()

        @pl.when(step < n - 1)
        def _():
            tile_hop(step + 1, owner_of(0, step)).start()

        tile_hand(step, core).start()

    def mixed_step(step, carry):
        pass_tile(step)
        for sub in range(2):
            for side in range(2):
                pass_on(small(sub, side), side, step)
        return carry

    lax.fori_loop(1, n - 1, mixed_step, 0)
    pass_tile(n - 1)
    for w in range(count):
        for side in range(2):
            begin(large(w, side), side)
        if w < 2:
            for side in range(2):
                pass_on(small(w, side), side, n - 1)

    def service(event):
        step, w = event // count + 1, event % count
        for side in range(2):
            pass_on(large(w, side), side, step)

    def gathered(step, carry):
        for sub in range(2):
            for side in range(2):
                hand(small(sub, side), side, step, 1 - core).wait_recv()
        tile_hand(step, 1 - core).wait_recv()
        return carry

    lax.fori_loop(0, n, gathered, 0)
    for sub in range(2):
        for side in range(2):
            keep_own(small(sub, side), side).wait()
    q_wide = (q_heads + 2 * kv_heads) * HD
    fetch_out = pltpu.make_async_copy(
        weights.at[pl.ds(0, model), pl.ds(q_wide, width - q_wide)], out_weight, load_sem.at[0]
    )
    turns = q_wide // columns.shape[2]
    deep = columns.shape[2]

    def fetch_columns(i):
        return pltpu.make_async_copy(
            weights.at[pl.ds(0, model), pl.ds(pl.multiple_of(i * deep, deep), deep)],
            columns.at[i % 2], column_sem.at[i % 2],
        )

    fetch_columns(0).start()
    fetch_out.start()
    dp = 2 * n
    share, head_share = model // dp, 2 * HD // dp
    for first, target, per in ((0, attn_gain, share), (1, mlp_gain, share)):
        for s in range(model // 128):
            owners = [d for d in range(dp) if d * per // 128 == s]
            total = box[owners[0], first : first + 1, :]
            for d in owners[1:]:
                total = total + box[d, first : first + 1, :]
            target[:, s * 128 : (s + 1) * 128] = total
    for s in range(2):
        owners = [d for d in range(dp) if d * head_share // HD == s]
        total = box[owners[0], 2:3, :]
        for d in owners[1:]:
            total = total + box[d, 2:3, :]
        gains[s : s + 1, :] = total
    swaps[0].wait_recv()
    strip = 32

    def norm_strip(i, carry):
        there = pl.ds(pl.multiple_of(i * strip, strip), strip)
        values = full_rows[there, :].astype(jnp.float32)
        full_two[there, :] = (values * row_scale(values) * attn_gain[...]).astype(jnp.bfloat16)
        return carry

    lax.fori_loop(0, seq // strip, norm_strip, 0)
    qkv = acc.at[count - 1]

    def project(i, carry):
        @pl.when(i < turns - 1)
        def _():
            fetch_columns(i + 1).start()

        fetch_columns(i).wait()
        qkv[:, pl.ds(pl.multiple_of(i * deep, deep), deep)] = product(full_two[...], columns[i % 2])
        return carry

    lax.fori_loop(0, turns, project, 0)
    save_qkv = pltpu.make_async_copy(qkv.at[:, pl.ds(0, q_wide)], qkv_out, load_sem.at[1])
    save_qkv.start()
    service(0)

    def load(job, side):
        step, w = job // count, job % count
        start = (w + 1) * model + chip_at(owner_of(side, step), n) * 2 * rows
        return pltpu.make_async_copy(
            weights.at[pl.ds(pl.multiple_of(start, 2 * rows), 2 * rows), pl.ds(side * wide, wide)],
            blocks.at[side], load_sem.at[side],
        )

    def work(job):
        step, w = job // count, job % count
        for side in range(2):
            hand(large(w, side), side, step, 1 - core).wait_recv()

            @pl.when(step == 0)
            def _():
                keep_own(large(w, side), side).wait()

            load(job, side).start()
        for side in range(2):
            load(job, side).wait()
            chip = chip_at(owner_of(side, step), n)

            def with_left(left):
                tile_width = wide // 3

                def one(i, carry):
                    there = pl.ds(pl.multiple_of(side * wide + i * tile_width, tile_width), tile_width)
                    gained = product(left, blocks[side, :, pl.ds(pl.multiple_of(i * tile_width, tile_width), tile_width)])

                    @pl.when(step == 0)
                    def _():
                        acc[w, :, there] = gained

                    @pl.when(step > 0)
                    def _():
                        acc[w, :, there] += gained

                    return carry

                lax.fori_loop(0, 3, one, 0)

            @pl.when(w < count - 1)
            def _():
                with_left(block_columns(full_two, chip, 2 * rows))

            @pl.when(w == count - 1)
            def _():
                with_left(block_columns(cot_full, chip, 2 * rows))

    def flip(source, target):
        flip_into(source, flipped.at[target], stage, stage_sem)

    groups = (qkv, tab, seg_col, seg_row, gains, attn, kept)

    def attend(first, last):
        def one(group, carry):
            attend_group(group, dims, *groups)
            return carry

        lax.fori_loop(first, last, one, 0)

    flip(full_two, 2)
    attend(0, kv_heads // 2)
    service(1)
    attend(kv_heads // 2, kv_heads)
    service(2)
    fetch_out.wait()
    part[...] = tail_product(attn[theirs, :], out_weight[...]).astype(jnp.bfloat16)
    swaps[1].wait_recv()
    send_part = remote(part, peer, swap_sem.at[2, 0], swap_sem.at[2, 1], twin)
    send_part.start()
    resid[...] = tokens[...].astype(jnp.float32) + tail_product(attn[ours, :], out_weight[...])
    service(3)
    service(4)
    flip(cot_full, 1)
    service(5)
    send_part.wait_recv()
    summed = resid[...] + peer[...].astype(jnp.float32)
    resid[...] = summed
    send_part.wait_send()
    part[...] = (summed * row_scale(summed) * mlp_gain[...]).astype(jnp.bfloat16)
    send_two = remote(part, full_two.at[ours], swap_sem.at[3, 0], swap_sem.at[3, 1], twin)
    send_two.start()
    full_two[ours, :] = part[...]
    ready = 9
    for event in range(6, ready):
        service(event)
    remote(part, full_two.at[theirs], swap_sem.at[3, 0], swap_sem.at[3, 1], twin).wait_recv()
    flip(full_two, 0)
    save_qkv.wait()

    def both(i, carry):
        service(ready + i)

        @pl.when(i < ready + 3)
        def _():
            def one(q, carry):
                work(2 * i + q)
                return carry

            lax.fori_loop(0, 2, one, 0)

        @pl.when(i >= ready + 3)
        def _():
            work(ready + 3 + i)

        return carry

    lax.fori_loop(0, count * (n - 1) - ready, both, 0)

    def finish(i, carry):
        there = pl.ds(pl.multiple_of(i * strip, strip), strip)
        gate = acc[0, there, :]
        up = acc[1, there, :]
        d_act = acc[2, there, :]
        sig = 1.0 / (1.0 + jnp.exp(-gate))
        silu = gate * sig
        act[0, there, :] = (d_act * up * sig * (1.0 + gate * (1.0 - sig))).astype(jnp.bfloat16)
        act[1, there, :] = (d_act * silu).astype(jnp.bfloat16)
        act[2, there, :] = (silu * up).astype(jnp.bfloat16)
        return carry

    lax.fori_loop(0, seq // strip, finish, 0)

    def drain(step, carry):
        for side in range(2):
            for message in [small(sub, side) for sub in range(2)] + [large(w, side) for w in range(count)]:
                hop(message, side, step).wait_send()
                hand(message, side, step, core).wait_send()
        tile_hop(step, owner_of(0, step)).wait_send()
        tile_hand(step, core).wait_send()
        return carry

    lax.fori_loop(1, n, drain, 0)
    for side in range(2):
        for message in [small(sub, side) for sub in range(2)] + [large(w, side) for w in range(count)]:
            hand(message, side, 0, core).wait_send()
    tile_hand(0, core).wait_send()
    for swap in (*swaps, send_two):
        swap.wait_send()


def forward_block(mixed, ffn_shards, tile, tokens, cot, tab, segments, q_heads, kv_heads, dp):
    n = dp // 2
    count, rows, width = ffn_shards.shape
    half, model = tokens.shape
    seq = 2 * half
    q_wide = (q_heads + 2 * kv_heads) * HD
    low, dma, vmem, hbm = jnp.bfloat16, pltpu.SemaphoreType.DMA, pltpu.VMEM, pltpu.HBM
    shape = jax.ShapeDtypeStruct
    place = lambda kind: pl.BlockSpec(memory_space=kind)
    return pl.pallas_call(
        functools.partial(forward_kernel, n, (q_heads, kv_heads, seq, seq // 2)),
        out_shape=[
            shape(((count + 1) * model, width), low),
            shape((seq, q_wide), jnp.float32),
            shape((seq, q_heads * HD), low),
            shape((half, model), jnp.float32),
            shape((3, model, seq), low),
            shape((count, seq, width), low),
            shape((1, model), jnp.float32),
            shape((1, model), jnp.float32),
            shape((2, HD), jnp.float32),
        ],
        in_specs=[place(vmem)] * 8,
        out_specs=[place(k) for k in (hbm, hbm, vmem, vmem, hbm, vmem, vmem, vmem, vmem)],
        scratch_shapes=[
            vmem((seq, model), low),
            vmem((seq, model), low),
            vmem((seq, model), low),
            vmem((model, width - q_wide), low),
            vmem((2, model, 256), low),
            vmem((dp, 8, 128), jnp.float32),
            vmem((2, seq, HD), low),
            vmem((half, model), low),
            vmem((half, model), low),
            vmem((count, seq, width), jnp.float32),
            vmem((2, 2 * rows, width // 2), low),
            vmem((2, 256, seq), low),
            dma((count + 2, 2)),
            dma((count + 2, 2, n)),
            dma((count + 2, 2, n)),
            dma((count + 2, 2, n)),
            dma((count + 2, 2, n)),
            dma((4, 2)),
            dma((2,)),
            dma((2,)),
            dma((2,)),
            dma((4, n)),
        ],
        compiler_params=pltpu.CompilerParams(
            collective_id=1, has_side_effects=True, vmem_limit_bytes=67043328
        ),
    )(mixed, ffn_shards, tile, tokens, cot, tab, segments.reshape(seq, 1), segments.reshape(1, seq))


SLOTS = 3


def undo(incoming, hat, inverse, gain, cosine, sine):
    turned = incoming * cosine - turn(incoming) * sine
    total = jnp.sum(turned * hat, axis=0, keepdims=True)
    scaled = turned * gain
    raw = inverse * (scaled - hat * jnp.mean(scaled * hat, axis=-1, keepdims=True))
    return total, raw.astype(jnp.bfloat16)


def attend_back(group, dims, heads, tab, seg_col, seg_row, gains, d_attn, d_proj, sums, kept):
    q_heads, kv_heads, seq, block = dims
    per_group = q_heads // kv_heads
    low = jnp.bfloat16
    scale = HD ** (-0.5)
    cosine, sine = tab[0], tab[1]
    keys = prepared(heads[per_group], gains[1:2, :], cosine, sine)[2]
    values = heads[per_group + 1].astype(low)
    for r in range(per_group):
        head = group * per_group + r
        q_inverse, q_hat, query = prepared(heads[r], gains[0:1, :], cosine, sine)
        for first in range(0, seq, block):
            width = first + block
            exps = exp_block(query[first:width], keys[:width], seg_col, seg_row, first)
            probs = exps / jnp.sum(exps, axis=-1, keepdims=True)
            incoming = d_attn[first:width, head_at(head)]
            d_probs = tail_product(incoming, values[:width])
            delta = jnp.sum(probs * d_probs, axis=-1, keepdims=True)
            d_scores = (probs * (d_probs - delta)).astype(low)
            kept[0, first:width, :] = product(d_scores, keys[:width]) * scale
            d_keys = lead_product(d_scores, query[first:width])
            d_values = lead_product(probs.astype(low), incoming)
            if r == 0 and first == 0:
                kept[1] = jnp.zeros_like(kept[1])
                kept[2] = jnp.zeros_like(kept[2])
            kept[1, :width, :] += d_keys
            kept[2, :width, :] += d_values
        total, raw = undo(kept[0], q_hat, q_inverse, gains[0:1, :], cosine, sine)
        sums[0:1, :] += total
        d_proj[0, :, head_at(head)] = raw
    k_inverse, k_hat, _ = prepared(heads[per_group], gains[1:2, :], cosine, sine)
    total, raw = undo(kept[1] * scale, k_hat, k_inverse, gains[1:2, :], cosine, sine)
    sums[1:2, :] += total
    d_proj[1, :, head_at(group)] = raw
    d_proj[1, :, head_at(kv_heads + group)] = kept[2].astype(low)


def reducer(n, pos, core, nexts, mate, refs, left_of):
    lefts, rights, out, mine, term, give, take, ship, land, give_sem, take_sem, ship_sem, land_sem, free_sem, out_sem = refs
    count = rights.shape[0]
    wide = rights.shape[2] // 2
    rows = out.shape[1]

    def owner_of(side, step):
        if side == 0:
            return (pos - 1 - step + 2 * n) % n
        return (pos + 1 + step) % n

    def given(m, side, step):
        return remote(
            give.at[m, side], take.at[m, side, step % 2],
            give_sem.at[m, side], take_sem.at[m, side, step % 2], mate,
        )

    def shipped(m, side, step):
        return remote(
            ship.at[m, side], land.at[m, side, step % SLOTS],
            ship_sem.at[m, side], land_sem.at[m, side, step % SLOTS], nexts[side],
        )

    def early(m, step):
        for side in range(2):
            start = pl.multiple_of(chip_at(owner_of(side, step), n) * 2 * rows, 2 * rows)
            left = lefts[left_of(m), pl.ds(start, 2 * rows), :]
            tile = min(512, wide)

            def one(i, carry):
                there = pl.multiple_of(i * tile, tile)
                term[:, pl.ds(there, tile)] = product(
                    left, rights[m, :, pl.ds(pl.multiple_of(side * wide + there, tile), tile)]
                )
                return carry

            lax.fori_loop(0, wide // tile, one, 0)

            @pl.when(step >= 1)
            def _():
                given(m, side, step - 1).wait_send()

            give[m, side] = term[pl.ds(pl.multiple_of((1 - core) * rows, rows), rows), :].astype(jnp.bfloat16)
            given(m, side, step).start()
            mine[m, side] = term[pl.ds(pl.multiple_of(core * rows, rows), rows), :]

    def event(e):
        step, m = e // count, e % count
        for side in range(2):
            given(m, side, step).wait_recv()

            @pl.when(step == 0)
            def _():
                mine[m, side] += take[m, side, 0].astype(jnp.float32)

            @pl.when(step > 0)
            def _():
                shipped(m, side, step - 1).wait_recv()
                mine[m, side] += take[m, side, step % 2].astype(jnp.float32) + land[
                    m, side, (step - 1) % SLOTS
                ].astype(jnp.float32)

                @pl.when(step - 1 + SLOTS <= n - 2)
                def _():
                    pl.semaphore_signal(
                        free_sem.at[m, side], inc=1, device_id=nexts[1 - side], device_id_type=MESH
                    )

                shipped(m, side, step - 1).wait_send()

            @pl.when(step < n - 1)
            def _():
                @pl.when(step >= SLOTS)
                def _():
                    pl.semaphore_wait(free_sem.at[m, side], 1)

                ship[m, side] = mine[m, side].astype(jnp.bfloat16)
                shipped(m, side, step).start()

            @pl.when(step == n - 1)
            def _():
                written(m, side).start()

        @pl.when(step < n - 1)
        def _():
            early(m, step + 1)

    def written(m, side):
        return pltpu.make_async_copy(mine.at[m, side], out.at[m, :, pl.ds(side * wide, wide)], out_sem.at[m, side])

    def finish():
        for m in range(count):
            for side in range(2):
                given(m, side, n - 1).wait_send()
                written(m, side).wait()

    return early, event, finish


def reduce_scratch(n, count, rows, wide):
    low, dma, vmem = jnp.bfloat16, pltpu.SemaphoreType.DMA, pltpu.VMEM
    return [
        vmem((count, 2, rows, wide), jnp.float32),
        vmem((2 * rows, wide), jnp.float32),
        vmem((count, 2, rows, wide), low),
        vmem((count, 2, 2, rows, wide), low),
        vmem((count, 2, rows, wide), low),
        vmem((count, 2, SLOTS, rows, wide), low),
        dma((count, 2)),
        dma((count, 2, 2)),
        dma((count, 2)),
        dma((count, 2, SLOTS)),
        pltpu.SemaphoreType.REGULAR((count, 2)),
        dma((count, 2)),
    ]


def backward_kernel(n, dims, *refs):
    (
        flipped, act, weights, qkv, attn, cot, resid, tab, seg_col, seg_row, gains, mlp_gain,
        grads, d_proj, d_flip, d_resid, mlp_sum, qk_sum,
        lefts, out_weight, d_full, gate_block, up_block, own, part, peer, d_attn, heads, kept, stage,
        swap_sem, load_sem, head_sem, left_sem, stage_sem,
    ) = refs[:35]
    q_heads, kv_heads, seq, block = dims
    pos, core = ring_place(n)
    lane = lax.axis_index("tensor")
    nexts = (at((pos + 1) % n, core, n), at((pos + n - 1) % n, core, n))
    mate = at(pos, 1 - core, n)
    twin = (lax.axis_index("dp"), 1 - lane)
    fetch_lefts = pltpu.make_async_copy(flipped.at[pl.ds(0, 2)], lefts, left_sem.at[0])
    fetch_lefts.start()
    fetch_attn = pltpu.make_async_copy(attn, d_proj.at[2], left_sem.at[1])
    fetch_attn.start()
    q_wide = qkv.shape[1]
    fetch_out = pltpu.make_async_copy(
        weights.at[pl.ds(0, out_weight.shape[0]), pl.ds(q_wide, out_weight.shape[1])], out_weight, left_sem.at[2]
    )
    meet((*nexts, mate, twin))
    fetch_lefts.wait()
    fetch_out.start()
    fetch_attn.wait()
    count = act.shape[0]
    model = resid.shape[1]
    half = seq // 2
    early, event, finish = reducer(
        n, pos, core, nexts, mate, (lefts, act, grads, *refs[35:]), lambda m: m // 2
    )
    for m in range(count):
        early(m, 0)
    for m in range(count):
        event(m)

    theirs = pl.ds(pl.multiple_of((1 - lane) * half, half), half)
    ours = pl.ds(pl.multiple_of(lane * half, half), half)
    deep = gate_block.shape[0]
    turns = model // deep

    def fetch(i, which):
        target = (gate_block, up_block)[which]
        start = (which + 1) * model + i * deep
        return pltpu.make_async_copy(
            weights.at[pl.ds(pl.multiple_of(start, deep), deep), :], target, load_sem.at[which]
        )

    fetch(0, 0).start()
    fetch(0, 1).start()

    def narrow(i, carry):
        there = pl.ds(pl.multiple_of(i * deep, deep), deep)
        for which, target in enumerate((gate_block, up_block)):
            fetch(i, which).wait()
            other = tail_product(act[which, theirs, :], target[...])
            same = tail_product(act[which, ours, :], target[...])
            if which == 0:
                own[:, there] = same
                d_resid[:, there] = other
            else:
                own[:, there] += same
                part[:, there] = (d_resid[:, there] + other).astype(jnp.bfloat16)

            @pl.when(i < turns - 1)
            def _():
                fetch(i + 1, which).start()

        @pl.when(i % 3 == 2)
        def _():
            event(count + i // 3)

        return carry

    lax.fori_loop(0, turns, narrow, 0)
    done = count + turns // 3
    send = remote(part, peer, swap_sem.at[0, 0], swap_sem.at[0, 1], twin)
    send.start()
    for e in range(done, done + 3):
        event(e)
    done = done + 3
    send.wait_recv()
    send.wait_send()
    strip = 32

    def norm_strip(i, carry):
        there = pl.ds(pl.multiple_of(i * strip, strip), strip)
        incoming = own[there, :] + peer[there, :].astype(jnp.float32)
        hidden = resid[there, :]
        inverse = row_scale(hidden)
        normed = hidden * inverse
        scaled = incoming * mlp_gain[...]
        change = cot[there, :].astype(jnp.float32) + inverse * (
            scaled - normed * jnp.mean(scaled * normed, axis=-1, keepdims=True)
        )
        d_resid[there, :] = change
        part[there, :] = change.astype(jnp.bfloat16)
        total = jnp.sum(incoming * normed, axis=0, keepdims=True)

        @pl.when(i == 0)
        def _():
            mlp_sum[...] = total

        @pl.when(i > 0)
        def _():
            mlp_sum[...] += total

        return carry

    lax.fori_loop(0, half // strip, norm_strip, 0)
    send = remote(part, d_full.at[ours], swap_sem.at[1, 0], swap_sem.at[1, 1], twin)
    send.start()
    d_full[ours, :] = part[...]
    fetch_out.wait()
    columns = out_weight.shape[1]
    quarter = columns // 4

    for e in range(done, done + 3):
        event(e)
    done = done + 3
    remote(part, d_full.at[theirs], swap_sem.at[1, 0], swap_sem.at[1, 1], twin).wait_recv()
    send.wait_send()
    for i in range(4):
        there = pl.ds(i * quarter, quarter)
        d_attn[:, there] = product(d_full[...], out_weight[:, there]).astype(jnp.bfloat16)
    event(done)
    done = done + 1
    flip_into(d_full, d_flip, stage, stage_sem)
    per_group = q_heads // kv_heads
    qk_sum[...] = jnp.zeros_like(qk_sum)

    def group_step(group, carry):
        places = [group * per_group + r for r in range(per_group)]
        places += [q_heads + group, q_heads + kv_heads + group]
        copies = [
            pltpu.make_async_copy(qkv.at[:, head_at(place)], heads.at[i], head_sem.at[i])
            for i, place in enumerate(places)
        ]
        for copy in copies:
            copy.start()
        for copy in copies:
            copy.wait()
        attend_back(group, dims, heads, tab, seg_col, seg_row, gains, d_attn, d_proj, qk_sum, kept)
        event(done + group)
        return carry

    lax.fori_loop(0, kv_heads, group_step, 0)
    done = done + kv_heads

    def rest(e, carry):
        event(e)
        return carry

    lax.fori_loop(done, count * n, rest, 0)
    finish()


def backward_block(
    flipped, act, weights, qkv, attn, cot, resid, tab, segments, gains, mlp_gain, q_heads, kv_heads, dp
):
    n = dp // 2
    count, seq, width = act.shape
    half, model = resid.shape
    rows = model // dp
    low, dma, vmem = jnp.bfloat16, pltpu.SemaphoreType.DMA, pltpu.VMEM
    shape = jax.ShapeDtypeStruct
    place = lambda kind: pl.BlockSpec(memory_space=kind)
    deep = 256
    return pl.pallas_call(
        functools.partial(backward_kernel, n, (q_heads, kv_heads, seq, seq // 2)),
        out_shape=[
            shape((count, rows, width), jnp.float32),
            shape((3, seq, q_heads * HD), low),
            shape((model, seq), low),
            shape((half, model), jnp.float32),
            shape((1, model), jnp.float32),
            shape((8, HD), jnp.float32),
        ],
        in_specs=[place(pltpu.HBM), place(vmem)] + [place(pltpu.HBM)] * 3 + [place(vmem)] * 7,
        out_specs=[place(pltpu.HBM), place(vmem), place(pltpu.HBM)] + [place(vmem)] * 3,
        scratch_shapes=[
            vmem((2, model, seq), low),
            vmem((model, q_heads * HD), low),
            vmem((seq, model), low),
            vmem((deep, width), low),
            vmem((deep, width), low),
            vmem((half, model), jnp.float32),
            vmem((half, model), low),
            vmem((half, model), low),
            vmem((seq, q_heads * HD), low),
            vmem((q_heads // kv_heads + 2, seq, HD), jnp.float32),
            vmem((3, seq, HD), jnp.float32),
            vmem((2, 256, seq), low),
            dma((2, 2)),
            dma((2,)),
            dma((q_heads // kv_heads + 2,)),
            dma((3,)),
            dma((2,)),
            *reduce_scratch(n, count, rows, width // 2),
        ],
        compiler_params=pltpu.CompilerParams(
            collective_id=2, has_side_effects=True, vmem_limit_bytes=67043328
        ),
    )(
        flipped, act, weights, qkv, attn, cot, resid, tab,
        segments.reshape(seq, 1), segments.reshape(1, seq), gains, mlp_gain,
    )


def closing_kernel(n, *refs):
    (
        flipped, d_flip, d_proj, weights, act, tokens, resid, d_resid, attn_gain, mlp_sum, qk_sum,
        grads, result, input_grad, gain_out,
        lefts, acts, first_block, second_block, own, part, peer, attn_sum, table, others, inbox,
        swap_sem, load_sem, first_sem, second_sem, trade_sem, post_sem, mail_sem,
    ) = refs[:33]
    pos, core = ring_place(n)
    me = lax.axis_index("dp")
    lane = lax.axis_index("tensor")
    nexts = (at((pos + 1) % n, core, n), at((pos + n - 1) % n, core, n))
    mate = at(pos, 1 - core, n)
    twin = (me, 1 - lane)
    fetches = [
        pltpu.make_async_copy(flipped.at[2], lefts.at[0], load_sem.at[0]),
        pltpu.make_async_copy(d_flip, lefts.at[1], load_sem.at[1]),
        pltpu.make_async_copy(act.at[2], acts, load_sem.at[2]),
    ]
    for fetch in fetches:
        fetch.start()
    barrier = pltpu.get_barrier_semaphore()

    def greet(o, carry):
        pl.semaphore_signal(barrier, inc=1, device_id=at((pos + o) % n, core, n), device_id_type=MESH)
        return carry

    lax.fori_loop(1, n, greet, 0)
    for other in (mate, twin):
        pl.semaphore_signal(barrier, inc=1, device_id=other, device_id_type=MESH)
    pl.semaphore_wait(barrier, n + 1)
    for fetch in fetches:
        fetch.wait()
    count, seq, width = d_proj.shape
    half, model = resid.shape
    early, event, finish = reducer(
        n, pos, core, nexts, mate, (lefts, d_proj, grads, *refs[33:]), lambda m: m // 2
    )
    for m in range(count):
        early(m, 0)
    for m in range(count):
        event(m)
    theirs = pl.ds(pl.multiple_of((1 - lane) * half, half), half)
    ours = pl.ds(pl.multiple_of(lane * half, half), half)
    deep = first_block.shape[1]
    turns = model // deep

    def stream(source, offset, block, sem):
        def fetch(i):
            return pltpu.make_async_copy(
                source.at[pl.ds(pl.multiple_of(offset + i * deep, deep), deep), pl.ds(0, block.shape[2])], block.at[i % 2], sem.at[i % 2]
            )

        return fetch

    first_fetch = stream(weights, 0, first_block, first_sem)
    second_fetch = stream(weights, 3 * model, second_block, second_sem)
    first_fetch(0).start()

    def narrow(which, fetch, block, rows_of, every, base):
        def one(i, carry):
            @pl.when(i < turns - 1)
            def _():
                fetch(i + 1).start()

            fetch(i).wait()
            there = pl.ds(pl.multiple_of(i * deep, deep), deep)
            for rows, target in ((theirs, part), (ours, own)):
                total = None
                for left, start in rows_of(rows):
                    gained = tail_product(left, block[i % 2, :, pl.ds(start, left.shape[1])])
                    total = gained if total is None else total + gained
                target[which, :, there] = total.astype(target.dtype)

            @pl.when(i % every == every - 1)
            def _():
                event(base + i // every)

            return carry

        lax.fori_loop(0, turns, one, 0)

    narrow(
        0, first_fetch, first_block,
        lambda rows: [(d_proj[0, rows, :], 0), (d_proj[1, rows, :], width)], 4, count,
    )
    sends = [remote(part.at[i], peer.at[i], swap_sem.at[i, 0], swap_sem.at[i, 1], twin) for i in range(2)]
    sends[0].start()
    second_fetch(0).start()
    done = count + turns // 4
    narrow(1, second_fetch, second_block, lambda rows: [(acts[rows, :], 0)], 2, done)
    sends[1].start()
    done = done + turns // 2

    def events(number):
        nonlocal done
        for e in range(done, done + number):
            event(e)
        done = done + number

    events(4)
    sends[0].wait_recv()
    strip = 32

    def norm_strip(i, carry):
        there = pl.ds(pl.multiple_of(i * strip, strip), strip)
        incoming = own[0, there, :] + peer[0, there, :].astype(jnp.float32)
        values = tokens[there, :].astype(jnp.float32)
        inverse = row_scale(values)
        normed = values * inverse
        scaled = incoming * attn_gain[...]
        change = d_resid[there, :] + inverse * (
            scaled - normed * jnp.mean(scaled * normed, axis=-1, keepdims=True)
        )
        input_grad[there, :] = change.astype(jnp.bfloat16)
        total = jnp.sum(incoming * normed, axis=0, keepdims=True)

        @pl.when(i == 0)
        def _():
            attn_sum[...] = total

        @pl.when(i > 0)
        def _():
            attn_sum[...] += total

        return carry

    lax.fori_loop(0, half // strip, norm_strip, 0)
    events(1)
    dp = 2 * n
    share, head_share = model // dp, 2 * HD // dp
    table[...] = jnp.zeros_like(table)
    for d in range(dp):
        start = d * share // 128 * 128
        row = d * head_share // HD
        table[d, 0:1, :] = attn_sum[:, start : start + 128]
        table[d, 1:2, :] = mlp_sum[:, start : start + 128]
        table[d, 2:3, :] = qk_sum[row : row + 1, :]
    for i, partner in enumerate((twin, mate)):
        trade = remote(table, others.at[i], trade_sem.at[i, 0], trade_sem.at[i, 1], partner)
        trade.start()
        events(1)
        trade.wait()
        table[...] += others[i]

    def mail(o, target):
        return remote(table.at[target], inbox.at[o], post_sem.at[o], mail_sem.at[o], at((pos + o) % n, core, n))

    def post(o, carry):
        mail(o, chip_at((pos + o) % n, n) * 2 + core).start()
        return carry

    lax.fori_loop(1, n, post, 0)
    events(3)
    sends[1].wait_recv()

    def last_strip(i, carry):
        there = pl.ds(pl.multiple_of(i * strip, strip), strip)
        result[there, :] = (
            resid[there, :] + (own[1, there, :] + peer[1, there, :].astype(jnp.float32))
        ).astype(jnp.bfloat16)
        return carry

    lax.fori_loop(0, half // strip, last_strip, 0)
    gain_out[...] = table[me]

    def collect(o, carry):
        mail(o, 0).wait_recv()
        gain_out[...] += inbox[o]
        return carry

    lax.fori_loop(1, n, collect, 0)

    def rest(e, carry):
        event(e)
        return carry

    lax.fori_loop(done, count * n, rest, 0)
    finish()
    for send in sends:
        send.wait_send()

    def sent(o, carry):
        mail(o, 0).wait_send()
        return carry

    lax.fori_loop(1, n, sent, 0)


def closing_block(
    flipped, d_flip, d_proj, weights, act, tokens, resid, d_resid, attn_gain, mlp_sum, qk_sum, dp
):
    n = dp // 2
    count, seq, width = d_proj.shape
    half, model = resid.shape
    hidden = act.shape[2]
    rows = model // dp
    deep = 256
    low, dma, vmem = jnp.bfloat16, pltpu.SemaphoreType.DMA, pltpu.VMEM
    shape = jax.ShapeDtypeStruct
    place = lambda kind: pl.BlockSpec(memory_space=kind)
    hbm = pltpu.HBM
    return pl.pallas_call(
        functools.partial(closing_kernel, n),
        out_shape=[
            shape((count, rows, width), jnp.float32),
            shape((half, model), low),
            shape((half, model), low),
            shape((8, 128), jnp.float32),
        ],
        in_specs=[place(k) for k in (hbm, hbm, vmem, hbm, hbm, *[vmem] * 6)],
        out_specs=[place(hbm), place(vmem), place(vmem), place(vmem)],
        scratch_shapes=[
            vmem((2, model, seq), low),
            vmem((seq, hidden), low),
            vmem((2, deep, 2 * width), low),
            vmem((2, deep, hidden), low),
            vmem((2, half, model), jnp.float32),
            vmem((2, half, model), low),
            vmem((2, half, model), low),
            vmem((1, model), jnp.float32),
            vmem((dp, 8, 128), jnp.float32),
            vmem((2, dp, 8, 128), jnp.float32),
            vmem((n, 8, 128), jnp.float32),
            dma((2, 2)),
            dma((3,)),
            dma((2,)),
            dma((2,)),
            dma((2, 2)),
            dma((n,)),
            dma((n,)),
            *reduce_scratch(n, count, rows, width // 2),
        ],
        compiler_params=pltpu.CompilerParams(
            collective_id=3, has_side_effects=True, vmem_limit_bytes=67043328
        ),
    )(flipped, d_flip, d_proj, weights, act, tokens, resid, d_resid, attn_gain, mlp_sum, qk_sum)


def on_device(
    tokens,
    seg_ids,
    w_query,
    w_key,
    w_value,
    w_output,
    w_gate,
    w_up,
    w_down,
    gain_attn,
    gain_mlp,
    gain_qk,
    cotangent,
):
    dp = lax.axis_size("dp")
    model = tokens.shape[1]
    me = lax.axis_index("dp")
    tile = jnp.zeros((8, 128), jnp.float32)
    for row, gain in enumerate((gain_attn, gain_mlp, gain_qk)):
        spot = me * gain.shape[0] % 128 if gain.shape[0] % 128 else 0
        tile = lax.dynamic_update_slice(tile, gain.astype(jnp.float32)[None, :], (row, spot))
    q_width = w_query.shape[1]
    kv_width = w_key.shape[1]
    q_heads = q_width // HD
    kv_heads = kv_width // HD
    cosine_table, sine_table, _ = tables(seg_ids[0])
    signed = jnp.concatenate([-sine_table[:, : HD // 2], sine_table[:, HD // 2 :]], axis=1)
    rope_tab = jnp.stack([cosine_table, signed])
    weights, projected, attn_rows, resid, flipped, act, attn_gain, mlp_gain, pair = forward_block(
        jnp.concatenate([w_query, w_key, w_value, w_output.T], axis=1),
        jnp.stack([w_gate, w_up, w_down.T]),
        tile,
        tokens,
        cotangent,
        rope_tab,
        seg_ids[0],
        q_heads,
        kv_heads,
        dp,
    )
    grads, d_projected, d_flip, d_resid, mlp_sum, qk_sum = backward_block(
        flipped,
        act,
        weights,
        projected,
        attn_rows,
        cotangent,
        resid,
        rope_tab,
        seg_ids[0],
        pair,
        mlp_gain,
        q_heads,
        kv_heads,
        dp,
    )
    grad_gate, grad_up, grad_down = grads[0], grads[1], grads[2]
    late_grads, result_rows, input_grad, gain_sums = closing_block(
        flipped,
        d_flip,
        d_projected,
        weights,
        act,
        tokens,
        resid,
        d_resid,
        attn_gain,
        mlp_sum,
        qk_sum,
        dp,
    )
    share = model // dp
    qk_share = 2 * HD // dp
    return (
        result_rows,
        input_grad,
        late_grads[0],
        late_grads[1, :, :kv_width],
        late_grads[1, :, kv_width:],
        late_grads[2].T,
        grad_gate,
        grad_up,
        grad_down.T,
        lax.dynamic_slice(gain_sums, (0, me * share % 128), (1, share))[0],
        lax.dynamic_slice(gain_sums, (1, me * share % 128), (1, share))[0],
        lax.dynamic_slice(gain_sums, (2, me * qk_share % HD), (1, qk_share))[0],
    )


def solution(mesh):
    return jax.shard_map(
        on_device,
        mesh=mesh,
        in_specs=(
            P(("dp", "tensor"), None),
            P("dp", None),
            P("dp", "tensor"),
            P("dp", "tensor"),
            P("dp", "tensor"),
            P("tensor", "dp"),
            P("dp", "tensor"),
            P("dp", "tensor"),
            P("tensor", "dp"),
            P("dp"),
            P("dp"),
            P("dp"),
            P(("dp", "tensor"), None),
        ),
        out_specs=(
            P(("dp", "tensor"), None),
            P(("dp", "tensor"), None),
            P("dp", "tensor"),
            P("dp", "tensor"),
            P("dp", "tensor"),
            P("tensor", "dp"),
            P("dp", "tensor"),
            P("dp", "tensor"),
            P("tensor", "dp"),
            P("dp"),
            P("dp"),
            P("dp"),
        ),
        check_vma=False,
    )
```

```python
import functools
import jax
import jax.numpy as jnp
from jax import lax
from jax.experimental import pallas as pl
from jax.experimental.pallas import tpu as pltpu

from jax.sharding import PartitionSpec as P

MESH = pl.DeviceIdType.MESH
HD = 128
epsilon = 1e-06
rope_base = 1000000.0


def ring_place(n):
    me = lax.axis_index("dp")
    chip = me // 2
    core = me % 2
    odd = chip % 2
    pos = (1 - odd) * (chip // 2) + odd * (n - 1 - chip // 2)
    return pos, core


def chip_at(pos, n):
    high = pos // (n // 2)
    return (1 - high) * (2 * pos) + high * (2 * (n - 1 - pos) + 1)


def at(pos, core, n):
    return (chip_at(pos, n) * 2 + core, lax.axis_index("tensor"))


def meet(peers):
    barrier = pltpu.get_barrier_semaphore()
    for peer in peers:
        pl.semaphore_signal(barrier, inc=1, device_id=peer, device_id_type=MESH)
    pl.semaphore_wait(barrier, len(peers))


def remote(src, dst, send, recv, peer):
    return pltpu.make_async_remote_copy(
        src_ref=src, dst_ref=dst, send_sem=send, recv_sem=recv, device_id=peer, device_id_type=MESH
    )


def product(left, right):
    return jnp.dot(left, right, preferred_element_type=jnp.float32)


def lead_product(left, right):
    return lax.dot_general(
        left, right, (((0,), (0,)), ((), ())), preferred_element_type=jnp.float32
    )


def tail_product(left, right):
    return lax.dot_general(
        left, right, (((1,), (1,)), ((), ())), preferred_element_type=jnp.float32
    )


def norm_rows(values):
    return lax.rsqrt(jnp.mean(values * values, axis=-1, keepdims=True) + epsilon)


def norm_back(incoming, normed, inverse):
    return inverse * (incoming - normed * jnp.mean(incoming * normed, axis=-1, keepdims=True))


def rotate(values, cosine_table, sine_table):
    half_width = values.shape[-1] // 2
    turned = jnp.concatenate([-values[..., half_width:], values[..., :half_width]], axis=-1)
    return values * cosine_table + turned * sine_table


def rotate_back(incoming, cosine_table, sine_table):
    half_width = incoming.shape[-1] // 2
    scaled = incoming * sine_table
    return incoming * cosine_table + jnp.concatenate(
        [scaled[..., half_width:], -scaled[..., :half_width]], axis=-1
    )


def tables(segments):
    seq_len = segments.shape[0]
    token_index = jnp.arange(seq_len, dtype=jnp.int32)
    doc_start = jnp.sum((segments[None, :] < segments[:, None]).astype(jnp.int32), axis=1)
    doc_pos = (token_index - doc_start).astype(jnp.float32)
    frequency = rope_base ** (-jnp.arange(0, HD, 2).astype(jnp.float32) / HD)
    angles = doc_pos[:, None] * frequency[None, :]
    cosine_table = jnp.concatenate([jnp.cos(angles), jnp.cos(angles)], axis=1)
    sine_table = jnp.concatenate([jnp.sin(angles), jnp.sin(angles)], axis=1)
    allowed = (segments[:, None] == segments[None, :]) & (
        token_index[None, :] <= token_index[:, None]
    )
    return (cosine_table, sine_table, allowed)


def turn(values):
    return pltpu.roll(values, values.shape[-1] // 2, 1)


def row_scale(values):
    return lax.rsqrt(jnp.mean(values * values, axis=-1, keepdims=True) + epsilon)


def head_at(index):
    return pl.ds(pl.multiple_of(index * HD, HD), HD)


def prepared(raw, gain, cosine, sine):
    inverse = row_scale(raw)
    hat = raw * inverse
    scaled = hat * gain
    return inverse, hat, (scaled * cosine + turn(scaled) * sine).astype(jnp.bfloat16)


def exp_block(query, keys, seg_col, seg_row, first):
    width = keys.shape[0]
    scores = tail_product(query, keys) * HD ** (-0.5)
    rows = lax.broadcasted_iota(jnp.int32, scores.shape, 0) + first
    columns = lax.broadcasted_iota(jnp.int32, scores.shape, 1)
    allowed = (seg_col[first : first + scores.shape[0], :] == seg_row[:, :width]) & (
        columns <= rows
    )
    return jnp.where(allowed, jnp.exp(scores), 0.0)


def attend_group(group, dims, qkv, tab, seg_col, seg_row, gains, attn, kept):
    q_heads, kv_heads, seq, block = dims
    per_group = q_heads // kv_heads
    cosine, sine = tab[0], tab[1]
    raw = qkv[:, head_at(q_heads + group)]
    kept[0] = prepared(raw, gains[1:2, :], cosine, sine)[2]
    kept[1] = qkv[:, head_at(q_heads + kv_heads + group)].astype(jnp.bfloat16)
    for r in range(per_group):
        head = group * per_group + r
        raw = qkv[:, head_at(head)]
        query = prepared(raw, gains[0:1, :], cosine, sine)[2]
        for first in range(0, seq, block):
            width = first + block
            exps = exp_block(query[first:width], kept[0, :width, :], seg_col, seg_row, first)
            probs = (exps / jnp.sum(exps, axis=-1, keepdims=True)).astype(jnp.bfloat16)
            attn[first:width, head_at(head)] = product(probs, kept[1, :width, :]).astype(jnp.bfloat16)


def block_columns(ref, index, width):
    if width % 128 == 0:
        return ref[:, pl.ds(pl.multiple_of(index * width, width), width)]
    fold = 128 // width
    tile = ref[:, pl.ds(pl.multiple_of((index // fold) * 128, 128), 128)]
    picked = tile[:, :width]
    for i in range(1, fold):
        picked = jnp.where(index % fold == i, tile[:, i * width : (i + 1) * width], picked)
    return picked


def flip_into(source, target, stage, stage_sem):
    deep = stage.shape[1]
    turns = source.shape[1] // deep

    def put(i):
        return pltpu.make_async_copy(
            stage.at[i % 2], target.at[pl.ds(pl.multiple_of(i * deep, deep), deep)], stage_sem.at[i % 2]
        )

    def one(i, carry):
        @pl.when(i >= 2)
        def _():
            put(i - 2).wait()

        stage[i % 2] = source[:, pl.ds(pl.multiple_of(i * deep, deep), deep)].T
        put(i).start()
        return carry

    lax.fori_loop(0, turns, one, 0)
    put(turns - 2).wait()
    put(turns - 1).wait()


def forward_kernel(n, dims, *refs):
    (
        mixed, ffn_shards, tile, tokens, cot, tab, seg_col, seg_row,
        weights, qkv_out, attn, resid, flipped, act, attn_gain, mlp_gain, gains,
        full_rows, cot_full, full_two, out_weight, columns, box, kept, part, peer, acc, blocks, stage,
        own_sem, send_sem, recv_sem, give_sem, take_sem, swap_sem, load_sem, stage_sem, column_sem, tile_sem,
    ) = refs
    q_heads, kv_heads, seq, block = dims
    pos, core = ring_place(n)
    me = lax.axis_index("dp")
    lane = lax.axis_index("tensor")
    nexts = (at((pos + 1) % n, core, n), at((pos + n - 1) % n, core, n))
    mate = at(pos, 1 - core, n)
    twin = (me, 1 - lane)
    count, rows, width = ffn_shards.shape
    wide = width // 2
    narrow = wide // 2
    model = 2 * n * rows
    half = seq // 2
    theirs = pl.ds(pl.multiple_of((1 - lane) * half, half), half)
    ours = pl.ds(pl.multiple_of(lane * half, half), half)
    meet((*nexts, mate, twin))

    def owner_of(side, step):
        if side == 0:
            return (pos - step + 2 * n) % n
        return (pos + step) % n

    def small(sub, side):
        return (sub, 0, pl.ds(side * wide + sub * narrow, narrow), mixed)

    def large(w, side):
        return (w + 2, (w + 1) * model, pl.ds(side * wide, wide), None if not isinstance(w, int) else ffn_shards.at[w])

    def spot(message, chip, who):
        start = message[1] + (chip * 2 + who) * rows
        return weights.at[pl.ds(pl.multiple_of(start, rows), rows), message[2]]

    def hop(message, side, step):
        k = message[0]
        here = spot(message, chip_at(owner_of(side, step - 1), n), core)
        return remote(here, here, send_sem.at[k, side, step], recv_sem.at[k, side, step], nexts[side])

    def arrived(message, side, step):
        k = message[0]
        here = spot(message, chip_at(owner_of(side, step), n), core)
        return remote(here, here, send_sem.at[k, side, step], recv_sem.at[k, side, step], nexts[side])

    def hand(message, side, step, who):
        k = message[0]
        here = spot(message, chip_at(owner_of(side, step), n), who)
        return remote(here, here, give_sem.at[k, side, step], take_sem.at[k, side, step], mate)

    def begin(message, side):
        k = message[0]
        source = message[3].at[:, message[2]]
        here = spot(message, chip_at(pos, n), core)
        remote(source, here, send_sem.at[k, side, 1], recv_sem.at[k, side, 1], nexts[side]).start()
        remote(source, here, give_sem.at[k, side, 0], take_sem.at[k, side, 0], mate).start()
        pltpu.make_async_copy(source, here, own_sem.at[k, side]).start()

    def keep_own(message, side):
        here = spot(message, chip_at(pos, n), core)
        return pltpu.make_async_copy(here, here, own_sem.at[message[0], side])

    def tile_hop(step, owner):
        place = chip_at(owner, n) * 2 + core
        return remote(box.at[place], box.at[place], tile_sem.at[0, step], tile_sem.at[1, step], nexts[0])

    def tile_hand(step, who):
        place = chip_at(owner_of(0, step), n) * 2 + who
        return remote(box.at[place], box.at[place], tile_sem.at[2, step], tile_sem.at[3, step], mate)

    box[me] = tile[...]
    swaps = [
        remote(source, target.at[ours], swap_sem.at[i, 0], swap_sem.at[i, 1], twin)
        for i, (source, target) in enumerate(((tokens, full_rows), (cot, cot_full)))
    ]
    remote(tile, box.at[me], tile_sem.at[0, 1], tile_sem.at[1, 1], nexts[0]).start()
    remote(tile, box.at[me], tile_sem.at[2, 0], tile_sem.at[3, 0], mate).start()
    for sub in range(2):
        for side in range(2):
            begin(small(sub, side), side)
    for swap in swaps:
        swap.start()
    full_rows[ours, :] = tokens[...]
    cot_full[ours, :] = cot[...]

    def pass_on(message, side, step):
        arrived(message, side, step).wait_recv()

        @pl.when(step < n - 1)
        def _():
            hop(message, side, step + 1).start()

        hand(message, side, step, core).start()

    def pass_tile(step):
        tile_hop(step, owner_of(0, step)).wait_recv()

        @pl.when(step < n - 1)
        def _():
            tile_hop(step + 1, owner_of(0, step)).start()

        tile_hand(step, core).start()

    def mixed_step(step, carry):
        pass_tile(step)
        for sub in range(2):
            for side in range(2):
                pass_on(small(sub, side), side, step)
        return carry

    lax.fori_loop(1, n - 1, mixed_step, 0)
    pass_tile(n - 1)
    for w in range(count):
        for side in range(2):
            begin(large(w, side), side)
        if w < 2:
            for side in range(2):
                pass_on(small(w, side), side, n - 1)

    def service(event):
        step, w = event // count + 1, event % count
        for side in range(2):
            pass_on(large(w, side), side, step)

    def gathered(step, carry):
        for sub in range(2):
            for side in range(2):
                hand(small(sub, side), side, step, 1 - core).wait_recv()
        tile_hand(step, 1 - core).wait_recv()
        return carry

    lax.fori_loop(0, n, gathered, 0)
    for sub in range(2):
        for side in range(2):
            keep_own(small(sub, side), side).wait()
    q_wide = (q_heads + 2 * kv_heads) * HD
    fetch_out = pltpu.make_async_copy(
        weights.at[pl.ds(0, model), pl.ds(q_wide, width - q_wide)], out_weight, load_sem.at[0]
    )
    turns = q_wide // columns.shape[2]
    deep = columns.shape[2]

    def fetch_columns(i):
        return pltpu.make_async_copy(
            weights.at[pl.ds(0, model), pl.ds(pl.multiple_of(i * deep, deep), deep)],
            columns.at[i % 2], column_sem.at[i % 2],
        )

    fetch_columns(0).start()
    fetch_out.start()
    dp = 2 * n
    share, head_share = model // dp, 2 * HD // dp
    for first, target, per in ((0, attn_gain, share), (1, mlp_gain, share)):
        for s in range(model // 128):
            owners = [d for d in range(dp) if d * per // 128 == s]
            total = box[owners[0], first : first + 1, :]
            for d in owners[1:]:
                total = total + box[d, first : first + 1, :]
            target[:, s * 128 : (s + 1) * 128] = total
    for s in range(2):
        owners = [d for d in range(dp) if d * head_share // HD == s]
        total = box[owners[0], 2:3, :]
        for d in owners[1:]:
            total = total + box[d, 2:3, :]
        gains[s : s + 1, :] = total
    swaps[0].wait_recv()
    strip = 32

    def norm_strip(i, carry):
        there = pl.ds(pl.multiple_of(i * strip, strip), strip)
        values = full_rows[there, :].astype(jnp.float32)
        full_two[there, :] = (values * row_scale(values) * attn_gain[...]).astype(jnp.bfloat16)
        return carry

    lax.fori_loop(0, seq // strip, norm_strip, 0)
    qkv = acc.at[count - 1]

    def project(i, carry):
        @pl.when(i < turns - 1)
        def _():
            fetch_columns(i + 1).start()

        fetch_columns(i).wait()
        qkv[:, pl.ds(pl.multiple_of(i * deep, deep), deep)] = product(full_two[...], columns[i % 2])
        return carry

    lax.fori_loop(0, turns, project, 0)
    save_qkv = pltpu.make_async_copy(qkv.at[:, pl.ds(0, q_wide)], qkv_out, load_sem.at[1])
    save_qkv.start()
    service(0)

    def load(job, side):
        step, w = job // count, job % count
        start = (w + 1) * model + chip_at(owner_of(side, step), n) * 2 * rows
        return pltpu.make_async_copy(
            weights.at[pl.ds(pl.multiple_of(start, 2 * rows), 2 * rows), pl.ds(side * wide, wide)],
            blocks.at[side], load_sem.at[side],
        )

    def work(job):
        step, w = job // count, job % count
        for side in range(2):
            hand(large(w, side), side, step, 1 - core).wait_recv()

            @pl.when(step == 0)
            def _():
                keep_own(large(w, side), side).wait()

            load(job, side).start()
        for side in range(2):
            load(job, side).wait()
            chip = chip_at(owner_of(side, step), n)

            def with_left(left):
                tile_width = wide // 3

                def one(i, carry):
                    there = pl.ds(pl.multiple_of(side * wide + i * tile_width, tile_width), tile_width)
                    gained = product(left, blocks[side, :, pl.ds(pl.multiple_of(i * tile_width, tile_width), tile_width)])

                    @pl.when(step == 0)
                    def _():
                        acc[w, :, there] = gained

                    @pl.when(step > 0)
                    def _():
                        acc[w, :, there] += gained

                    return carry

                lax.fori_loop(0, 3, one, 0)

            @pl.when(w < count - 1)
            def _():
                with_left(block_columns(full_two, chip, 2 * rows))

            @pl.when(w == count - 1)
            def _():
                with_left(block_columns(cot_full, chip, 2 * rows))

    def flip(source, target):
        flip_into(source, flipped.at[target], stage, stage_sem)

    groups = (qkv, tab, seg_col, seg_row, gains, attn, kept)

    def attend(first, last):
        def one(group, carry):
            attend_group(group, dims, *groups)
            return carry

        lax.fori_loop(first, last, one, 0)

    flip(full_two, 2)
    attend(0, kv_heads // 2)
    service(1)
    attend(kv_heads // 2, kv_heads)
    service(2)
    fetch_out.wait()
    part[...] = tail_product(attn[theirs, :], out_weight[...]).astype(jnp.bfloat16)
    swaps[1].wait_recv()
    send_part = remote(part, peer, swap_sem.at[2, 0], swap_sem.at[2, 1], twin)
    send_part.start()
    resid[...] = tokens[...].astype(jnp.float32) + tail_product(attn[ours, :], out_weight[...])
    service(3)
    service(4)
    flip(cot_full, 1)
    service(5)
    send_part.wait_recv()
    summed = resid[...] + peer[...].astype(jnp.float32)
    resid[...] = summed
    send_part.wait_send()
    part[...] = (summed * row_scale(summed) * mlp_gain[...]).astype(jnp.bfloat16)
    send_two = remote(part, full_two.at[ours], swap_sem.at[3, 0], swap_sem.at[3, 1], twin)
    send_two.start()
    full_two[ours, :] = part[...]
    ready = 9
    for event in range(6, ready):
        service(event)
    remote(part, full_two.at[theirs], swap_sem.at[3, 0], swap_sem.at[3, 1], twin).wait_recv()
    flip(full_two, 0)
    save_qkv.wait()

    def both(i, carry):
        service(ready + i)

        @pl.when(i < ready + 3)
        def _():
            def one(q, carry):
                work(2 * i + q)
                return carry

            lax.fori_loop(0, 2, one, 0)

        @pl.when(i >= ready + 3)
        def _():
            work(ready + 3 + i)

        return carry

    lax.fori_loop(0, count * (n - 1) - ready, both, 0)

    def finish(i, carry):
        there = pl.ds(pl.multiple_of(i * strip, strip), strip)
        gate = acc[0, there, :]
        up = acc[1, there, :]
        d_act = acc[2, there, :]
        sig = 1.0 / (1.0 + jnp.exp(-gate))
        silu = gate * sig
        act[0, there, :] = (d_act * up * sig * (1.0 + gate * (1.0 - sig))).astype(jnp.bfloat16)
        act[1, there, :] = (d_act * silu).astype(jnp.bfloat16)
        act[2, there, :] = (silu * up).astype(jnp.bfloat16)
        return carry

    lax.fori_loop(0, seq // strip, finish, 0)

    def drain(step, carry):
        for side in range(2):
            for message in [small(sub, side) for sub in range(2)] + [large(w, side) for w in range(count)]:
                hop(message, side, step).wait_send()
                hand(message, side, step, core).wait_send()
        tile_hop(step, owner_of(0, step)).wait_send()
        tile_hand(step, core).wait_send()
        return carry

    lax.fori_loop(1, n, drain, 0)
    for side in range(2):
        for message in [small(sub, side) for sub in range(2)] + [large(w, side) for w in range(count)]:
            hand(message, side, 0, core).wait_send()
    tile_hand(0, core).wait_send()
    for swap in (*swaps, send_two):
        swap.wait_send()


def forward_block(mixed, ffn_shards, tile, tokens, cot, tab, segments, q_heads, kv_heads, dp):
    n = dp // 2
    count, rows, width = ffn_shards.shape
    half, model = tokens.shape
    seq = 2 * half
    q_wide = (q_heads + 2 * kv_heads) * HD
    low, dma, vmem, hbm = jnp.bfloat16, pltpu.SemaphoreType.DMA, pltpu.VMEM, pltpu.HBM
    shape = jax.ShapeDtypeStruct
    place = lambda kind: pl.BlockSpec(memory_space=kind)
    return pl.pallas_call(
        functools.partial(forward_kernel, n, (q_heads, kv_heads, seq, seq // 2)),
        out_shape=[
            shape(((count + 1) * model, width), low),
            shape((seq, q_wide), jnp.float32),
            shape((seq, q_heads * HD), low),
            shape((half, model), jnp.float32),
            shape((3, model, seq), low),
            shape((count, seq, width), low),
            shape((1, model), jnp.float32),
            shape((1, model), jnp.float32),
            shape((2, HD), jnp.float32),
        ],
        in_specs=[place(vmem)] * 8,
        out_specs=[place(k) for k in (hbm, hbm, vmem, vmem, hbm, vmem, vmem, vmem, vmem)],
        scratch_shapes=[
            vmem((seq, model), low),
            vmem((seq, model), low),
            vmem((seq, model), low),
            vmem((model, width - q_wide), low),
            vmem((2, model, 256), low),
            vmem((dp, 8, 128), jnp.float32),
            vmem((2, seq, HD), low),
            vmem((half, model), low),
            vmem((half, model), low),
            vmem((count, seq, width), jnp.float32),
            vmem((2, 2 * rows, width // 2), low),
            vmem((2, 256, seq), low),
            dma((count + 2, 2)),
            dma((count + 2, 2, n)),
            dma((count + 2, 2, n)),
            dma((count + 2, 2, n)),
            dma((count + 2, 2, n)),
            dma((4, 2)),
            dma((2,)),
            dma((2,)),
            dma((2,)),
            dma((4, n)),
        ],
        compiler_params=pltpu.CompilerParams(
            collective_id=1, has_side_effects=True, vmem_limit_bytes=67043328
        ),
    )(mixed, ffn_shards, tile, tokens, cot, tab, segments.reshape(seq, 1), segments.reshape(1, seq))


SLOTS = 3


def undo(incoming, hat, inverse, gain, cosine, sine):
    turned = incoming * cosine - turn(incoming) * sine
    total = jnp.sum(turned * hat, axis=0, keepdims=True)
    scaled = turned * gain
    raw = inverse * (scaled - hat * jnp.mean(scaled * hat, axis=-1, keepdims=True))
    return total, raw.astype(jnp.bfloat16)


def attend_back(group, dims, heads, tab, seg_col, seg_row, gains, d_attn, d_proj, sums, kept):
    q_heads, kv_heads, seq, block = dims
    per_group = q_heads // kv_heads
    low = jnp.bfloat16
    scale = HD ** (-0.5)
    cosine, sine = tab[0], tab[1]
    keys = prepared(heads[per_group], gains[1:2, :], cosine, sine)[2]
    values = heads[per_group + 1].astype(low)
    for r in range(per_group):
        head = group * per_group + r
        q_inverse, q_hat, query = prepared(heads[r], gains[0:1, :], cosine, sine)
        for first in range(0, seq, block):
            width = first + block
            exps = exp_block(query[first:width], keys[:width], seg_col, seg_row, first)
            probs = exps / jnp.sum(exps, axis=-1, keepdims=True)
            incoming = d_attn[first:width, head_at(r)]
            d_probs = tail_product(incoming, values[:width])
            delta = jnp.sum(probs * d_probs, axis=-1, keepdims=True)
            d_scores = (probs * (d_probs - delta)).astype(low)
            kept[0, first:width, :] = product(d_scores, keys[:width]) * scale
            d_keys = lead_product(d_scores, query[first:width])
            d_values = lead_product(probs.astype(low), incoming)
            if r == 0 and first == 0:
                kept[1] = jnp.zeros_like(kept[1])
                kept[2] = jnp.zeros_like(kept[2])
            kept[1, :width, :] += d_keys
            kept[2, :width, :] += d_values
        total, raw = undo(kept[0], q_hat, q_inverse, gains[0:1, :], cosine, sine)
        sums[0:1, :] += total
        d_proj[0, :, head_at(head)] = raw
    k_inverse, k_hat, _ = prepared(heads[per_group], gains[1:2, :], cosine, sine)
    total, raw = undo(kept[1] * scale, k_hat, k_inverse, gains[1:2, :], cosine, sine)
    sums[1:2, :] += total
    d_proj[1, :, head_at(group)] = raw
    d_proj[1, :, head_at(kv_heads + group)] = kept[2].astype(low)


def reducer(n, pos, core, nexts, mate, rights, outs, fetch_left, scratch, stage_of):
    lefts, mine, term, give, take, ship, land, give_sem, take_sem, ship_sem, land_sem, free_sem, out_sem = scratch
    before, sends_before, sends_total = stage_of
    count = rights.shape[0]
    wide = rights.shape[2] // 2
    rows = outs[0].shape[0]
    span = pl.ds(0, wide)

    def owner_of(side, step):
        if side == 0:
            return (pos - 1 - step + 2 * n) % n
        return (pos + 1 + step) % n

    def given(m, side, step):
        slot = (before + step) % 2
        return remote(
            give.at[m, side, :, span], take.at[m, side, slot, :, span],
            give_sem.at[m, side], take_sem.at[m, side, slot], mate,
        )

    def shipped(m, side, step):
        slot = (sends_before + step) % SLOTS
        return remote(
            ship.at[m, side, :, span], land.at[m, side, slot, :, span],
            ship_sem.at[m, side], land_sem.at[m, side, slot], nexts[side],
        )

    def fetch(m, step):
        for side in range(2):
            start = pl.multiple_of(chip_at(owner_of(side, step), n) * 2 * rows, 2 * rows)
            fetch_left(m, side, pl.ds(start, 2 * rows))

    def early(m, step):
        for side in range(2):
            fetch_left(m, side, None)
        for side in range(2):
            tile = min(512, wide)

            def one(i, carry):
                there = pl.multiple_of(i * tile, tile)
                term[:, pl.ds(there, tile)] = product(
                    lefts[side], rights[m, :, pl.ds(pl.multiple_of(side * wide + there, tile), tile)]
                )
                return carry

            lax.fori_loop(0, wide // tile, one, 0)

            @pl.when(step >= 1)
            def _():
                given(m, side, step - 1).wait_send()

            other = term[pl.ds(pl.multiple_of((1 - core) * rows, rows), rows), span]
            give[m, side, :, span] = other.astype(jnp.bfloat16)
            given(m, side, step).start()
            mine[m, side, :, span] = term[pl.ds(pl.multiple_of(core * rows, rows), rows), span]

    def event(e):
        step, m = e // count, e % count

        @pl.when(step < n - 1)
        def _():
            fetch(m, step + 1)

        for side in range(2):
            given(m, side, step).wait_recv()
            near = take[m, side, (before + step) % 2, :, span].astype(jnp.float32)

            @pl.when(step == 0)
            def _():
                mine[m, side, :, span] += near

            @pl.when(step > 0)
            def _():
                shipped(m, side, step - 1).wait_recv()
                far = land[m, side, (sends_before + step - 1) % SLOTS, :, span].astype(jnp.float32)
                mine[m, side, :, span] += near + far

                @pl.when(sends_before + step - 1 + SLOTS < sends_total)
                def _():
                    pl.semaphore_signal(
                        free_sem.at[m, side], inc=1, device_id=nexts[1 - side], device_id_type=MESH
                    )

                shipped(m, side, step - 1).wait_send()

            @pl.when(step < n - 1)
            def _():
                @pl.when(sends_before + step >= SLOTS)
                def _():
                    pl.semaphore_wait(free_sem.at[m, side], 1)

                ship[m, side, :, span] = mine[m, side, :, span].astype(jnp.bfloat16)
                shipped(m, side, step).start()

            @pl.when(step == n - 1)
            def _():
                for i in range(count):
                    @pl.when(m == i)
                    def _():
                        written(m, side, i).start()

        @pl.when(step < n - 1)
        def _():
            early(m, step + 1)

    def written(m, side, i):
        return pltpu.make_async_copy(
            mine.at[m, side, :, span], outs[i].at[:, pl.ds(side * wide, wide)], out_sem.at[m, side]
        )

    def begin(m):
        fetch(m, 0)
        early(m, 0)

    def finish(m):
        for side in range(2):
            given(m, side, n - 1).wait_send()
            written(m, side, m).wait()

    return begin, event, finish


def backward_kernel(n, dims, *refs):
    (
        flipped, act, weights, qkv, attn, cot, tokens, resid, tab, seg_col, seg_row, gains, attn_gain, mlp_gain,
        grad_gate, grad_up, grad_down, grad_query, grad_pair, grad_out, result, input_grad, gain_out, d_flip,
        d_proj, d_full, d_resid, blocks, columns, own, part, peer, d_attn, heads, kept, stage,
        attn_sum, mlp_sum, qk_sum, table, others, inbox,
        swap_sem, load_sem, head_sem, attn_sem, stage_sem, column_sem, trade_sem, post_sem, mail_sem, left_sem,
        *scratch,
    ) = refs
    q_heads, kv_heads, seq, block = dims
    pos, core = ring_place(n)
    me = lax.axis_index("dp")
    lane = lax.axis_index("tensor")
    nexts = (at((pos + 1) % n, core, n), at((pos + n - 1) % n, core, n))
    mate = at(pos, 1 - core, n)
    twin = (me, 1 - lane)
    fetch_attn = pltpu.make_async_copy(attn, d_proj.at[2], attn_sem.at[0])
    fetch_attn.start()
    barrier = pltpu.get_barrier_semaphore()

    def greet(o, carry):
        pl.semaphore_signal(barrier, inc=1, device_id=at((pos + o) % n, core, n), device_id_type=MESH)
        return carry

    lax.fori_loop(1, n, greet, 0)
    for other in (mate, twin):
        pl.semaphore_signal(barrier, inc=1, device_id=other, device_id_type=MESH)
    pl.semaphore_wait(barrier, n + 1)
    count, _, hidden = act.shape
    half, model = resid.shape
    q_wide = qkv.shape[1]
    per_group = q_heads // kv_heads
    lefts = scratch[0]

    def from_flipped(first):
        def fetch_left(m, side, there):
            if there is None:
                pltpu.make_async_copy(
                    flipped.at[0, pl.ds(0, lefts.shape[1])], lefts.at[side], left_sem.at[side]
                ).wait()
            elif first == 0:
                pltpu.make_async_copy(flipped.at[m // 2, there], lefts.at[side], left_sem.at[side]).start()
            else:
                @pl.when(m < 2)
                def _():
                    pltpu.make_async_copy(flipped.at[2, there], lefts.at[side], left_sem.at[side]).start()

                @pl.when(m == 2)
                def _():
                    pltpu.make_async_copy(d_flip.at[there], lefts.at[side], left_sem.at[side]).start()

        return fetch_left

    links = (n, pos, core, nexts, mate)
    begin, event, finish = reducer(
        *links, act, (grad_gate, grad_up, grad_down), from_flipped(0), scratch, (0, 0, 2 * (n - 1))
    )
    late_begin, late_event, late_finish = reducer(
        *links, d_proj, (grad_query, grad_pair, grad_out), from_flipped(2), scratch, (n, n - 1, 2 * (n - 1))
    )
    deep = blocks.shape[1]
    turns = model // deep

    def fetch(which, i, slot, width):
        start = which * model + i * deep
        return pltpu.make_async_copy(
            weights.at[pl.ds(pl.multiple_of(start, deep), deep), pl.ds(0, width)],
            blocks.at[slot, :, pl.ds(0, width)], load_sem.at[slot],
        )

    for m in range(count):
        begin(m)
    fetch(1, 0, 0, hidden).start()
    fetch(2, 0, 1, hidden).start()
    for m in range(count):
        event(m)
    theirs = pl.ds(pl.multiple_of((1 - lane) * half, half), half)
    ours = pl.ds(pl.multiple_of(lane * half, half), half)
    done = count

    def events(number):
        nonlocal done
        for e in range(done, done + number):
            event(e)
        done = done + number

    def send_part(slot, target, i):
        return remote(part.at[slot], target, swap_sem.at[i, 0], swap_sem.at[i, 1], twin)

    def dn_two(i, carry):
        there = pl.ds(pl.multiple_of(i * deep, deep), deep)
        for which in range(2):
            fetch(which + 1, i, which, hidden).wait()
            other = tail_product(act[which, theirs, :], blocks[which])
            same = tail_product(act[which, ours, :], blocks[which])
            if which == 0:
                own[:, there] = same
                d_resid[:, there] = other
            else:
                own[:, there] += same
                part[0, :, there] = (d_resid[:, there] + other).astype(jnp.bfloat16)

            @pl.when(i < turns - 1)
            def _():
                fetch(which + 1, i + 1, which, hidden).start()

        @pl.when(i % 3 == 2)
        def _():
            event(count + i // 3)

        return carry

    lax.fori_loop(0, turns, dn_two, 0)
    done = done + turns // 3
    sends = [send_part(0, peer.at[0], 0)]
    sends[0].start()
    fetch(3, 0, 0, hidden).start()
    events(3)
    sends[0].wait_recv()
    sends[0].wait_send()
    strip = 32

    def over_strips(body):
        lax.fori_loop(0, half // strip, body, 0)

    def gather_sum(target, i, total):
        @pl.when(i == 0)
        def _():
            target[...] = total

        @pl.when(i > 0)
        def _():
            target[...] += total

    def norm_two(i, carry):
        there = pl.ds(pl.multiple_of(i * strip, strip), strip)
        incoming = own[there, :] + peer[0, there, :].astype(jnp.float32)
        values = resid[there, :]
        inverse = row_scale(values)
        normed = values * inverse
        scaled = incoming * mlp_gain[...]
        change = cot[there, :].astype(jnp.float32) + inverse * (
            scaled - normed * jnp.mean(scaled * normed, axis=-1, keepdims=True)
        )
        d_resid[there, :] = change
        part[0, there, :] = change.astype(jnp.bfloat16)
        gather_sum(mlp_sum, i, jnp.sum(incoming * normed, axis=0, keepdims=True))
        return carry

    over_strips(norm_two)
    sends.append(send_part(0, d_full.at[ours], 1))
    sends[1].start()
    d_full[ours, :] = part[0]

    def narrow(which, width, slot, base, rows_of):
        def one(i, carry):
            @pl.when(i < turns - 1)
            def _():
                fetch(which, i + 1, (i + 1) % 2, width).start()

            fetch(which, i, i % 2, width).wait()
            there = pl.ds(pl.multiple_of(i * deep, deep), deep)
            for rows, mine in ((theirs, False), (ours, True)):
                total = None
                for left, start in rows_of(rows):
                    gained = tail_product(left, blocks[i % 2, :, pl.ds(start, left.shape[1])])
                    total = gained if total is None else total + gained
                if mine:
                    own[:, there] = total
                else:
                    part[slot, :, there] = total.astype(jnp.bfloat16)

            @pl.when(i % 4 == 3)
            def _():
                event(base + i // 4)

            return carry

        lax.fori_loop(0, turns, one, 0)

    narrow(3, hidden, 1, done, lambda rows: [(act[2, rows, :], 0)])
    done = done + turns // 4
    sends.append(send_part(1, peer.at[1], 2))
    sends[2].start()
    group_wide = per_group * HD

    def fetch_columns(g):
        return pltpu.make_async_copy(
            weights.at[pl.ds(0, model), pl.ds(pl.multiple_of(q_wide + g * group_wide, group_wide), group_wide)],
            columns.at[g % 2], column_sem.at[g % 2],
        )

    fetch_columns(0).start()
    events(1)
    remote(part.at[0], d_full.at[theirs], swap_sem.at[1, 0], swap_sem.at[1, 1], twin).wait_recv()
    flip_into(d_full, d_flip, stage, stage_sem)
    qk_sum[...] = jnp.zeros_like(qk_sum)
    fetch_attn.wait()

    def group_step(group, carry):
        places = [group * per_group + r for r in range(per_group)]
        places += [q_heads + group, q_heads + kv_heads + group]
        copies = [
            pltpu.make_async_copy(qkv.at[:, head_at(place)], heads.at[i], head_sem.at[i])
            for i, place in enumerate(places)
        ]
        for copy in copies:
            copy.start()

        @pl.when(group < kv_heads - 1)
        def _():
            fetch_columns(group + 1).start()

        fetch_columns(group).wait()
        d_attn[...] = product(d_full[...], columns[group % 2]).astype(jnp.bfloat16)
        for copy in copies:
            copy.wait()
        attend_back(group, dims, heads, tab, seg_col, seg_row, gains, d_attn, d_proj, qk_sum, kept)
        event(done + group)
        return carry

    lax.fori_loop(0, kv_heads, group_step, 0)
    done = done + kv_heads
    sends[2].wait_recv()

    def last_strip(i, carry):
        there = pl.ds(pl.multiple_of(i * strip, strip), strip)
        result[there, :] = (
            resid[there, :] + (own[there, :] + peer[1, there, :].astype(jnp.float32))
        ).astype(jnp.bfloat16)
        return carry

    over_strips(last_strip)
    fetch(0, 0, 0, q_wide).start()
    sends[1].wait_send()
    events(1)
    width = d_proj.shape[2]
    narrow(0, q_wide, 0, done, lambda rows: [(d_proj[0, rows, :], 0), (d_proj[1, rows, :], width)])
    done = done + turns // 4
    sends.append(send_part(0, peer.at[0], 3))
    sends[3].start()
    events(1)
    sends[3].wait_recv()

    def norm_one(i, carry):
        there = pl.ds(pl.multiple_of(i * strip, strip), strip)
        incoming = own[there, :] + peer[0, there, :].astype(jnp.float32)
        values = tokens[there, :].astype(jnp.float32)
        inverse = row_scale(values)
        normed = values * inverse
        scaled = incoming * attn_gain[...]
        change = d_resid[there, :] + inverse * (
            scaled - normed * jnp.mean(scaled * normed, axis=-1, keepdims=True)
        )
        input_grad[there, :] = change.astype(jnp.bfloat16)
        gather_sum(attn_sum, i, jnp.sum(incoming * normed, axis=0, keepdims=True))
        return carry

    over_strips(norm_one)
    dp = 2 * n
    share, head_share = model // dp, 2 * HD // dp
    table[...] = jnp.zeros_like(table)
    for d in range(dp):
        start = d * share // 128 * 128
        row = d * head_share // HD
        table[d, 0:1, :] = attn_sum[:, start : start + 128]
        table[d, 1:2, :] = mlp_sum[:, start : start + 128]
        table[d, 2:3, :] = qk_sum[row : row + 1, :]
    for i, partner in enumerate((twin, mate)):
        trade = remote(table, others.at[i], trade_sem.at[i, 0], trade_sem.at[i, 1], partner)
        trade.start()
        events(1)
        trade.wait()
        table[...] += others[i]

    def mail(o, target):
        return remote(table.at[target], inbox.at[o], post_sem.at[o], mail_sem.at[o], at((pos + o) % n, core, n))

    def post(o, carry):
        mail(o, chip_at((pos + o) % n, n) * 2 + core).start()
        return carry

    lax.fori_loop(1, n, post, 0)

    def rest(e, carry):
        event(e)
        return carry

    last = count * (n - 1)
    lax.fori_loop(done, last, rest, 0)
    for m in range(count):
        event(last + m)
        finish(m)
        late_begin(m)
        late_event(m)
    gain_out[...] = table[me]

    def collect(o, carry):
        mail(o, 0).wait_recv()
        gain_out[...] += inbox[o]
        return carry

    lax.fori_loop(1, n, collect, 0)

    def late_rest(e, carry):
        late_event(e)
        return carry

    lax.fori_loop(count, count * n, late_rest, 0)
    for m in range(count):
        late_finish(m)
    sends[2].wait_send()
    sends[3].wait_send()

    def sent(o, carry):
        mail(o, 0).wait_send()
        return carry

    lax.fori_loop(1, n, sent, 0)


def backward_block(
    flipped, act, weights, qkv, attn, cot, tokens, resid, tab, segments, gains, attn_gain, mlp_gain,
    q_heads, kv_heads, dp,
):
    n = dp // 2
    count, seq, hidden = act.shape
    half, model = resid.shape
    rows = model // dp
    wide = hidden // 2
    width = q_heads * HD
    low, full, dma, vmem, hbm = jnp.bfloat16, jnp.float32, pltpu.SemaphoreType.DMA, pltpu.VMEM, pltpu.HBM
    shape = jax.ShapeDtypeStruct
    place = lambda kind: pl.BlockSpec(memory_space=kind)
    per_group = q_heads // kv_heads
    return pl.pallas_call(
        functools.partial(backward_kernel, n, (q_heads, kv_heads, seq, seq // 2)),
        out_shape=[
            *[shape((rows, hidden), full)] * 3,
            *[shape((rows, width), full)] * 3,
            shape((half, model), low),
            shape((half, model), low),
            shape((8, 128), full),
            shape((model, seq), low),
        ],
        in_specs=[place(k) for k in (hbm, vmem, hbm, hbm, hbm, *[vmem] * 9)],
        out_specs=[place(k) for k in (*[hbm] * 6, vmem, vmem, vmem, hbm)],
        scratch_shapes=[
            vmem((3, seq, width), low),
            vmem((seq, model), low),
            vmem((half, model), full),
            vmem((2, 256, hidden), low),
            vmem((2, model, per_group * HD), low),
            vmem((half, model), full),
            vmem((2, half, model), low),
            vmem((2, half, model), low),
            vmem((seq, per_group * HD), low),
            vmem((per_group + 2, seq, HD), full),
            vmem((3, seq, HD), full),
            vmem((2, 256, seq), low),
            vmem((1, model), full),
            vmem((1, model), full),
            vmem((8, HD), full),
            vmem((dp, 8, 128), full),
            vmem((2, dp, 8, 128), full),
            vmem((n, 8, 128), full),
            dma((4, 2)),
            dma((2,)),
            dma((per_group + 2,)),
            dma((1,)),
            dma((2,)),
            dma((2,)),
            dma((2, 2)),
            dma((n,)),
            dma((n,)),
            dma((2,)),
            vmem((2, 2 * rows, seq), low),
            vmem((count, 2, rows, wide), full),
            vmem((2 * rows, wide), full),
            vmem((count, 2, rows, wide), low),
            vmem((count, 2, 2, rows, wide), low),
            vmem((count, 2, rows, wide), low),
            vmem((count, 2, SLOTS, rows, wide), low),
            dma((count, 2)),
            dma((count, 2, 2)),
            dma((count, 2)),
            dma((count, 2, SLOTS)),
            pltpu.SemaphoreType.REGULAR((count, 2)),
            dma((count, 2)),
        ],
        compiler_params=pltpu.CompilerParams(
            collective_id=2, has_side_effects=True, vmem_limit_bytes=67043328
        ),
    )(
        flipped, act, weights, qkv, attn, cot, tokens, resid, tab,
        segments.reshape(seq, 1), segments.reshape(1, seq), gains, attn_gain, mlp_gain,
    )


def on_device(
    tokens,
    seg_ids,
    w_query,
    w_key,
    w_value,
    w_output,
    w_gate,
    w_up,
    w_down,
    gain_attn,
    gain_mlp,
    gain_qk,
    cotangent,
):
    dp = lax.axis_size("dp")
    model = tokens.shape[1]
    me = lax.axis_index("dp")
    tile = jnp.zeros((8, 128), jnp.float32)
    for row, gain in enumerate((gain_attn, gain_mlp, gain_qk)):
        spot = me * gain.shape[0] % 128 if gain.shape[0] % 128 else 0
        tile = lax.dynamic_update_slice(tile, gain.astype(jnp.float32)[None, :], (row, spot))
    q_width = w_query.shape[1]
    kv_width = w_key.shape[1]
    q_heads = q_width // HD
    kv_heads = kv_width // HD
    cosine_table, sine_table, _ = tables(seg_ids[0])
    signed = jnp.concatenate([-sine_table[:, : HD // 2], sine_table[:, HD // 2 :]], axis=1)
    rope_tab = jnp.stack([cosine_table, signed])
    weights, projected, attn_rows, resid, flipped, act, attn_gain, mlp_gain, pair = forward_block(
        jnp.concatenate([w_query, w_key, w_value, w_output.T], axis=1),
        jnp.stack([w_gate, w_up, w_down.T]),
        tile,
        tokens,
        cotangent,
        rope_tab,
        seg_ids[0],
        q_heads,
        kv_heads,
        dp,
    )
    (
        grad_gate, grad_up, grad_down, grad_query, grad_pair, grad_out, result_rows, input_grad, gain_sums, _,
    ) = backward_block(
        flipped,
        act,
        weights,
        projected,
        attn_rows,
        cotangent,
        tokens,
        resid,
        rope_tab,
        seg_ids[0],
        pair,
        attn_gain,
        mlp_gain,
        q_heads,
        kv_heads,
        dp,
    )
    share = model // dp
    qk_share = 2 * HD // dp
    return (
        result_rows,
        input_grad,
        grad_query,
        grad_pair[:, :kv_width],
        grad_pair[:, kv_width:],
        grad_out.T,
        grad_gate,
        grad_up,
        grad_down.T,
        lax.dynamic_slice(gain_sums, (0, me * share % 128), (1, share))[0],
        lax.dynamic_slice(gain_sums, (1, me * share % 128), (1, share))[0],
        lax.dynamic_slice(gain_sums, (2, me * qk_share % HD), (1, qk_share))[0],
    )


def solution(mesh):
    return jax.shard_map(
        on_device,
        mesh=mesh,
        in_specs=(
            P(("dp", "tensor"), None),
            P("dp", None),
            P("dp", "tensor"),
            P("dp", "tensor"),
            P("dp", "tensor"),
            P("tensor", "dp"),
            P("dp", "tensor"),
            P("dp", "tensor"),
            P("tensor", "dp"),
            P("dp"),
            P("dp"),
            P("dp"),
            P(("dp", "tensor"), None),
        ),
        out_specs=(
            P(("dp", "tensor"), None),
            P(("dp", "tensor"), None),
            P("dp", "tensor"),
            P("dp", "tensor"),
            P("dp", "tensor"),
            P("tensor", "dp"),
            P("dp", "tensor"),
            P("dp", "tensor"),
            P("tensor", "dp"),
            P("dp"),
            P("dp"),
            P("dp"),
        ),
        check_vma=False,
    )
```

```python
import functools
import jax
import jax.numpy as jnp
import numpy as np
from jax import lax
from jax.experimental import pallas as pl
from jax.experimental.pallas import tpu as pltpu

from jax.sharding import PartitionSpec as P

MESH = pl.DeviceIdType.MESH
HD = 128
epsilon = 1e-06
rope_base = 1000000.0


def ring_place(n):
    me = lax.axis_index("dp")
    chip = me // 2
    core = me % 2
    odd = chip % 2
    pos = (1 - odd) * (chip // 2) + odd * (n - 1 - chip // 2)
    return pos, core


def chip_at(pos, n):
    high = pos // (n // 2)
    return (1 - high) * (2 * pos) + high * (2 * (n - 1 - pos) + 1)


def at(pos, core, n):
    return (chip_at(pos, n) * 2 + core, lax.axis_index("tensor"))


def meet(peers):
    barrier = pltpu.get_barrier_semaphore()
    for peer in peers:
        pl.semaphore_signal(barrier, inc=1, device_id=peer, device_id_type=MESH)
    pl.semaphore_wait(barrier, len(peers))


def remote(src, dst, send, recv, peer):
    return pltpu.make_async_remote_copy(
        src_ref=src, dst_ref=dst, send_sem=send, recv_sem=recv, device_id=peer, device_id_type=MESH
    )


def product(left, right):
    return jnp.dot(left, right, preferred_element_type=jnp.float32)


def lead_product(left, right):
    return lax.dot_general(
        left, right, (((0,), (0,)), ((), ())), preferred_element_type=jnp.float32
    )


def tail_product(left, right):
    return lax.dot_general(
        left, right, (((1,), (1,)), ((), ())), preferred_element_type=jnp.float32
    )


def turn(values):
    return pltpu.roll(values, values.shape[-1] // 2, 1)


def row_scale(values):
    return lax.rsqrt(jnp.mean(values * values, axis=-1, keepdims=True) + epsilon)


def head_at(index):
    return pl.ds(pl.multiple_of(index * HD, HD), HD)


def prepared(raw, gain, cosine, sine):
    inverse = row_scale(raw)
    hat = raw * inverse
    scaled = hat * gain
    return inverse, hat, (scaled * cosine + turn(scaled) * sine).astype(jnp.bfloat16)


def exp_block(query, keys, seg_col, seg_row, first):
    width = keys.shape[0]
    scores = tail_product(query, keys) * HD ** (-0.5)
    rows = lax.broadcasted_iota(jnp.int32, scores.shape, 0) + first
    columns = lax.broadcasted_iota(jnp.int32, scores.shape, 1)
    allowed = (seg_col[first : first + scores.shape[0], :] == seg_row[:, :width]) & (
        columns <= rows
    )
    return jnp.where(allowed, jnp.exp(scores), 0.0)


def attend_group(group, dims, qkv, tab, seg_col, seg_row, gains, attn, kept):
    q_heads, kv_heads, seq, block = dims
    per_group = q_heads // kv_heads
    cosine, sine = tab[0], tab[1]
    raw = qkv[:, head_at(q_heads + group)]
    kept[0] = prepared(raw, gains[1:2, :], cosine, sine)[2]
    kept[1] = qkv[:, head_at(q_heads + kv_heads + group)].astype(jnp.bfloat16)
    for r in range(per_group):
        head = group * per_group + r
        raw = qkv[:, head_at(head)]
        query = prepared(raw, gains[0:1, :], cosine, sine)[2]
        for first in range(0, seq, block):
            width = first + block
            exps = exp_block(query[first:width], kept[0, :width, :], seg_col, seg_row, first)
            probs = (exps / jnp.sum(exps, axis=-1, keepdims=True)).astype(jnp.bfloat16)
            attn[first:width, head_at(head)] = product(probs, kept[1, :width, :]).astype(jnp.bfloat16)


def block_columns(ref, index, width):
    if width % 128 == 0:
        return ref[:, pl.ds(pl.multiple_of(index * width, width), width)]
    fold = 128 // width
    tile = ref[:, pl.ds(pl.multiple_of((index // fold) * 128, 128), 128)]
    picked = tile[:, :width]
    for i in range(1, fold):
        picked = jnp.where(index % fold == i, tile[:, i * width : (i + 1) * width], picked)
    return picked


def flip_into(source, target, stage, stage_sem):
    deep = stage.shape[1]
    turns = source.shape[1] // deep

    def put(i):
        return pltpu.make_async_copy(
            stage.at[i % 2], target.at[pl.ds(pl.multiple_of(i * deep, deep), deep)], stage_sem.at[i % 2]
        )

    def one(i, carry):
        @pl.when(i >= 2)
        def _():
            put(i - 2).wait()

        stage[i % 2] = source[:, pl.ds(pl.multiple_of(i * deep, deep), deep)].T
        put(i).start()
        return carry

    lax.fori_loop(0, turns, one, 0)
    put(turns - 2).wait()
    put(turns - 1).wait()


def forward_kernel(n, dims, *refs):
    (
        query_shard, key_shard, value_shard, out_shard, gate_shard, up_shard, down_shard,
        tokens, cot, frequency, seg_row, attn_share, mlp_share, qk_share,
        weights, qkv_out, attn, resid, flipped, act, attn_gain, mlp_gain, gains, tab, seg_col,
        full_rows, cot_full, full_two, out_weight, columns, box, kept, part, peer, acc, blocks, stage,
        own_sem, send_sem, recv_sem, give_sem, take_sem, swap_sem, load_sem, stage_sem, column_sem, tile_sem,
    ) = refs
    q_heads, kv_heads, seq, block = dims
    pos, core = ring_place(n)
    me = lax.axis_index("dp")
    lane = lax.axis_index("tensor")
    nexts = (at((pos + 1) % n, core, n), at((pos + n - 1) % n, core, n))
    mate = at(pos, 1 - core, n)
    twin = (me, 1 - lane)
    ffn_shards = (gate_shard, up_shard, down_shard)
    count = len(ffn_shards)
    rows, width = gate_shard.shape
    wide = width // 2
    q_span, kv_span = query_shard.shape[1], key_shard.shape[1]
    model = 2 * n * rows
    half = seq // 2
    theirs = pl.ds(pl.multiple_of((1 - lane) * half, half), half)
    ours = pl.ds(pl.multiple_of(lane * half, half), half)
    tile = box.at[me]
    tile[...] = jnp.zeros(tile.shape, jnp.float32)
    for i, gain in enumerate((attn_share, mlp_share, qk_share)):
        size = gain.shape[1]
        tile[i : i + 1, 0:size] = gain[...].astype(jnp.float32)
        if size % 128:
            tile[i : i + 1, :] = pltpu.roll(tile[i : i + 1, :], me * size % 128, 1)
    meet((*nexts, mate, twin))

    def owner_of(side, step):
        if side == 0:
            return (pos - step + 2 * n) % n
        return (pos + step) % n

    def small(sub, side):
        start, source = (
            ((0, query_shard), (q_span + 2 * kv_span, out_shard)),
            ((q_span, key_shard), (q_span + kv_span, value_shard)),
        )[sub][side]
        return (sub, 0, pl.ds(start, source.shape[1]), source)

    def large(w, side):
        columns = pl.ds(side * wide, wide)
        source = ffn_shards[w].at[:, columns] if isinstance(w, int) else None
        return (w + 2, (w + 1) * model, columns, source)

    def spot(message, chip, who):
        start = message[1] + (chip * 2 + who) * rows
        return weights.at[pl.ds(pl.multiple_of(start, rows), rows), message[2]]

    def hop(message, side, step):
        k = message[0]
        here = spot(message, chip_at(owner_of(side, step - 1), n), core)
        return remote(here, here, send_sem.at[k, side, step], recv_sem.at[k, side, step], nexts[side])

    def arrived(message, side, step):
        k = message[0]
        here = spot(message, chip_at(owner_of(side, step), n), core)
        return remote(here, here, send_sem.at[k, side, step], recv_sem.at[k, side, step], nexts[side])

    def hand(message, side, step, who):
        k = message[0]
        here = spot(message, chip_at(owner_of(side, step), n), who)
        return remote(here, here, give_sem.at[k, side, step], take_sem.at[k, side, step], mate)

    def begin(message, side):
        k = message[0]
        source = message[3]
        here = spot(message, chip_at(pos, n), core)
        remote(source, here, send_sem.at[k, side, 1], recv_sem.at[k, side, 1], nexts[side]).start()
        remote(source, here, give_sem.at[k, side, 0], take_sem.at[k, side, 0], mate).start()
        pltpu.make_async_copy(source, here, own_sem.at[k, side]).start()

    def keep_own(message, side):
        here = spot(message, chip_at(pos, n), core)
        return pltpu.make_async_copy(here, here, own_sem.at[message[0], side])

    def tile_hop(step, owner):
        place = chip_at(owner, n) * 2 + core
        return remote(box.at[place], box.at[place], tile_sem.at[0, step], tile_sem.at[1, step], nexts[0])

    def tile_hand(step, who):
        place = chip_at(owner_of(0, step), n) * 2 + who
        return remote(box.at[place], box.at[place], tile_sem.at[2, step], tile_sem.at[3, step], mate)

    swaps = [
        remote(source, target.at[ours], swap_sem.at[i, 0], swap_sem.at[i, 1], twin)
        for i, (source, target) in enumerate(((tokens, full_rows), (cot, cot_full)))
    ]
    remote(tile, box.at[me], tile_sem.at[0, 1], tile_sem.at[1, 1], nexts[0]).start()
    remote(tile, box.at[me], tile_sem.at[2, 0], tile_sem.at[3, 0], mate).start()
    for sub in range(2):
        for side in range(2):
            begin(small(sub, side), side)
    for swap in swaps:
        swap.start()
    full_rows[ours, :] = tokens[...]
    cot_full[ours, :] = cot[...]

    def pass_on(message, side, step):
        arrived(message, side, step).wait_recv()

        @pl.when(step < n - 1)
        def _():
            hop(message, side, step + 1).start()

        hand(message, side, step, core).start()

    def pass_tile(step):
        tile_hop(step, owner_of(0, step)).wait_recv()

        @pl.when(step < n - 1)
        def _():
            tile_hop(step + 1, owner_of(0, step)).start()

        tile_hand(step, core).start()

    def mixed_step(step, carry):
        pass_tile(step)
        for sub in range(2):
            for side in range(2):
                pass_on(small(sub, side), side, step)
        return carry

    def mixed_steps(first, last):
        lax.fori_loop(first, last, mixed_step, 0)

    mixed_steps(1, 3)
    row = lax.broadcasted_iota(jnp.int32, (seq, seq), 0)
    column = lax.broadcasted_iota(jnp.int32, (seq, seq), 1)
    ids = jnp.broadcast_to(seg_row[...], (seq, seq)).astype(jnp.float32)
    own_id = jnp.sum(jnp.where(row == column, ids, 0.0), axis=1, keepdims=True)
    doc_start = jnp.sum(jnp.where(ids < own_id, 1.0, 0.0), axis=1, keepdims=True)
    place = lax.broadcasted_iota(jnp.int32, (seq, 1), 0).astype(jnp.float32)
    seg_col[...] = own_id.astype(jnp.int32)
    angles = (place - doc_start) * frequency[...]
    tab[0] = jnp.cos(angles)
    sign = jnp.where(lax.broadcasted_iota(jnp.int32, angles.shape, 1) < HD // 2, -1.0, 1.0)
    tab[1] = jnp.sin(angles) * sign
    mixed_steps(3, n - 1)
    pass_tile(n - 1)
    for w in range(count):
        for side in range(2):
            begin(large(w, side), side)
        if w < 2:
            for side in range(2):
                pass_on(small(w, side), side, n - 1)

    def service(event):
        step, w = event // count + 1, event % count
        for side in range(2):
            pass_on(large(w, side), side, step)

    def services(first, last):
        def one(event, carry):
            service(event)
            return carry

        lax.fori_loop(first, last, one, 0)

    def gathered(step, carry):
        for sub in range(2):
            for side in range(2):
                hand(small(sub, side), side, step, 1 - core).wait_recv()
        tile_hand(step, 1 - core).wait_recv()
        return carry

    lax.fori_loop(0, n, gathered, 0)
    for sub in range(2):
        for side in range(2):
            keep_own(small(sub, side), side).wait()
    q_wide = (q_heads + 2 * kv_heads) * HD
    fetch_out = pltpu.make_async_copy(
        weights.at[pl.ds(0, model), pl.ds(q_wide, width - q_wide)], out_weight, load_sem.at[0]
    )
    turns = q_wide // columns.shape[2]
    deep = columns.shape[2]

    def fetch_columns(i):
        return pltpu.make_async_copy(
            weights.at[pl.ds(0, model), pl.ds(pl.multiple_of(i * deep, deep), deep)],
            columns.at[i % 2], column_sem.at[i % 2],
        )

    fetch_columns(0).start()
    fetch_out.start()
    dp = 2 * n
    share, head_share = model // dp, 2 * HD // dp
    for first, target, per in ((0, attn_gain, share), (1, mlp_gain, share)):
        for s in range(model // 128):
            owners = [d for d in range(dp) if d * per // 128 == s]
            total = box[owners[0], first : first + 1, :]
            for d in owners[1:]:
                total = total + box[d, first : first + 1, :]
            target[:, s * 128 : (s + 1) * 128] = total
    for s in range(2):
        owners = [d for d in range(dp) if d * head_share // HD == s]
        total = box[owners[0], 2:3, :]
        for d in owners[1:]:
            total = total + box[d, 2:3, :]
        gains[s : s + 1, :] = total
    swaps[0].wait_recv()
    strip = 32

    def norm_strip(i, carry):
        there = pl.ds(pl.multiple_of(i * strip, strip), strip)
        values = full_rows[there, :].astype(jnp.float32)
        full_two[there, :] = (values * row_scale(values) * attn_gain[...]).astype(jnp.bfloat16)
        return carry

    lax.fori_loop(0, seq // strip, norm_strip, 0)
    qkv = acc.at[count - 1]

    def project(i, carry):
        @pl.when(i < turns - 1)
        def _():
            fetch_columns(i + 1).start()

        fetch_columns(i).wait()
        qkv[:, pl.ds(pl.multiple_of(i * deep, deep), deep)] = product(full_two[...], columns[i % 2])
        return carry

    lax.fori_loop(0, turns, project, 0)
    save_qkv = pltpu.make_async_copy(qkv.at[:, pl.ds(0, q_wide)], qkv_out, load_sem.at[1])
    save_qkv.start()
    service(0)

    def load(step, w, side):
        start = (w + 1) * model + chip_at(owner_of(side, step), n) * 2 * rows
        return pltpu.make_async_copy(
            weights.at[pl.ds(pl.multiple_of(start, 2 * rows), 2 * rows), pl.ds(side * wide, wide)],
            blocks.at[side], load_sem.at[side],
        )

    def work(job):
        step, w = job // count, job % count
        for side in range(2):
            hand(large(w, side), side, step, 1 - core).wait_recv()

            @pl.when(step == 0)
            def _():
                keep_own(large(w, side), side).wait()

            load(step, w, side).start()
        for side in range(2):
            load(step, w, side).wait()
            chip = chip_at(owner_of(side, step), n)

            def with_left(left):
                tile_width = wide // 3

                def one(i, carry):
                    there = pl.ds(pl.multiple_of(side * wide + i * tile_width, tile_width), tile_width)
                    gained = product(left, blocks[side, :, pl.ds(pl.multiple_of(i * tile_width, tile_width), tile_width)])

                    @pl.when(step == 0)
                    def _():
                        acc[w, :, there] = gained

                    @pl.when(step > 0)
                    def _():
                        acc[w, :, there] += gained

                    return carry

                lax.fori_loop(0, 3, one, 0)

            @pl.when(w < count - 1)
            def _():
                with_left(block_columns(full_two, chip, 2 * rows))

            @pl.when(w == count - 1)
            def _():
                with_left(block_columns(cot_full, chip, 2 * rows))

    def flip(source, target):
        flip_into(source, flipped.at[target], stage, stage_sem)

    groups = (qkv, tab, seg_col, seg_row, gains, attn, kept)

    def attend():
        def one(group, carry):
            attend_group(group, dims, *groups)

            @pl.when(group % (kv_heads // 2) == kv_heads // 2 - 1)
            def _():
                service(1 + group // (kv_heads // 2))

            return carry

        lax.fori_loop(0, kv_heads, one, 0)

    flip(full_two, 2)
    attend()
    fetch_out.wait()
    part[...] = tail_product(attn[theirs, :], out_weight[...]).astype(jnp.bfloat16)
    swaps[1].wait_recv()
    send_part = remote(part, peer, swap_sem.at[2, 0], swap_sem.at[2, 1], twin)
    send_part.start()
    resid[...] = tokens[...].astype(jnp.float32) + tail_product(attn[ours, :], out_weight[...])
    services(3, 5)
    flip(cot_full, 1)
    service(5)
    send_part.wait_recv()
    summed = resid[...] + peer[...].astype(jnp.float32)
    resid[...] = summed
    send_part.wait_send()
    part[...] = (summed * row_scale(summed) * mlp_gain[...]).astype(jnp.bfloat16)
    send_two = remote(part, full_two.at[ours], swap_sem.at[3, 0], swap_sem.at[3, 1], twin)
    send_two.start()
    full_two[ours, :] = part[...]
    ready = 9
    services(6, ready)
    remote(part, full_two.at[theirs], swap_sem.at[3, 0], swap_sem.at[3, 1], twin).wait_recv()
    flip(full_two, 0)
    save_qkv.wait()

    def works(first, last):
        def one(job, carry):
            work(job)
            return carry

        lax.fori_loop(first, last, one, 0)

    pairs = ready + 3

    def both(i, carry):
        service(ready + i)
        several = 1 - jnp.minimum(i // pairs, 1)
        first = several * 2 * i + (1 - several) * (pairs + i)
        works(first, first + 1 + several)
        return carry

    lax.fori_loop(0, count * (n - 1) - ready, both, 0)

    def finish(i, carry):
        there = pl.ds(pl.multiple_of(i * strip, strip), strip)
        gate = acc[0, there, :]
        up = acc[1, there, :]
        d_act = acc[2, there, :]
        sig = 1.0 / (1.0 + jnp.exp(-gate))
        silu = gate * sig
        act[0, there, :] = (d_act * up * sig * (1.0 + gate * (1.0 - sig))).astype(jnp.bfloat16)
        act[1, there, :] = (d_act * silu).astype(jnp.bfloat16)
        act[2, there, :] = (silu * up).astype(jnp.bfloat16)
        return carry

    lax.fori_loop(0, seq // strip, finish, 0)

    def drain(step, carry):
        for side in range(2):
            for message in [small(sub, side) for sub in range(2)] + [large(w, side) for w in range(count)]:
                hop(message, side, step).wait_send()
                hand(message, side, step, core).wait_send()
        tile_hop(step, owner_of(0, step)).wait_send()
        tile_hand(step, core).wait_send()
        return carry

    lax.fori_loop(1, n, drain, 0)
    for side in range(2):
        for message in [small(sub, side) for sub in range(2)] + [large(w, side) for w in range(count)]:
            hand(message, side, 0, core).wait_send()
    tile_hand(0, core).wait_send()
    for swap in (*swaps, send_two):
        swap.wait_send()


def forward_block(shards, tokens, cot, frequency, seg_row, shares, q_heads, kv_heads, dp):
    n = dp // 2
    rows, width = shards[-1].shape
    count = 3
    half, model = tokens.shape
    seq = 2 * half
    q_wide = (q_heads + 2 * kv_heads) * HD
    low, full, dma, vmem, hbm = jnp.bfloat16, jnp.float32, pltpu.SemaphoreType.DMA, pltpu.VMEM, pltpu.HBM
    shape = jax.ShapeDtypeStruct
    place = lambda kind: pl.BlockSpec(memory_space=kind)
    return pl.pallas_call(
        functools.partial(forward_kernel, n, (q_heads, kv_heads, seq, seq // 2)),
        out_shape=[
            shape(((count + 1) * model, width), low),
            shape((seq, q_wide), full),
            shape((seq, q_heads * HD), low),
            shape((half, model), full),
            shape((3, model, seq), low),
            shape((count, seq, width), low),
            shape((1, model), full),
            shape((1, model), full),
            shape((2, HD), full),
            shape((2, seq, HD), full),
            shape((seq, 1), jnp.int32),
        ],
        in_specs=[place(vmem)] * 14,
        out_specs=[place(k) for k in (hbm, hbm, vmem, vmem, hbm, *[vmem] * 6)],
        scratch_shapes=[
            vmem((seq, model), low),
            vmem((seq, model), low),
            vmem((seq, model), low),
            vmem((model, width - q_wide), low),
            vmem((2, model, 256), low),
            vmem((dp, 8, 128), full),
            vmem((2, seq, HD), low),
            vmem((half, model), low),
            vmem((half, model), low),
            vmem((count, seq, width), full),
            vmem((2, 2 * rows, width // 2), low),
            vmem((2, 256, seq), low),
            dma((count + 2, 2)),
            dma((count + 2, 2, n)),
            dma((count + 2, 2, n)),
            dma((count + 2, 2, n)),
            dma((count + 2, 2, n)),
            dma((4, 2)),
            dma((2,)),
            dma((2,)),
            dma((2,)),
            dma((4, n)),
        ],
        compiler_params=pltpu.CompilerParams(
            collective_id=1, has_side_effects=True, vmem_limit_bytes=67043328
        ),
    )(*shards, tokens, cot, frequency, seg_row, *shares)


SLOTS = 3


def undo(incoming, hat, inverse, gain, cosine, sine):
    turned = incoming * cosine - turn(incoming) * sine
    total = jnp.sum(turned * hat, axis=0, keepdims=True)
    scaled = turned * gain
    raw = inverse * (scaled - hat * jnp.mean(scaled * hat, axis=-1, keepdims=True))
    return total, raw.astype(jnp.bfloat16)


def attend_back(group, dims, heads, tab, seg_col, seg_row, gains, d_attn, d_proj, sums, kept):
    q_heads, kv_heads, seq, block = dims
    per_group = q_heads // kv_heads
    low = jnp.bfloat16
    scale = HD ** (-0.5)
    cosine, sine = tab[0], tab[1]
    keys = prepared(heads[per_group], gains[1:2, :], cosine, sine)[2]
    values = heads[per_group + 1].astype(low)
    for r in range(per_group):
        head = group * per_group + r
        q_inverse, q_hat, query = prepared(heads[r], gains[0:1, :], cosine, sine)
        for first in range(0, seq, block):
            width = first + block
            exps = exp_block(query[first:width], keys[:width], seg_col, seg_row, first)
            probs = exps / jnp.sum(exps, axis=-1, keepdims=True)
            incoming = d_attn[first:width, head_at(r)]
            d_probs = tail_product(incoming, values[:width])
            delta = jnp.sum(probs * d_probs, axis=-1, keepdims=True)
            d_scores = (probs * (d_probs - delta)).astype(low)
            kept[0, first:width, :] = product(d_scores, keys[:width]) * scale
            d_keys = lead_product(d_scores, query[first:width])
            d_values = lead_product(probs.astype(low), incoming)
            if r == 0 and first == 0:
                kept[1] = jnp.zeros_like(kept[1])
                kept[2] = jnp.zeros_like(kept[2])
            kept[1, :width, :] += d_keys
            kept[2, :width, :] += d_values
        total, raw = undo(kept[0], q_hat, q_inverse, gains[0:1, :], cosine, sine)
        sums[0:1, :] += total
        d_proj[0, :, head_at(head)] = raw
    k_inverse, k_hat, _ = prepared(heads[per_group], gains[1:2, :], cosine, sine)
    total, raw = undo(kept[1] * scale, k_hat, k_inverse, gains[1:2, :], cosine, sine)
    sums[1:2, :] += total
    d_proj[1, :, head_at(group)] = raw
    d_proj[1, :, head_at(kv_heads + group)] = kept[2].astype(low)


def reducer(n, pos, core, nexts, mate, rights, outs, fetch_left, scratch, stage_of):
    lefts, mine, term, give, take, ship, land, give_sem, take_sem, ship_sem, land_sem, free_sem, out_sem = scratch
    before, sends_before, sends_total = stage_of
    count = rights.shape[0]
    wide = rights.shape[2] // 2
    rows = outs[0].shape[0]
    span = pl.ds(0, wide)

    def owner_of(side, step):
        if side == 0:
            return (pos - 1 - step + 2 * n) % n
        return (pos + 1 + step) % n

    def given(m, side, step):
        slot = (before + step) % 2
        return remote(
            give.at[m, side, :, span], take.at[m, side, slot, :, span],
            give_sem.at[m, side], take_sem.at[m, side, slot], mate,
        )

    def shipped(m, side, step):
        slot = (sends_before + step) % SLOTS
        return remote(
            ship.at[m, side, :, span], land.at[m, side, slot, :, span],
            ship_sem.at[m, side], land_sem.at[m, side, slot], nexts[side],
        )

    def fetch(m, step):
        for side in range(2):
            start = pl.multiple_of(chip_at(owner_of(side, step), n) * 2 * rows, 2 * rows)
            fetch_left(m, side, pl.ds(start, 2 * rows))

    def early(m, step):
        for side in range(2):
            fetch_left(m, side, None)
        for side in range(2):
            tile = min(512, wide)

            def one(i, carry):
                there = pl.multiple_of(i * tile, tile)
                term[:, pl.ds(there, tile)] = product(
                    lefts[side], rights[m, :, pl.ds(pl.multiple_of(side * wide + there, tile), tile)]
                )
                return carry

            lax.fori_loop(0, wide // tile, one, 0)

            @pl.when(step >= 1)
            def _():
                given(m, side, step - 1).wait_send()

            other = term[pl.ds(pl.multiple_of((1 - core) * rows, rows), rows), span]
            give[m, side, :, span] = other.astype(jnp.bfloat16)
            given(m, side, step).start()
            mine[m, side, :, span] = term[pl.ds(pl.multiple_of(core * rows, rows), rows), span]

    def event(e):
        step, m = e // count, e % count

        @pl.when(step < n - 1)
        def _():
            fetch(m, step + 1)

        for side in range(2):
            given(m, side, step).wait_recv()
            near = take[m, side, (before + step) % 2, :, span].astype(jnp.float32)

            @pl.when(step == 0)
            def _():
                mine[m, side, :, span] += near

            @pl.when(step > 0)
            def _():
                shipped(m, side, step - 1).wait_recv()
                far = land[m, side, (sends_before + step - 1) % SLOTS, :, span].astype(jnp.float32)
                mine[m, side, :, span] += near + far

                @pl.when(sends_before + step - 1 + SLOTS < sends_total)
                def _():
                    pl.semaphore_signal(
                        free_sem.at[m, side], inc=1, device_id=nexts[1 - side], device_id_type=MESH
                    )

                shipped(m, side, step - 1).wait_send()

            @pl.when(step < n - 1)
            def _():
                @pl.when(sends_before + step >= SLOTS)
                def _():
                    pl.semaphore_wait(free_sem.at[m, side], 1)

                ship[m, side, :, span] = mine[m, side, :, span].astype(jnp.bfloat16)
                shipped(m, side, step).start()

            @pl.when(step == n - 1)
            def _():
                for i in range(count):
                    @pl.when(m == i)
                    def _():
                        written(m, side, i).start()

        @pl.when(step < n - 1)
        def _():
            early(m, step + 1)

    def written(m, side, i):
        return pltpu.make_async_copy(
            mine.at[m, side, :, span], outs[i].at[:, pl.ds(side * wide, wide)], out_sem.at[m, side]
        )

    def begin(m):
        fetch(m, 0)
        early(m, 0)

    def finish(m):
        for side in range(2):
            given(m, side, n - 1).wait_send()
            written(m, side, 0).wait()

    return begin, event, finish


def backward_kernel(n, dims, *refs):
    (
        flipped, act, weights, qkv, attn, cot, tokens, resid, tab, seg_col, seg_row, gains, attn_gain, mlp_gain,
        grad_gate, grad_up, grad_down, grad_query, grad_pair, grad_out, result, input_grad, gain_out, d_flip,
        d_proj, d_full, d_resid, blocks, columns, own, part, peer, d_attn, heads, kept, stage,
        attn_sum, mlp_sum, qk_sum, table, others, inbox,
        swap_sem, load_sem, head_sem, attn_sem, stage_sem, column_sem, trade_sem, post_sem, mail_sem, left_sem,
        *scratch,
    ) = refs
    q_heads, kv_heads, seq, block = dims
    pos, core = ring_place(n)
    me = lax.axis_index("dp")
    lane = lax.axis_index("tensor")
    nexts = (at((pos + 1) % n, core, n), at((pos + n - 1) % n, core, n))
    mate = at(pos, 1 - core, n)
    twin = (me, 1 - lane)
    fetch_attn = pltpu.make_async_copy(attn, d_proj.at[2], attn_sem.at[0])
    fetch_attn.start()
    barrier = pltpu.get_barrier_semaphore()

    def greet(o, carry):
        pl.semaphore_signal(barrier, inc=1, device_id=at((pos + o) % n, core, n), device_id_type=MESH)
        return carry

    lax.fori_loop(1, n, greet, 0)
    for other in (mate, twin):
        pl.semaphore_signal(barrier, inc=1, device_id=other, device_id_type=MESH)
    pl.semaphore_wait(barrier, n + 1)
    count, _, hidden = act.shape
    half, model = resid.shape
    q_wide = qkv.shape[1]
    per_group = q_heads // kv_heads
    lefts = scratch[0]

    def from_flipped(first):
        def fetch_left(m, side, there):
            if there is None:
                pltpu.make_async_copy(
                    flipped.at[0, pl.ds(0, lefts.shape[1])], lefts.at[side], left_sem.at[side]
                ).wait()
            elif first == 0:
                pltpu.make_async_copy(flipped.at[m // 2, there], lefts.at[side], left_sem.at[side]).start()
            else:
                @pl.when(m < 2)
                def _():
                    pltpu.make_async_copy(flipped.at[2, there], lefts.at[side], left_sem.at[side]).start()

                @pl.when(m == 2)
                def _():
                    pltpu.make_async_copy(d_flip.at[there], lefts.at[side], left_sem.at[side]).start()

        return fetch_left

    links = (n, pos, core, nexts, mate)
    begin, event, finish = reducer(
        *links, act, (grad_gate, grad_up, grad_down), from_flipped(0), scratch, (0, 0, 2 * (n - 1))
    )
    late_begin, late_event, late_finish = reducer(
        *links, d_proj, (grad_query, grad_pair, grad_out), from_flipped(2), scratch, (n, n - 1, 2 * (n - 1))
    )
    deep = blocks.shape[1]
    turns = model // deep

    def fetch(which, i, slot, width):
        start = which * model + i * deep
        return pltpu.make_async_copy(
            weights.at[pl.ds(pl.multiple_of(start, deep), deep), pl.ds(0, width)],
            blocks.at[slot, :, pl.ds(0, width)], load_sem.at[slot],
        )

    def first_m(m, carry):
        begin(m)
        return carry

    lax.fori_loop(0, count, first_m, 0)
    fetch(1, 0, 0, hidden).start()
    fetch(2, 0, 1, hidden).start()
    def run(first, last):
        def one(e, carry):
            event(e)
            return carry

        lax.fori_loop(first, last, one, 0)

    run(0, count)
    theirs = pl.ds(pl.multiple_of((1 - lane) * half, half), half)
    ours = pl.ds(pl.multiple_of(lane * half, half), half)
    done = count

    def events(number):
        nonlocal done
        run(done, done + number)
        done = done + number

    def send_part(slot, target, i):
        return remote(part.at[slot], target, swap_sem.at[i, 0], swap_sem.at[i, 1], twin)

    def dn_two(i, carry):
        there = pl.ds(pl.multiple_of(i * deep, deep), deep)
        for which in range(2):
            fetch(which + 1, i, which, hidden).wait()
            other = tail_product(act[which, theirs, :], blocks[which])
            same = tail_product(act[which, ours, :], blocks[which])
            if which == 0:
                own[:, there] = same
                d_resid[:, there] = other
            else:
                own[:, there] += same
                part[0, :, there] = (d_resid[:, there] + other).astype(jnp.bfloat16)

            @pl.when(i < turns - 1)
            def _():
                fetch(which + 1, i + 1, which, hidden).start()

        @pl.when(i % 3 == 2)
        def _():
            event(count + i // 3)

        return carry

    lax.fori_loop(0, turns, dn_two, 0)
    done = done + turns // 3
    sends = [send_part(0, peer.at[0], 0)]
    sends[0].start()
    fetch(3, 0, 0, hidden).start()
    events(3)
    sends[0].wait_recv()
    sends[0].wait_send()
    strip = 32

    def over_strips(body):
        lax.fori_loop(0, half // strip, body, 0)

    def gather_sum(target, i, total):
        @pl.when(i == 0)
        def _():
            target[...] = total

        @pl.when(i > 0)
        def _():
            target[...] += total

    def norm_two(i, carry):
        there = pl.ds(pl.multiple_of(i * strip, strip), strip)
        incoming = own[there, :] + peer[0, there, :].astype(jnp.float32)
        values = resid[there, :]
        inverse = row_scale(values)
        normed = values * inverse
        scaled = incoming * mlp_gain[...]
        change = cot[there, :].astype(jnp.float32) + inverse * (
            scaled - normed * jnp.mean(scaled * normed, axis=-1, keepdims=True)
        )
        d_resid[there, :] = change
        part[0, there, :] = change.astype(jnp.bfloat16)
        gather_sum(mlp_sum, i, jnp.sum(incoming * normed, axis=0, keepdims=True))
        return carry

    over_strips(norm_two)
    sends.append(send_part(0, d_full.at[ours], 1))
    sends[1].start()
    d_full[ours, :] = part[0]

    def narrow(which, width, slot, base, rows_of):
        def one(i, carry):
            @pl.when(i < turns - 1)
            def _():
                fetch(which, i + 1, (i + 1) % 2, width).start()

            fetch(which, i, i % 2, width).wait()
            there = pl.ds(pl.multiple_of(i * deep, deep), deep)
            for rows, mine in ((theirs, False), (ours, True)):
                total = None
                for left, start in rows_of(rows):
                    gained = tail_product(left, blocks[i % 2, :, pl.ds(start, left.shape[1])])
                    total = gained if total is None else total + gained
                if mine:
                    own[:, there] = total
                else:
                    part[slot, :, there] = total.astype(jnp.bfloat16)

            @pl.when(i % 4 == 3)
            def _():
                event(base + i // 4)

            return carry

        lax.fori_loop(0, turns, one, 0)

    narrow(3, hidden, 1, done, lambda rows: [(act[2, rows, :], 0)])
    done = done + turns // 4
    sends.append(send_part(1, peer.at[1], 2))
    sends[2].start()
    group_wide = per_group * HD

    def fetch_columns(g):
        return pltpu.make_async_copy(
            weights.at[pl.ds(0, model), pl.ds(pl.multiple_of(q_wide + g * group_wide, group_wide), group_wide)],
            columns.at[g % 2], column_sem.at[g % 2],
        )

    fetch_columns(0).start()
    events(1)
    remote(part.at[0], d_full.at[theirs], swap_sem.at[1, 0], swap_sem.at[1, 1], twin).wait_recv()
    flip_into(d_full, d_flip, stage, stage_sem)
    qk_sum[...] = jnp.zeros_like(qk_sum)
    fetch_attn.wait()

    def group_step(group, carry):
        places = [group * per_group + r for r in range(per_group)]
        places += [q_heads + group, q_heads + kv_heads + group]
        copies = [
            pltpu.make_async_copy(qkv.at[:, head_at(place)], heads.at[i], head_sem.at[i])
            for i, place in enumerate(places)
        ]
        for copy in copies:
            copy.start()

        @pl.when(group < kv_heads - 1)
        def _():
            fetch_columns(group + 1).start()

        fetch_columns(group).wait()
        d_attn[...] = product(d_full[...], columns[group % 2]).astype(jnp.bfloat16)
        for copy in copies:
            copy.wait()
        attend_back(group, dims, heads, tab, seg_col, seg_row, gains, d_attn, d_proj, qk_sum, kept)
        event(done + group)
        return carry

    lax.fori_loop(0, kv_heads, group_step, 0)
    done = done + kv_heads
    sends[2].wait_recv()

    def last_strip(i, carry):
        there = pl.ds(pl.multiple_of(i * strip, strip), strip)
        result[there, :] = (
            resid[there, :] + (own[there, :] + peer[1, there, :].astype(jnp.float32))
        ).astype(jnp.bfloat16)
        return carry

    over_strips(last_strip)
    fetch(0, 0, 0, q_wide).start()
    sends[1].wait_send()
    events(1)
    width = d_proj.shape[2]
    narrow(0, q_wide, 0, done, lambda rows: [(d_proj[0, rows, :], 0), (d_proj[1, rows, :], width)])
    done = done + turns // 4
    sends.append(send_part(0, peer.at[0], 3))
    sends[3].start()
    events(1)
    sends[3].wait_recv()

    def norm_one(i, carry):
        there = pl.ds(pl.multiple_of(i * strip, strip), strip)
        incoming = own[there, :] + peer[0, there, :].astype(jnp.float32)
        values = tokens[there, :].astype(jnp.float32)
        inverse = row_scale(values)
        normed = values * inverse
        scaled = incoming * attn_gain[...]
        change = d_resid[there, :] + inverse * (
            scaled - normed * jnp.mean(scaled * normed, axis=-1, keepdims=True)
        )
        input_grad[there, :] = change.astype(jnp.bfloat16)
        gather_sum(attn_sum, i, jnp.sum(incoming * normed, axis=0, keepdims=True))
        return carry

    over_strips(norm_one)
    dp = 2 * n
    share, head_share = model // dp, 2 * HD // dp
    table[...] = jnp.zeros_like(table)
    for d in range(dp):
        start = d * share // 128 * 128
        row = d * head_share // HD
        table[d, 0:1, :] = attn_sum[:, start : start + 128]
        table[d, 1:2, :] = mlp_sum[:, start : start + 128]
        table[d, 2:3, :] = qk_sum[row : row + 1, :]
    def trade(i, carry):
        partner = ((1 - i) * me + i * mate[0], (1 - i) * twin[1] + i * lane)
        swap = remote(table, others.at[i], trade_sem.at[i, 0], trade_sem.at[i, 1], partner)
        swap.start()
        event(done + i)
        swap.wait()
        table[...] += others[i]
        return carry

    lax.fori_loop(0, 2, trade, 0)
    done = done + 2

    def mail(o, target):
        return remote(table.at[target], inbox.at[o], post_sem.at[o], mail_sem.at[o], at((pos + o) % n, core, n))

    def post(o, carry):
        mail(o, chip_at((pos + o) % n, n) * 2 + core).start()
        return carry

    lax.fori_loop(1, n, post, 0)

    last = count * (n - 1)
    run(done, last)

    def hand_over(m, carry):
        event(last + m)
        finish(m)
        late_begin(m)
        late_event(m)
        return carry

    lax.fori_loop(0, count, hand_over, 0)
    gain_out[...] = table[me]

    def collect(o, carry):
        mail(o, 0).wait_recv()
        gain_out[...] += inbox[o]
        return carry

    lax.fori_loop(1, n, collect, 0)

    def late_rest(e, carry):
        late_event(e)
        return carry

    lax.fori_loop(count, count * n, late_rest, 0)
    for m in range(count):
        late_finish(m)
    sends[2].wait_send()
    sends[3].wait_send()

    def sent(o, carry):
        mail(o, 0).wait_send()
        return carry

    lax.fori_loop(1, n, sent, 0)


def backward_block(
    flipped, act, weights, qkv, attn, cot, tokens, resid, tab, seg_col, seg_row, gains, attn_gain, mlp_gain,
    q_heads, kv_heads, dp,
):
    n = dp // 2
    count, seq, hidden = act.shape
    half, model = resid.shape
    rows = model // dp
    wide = hidden // 2
    width = q_heads * HD
    low, full, dma, vmem, hbm = jnp.bfloat16, jnp.float32, pltpu.SemaphoreType.DMA, pltpu.VMEM, pltpu.HBM
    shape = jax.ShapeDtypeStruct
    place = lambda kind: pl.BlockSpec(memory_space=kind)
    per_group = q_heads // kv_heads
    return pl.pallas_call(
        functools.partial(backward_kernel, n, (q_heads, kv_heads, seq, seq // 2)),
        out_shape=[
            *[shape((rows, hidden), full)] * 3,
            *[shape((rows, width), full)] * 3,
            shape((half, model), low),
            shape((half, model), low),
            shape((8, 128), full),
            shape((model, seq), low),
        ],
        in_specs=[place(k) for k in (hbm, vmem, hbm, hbm, hbm, *[vmem] * 9)],
        out_specs=[place(k) for k in (*[hbm] * 6, vmem, vmem, vmem, hbm)],
        scratch_shapes=[
            vmem((3, seq, width), low),
            vmem((seq, model), low),
            vmem((half, model), full),
            vmem((2, 256, hidden), low),
            vmem((2, model, per_group * HD), low),
            vmem((half, model), full),
            vmem((2, half, model), low),
            vmem((2, half, model), low),
            vmem((seq, per_group * HD), low),
            vmem((per_group + 2, seq, HD), full),
            vmem((3, seq, HD), full),
            vmem((2, 256, seq), low),
            vmem((1, model), full),
            vmem((1, model), full),
            vmem((8, HD), full),
            vmem((dp, 8, 128), full),
            vmem((2, dp, 8, 128), full),
            vmem((n, 8, 128), full),
            dma((4, 2)),
            dma((2,)),
            dma((per_group + 2,)),
            dma((1,)),
            dma((2,)),
            dma((2,)),
            dma((2, 2)),
            dma((n,)),
            dma((n,)),
            dma((2,)),
            vmem((2, 2 * rows, seq), low),
            vmem((count, 2, rows, wide), full),
            vmem((2 * rows, wide), full),
            vmem((count, 2, rows, wide), low),
            vmem((count, 2, 2, rows, wide), low),
            vmem((count, 2, rows, wide), low),
            vmem((count, 2, SLOTS, rows, wide), low),
            dma((count, 2)),
            dma((count, 2, 2)),
            dma((count, 2)),
            dma((count, 2, SLOTS)),
            pltpu.SemaphoreType.REGULAR((count, 2)),
            dma((count, 2)),
        ],
        compiler_params=pltpu.CompilerParams(
            collective_id=2, has_side_effects=True, vmem_limit_bytes=67043328
        ),
    )(
        flipped, act, weights, qkv, attn, cot, tokens, resid, tab, seg_col, seg_row, gains, attn_gain, mlp_gain,
    )


def finishing_kernel(dp, *refs):
    gains = refs[0]
    sources, outs = refs[1:9], refs[9:21]
    bufs, turned, in_sem, out_sem = refs[21:29], refs[29:31], refs[31], refs[32]
    loads = [pltpu.make_async_copy(source, buf, in_sem.at[i]) for i, (source, buf) in enumerate(zip(sources, bufs))]
    for load in loads:
        load.start()
    half = outs[3].shape[1]
    stores = [None] * 9

    def store(i, buf, out):
        stores[i] = pltpu.make_async_copy(buf, out, out_sem.at[i])
        stores[i].start()

    for i, (which, out) in enumerate(((6, 0), (7, 1), (3, 2), (0, 6), (1, 7))):
        loads[which].wait()
        store(i, bufs[which], outs[out])
    loads[4].wait()
    store(5, bufs[4].at[:, pl.ds(0, half)], outs[3])
    store(6, bufs[4].at[:, pl.ds(half, half)], outs[4])
    for i, (which, out) in enumerate(((2, 8), (5, 5))):
        loads[which].wait()
        turned[i][...] = bufs[which][...].T
        store(7 + i, turned[i], outs[out])
    me = lax.axis_index("dp")
    for row in range(3):
        target = outs[9 + row]
        size = target.shape[1]
        line = gains[row : row + 1, :]
        if size % 128:
            line = pltpu.roll(line, (128 - me * size % 128) % 128, 1)
        target[...] = line[:, :size]
    for copy in stores:
        copy.wait()


def finishing_block(gains, arrays, shapes, dp):
    full, dma, vmem, hbm = jnp.float32, pltpu.SemaphoreType.DMA, pltpu.VMEM, pltpu.HBM
    place = lambda kind: pl.BlockSpec(memory_space=kind)
    return pl.pallas_call(
        functools.partial(finishing_kernel, dp),
        out_shape=shapes,
        in_specs=[place(vmem)] + [place(hbm)] * 8,
        out_specs=[place(hbm)] * 9 + [place(vmem)] * 3,
        scratch_shapes=[
            *[vmem(a.shape, a.dtype) for a in arrays],
            vmem(arrays[2].shape[::-1], full),
            vmem(arrays[5].shape[::-1], full),
            dma((8,)),
            dma((9,)),
        ],
        compiler_params=pltpu.CompilerParams(vmem_limit_bytes=67043328),
    )(gains, *arrays)


def on_device(
    tokens,
    seg_ids,
    w_query,
    w_key,
    w_value,
    w_output,
    w_gate,
    w_up,
    w_down,
    gain_attn,
    gain_mlp,
    gain_qk,
    cotangent,
):
    dp = lax.axis_size("dp")
    q_heads = w_query.shape[1] // HD
    kv_heads = w_key.shape[1] // HD
    places = np.arange(HD) % (HD // 2) * 2
    frequency = jnp.asarray((rope_base ** (-places / HD)).astype(np.float32)[None, :])
    (
        weights, projected, attn_rows, resid, flipped, act, attn_gain, mlp_gain, pair, rope_tab, seg_col,
    ) = forward_block(
        (w_query, w_key, w_value, w_output.T, w_gate, w_up, w_down.T),
        tokens,
        cotangent,
        frequency,
        seg_ids,
        [g[None, :] for g in (gain_attn, gain_mlp, gain_qk)],
        q_heads,
        kv_heads,
        dp,
    )
    (
        grad_gate, grad_up, grad_down, grad_query, grad_pair, grad_out, result_rows, input_grad, gain_sums, _,
    ) = backward_block(
        flipped,
        act,
        weights,
        projected,
        attn_rows,
        cotangent,
        tokens,
        resid,
        rope_tab,
        seg_col,
        seg_ids,
        pair,
        attn_gain,
        mlp_gain,
        q_heads,
        kv_heads,
        dp,
    )
    full = jnp.float32
    shapes = [jax.ShapeDtypeStruct(tokens.shape, jnp.bfloat16)] * 2
    shapes += [
        jax.ShapeDtypeStruct(w.shape, full)
        for w in (w_query, w_key, w_value, w_output, w_gate, w_up, w_down)
    ]
    shapes += [jax.ShapeDtypeStruct((1, g.shape[0]), full) for g in (gain_attn, gain_mlp, gain_qk)]
    outs = finishing_block(
        gain_sums,
        [grad_gate, grad_up, grad_down, grad_query, grad_pair, grad_out, result_rows, input_grad],
        shapes,
        dp,
    )
    return (*outs[:9], *(g.reshape(-1) for g in outs[9:]))


def solution(mesh):
    return jax.shard_map(
        on_device,
        mesh=mesh,
        in_specs=(
            P(("dp", "tensor"), None),
            P("dp", None),
            P("dp", "tensor"),
            P("dp", "tensor"),
            P("dp", "tensor"),
            P("tensor", "dp"),
            P("dp", "tensor"),
            P("dp", "tensor"),
            P("tensor", "dp"),
            P("dp"),
            P("dp"),
            P("dp"),
            P(("dp", "tensor"), None),
        ),
        out_specs=(
            P(("dp", "tensor"), None),
            P(("dp", "tensor"), None),
            P("dp", "tensor"),
            P("dp", "tensor"),
            P("dp", "tensor"),
            P("tensor", "dp"),
            P("dp", "tensor"),
            P("dp", "tensor"),
            P("tensor", "dp"),
            P("dp"),
            P("dp"),
            P("dp"),
        ),
        check_vma=False,
    )
```

```python
import functools
import jax
import jax.numpy as jnp
import numpy as np
from jax import lax
from jax.experimental import pallas as pl
from jax.experimental.pallas import tpu as pltpu

from jax.sharding import PartitionSpec as P

MESH = pl.DeviceIdType.MESH
HD = 128
epsilon = 1e-06
rope_base = 1000000.0


def ring_place(n):
    me = lax.axis_index("dp")
    chip = me // 2
    core = me % 2
    odd = chip % 2
    pos = (1 - odd) * (chip // 2) + odd * (n - 1 - chip // 2)
    return pos, core


def chip_at(pos, n):
    high = pos // (n // 2)
    return (1 - high) * (2 * pos) + high * (2 * (n - 1 - pos) + 1)


def at(pos, core, n):
    return (chip_at(pos, n) * 2 + core, lax.axis_index("tensor"))


def meet(peers):
    barrier = pltpu.get_barrier_semaphore()
    for peer in peers:
        pl.semaphore_signal(barrier, inc=1, device_id=peer, device_id_type=MESH)
    pl.semaphore_wait(barrier, len(peers))


def remote(src, dst, send, recv, peer):
    return pltpu.make_async_remote_copy(
        src_ref=src, dst_ref=dst, send_sem=send, recv_sem=recv, device_id=peer, device_id_type=MESH
    )


def product(left, right):
    return jnp.dot(left, right, preferred_element_type=jnp.float32)


def lead_product(left, right):
    return lax.dot_general(
        left, right, (((0,), (0,)), ((), ())), preferred_element_type=jnp.float32
    )


def tail_product(left, right):
    return lax.dot_general(
        left, right, (((1,), (1,)), ((), ())), preferred_element_type=jnp.float32
    )


def turn(values):
    return pltpu.roll(values, values.shape[-1] // 2, 1)


def row_scale(values):
    return lax.rsqrt(jnp.mean(values * values, axis=-1, keepdims=True) + epsilon)


def head_at(index):
    return pl.ds(pl.multiple_of(index * HD, HD), HD)


def prepared(raw, gain, cosine, sine):
    inverse = row_scale(raw)
    hat = raw * inverse
    scaled = hat * gain
    return inverse, hat, (scaled * cosine + turn(scaled) * sine).astype(jnp.bfloat16)


def exp_block(query, keys, seg_col, seg_row, first):
    width = keys.shape[0]
    scores = tail_product(query, keys) * HD ** (-0.5)
    rows = lax.broadcasted_iota(jnp.int32, scores.shape, 0) + first
    columns = lax.broadcasted_iota(jnp.int32, scores.shape, 1)
    allowed = (seg_col[first : first + scores.shape[0], :] == seg_row[:, :width]) & (
        columns <= rows
    )
    return jnp.where(allowed, jnp.exp(scores), 0.0)


def attend_group(group, dims, qkv, tab, seg_col, seg_row, gains, attn, kept):
    q_heads, kv_heads, seq, block = dims
    per_group = q_heads // kv_heads
    cosine, sine = tab[0], tab[1]
    raw = qkv[:, head_at(q_heads + group)]
    kept[0] = prepared(raw, gains[1:2, :], cosine, sine)[2]
    kept[1] = qkv[:, head_at(q_heads + kv_heads + group)].astype(jnp.bfloat16)
    for r in range(per_group):
        head = group * per_group + r
        raw = qkv[:, head_at(head)]
        query = prepared(raw, gains[0:1, :], cosine, sine)[2]
        for first in range(0, seq, block):
            width = first + block
            exps = exp_block(query[first:width], kept[0, :width, :], seg_col, seg_row, first)
            probs = (exps / jnp.sum(exps, axis=-1, keepdims=True)).astype(jnp.bfloat16)
            attn[first:width, head_at(head)] = product(probs, kept[1, :width, :]).astype(jnp.bfloat16)


def block_columns(ref, index, width):
    if width % 128 == 0:
        return ref[:, pl.ds(pl.multiple_of(index * width, width), width)]
    fold = 128 // width
    tile = ref[:, pl.ds(pl.multiple_of((index // fold) * 128, 128), 128)]
    picked = tile[:, :width]
    for i in range(1, fold):
        picked = jnp.where(index % fold == i, tile[:, i * width : (i + 1) * width], picked)
    return picked


HALFWAY = 6
READY = 9


def flip_into(source, target, stage, stage_sem):
    deep = stage.shape[1]
    turns = source.shape[1] // deep

    def put(i):
        return pltpu.make_async_copy(
            stage.at[i % 2], target.at[pl.ds(pl.multiple_of(i * deep, deep), deep)], stage_sem.at[i % 2]
        )

    def one(i, carry):
        @pl.when(i >= 2)
        def _():
            put(i - 2).wait()

        stage[i % 2] = source[:, pl.ds(pl.multiple_of(i * deep, deep), deep)].T
        put(i).start()
        return carry

    lax.fori_loop(0, turns, one, 0)
    put(turns - 2).wait()
    put(turns - 1).wait()


def forward_kernel(n, dims, *refs):
    (
        query_shard, key_shard, value_shard, out_shard, gate_shard, up_shard, down_shard,
        tokens, cot, frequency, seg_row, attn_share, mlp_share, qk_share,
        weights, qkv_out, attn, resid, flipped, act, attn_gain, mlp_gain, gains, tab, seg_col,
        full_rows, cot_full, full_two, out_weight, columns, box, kept, part, peer, acc, blocks, stage,
        own_sem, send_sem, recv_sem, give_sem, take_sem, swap_sem, load_sem, stage_sem, column_sem, tile_sem,
    ) = refs
    q_heads, kv_heads, seq, block = dims
    pos, core = ring_place(n)
    me = lax.axis_index("dp")
    lane = lax.axis_index("tensor")
    nexts = (at((pos + 1) % n, core, n), at((pos + n - 1) % n, core, n))
    mate = at(pos, 1 - core, n)
    twin = (me, 1 - lane)
    ffn_shards = (gate_shard, up_shard, down_shard)
    count = len(ffn_shards)
    rows, width = gate_shard.shape
    wide = width // 2
    q_span, kv_span = query_shard.shape[1], key_shard.shape[1]
    model = 2 * n * rows
    half = seq // 2
    theirs = pl.ds(pl.multiple_of((1 - lane) * half, half), half)
    ours = pl.ds(pl.multiple_of(lane * half, half), half)
    tile = box.at[me]
    tile[...] = jnp.zeros(tile.shape, jnp.float32)
    for i, gain in enumerate((attn_share, mlp_share, qk_share)):
        size = gain.shape[1]
        tile[i : i + 1, 0:size] = gain[...].astype(jnp.float32)
        if size % 128:
            tile[i : i + 1, :] = pltpu.roll(tile[i : i + 1, :], me * size % 128, 1)
    meet((*nexts, mate, twin))

    def owner_of(side, step):
        if side == 0:
            return (pos - step + 2 * n) % n
        return (pos + step) % n

    def small(sub, side):
        start, source = (
            ((0, query_shard), (q_span + 2 * kv_span, out_shard)),
            ((q_span, key_shard), (q_span + kv_span, value_shard)),
        )[sub][side]
        return (sub, 0, pl.ds(start, source.shape[1]), source)

    def large(w, side):
        columns = pl.ds(side * wide, wide)
        source = ffn_shards[w].at[:, columns] if isinstance(w, int) else None
        return (w + 2, (w + 1) * model, columns, source)

    def spot(message, chip, who):
        start = message[1] + (chip * 2 + who) * rows
        return weights.at[pl.ds(pl.multiple_of(start, rows), rows), message[2]]

    def hop(message, side, step):
        k = message[0]
        here = spot(message, chip_at(owner_of(side, step - 1), n), core)
        return remote(here, here, send_sem.at[k, side, step], recv_sem.at[k, side, step], nexts[side])

    def arrived(message, side, step):
        k = message[0]
        here = spot(message, chip_at(owner_of(side, step), n), core)
        return remote(here, here, send_sem.at[k, side, step], recv_sem.at[k, side, step], nexts[side])

    def hand(message, side, step, who):
        k = message[0]
        here = spot(message, chip_at(owner_of(side, step), n), who)
        return remote(here, here, give_sem.at[k, side, step], take_sem.at[k, side, step], mate)

    def begin(message, side):
        k = message[0]
        source = message[3]
        here = spot(message, chip_at(pos, n), core)
        remote(source, here, send_sem.at[k, side, 1], recv_sem.at[k, side, 1], nexts[side]).start()
        remote(source, here, give_sem.at[k, side, 0], take_sem.at[k, side, 0], mate).start()
        pltpu.make_async_copy(source, here, own_sem.at[k, side]).start()

    def keep_own(message, side):
        here = spot(message, chip_at(pos, n), core)
        return pltpu.make_async_copy(here, here, own_sem.at[message[0], side])

    def tile_hop(step, owner):
        place = chip_at(owner, n) * 2 + core
        return remote(box.at[place], box.at[place], tile_sem.at[0, step], tile_sem.at[1, step], nexts[0])

    def tile_hand(step, who):
        place = chip_at(owner_of(0, step), n) * 2 + who
        return remote(box.at[place], box.at[place], tile_sem.at[2, step], tile_sem.at[3, step], mate)

    swaps = [
        remote(source, target.at[ours], swap_sem.at[i, 0], swap_sem.at[i, 1], twin)
        for i, (source, target) in enumerate(((tokens, full_rows), (cot, cot_full)))
    ]
    remote(tile, box.at[me], tile_sem.at[0, 1], tile_sem.at[1, 1], nexts[0]).start()
    remote(tile, box.at[me], tile_sem.at[2, 0], tile_sem.at[3, 0], mate).start()
    for side in range(2):
        begin(small(0, side), side)
    for swap in swaps:
        swap.start()
    full_rows[ours, :] = tokens[...]
    cot_full[ours, :] = cot[...]

    def pass_on(message, side, step):
        arrived(message, side, step).wait_recv()

        @pl.when(step < n - 1)
        def _():
            hop(message, side, step + 1).start()

        hand(message, side, step, core).start()

    def pass_tile(step):
        tile_hop(step, owner_of(0, step)).wait_recv()

        @pl.when(step < n - 1)
        def _():
            tile_hop(step + 1, owner_of(0, step)).start()

        tile_hand(step, core).start()

    def mixed_step(step, carry):
        pass_tile(step)
        for sub in range(2):
            for side in range(2):
                pass_on(small(sub, side), side, step)
        return carry

    def mixed_steps(first, last):
        lax.fori_loop(first, last, mixed_step, 0)

    row = lax.broadcasted_iota(jnp.int32, (seq, seq), 0)
    column = lax.broadcasted_iota(jnp.int32, (seq, seq), 1)
    ids = jnp.broadcast_to(seg_row[...], (seq, seq)).astype(jnp.float32)
    own_id = jnp.sum(jnp.where(row == column, ids, 0.0), axis=1, keepdims=True)
    doc_start = jnp.sum(jnp.where(ids < own_id, 1.0, 0.0), axis=1, keepdims=True)
    place = lax.broadcasted_iota(jnp.int32, (seq, 1), 0).astype(jnp.float32)
    seg_col[...] = own_id.astype(jnp.int32)
    angles = (place - doc_start) * frequency[...]
    tab[0] = jnp.cos(angles)
    sign = jnp.where(lax.broadcasted_iota(jnp.int32, angles.shape, 1) < HD // 2, -1.0, 1.0)
    tab[1] = jnp.sin(angles) * sign
    for side in range(2):
        begin(small(1, side), side)
    mixed_steps(1, n - 1)
    pass_tile(n - 1)
    for side in range(2):
        pass_on(small(0, side), side, n - 1)
    for side in range(2):
        begin(large(0, side), side)
    for side in range(2):
        pass_on(small(1, side), side, n - 1)

    def service(event):
        step, w = event // count + 1, event % count
        for side in range(2):
            pass_on(large(w, side), side, step)

    def services(first, last):
        def one(event, carry):
            service(event)
            return carry

        lax.fori_loop(first, last, one, 0)

    def gathered(step, carry):
        for sub in range(2):
            for side in range(2):
                hand(small(sub, side), side, step, 1 - core).wait_recv()
        tile_hand(step, 1 - core).wait_recv()
        return carry

    lax.fori_loop(0, n, gathered, 0)
    for sub in range(2):
        for side in range(2):
            keep_own(small(sub, side), side).wait()
    q_wide = (q_heads + 2 * kv_heads) * HD
    fetch_out = pltpu.make_async_copy(
        weights.at[pl.ds(0, model), pl.ds(q_wide, width - q_wide)], out_weight, load_sem.at[0, 0]
    )
    turns = q_wide // columns.shape[2]
    deep = columns.shape[2]

    def fetch_columns(i):
        return pltpu.make_async_copy(
            weights.at[pl.ds(0, model), pl.ds(pl.multiple_of(i * deep, deep), deep)],
            columns.at[i % 2], column_sem.at[i % 2],
        )

    fetch_columns(0).start()
    fetch_out.start()
    dp = 2 * n
    share, head_share = model // dp, 2 * HD // dp
    for first, target, per in ((0, attn_gain, share), (1, mlp_gain, share)):
        for s in range(model // 128):
            owners = [d for d in range(dp) if d * per // 128 == s]
            total = box[owners[0], first : first + 1, :]
            for d in owners[1:]:
                total = total + box[d, first : first + 1, :]
            target[:, s * 128 : (s + 1) * 128] = total
    for s in range(2):
        owners = [d for d in range(dp) if d * head_share // HD == s]
        total = box[owners[0], 2:3, :]
        for d in owners[1:]:
            total = total + box[d, 2:3, :]
        gains[s : s + 1, :] = total
    swaps[0].wait_recv()
    strip = 32

    def norm_strip(i, carry):
        there = pl.ds(pl.multiple_of(i * strip, strip), strip)
        values = full_rows[there, :].astype(jnp.float32)
        full_two[there, :] = (values * row_scale(values) * attn_gain[...]).astype(jnp.bfloat16)
        return carry

    lax.fori_loop(0, seq // strip, norm_strip, 0)
    for side in range(2):
        begin(large(1, side), side)
    qkv = acc.at[count - 1]

    def project(i, carry):
        @pl.when(i < turns - 1)
        def _():
            fetch_columns(i + 1).start()

        fetch_columns(i).wait()
        qkv[:, pl.ds(pl.multiple_of(i * deep, deep), deep)] = product(full_two[...], columns[i % 2])
        return carry

    lax.fori_loop(0, turns, project, 0)
    save_qkv = pltpu.make_async_copy(qkv.at[:, pl.ds(0, q_wide)], qkv_out, load_sem.at[0, 1])
    save_qkv.start()
    for side in range(2):
        begin(large(2, side), side)
    service(0)

    def load(job, side):
        step, w = job // count, job % count
        start = (w + 1) * model + chip_at(owner_of(side, step), n) * 2 * rows
        return pltpu.make_async_copy(
            weights.at[pl.ds(pl.multiple_of(start, 2 * rows), 2 * rows), pl.ds(side * wide, wide)],
            blocks.at[job % 2, side], load_sem.at[job % 2, side],
        )

    def prepare(job):
        step, w = job // count, job % count
        for side in range(2):
            hand(large(w, side), side, step, 1 - core).wait_recv()

            @pl.when(step == 0)
            def _():
                keep_own(large(w, side), side).wait()

            load(job, side).start()

    def work(job):
        step, w = job // count, job % count
        for side in range(2):
            load(job, side).wait()
            chip = chip_at(owner_of(side, step), n)

            def with_left(left):
                tile_width = wide // 3

                def one(i, carry):
                    there = pl.ds(pl.multiple_of(side * wide + i * tile_width, tile_width), tile_width)
                    gained = product(
                        left, blocks[job % 2, side, :, pl.ds(pl.multiple_of(i * tile_width, tile_width), tile_width)]
                    )

                    @pl.when(step == 0)
                    def _():
                        acc[w, :, there] = gained

                    @pl.when(step > 0)
                    def _():
                        acc[w, :, there] += gained

                    return carry

                lax.fori_loop(0, 3, one, 0)

            @pl.when(w < count - 1)
            def _():
                with_left(block_columns(full_two, chip, 2 * rows))

            @pl.when(w == count - 1)
            def _():
                with_left(block_columns(cot_full, chip, 2 * rows))

    def flip(source, target):
        flip_into(source, flipped.at[target], stage, stage_sem)

    groups = (qkv, tab, seg_col, seg_row, gains, attn, kept)

    def attend():
        def one(group, carry):
            attend_group(group, dims, *groups)

            @pl.when(group % (kv_heads // 2) == kv_heads // 2 - 1)
            def _():
                service(1 + group // (kv_heads // 2))

            return carry

        lax.fori_loop(0, kv_heads, one, 0)

    flip(full_two, 2)
    attend()
    fetch_out.wait()
    part[...] = tail_product(attn[theirs, :], out_weight[...]).astype(jnp.bfloat16)
    swaps[1].wait_recv()
    send_part = remote(part, peer, swap_sem.at[2, 0], swap_sem.at[2, 1], twin)
    send_part.start()
    resid[...] = tokens[...].astype(jnp.float32) + tail_product(attn[ours, :], out_weight[...])
    services(3, 5)
    flip(cot_full, 1)
    services(5, HALFWAY)
    send_part.wait_recv()
    summed = resid[...] + peer[...].astype(jnp.float32)
    resid[...] = summed
    send_part.wait_send()
    part[...] = (summed * row_scale(summed) * mlp_gain[...]).astype(jnp.bfloat16)
    send_two = remote(part, full_two.at[ours], swap_sem.at[3, 0], swap_sem.at[3, 1], twin)
    send_two.start()
    full_two[ours, :] = part[...]
    ready = READY
    services(HALFWAY, ready)
    remote(part, full_two.at[theirs], swap_sem.at[3, 0], swap_sem.at[3, 1], twin).wait_recv()
    flip(full_two, 0)
    save_qkv.wait()

    jobs, turns_left = count * n, count * (n - 1) - ready
    most = 2 if 2 * (turns_left - 1) >= jobs - 2 else 3

    def done_before(i):
        return jnp.minimum(jnp.minimum(most * i, i + ready + count), jobs - 2)

    def both(i, carry):
        service(ready + i)
        first, last = done_before(i), done_before(i + 1)

        def one(job, carry):
            @pl.when((job == first) & ((i == 0) | (job == i + ready + count)))
            def _():
                prepare(job)

            @pl.when(job + 1 <= i + ready + count)
            def _():
                prepare(job + 1)

            work(job)
            return carry

        lax.fori_loop(first, last, one, 0)
        return carry

    lax.fori_loop(0, turns_left - 1, both, 0)
    full_turn = next(i for i in range(turns_left) if min(most * (i + 1), i + 1 + ready + count) > jobs - 3)
    if jobs - 2 > full_turn + ready + count:
        prepare(jobs - 2)
    work(jobs - 2)

    def partly(i, carry):
        there = pl.ds(pl.multiple_of(i * strip, strip), strip)
        gate = acc[0, there, :]
        up = acc[1, there, :]
        sig = 1.0 / (1.0 + jnp.exp(-gate))
        silu = gate * sig
        acc[0, there, :] = up * sig * (1.0 + gate * (1.0 - sig))
        acc[1, there, :] = silu
        act[2, there, :] = (silu * up).astype(jnp.bfloat16)
        return carry

    lax.fori_loop(0, seq // strip, partly, 0)
    service(count * (n - 1) - 1)
    prepare(jobs - 1)
    work(jobs - 1)

    def complete(i, carry):
        there = pl.ds(pl.multiple_of(i * strip, strip), strip)
        d_act = acc[2, there, :]
        act[0, there, :] = (d_act * acc[0, there, :]).astype(jnp.bfloat16)
        act[1, there, :] = (d_act * acc[1, there, :]).astype(jnp.bfloat16)
        return carry

    lax.fori_loop(0, seq // strip, complete, 0)

    def drain(step, carry):
        for side in range(2):
            for message in [small(sub, side) for sub in range(2)] + [large(w, side) for w in range(count)]:
                hop(message, side, step).wait_send()
                hand(message, side, step, core).wait_send()
        tile_hop(step, owner_of(0, step)).wait_send()
        tile_hand(step, core).wait_send()
        return carry

    lax.fori_loop(1, n, drain, 0)
    for side in range(2):
        for message in [small(sub, side) for sub in range(2)] + [large(w, side) for w in range(count)]:
            hand(message, side, 0, core).wait_send()
    tile_hand(0, core).wait_send()
    for swap in (*swaps, send_two):
        swap.wait_send()


def forward_block(shards, tokens, cot, frequency, seg_row, shares, q_heads, kv_heads, dp):
    n = dp // 2
    rows, width = shards[-1].shape
    count = 3
    half, model = tokens.shape
    seq = 2 * half
    q_wide = (q_heads + 2 * kv_heads) * HD
    low, full, dma, vmem, hbm = jnp.bfloat16, jnp.float32, pltpu.SemaphoreType.DMA, pltpu.VMEM, pltpu.HBM
    shape = jax.ShapeDtypeStruct
    place = lambda kind: pl.BlockSpec(memory_space=kind)
    return pl.pallas_call(
        functools.partial(forward_kernel, n, (q_heads, kv_heads, seq, seq // 2)),
        out_shape=[
            shape(((count + 1) * model, width), low),
            shape((seq, q_wide), full),
            shape((seq, q_heads * HD), low),
            shape((half, model), full),
            shape((3, model, seq), low),
            shape((count, seq, width), low),
            shape((1, model), full),
            shape((1, model), full),
            shape((2, HD), full),
            shape((2, seq, HD), full),
            shape((seq, 1), jnp.int32),
        ],
        in_specs=[place(vmem)] * 14,
        out_specs=[place(k) for k in (hbm, hbm, vmem, vmem, hbm, *[vmem] * 6)],
        scratch_shapes=[
            vmem((seq, model), low),
            vmem((seq, model), low),
            vmem((seq, model), low),
            vmem((model, width - q_wide), low),
            vmem((2, model, 256), low),
            vmem((dp, 8, 128), full),
            vmem((2, seq, HD), low),
            vmem((half, model), low),
            vmem((half, model), low),
            vmem((count, seq, width), full),
            vmem((2, 2, 2 * rows, width // 2), low),
            vmem((2, 256, seq), low),
            dma((count + 2, 2)),
            dma((count + 2, 2, n)),
            dma((count + 2, 2, n)),
            dma((count + 2, 2, n)),
            dma((count + 2, 2, n)),
            dma((4, 2)),
            dma((2, 2)),
            dma((2,)),
            dma((2,)),
            dma((4, n)),
        ],
        compiler_params=pltpu.CompilerParams(
            collective_id=1, has_side_effects=True, vmem_limit_bytes=67043328
        ),
    )(*shards, tokens, cot, frequency, seg_row, *shares)


SLOTS = 3


def undo(incoming, hat, inverse, gain, cosine, sine):
    turned = incoming * cosine - turn(incoming) * sine
    total = jnp.sum(turned * hat, axis=0, keepdims=True)
    scaled = turned * gain
    raw = inverse * (scaled - hat * jnp.mean(scaled * hat, axis=-1, keepdims=True))
    return total, raw.astype(jnp.bfloat16)


def attend_back(group, dims, heads, tab, seg_col, seg_row, gains, d_attn, d_proj, sums, kept):
    q_heads, kv_heads, seq, block = dims
    per_group = q_heads // kv_heads
    low = jnp.bfloat16
    scale = HD ** (-0.5)
    cosine, sine = tab[0], tab[1]
    keys = prepared(heads[per_group], gains[1:2, :], cosine, sine)[2]
    values = heads[per_group + 1].astype(low)
    for r in range(per_group):
        head = group * per_group + r
        q_inverse, q_hat, query = prepared(heads[r], gains[0:1, :], cosine, sine)
        for first in range(0, seq, block):
            width = first + block
            exps = exp_block(query[first:width], keys[:width], seg_col, seg_row, first)
            probs = exps / jnp.sum(exps, axis=-1, keepdims=True)
            incoming = d_attn[first:width, head_at(r)]
            d_probs = tail_product(incoming, values[:width])
            delta = jnp.sum(probs * d_probs, axis=-1, keepdims=True)
            d_scores = (probs * (d_probs - delta)).astype(low)
            kept[0, first:width, :] = product(d_scores, keys[:width]) * scale
            d_keys = lead_product(d_scores, query[first:width])
            d_values = lead_product(probs.astype(low), incoming)
            if r == 0 and first == 0:
                kept[1] = jnp.zeros_like(kept[1])
                kept[2] = jnp.zeros_like(kept[2])
            kept[1, :width, :] += d_keys
            kept[2, :width, :] += d_values
        total, raw = undo(kept[0], q_hat, q_inverse, gains[0:1, :], cosine, sine)
        sums[0:1, :] += total
        d_proj[0, :, head_at(head)] = raw
    k_inverse, k_hat, _ = prepared(heads[per_group], gains[1:2, :], cosine, sine)
    total, raw = undo(kept[1] * scale, k_hat, k_inverse, gains[1:2, :], cosine, sine)
    sums[1:2, :] += total
    d_proj[1, :, head_at(group)] = raw
    d_proj[1, :, head_at(kv_heads + group)] = kept[2].astype(low)


def reducer(n, pos, core, nexts, mate, rights, outs, fetch_left, scratch, stage_of):
    lefts, mine, term, give, take, ship, land, give_sem, take_sem, ship_sem, land_sem, free_sem, out_sem = scratch
    before, sends_before, sends_total = stage_of
    count = rights.shape[0]
    wide = rights.shape[2] // 2
    rows = outs[0].shape[0]
    span = pl.ds(0, wide)

    def owner_of(side, step):
        if side == 0:
            return (pos - 1 - step + 2 * n) % n
        return (pos + 1 + step) % n

    def given(m, side, step):
        slot = (before + step) % 2
        return remote(
            give.at[m, side, :, span], take.at[m, side, slot, :, span],
            give_sem.at[m, side], take_sem.at[m, side, slot], mate,
        )

    def shipped(m, side, step):
        slot = (sends_before + step) % SLOTS
        return remote(
            ship.at[m, side, :, span], land.at[m, side, slot, :, span],
            ship_sem.at[m, side], land_sem.at[m, side, slot], nexts[side],
        )

    def fetch(m, step):
        for side in range(2):
            start = pl.multiple_of(chip_at(owner_of(side, step), n) * 2 * rows, 2 * rows)
            fetch_left(m, side, pl.ds(start, 2 * rows))

    def early(m, step):
        for side in range(2):
            fetch_left(m, side, None)
        for side in range(2):
            tile = min(512, wide)

            def one(i, carry):
                there = pl.multiple_of(i * tile, tile)
                term[:, pl.ds(there, tile)] = product(
                    lefts[side], rights[m, :, pl.ds(pl.multiple_of(side * wide + there, tile), tile)]
                )
                return carry

            lax.fori_loop(0, wide // tile, one, 0)

            @pl.when(step >= 1)
            def _():
                given(m, side, step - 1).wait_send()

            other = term[pl.ds(pl.multiple_of((1 - core) * rows, rows), rows), span]
            give[m, side, :, span] = other.astype(jnp.bfloat16)
            given(m, side, step).start()
            mine[m, side, :, span] = term[pl.ds(pl.multiple_of(core * rows, rows), rows), span]

    def event(e):
        step, m = e // count, e % count

        @pl.when(step < n - 1)
        def _():
            fetch(m, step + 1)

        for side in range(2):
            given(m, side, step).wait_recv()
            near = take[m, side, (before + step) % 2, :, span].astype(jnp.float32)

            @pl.when(step == 0)
            def _():
                mine[m, side, :, span] += near

            @pl.when(step > 0)
            def _():
                shipped(m, side, step - 1).wait_recv()
                far = land[m, side, (sends_before + step - 1) % SLOTS, :, span].astype(jnp.float32)
                mine[m, side, :, span] += near + far

                @pl.when(sends_before + step - 1 + SLOTS < sends_total)
                def _():
                    pl.semaphore_signal(
                        free_sem.at[m, side], inc=1, device_id=nexts[1 - side], device_id_type=MESH
                    )

                shipped(m, side, step - 1).wait_send()

            @pl.when(step < n - 1)
            def _():
                @pl.when(sends_before + step >= SLOTS)
                def _():
                    pl.semaphore_wait(free_sem.at[m, side], 1)

                ship[m, side, :, span] = mine[m, side, :, span].astype(jnp.bfloat16)
                shipped(m, side, step).start()

            @pl.when(step == n - 1)
            def _():
                for i in range(count):
                    @pl.when(m == i)
                    def _():
                        written(m, side, i).start()

        @pl.when(step < n - 1)
        def _():
            early(m, step + 1)

    def written(m, side, i):
        return pltpu.make_async_copy(
            mine.at[m, side, :, span], outs[i].at[:, pl.ds(side * wide, wide)], out_sem.at[m, side]
        )

    def begin(m):
        fetch(m, 0)
        early(m, 0)

    def finish(m):
        for side in range(2):
            given(m, side, n - 1).wait_send()
            written(m, side, 0).wait()

    return begin, event, finish


def backward_kernel(n, dims, *refs):
    (
        flipped, act, weights, qkv, attn, cot, tokens, resid, tab, seg_col, seg_row, gains, attn_gain, mlp_gain,
        grad_gate, grad_up, grad_down, grad_query, grad_pair, grad_out, result, input_grad, gain_out, d_flip,
        d_proj, d_full, d_resid, blocks, columns, own, part, peer, d_attn, heads, kept, stage,
        attn_sum, mlp_sum, qk_sum, table, others, inbox,
        swap_sem, load_sem, head_sem, attn_sem, stage_sem, column_sem, trade_sem, post_sem, mail_sem, left_sem,
        *scratch,
    ) = refs
    q_heads, kv_heads, seq, block = dims
    pos, core = ring_place(n)
    me = lax.axis_index("dp")
    lane = lax.axis_index("tensor")
    nexts = (at((pos + 1) % n, core, n), at((pos + n - 1) % n, core, n))
    mate = at(pos, 1 - core, n)
    twin = (me, 1 - lane)
    fetch_attn = pltpu.make_async_copy(attn, d_proj.at[2], attn_sem.at[0])
    fetch_attn.start()
    barrier = pltpu.get_barrier_semaphore()

    def greet(o, carry):
        pl.semaphore_signal(barrier, inc=1, device_id=at((pos + o) % n, core, n), device_id_type=MESH)
        return carry

    lax.fori_loop(1, n, greet, 0)
    for other in (mate, twin):
        pl.semaphore_signal(barrier, inc=1, device_id=other, device_id_type=MESH)
    pl.semaphore_wait(barrier, n + 1)
    count, _, hidden = act.shape
    half, model = resid.shape
    q_wide = qkv.shape[1]
    per_group = q_heads // kv_heads
    lefts = scratch[0]

    def from_flipped(first):
        def fetch_left(m, side, there):
            if there is None:
                pltpu.make_async_copy(
                    flipped.at[0, pl.ds(0, lefts.shape[1])], lefts.at[side], left_sem.at[side]
                ).wait()
            elif first == 0:
                pltpu.make_async_copy(flipped.at[m // 2, there], lefts.at[side], left_sem.at[side]).start()
            else:
                @pl.when(m < 2)
                def _():
                    pltpu.make_async_copy(flipped.at[2, there], lefts.at[side], left_sem.at[side]).start()

                @pl.when(m == 2)
                def _():
                    pltpu.make_async_copy(d_flip.at[there], lefts.at[side], left_sem.at[side]).start()

        return fetch_left

    links = (n, pos, core, nexts, mate)
    begin, event, finish = reducer(
        *links, act, (grad_gate, grad_up, grad_down), from_flipped(0), scratch, (0, 0, 2 * (n - 1))
    )
    late_begin, late_event, late_finish = reducer(
        *links, d_proj, (grad_query, grad_pair, grad_out), from_flipped(2), scratch, (n, n - 1, 2 * (n - 1))
    )
    deep = blocks.shape[1]
    turns = model // deep

    def fetch(which, i, slot, width):
        start = which * model + i * deep
        return pltpu.make_async_copy(
            weights.at[pl.ds(pl.multiple_of(start, deep), deep), pl.ds(0, width)],
            blocks.at[slot, :, pl.ds(0, width)], load_sem.at[slot],
        )

    def first_m(m, carry):
        begin(m)
        return carry

    lax.fori_loop(0, count, first_m, 0)
    fetch(1, 0, 0, hidden).start()
    fetch(2, 0, 1, hidden).start()
    def run(first, last):
        def one(e, carry):
            event(e)
            return carry

        lax.fori_loop(first, last, one, 0)

    run(0, count)
    theirs = pl.ds(pl.multiple_of((1 - lane) * half, half), half)
    ours = pl.ds(pl.multiple_of(lane * half, half), half)
    done = count

    def events(number):
        nonlocal done
        run(done, done + number)
        done = done + number

    def send_part(slot, target, i):
        return remote(part.at[slot], target, swap_sem.at[i, 0], swap_sem.at[i, 1], twin)

    def dn_two(i, carry):
        there = pl.ds(pl.multiple_of(i * deep, deep), deep)
        for which in range(2):
            fetch(which + 1, i, which, hidden).wait()
            other = tail_product(act[which, theirs, :], blocks[which])
            same = tail_product(act[which, ours, :], blocks[which])
            if which == 0:
                own[:, there] = same
                d_resid[:, there] = other
            else:
                own[:, there] += same
                part[0, :, there] = (d_resid[:, there] + other).astype(jnp.bfloat16)

            @pl.when(i < turns - 1)
            def _():
                fetch(which + 1, i + 1, which, hidden).start()

        @pl.when(i % 4 == 3)
        def _():
            event(count + i // 4)

        return carry

    lax.fori_loop(0, turns, dn_two, 0)
    done = done + turns // 4
    sends = [send_part(0, peer.at[0], 0)]
    sends[0].start()
    fetch(3, 0, 0, hidden).start()
    events(4)
    sends[0].wait_recv()
    sends[0].wait_send()
    strip = 32

    def over_strips(body):
        lax.fori_loop(0, half // strip, body, 0)

    def gather_sum(target, i, total):
        @pl.when(i == 0)
        def _():
            target[...] = total

        @pl.when(i > 0)
        def _():
            target[...] += total

    def norm_two(i, carry):
        there = pl.ds(pl.multiple_of(i * strip, strip), strip)
        incoming = own[there, :] + peer[0, there, :].astype(jnp.float32)
        values = resid[there, :]
        inverse = row_scale(values)
        normed = values * inverse
        scaled = incoming * mlp_gain[...]
        change = cot[there, :].astype(jnp.float32) + inverse * (
            scaled - normed * jnp.mean(scaled * normed, axis=-1, keepdims=True)
        )
        d_resid[there, :] = change
        part[0, there, :] = change.astype(jnp.bfloat16)
        gather_sum(mlp_sum, i, jnp.sum(incoming * normed, axis=0, keepdims=True))
        return carry

    over_strips(norm_two)
    sends.append(send_part(0, d_full.at[ours], 1))
    sends[1].start()
    d_full[ours, :] = part[0]

    def narrow(which, width, slot, base, every, rows_of):
        def one(i, carry):
            @pl.when(i < turns - 1)
            def _():
                fetch(which, i + 1, (i + 1) % 2, width).start()

            fetch(which, i, i % 2, width).wait()
            there = pl.ds(pl.multiple_of(i * deep, deep), deep)
            for rows, mine in ((theirs, False), (ours, True)):
                total = None
                for left, start in rows_of(rows):
                    gained = tail_product(left, blocks[i % 2, :, pl.ds(start, left.shape[1])])
                    total = gained if total is None else total + gained
                if mine:
                    own[:, there] = total
                else:
                    part[slot, :, there] = total.astype(jnp.bfloat16)

            @pl.when(i % every == every - 1)
            def _():
                event(base + i // every)

            return carry

        lax.fori_loop(0, turns, one, 0)

    narrow(3, hidden, 1, done, 4, lambda rows: [(act[2, rows, :], 0)])
    done = done + turns // 4
    sends.append(send_part(1, peer.at[1], 2))
    sends[2].start()
    group_wide = per_group * HD

    def fetch_columns(g):
        return pltpu.make_async_copy(
            weights.at[pl.ds(0, model), pl.ds(pl.multiple_of(q_wide + g * group_wide, group_wide), group_wide)],
            columns.at[g % 2], column_sem.at[g % 2],
        )

    fetch_columns(0).start()
    events(1)
    remote(part.at[0], d_full.at[theirs], swap_sem.at[1, 0], swap_sem.at[1, 1], twin).wait_recv()
    flip_into(d_full, d_flip, stage, stage_sem)
    qk_sum[...] = jnp.zeros_like(qk_sum)
    fetch_attn.wait()

    def group_step(group, carry):
        places = [group * per_group + r for r in range(per_group)]
        places += [q_heads + group, q_heads + kv_heads + group]
        copies = [
            pltpu.make_async_copy(qkv.at[:, head_at(place)], heads.at[i], head_sem.at[i])
            for i, place in enumerate(places)
        ]
        for copy in copies:
            copy.start()

        @pl.when(group < kv_heads - 1)
        def _():
            fetch_columns(group + 1).start()

        fetch_columns(group).wait()
        d_attn[...] = product(d_full[...], columns[group % 2]).astype(jnp.bfloat16)
        for copy in copies:
            copy.wait()
        attend_back(group, dims, heads, tab, seg_col, seg_row, gains, d_attn, d_proj, qk_sum, kept)
        event(done + group)
        return carry

    lax.fori_loop(0, kv_heads, group_step, 0)
    done = done + kv_heads
    sends[2].wait_recv()

    def last_strip(i, carry):
        there = pl.ds(pl.multiple_of(i * strip, strip), strip)
        result[there, :] = (
            resid[there, :] + (own[there, :] + peer[1, there, :].astype(jnp.float32))
        ).astype(jnp.bfloat16)
        return carry

    over_strips(last_strip)
    fetch(0, 0, 0, q_wide).start()
    sends[1].wait_send()
    events(1)
    width = d_proj.shape[2]
    narrow(0, q_wide, 0, done, 8, lambda rows: [(d_proj[0, rows, :], 0), (d_proj[1, rows, :], width)])
    done = done + turns // 8
    sends.append(send_part(0, peer.at[0], 3))
    sends[3].start()
    events(3)
    sends[3].wait_recv()

    def norm_one(i, carry):
        there = pl.ds(pl.multiple_of(i * strip, strip), strip)
        incoming = own[there, :] + peer[0, there, :].astype(jnp.float32)
        values = tokens[there, :].astype(jnp.float32)
        inverse = row_scale(values)
        normed = values * inverse
        scaled = incoming * attn_gain[...]
        change = d_resid[there, :] + inverse * (
            scaled - normed * jnp.mean(scaled * normed, axis=-1, keepdims=True)
        )
        input_grad[there, :] = change.astype(jnp.bfloat16)
        gather_sum(attn_sum, i, jnp.sum(incoming * normed, axis=0, keepdims=True))
        return carry

    over_strips(norm_one)
    dp = 2 * n
    share, head_share = model // dp, 2 * HD // dp
    table[...] = jnp.zeros_like(table)
    for d in range(dp):
        start = d * share // 128 * 128
        row = d * head_share // HD
        table[d, 0:1, :] = attn_sum[:, start : start + 128]
        table[d, 1:2, :] = mlp_sum[:, start : start + 128]
        table[d, 2:3, :] = qk_sum[row : row + 1, :]
    def trade(i, carry):
        partner = ((1 - i) * me + i * mate[0], (1 - i) * twin[1] + i * lane)
        swap = remote(table, others.at[i], trade_sem.at[i, 0], trade_sem.at[i, 1], partner)
        swap.start()
        swap.wait()
        table[...] += others[i]
        return carry

    lax.fori_loop(0, 2, trade, 0)

    def mail(o, target):
        return remote(table.at[target], inbox.at[o], post_sem.at[o], mail_sem.at[o], at((pos + o) % n, core, n))

    def post(o, carry):
        mail(o, chip_at((pos + o) % n, n) * 2 + core).start()
        return carry

    lax.fori_loop(1, n, post, 0)

    last = count * (n - 1)
    run(done, last)

    def hand_over(m, carry):
        event(last + m)
        finish(m)
        late_begin(m)
        late_event(m)
        return carry

    lax.fori_loop(0, count, hand_over, 0)
    gain_out[...] = table[me]

    def collect(o, carry):
        mail(o, 0).wait_recv()
        gain_out[...] += inbox[o]
        return carry

    lax.fori_loop(1, n, collect, 0)

    def late_rest(e, carry):
        late_event(e)
        return carry

    lax.fori_loop(count, count * n, late_rest, 0)
    for m in range(count):
        late_finish(m)
    sends[2].wait_send()
    sends[3].wait_send()

    def sent(o, carry):
        mail(o, 0).wait_send()
        return carry

    lax.fori_loop(1, n, sent, 0)


def backward_block(
    flipped, act, weights, qkv, attn, cot, tokens, resid, tab, seg_col, seg_row, gains, attn_gain, mlp_gain,
    q_heads, kv_heads, dp,
):
    n = dp // 2
    count, seq, hidden = act.shape
    half, model = resid.shape
    rows = model // dp
    wide = hidden // 2
    width = q_heads * HD
    low, full, dma, vmem, hbm = jnp.bfloat16, jnp.float32, pltpu.SemaphoreType.DMA, pltpu.VMEM, pltpu.HBM
    shape = jax.ShapeDtypeStruct
    place = lambda kind: pl.BlockSpec(memory_space=kind)
    per_group = q_heads // kv_heads
    return pl.pallas_call(
        functools.partial(backward_kernel, n, (q_heads, kv_heads, seq, seq // 2)),
        out_shape=[
            *[shape((rows, hidden), full)] * 3,
            *[shape((rows, width), full)] * 3,
            shape((half, model), low),
            shape((half, model), low),
            shape((8, 128), full),
            shape((model, seq), low),
        ],
        in_specs=[place(k) for k in (hbm, vmem, hbm, hbm, hbm, *[vmem] * 9)],
        out_specs=[place(k) for k in (*[hbm] * 6, vmem, vmem, vmem, hbm)],
        scratch_shapes=[
            vmem((3, seq, width), low),
            vmem((seq, model), low),
            vmem((half, model), full),
            vmem((2, 256, hidden), low),
            vmem((2, model, per_group * HD), low),
            vmem((half, model), full),
            vmem((2, half, model), low),
            vmem((2, half, model), low),
            vmem((seq, per_group * HD), low),
            vmem((per_group + 2, seq, HD), full),
            vmem((3, seq, HD), full),
            vmem((2, 256, seq), low),
            vmem((1, model), full),
            vmem((1, model), full),
            vmem((8, HD), full),
            vmem((dp, 8, 128), full),
            vmem((2, dp, 8, 128), full),
            vmem((n, 8, 128), full),
            dma((4, 2)),
            dma((2,)),
            dma((per_group + 2,)),
            dma((1,)),
            dma((2,)),
            dma((2,)),
            dma((2, 2)),
            dma((n,)),
            dma((n,)),
            dma((2,)),
            vmem((2, 2 * rows, seq), low),
            vmem((count, 2, rows, wide), full),
            vmem((2 * rows, wide), full),
            vmem((count, 2, rows, wide), low),
            vmem((count, 2, 2, rows, wide), low),
            vmem((count, 2, rows, wide), low),
            vmem((count, 2, SLOTS, rows, wide), low),
            dma((count, 2)),
            dma((count, 2, 2)),
            dma((count, 2)),
            dma((count, 2, SLOTS)),
            pltpu.SemaphoreType.REGULAR((count, 2)),
            dma((count, 2)),
        ],
        compiler_params=pltpu.CompilerParams(
            collective_id=2, has_side_effects=True, vmem_limit_bytes=67043328
        ),
    )(
        flipped, act, weights, qkv, attn, cot, tokens, resid, tab, seg_col, seg_row, gains, attn_gain, mlp_gain,
    )


def finishing_kernel(dp, *refs):
    gains = refs[0]
    sources, outs = refs[1:9], refs[9:21]
    bufs, turned, in_sem, out_sem = refs[21:29], refs[29:31], refs[31], refs[32]
    loads = [pltpu.make_async_copy(source, buf, in_sem.at[i]) for i, (source, buf) in enumerate(zip(sources, bufs))]
    for load in loads:
        load.start()
    half = outs[3].shape[1]
    stores = [None] * 9

    def store(i, buf, out):
        stores[i] = pltpu.make_async_copy(buf, out, out_sem.at[i])
        stores[i].start()

    for i, (which, out) in enumerate(((6, 0), (7, 1), (3, 2), (0, 6), (1, 7))):
        loads[which].wait()
        store(i, bufs[which], outs[out])
    loads[4].wait()
    store(5, bufs[4].at[:, pl.ds(0, half)], outs[3])
    store(6, bufs[4].at[:, pl.ds(half, half)], outs[4])
    for i, (which, out) in enumerate(((2, 8), (5, 5))):
        loads[which].wait()
        turned[i][...] = bufs[which][...].T
        store(7 + i, turned[i], outs[out])
    me = lax.axis_index("dp")
    for row in range(3):
        target = outs[9 + row]
        size = target.shape[1]
        line = gains[row : row + 1, :]
        if size % 128:
            line = pltpu.roll(line, (128 - me * size % 128) % 128, 1)
        target[...] = line[:, :size]
    for copy in stores:
        copy.wait()


def finishing_block(gains, arrays, shapes, dp):
    full, dma, vmem, hbm = jnp.float32, pltpu.SemaphoreType.DMA, pltpu.VMEM, pltpu.HBM
    place = lambda kind: pl.BlockSpec(memory_space=kind)
    return pl.pallas_call(
        functools.partial(finishing_kernel, dp),
        out_shape=shapes,
        in_specs=[place(vmem)] + [place(hbm)] * 8,
        out_specs=[place(hbm)] * 9 + [place(vmem)] * 3,
        scratch_shapes=[
            *[vmem(a.shape, a.dtype) for a in arrays],
            vmem(arrays[2].shape[::-1], full),
            vmem(arrays[5].shape[::-1], full),
            dma((8,)),
            dma((9,)),
        ],
        compiler_params=pltpu.CompilerParams(vmem_limit_bytes=67043328),
    )(gains, *arrays)


def on_device(
    tokens,
    seg_ids,
    w_query,
    w_key,
    w_value,
    w_output,
    w_gate,
    w_up,
    w_down,
    gain_attn,
    gain_mlp,
    gain_qk,
    cotangent,
):
    dp = lax.axis_size("dp")
    q_heads = w_query.shape[1] // HD
    kv_heads = w_key.shape[1] // HD
    places = np.arange(HD) % (HD // 2) * 2
    frequency = jnp.asarray((rope_base ** (-places / HD)).astype(np.float32)[None, :])
    (
        weights, projected, attn_rows, resid, flipped, act, attn_gain, mlp_gain, pair, rope_tab, seg_col,
    ) = forward_block(
        (w_query, w_key, w_value, w_output.T, w_gate, w_up, w_down.T),
        tokens,
        cotangent,
        frequency,
        seg_ids,
        [g[None, :] for g in (gain_attn, gain_mlp, gain_qk)],
        q_heads,
        kv_heads,
        dp,
    )
    (
        grad_gate, grad_up, grad_down, grad_query, grad_pair, grad_out, result_rows, input_grad, gain_sums, _,
    ) = backward_block(
        flipped,
        act,
        weights,
        projected,
        attn_rows,
        cotangent,
        tokens,
        resid,
        rope_tab,
        seg_col,
        seg_ids,
        pair,
        attn_gain,
        mlp_gain,
        q_heads,
        kv_heads,
        dp,
    )
    full = jnp.float32
    shapes = [jax.ShapeDtypeStruct(tokens.shape, jnp.bfloat16)] * 2
    shapes += [
        jax.ShapeDtypeStruct(w.shape, full)
        for w in (w_query, w_key, w_value, w_output, w_gate, w_up, w_down)
    ]
    shapes += [jax.ShapeDtypeStruct((1, g.shape[0]), full) for g in (gain_attn, gain_mlp, gain_qk)]
    outs = finishing_block(
        gain_sums,
        [grad_gate, grad_up, grad_down, grad_query, grad_pair, grad_out, result_rows, input_grad],
        shapes,
        dp,
    )
    return (*outs[:9], *(g.reshape(-1) for g in outs[9:]))


def solution(mesh):
    return jax.shard_map(
        on_device,
        mesh=mesh,
        in_specs=(
            P(("dp", "tensor"), None),
            P("dp", None),
            P("dp", "tensor"),
            P("dp", "tensor"),
            P("dp", "tensor"),
            P("tensor", "dp"),
            P("dp", "tensor"),
            P("dp", "tensor"),
            P("tensor", "dp"),
            P("dp"),
            P("dp"),
            P("dp"),
            P(("dp", "tensor"), None),
        ),
        out_specs=(
            P(("dp", "tensor"), None),
            P(("dp", "tensor"), None),
            P("dp", "tensor"),
            P("dp", "tensor"),
            P("dp", "tensor"),
            P("tensor", "dp"),
            P("dp", "tensor"),
            P("dp", "tensor"),
            P("tensor", "dp"),
            P("dp"),
            P("dp"),
            P("dp"),
        ),
        check_vma=False,
    )
```

```python
import functools
import jax
import jax.numpy as jnp
import numpy as np
from jax import lax
from jax.experimental import pallas as pl
from jax.experimental.pallas import tpu as pltpu

from jax.sharding import PartitionSpec as P

MESH = pl.DeviceIdType.MESH
HD = 128
epsilon = 1e-06
rope_base = 1000000.0


def ring_place(n):
    me = lax.axis_index("dp")
    chip = me // 2
    core = me % 2
    odd = chip % 2
    pos = (1 - odd) * (chip // 2) + odd * (n - 1 - chip // 2)
    return pos, core


def chip_at(pos, n):
    high = pos // (n // 2)
    return (1 - high) * (2 * pos) + high * (2 * (n - 1 - pos) + 1)


def at(pos, core, n):
    return (chip_at(pos, n) * 2 + core, lax.axis_index("tensor"))


def meet(peers):
    barrier = pltpu.get_barrier_semaphore()
    for peer in peers:
        pl.semaphore_signal(barrier, inc=1, device_id=peer, device_id_type=MESH)
    pl.semaphore_wait(barrier, len(peers))


def remote(src, dst, send, recv, peer):
    return pltpu.make_async_remote_copy(
        src_ref=src, dst_ref=dst, send_sem=send, recv_sem=recv, device_id=peer, device_id_type=MESH
    )


def product(left, right):
    return jnp.dot(left, right, preferred_element_type=jnp.float32)


def lead_product(left, right):
    return lax.dot_general(
        left, right, (((0,), (0,)), ((), ())), preferred_element_type=jnp.float32
    )


def tail_product(left, right):
    return lax.dot_general(
        left, right, (((1,), (1,)), ((), ())), preferred_element_type=jnp.float32
    )


def turn(values):
    return pltpu.roll(values, values.shape[-1] // 2, 1)


def row_scale(values):
    return lax.rsqrt(jnp.mean(values * values, axis=-1, keepdims=True) + epsilon)


def head_at(index):
    return pl.ds(pl.multiple_of(index * HD, HD), HD)


def prepared(raw, gain, cosine, sine):
    inverse = row_scale(raw)
    hat = raw * inverse
    scaled = hat * gain
    return inverse, hat, (scaled * cosine + turn(scaled) * sine).astype(jnp.bfloat16)


def exp_block(query, keys, seg_col, seg_row, first):
    width = keys.shape[0]
    scores = tail_product(query, keys) * HD ** (-0.5)
    rows = lax.broadcasted_iota(jnp.int32, scores.shape, 0) + first
    columns = lax.broadcasted_iota(jnp.int32, scores.shape, 1)
    allowed = (seg_col[first : first + scores.shape[0], :] == seg_row[:, :width]) & (
        columns <= rows
    )
    return jnp.where(allowed, jnp.exp(scores), 0.0)


def attend_group(group, dims, qkv, tab, seg_col, seg_row, gains, attn, kept):
    q_heads, kv_heads, seq, block = dims
    per_group = q_heads // kv_heads
    cosine, sine = tab[0], tab[1]
    raw = qkv[:, head_at(q_heads + group)]
    kept[0] = prepared(raw, gains[1:2, :], cosine, sine)[2]
    kept[1] = qkv[:, head_at(q_heads + kv_heads + group)].astype(jnp.bfloat16)
    for r in range(per_group):
        head = group * per_group + r
        raw = qkv[:, head_at(head)]
        query = prepared(raw, gains[0:1, :], cosine, sine)[2]
        for first in range(0, seq, block):
            width = first + block
            exps = exp_block(query[first:width], kept[0, :width, :], seg_col, seg_row, first)
            probs = (exps / jnp.sum(exps, axis=-1, keepdims=True)).astype(jnp.bfloat16)
            attn[first:width, head_at(head)] = product(probs, kept[1, :width, :]).astype(jnp.bfloat16)


def block_columns(ref, index, width):
    if width % 128 == 0:
        return ref[:, pl.ds(pl.multiple_of(index * width, width), width)]
    fold = 128 // width
    tile = ref[:, pl.ds(pl.multiple_of((index // fold) * 128, 128), 128)]
    picked = tile[:, :width]
    for i in range(1, fold):
        picked = jnp.where(index % fold == i, tile[:, i * width : (i + 1) * width], picked)
    return picked


HALFWAY = 6
READY = 9


def flip_into(source, target, stage, stage_sem):
    deep = stage.shape[1]
    turns = source.shape[1] // deep

    def put(i):
        return pltpu.make_async_copy(
            stage.at[i % 2], target.at[pl.ds(pl.multiple_of(i * deep, deep), deep)], stage_sem.at[i % 2]
        )

    def one(i, carry):
        @pl.when(i >= 2)
        def _():
            put(i - 2).wait()

        stage[i % 2] = source[:, pl.ds(pl.multiple_of(i * deep, deep), deep)].T
        put(i).start()
        return carry

    lax.fori_loop(0, turns, one, 0)
    put(turns - 2).wait()
    put(turns - 1).wait()


def forward_kernel(n, dims, *refs):
    (
        query_shard, key_shard, value_shard, out_shard, gate_shard, up_shard, down_given,
        tokens, cot, frequency, seg_row, attn_share, mlp_share, qk_share,
        weights, qkv_out, attn, resid, flipped, act, attn_gain, mlp_gain, gains, tab, seg_col,
        full_rows, cot_full, full_two, out_weight, columns, box, kept, part, peer, acc, blocks, stage,
        own_sem, send_sem, recv_sem, give_sem, take_sem, swap_sem, load_sem, stage_sem, column_sem, tile_sem, down_shard,
    ) = refs
    q_heads, kv_heads, seq, block = dims
    pos, core = ring_place(n)
    me = lax.axis_index("dp")
    lane = lax.axis_index("tensor")
    nexts = (at((pos + 1) % n, core, n), at((pos + n - 1) % n, core, n))
    mate = at(pos, 1 - core, n)
    twin = (me, 1 - lane)
    ffn_shards = (gate_shard, up_shard, down_shard)
    count = len(ffn_shards)
    rows, width = gate_shard.shape
    wide = width // 2
    q_span, kv_span = query_shard.shape[1], key_shard.shape[1]
    model = 2 * n * rows
    half = seq // 2
    theirs = pl.ds(pl.multiple_of((1 - lane) * half, half), half)
    ours = pl.ds(pl.multiple_of(lane * half, half), half)
    tile = box.at[me]
    tile[...] = jnp.zeros(tile.shape, jnp.float32)
    for i, gain in enumerate((attn_share, mlp_share, qk_share)):
        size = gain.shape[1]
        tile[i : i + 1, 0:size] = gain[...].astype(jnp.float32)
        if size % 128:
            tile[i : i + 1, :] = pltpu.roll(tile[i : i + 1, :], me * size % 128, 1)
    meet((*nexts, mate, twin))

    def owner_of(side, step):
        if side == 0:
            return (pos - step + 2 * n) % n
        return (pos + step) % n

    def small(sub, side):
        start, source = (
            ((0, query_shard), (q_span + 2 * kv_span, out_shard)),
            ((q_span, key_shard), (q_span + kv_span, value_shard)),
        )[sub][side]
        return (sub, 0, pl.ds(start, source.shape[1]), source)

    def large(w, side):
        columns = pl.ds(side * wide, wide)
        source = ffn_shards[w].at[:, columns] if isinstance(w, int) else None
        return (w + 2, (w + 1) * model, columns, source)

    def spot(message, chip, who):
        start = message[1] + (chip * 2 + who) * rows
        return weights.at[pl.ds(pl.multiple_of(start, rows), rows), message[2]]

    def hop(message, side, step):
        k = message[0]
        here = spot(message, chip_at(owner_of(side, step - 1), n), core)
        return remote(here, here, send_sem.at[k, side, step], recv_sem.at[k, side, step], nexts[side])

    def arrived(message, side, step):
        k = message[0]
        here = spot(message, chip_at(owner_of(side, step), n), core)
        return remote(here, here, send_sem.at[k, side, step], recv_sem.at[k, side, step], nexts[side])

    def hand(message, side, step, who):
        k = message[0]
        here = spot(message, chip_at(owner_of(side, step), n), who)
        return remote(here, here, give_sem.at[k, side, step], take_sem.at[k, side, step], mate)

    def begin(message, side):
        k = message[0]
        source = message[3]
        here = spot(message, chip_at(pos, n), core)
        remote(source, here, send_sem.at[k, side, 1], recv_sem.at[k, side, 1], nexts[side]).start()
        remote(source, here, give_sem.at[k, side, 0], take_sem.at[k, side, 0], mate).start()
        pltpu.make_async_copy(source, here, own_sem.at[k, side]).start()

    def keep_own(message, side):
        here = spot(message, chip_at(pos, n), core)
        return pltpu.make_async_copy(here, here, own_sem.at[message[0], side])

    def tile_hop(step, owner):
        place = chip_at(owner, n) * 2 + core
        return remote(box.at[place], box.at[place], tile_sem.at[0, step], tile_sem.at[1, step], nexts[0])

    def tile_hand(step, who):
        place = chip_at(owner_of(0, step), n) * 2 + who
        return remote(box.at[place], box.at[place], tile_sem.at[2, step], tile_sem.at[3, step], mate)

    swaps = [
        remote(source, target.at[ours], swap_sem.at[i, 0], swap_sem.at[i, 1], twin)
        for i, (source, target) in enumerate(((tokens, full_rows), (cot, cot_full)))
    ]
    remote(tile, box.at[me], tile_sem.at[0, 1], tile_sem.at[1, 1], nexts[0]).start()
    remote(tile, box.at[me], tile_sem.at[2, 0], tile_sem.at[3, 0], mate).start()
    for side in range(2):
        begin(small(0, side), side)
    for swap in swaps:
        swap.start()
    full_rows[ours, :] = tokens[...]
    cot_full[ours, :] = cot[...]

    def pass_on(message, side, step):
        arrived(message, side, step).wait_recv()

        @pl.when(step < n - 1)
        def _():
            hop(message, side, step + 1).start()

        hand(message, side, step, core).start()

    def pass_tile(step):
        tile_hop(step, owner_of(0, step)).wait_recv()

        @pl.when(step < n - 1)
        def _():
            tile_hop(step + 1, owner_of(0, step)).start()

        tile_hand(step, core).start()

    def mixed_step(step, carry):
        pass_tile(step)
        for sub in range(2):
            for side in range(2):
                pass_on(small(sub, side), side, step)
        return carry

    def mixed_steps(first, last):
        lax.fori_loop(first, last, mixed_step, 0)

    row = lax.broadcasted_iota(jnp.int32, (seq, seq), 0)
    column = lax.broadcasted_iota(jnp.int32, (seq, seq), 1)
    ids = jnp.broadcast_to(seg_row[...], (seq, seq)).astype(jnp.float32)
    own_id = jnp.sum(jnp.where(row == column, ids, 0.0), axis=1, keepdims=True)
    doc_start = jnp.sum(jnp.where(ids < own_id, 1.0, 0.0), axis=1, keepdims=True)
    place = lax.broadcasted_iota(jnp.int32, (seq, 1), 0).astype(jnp.float32)
    seg_col[...] = own_id.astype(jnp.int32)
    for i in range(0, width, 512):
        down_shard[:, i : i + 512] = down_given[i : i + 512, :].T
    angles = (place - doc_start) * frequency[...]
    tab[0] = jnp.cos(angles)
    sign = jnp.where(lax.broadcasted_iota(jnp.int32, angles.shape, 1) < HD // 2, -1.0, 1.0)
    tab[1] = jnp.sin(angles) * sign
    for side in range(2):
        begin(small(1, side), side)
    mixed_steps(1, n - 1)
    pass_tile(n - 1)
    for side in range(2):
        pass_on(small(0, side), side, n - 1)
    for side in range(2):
        begin(large(0, side), side)
    for side in range(2):
        pass_on(small(1, side), side, n - 1)

    def service(event):
        step, w = event // count + 1, event % count
        for side in range(2):
            pass_on(large(w, side), side, step)

    def services(first, last):
        def one(event, carry):
            service(event)
            return carry

        lax.fori_loop(first, last, one, 0)

    def gathered(step, carry):
        for sub in range(2):
            for side in range(2):
                hand(small(sub, side), side, step, 1 - core).wait_recv()
        tile_hand(step, 1 - core).wait_recv()
        return carry

    lax.fori_loop(0, n, gathered, 0)
    for sub in range(2):
        for side in range(2):
            keep_own(small(sub, side), side).wait()
    q_wide = (q_heads + 2 * kv_heads) * HD
    fetch_out = pltpu.make_async_copy(
        weights.at[pl.ds(0, model), pl.ds(q_wide, width - q_wide)], out_weight, load_sem.at[0, 0]
    )
    turns = q_wide // columns.shape[2]
    deep = columns.shape[2]

    def fetch_columns(i):
        return pltpu.make_async_copy(
            weights.at[pl.ds(0, model), pl.ds(pl.multiple_of(i * deep, deep), deep)],
            columns.at[i % 2], column_sem.at[i % 2],
        )

    fetch_columns(0).start()
    fetch_out.start()
    dp = 2 * n
    share, head_share = model // dp, 2 * HD // dp
    for first, target, per in ((0, attn_gain, share), (1, mlp_gain, share)):
        for s in range(model // 128):
            owners = [d for d in range(dp) if d * per // 128 == s]
            total = box[owners[0], first : first + 1, :]
            for d in owners[1:]:
                total = total + box[d, first : first + 1, :]
            target[:, s * 128 : (s + 1) * 128] = total
    for s in range(2):
        owners = [d for d in range(dp) if d * head_share // HD == s]
        total = box[owners[0], 2:3, :]
        for d in owners[1:]:
            total = total + box[d, 2:3, :]
        gains[s : s + 1, :] = total
    swaps[0].wait_recv()
    strip = 32

    def norm_strip(i, carry):
        there = pl.ds(pl.multiple_of(i * strip, strip), strip)
        values = full_rows[there, :].astype(jnp.float32)
        full_two[there, :] = (values * row_scale(values) * attn_gain[...]).astype(jnp.bfloat16)
        return carry

    lax.fori_loop(0, seq // strip, norm_strip, 0)
    for side in range(2):
        begin(large(1, side), side)
    qkv = acc.at[count - 1]

    def project(i, carry):
        @pl.when(i < turns - 1)
        def _():
            fetch_columns(i + 1).start()

        fetch_columns(i).wait()
        qkv[:, pl.ds(pl.multiple_of(i * deep, deep), deep)] = product(full_two[...], columns[i % 2])
        return carry

    lax.fori_loop(0, turns, project, 0)
    save_qkv = pltpu.make_async_copy(qkv.at[:, pl.ds(0, q_wide)], qkv_out, load_sem.at[0, 1])
    save_qkv.start()
    for side in range(2):
        begin(large(2, side), side)
    service(0)

    def load(job, side):
        step, w = job // count, job % count
        start = (w + 1) * model + chip_at(owner_of(side, step), n) * 2 * rows
        return pltpu.make_async_copy(
            weights.at[pl.ds(pl.multiple_of(start, 2 * rows), 2 * rows), pl.ds(side * wide, wide)],
            blocks.at[job % 2, side], load_sem.at[job % 2, side],
        )

    def prepare(job):
        step, w = job // count, job % count
        for side in range(2):
            hand(large(w, side), side, step, 1 - core).wait_recv()

            @pl.when(step == 0)
            def _():
                keep_own(large(w, side), side).wait()

            load(job, side).start()

    def work(job):
        step, w = job // count, job % count
        for side in range(2):
            load(job, side).wait()
            chip = chip_at(owner_of(side, step), n)

            def with_left(left):
                tile_width = wide // 3

                def one(i, carry):
                    there = pl.ds(pl.multiple_of(side * wide + i * tile_width, tile_width), tile_width)
                    gained = product(
                        left, blocks[job % 2, side, :, pl.ds(pl.multiple_of(i * tile_width, tile_width), tile_width)]
                    )

                    @pl.when(step == 0)
                    def _():
                        acc[w, :, there] = gained

                    @pl.when(step > 0)
                    def _():
                        acc[w, :, there] += gained

                    return carry

                lax.fori_loop(0, 3, one, 0)

            @pl.when(w < count - 1)
            def _():
                with_left(block_columns(full_two, chip, 2 * rows))

            @pl.when(w == count - 1)
            def _():
                with_left(block_columns(cot_full, chip, 2 * rows))

    def flip(source, target):
        flip_into(source, flipped.at[target], stage, stage_sem)

    groups = (qkv, tab, seg_col, seg_row, gains, attn, kept)

    def attend():
        def one(group, carry):
            attend_group(group, dims, *groups)

            @pl.when(group % (kv_heads // 2) == kv_heads // 2 - 1)
            def _():
                service(1 + group // (kv_heads // 2))

            return carry

        lax.fori_loop(0, kv_heads, one, 0)

    flip(full_two, 2)
    attend()
    fetch_out.wait()
    part[...] = tail_product(attn[theirs, :], out_weight[...]).astype(jnp.bfloat16)
    swaps[1].wait_recv()
    send_part = remote(part, peer, swap_sem.at[2, 0], swap_sem.at[2, 1], twin)
    send_part.start()
    resid[...] = tokens[...].astype(jnp.float32) + tail_product(attn[ours, :], out_weight[...])
    services(3, 5)
    flip(cot_full, 1)
    services(5, HALFWAY)
    send_part.wait_recv()
    summed = resid[...] + peer[...].astype(jnp.float32)
    resid[...] = summed
    send_part.wait_send()
    part[...] = (summed * row_scale(summed) * mlp_gain[...]).astype(jnp.bfloat16)
    send_two = remote(part, full_two.at[ours], swap_sem.at[3, 0], swap_sem.at[3, 1], twin)
    send_two.start()
    full_two[ours, :] = part[...]
    ready = READY
    services(HALFWAY, ready)
    remote(part, full_two.at[theirs], swap_sem.at[3, 0], swap_sem.at[3, 1], twin).wait_recv()
    flip(full_two, 0)
    save_qkv.wait()

    jobs, turns_left = count * n, count * (n - 1) - ready
    most = 2 if 2 * (turns_left - 1) >= jobs - 2 else 3

    def done_before(i):
        return jnp.minimum(jnp.minimum(most * i, i + ready + count), jobs - 2)

    def both(i, carry):
        service(ready + i)
        first, last = done_before(i), done_before(i + 1)

        def one(job, carry):
            @pl.when((job == first) & ((i == 0) | (job == i + ready + count)))
            def _():
                prepare(job)

            @pl.when(job + 1 <= i + ready + count)
            def _():
                prepare(job + 1)

            work(job)
            return carry

        lax.fori_loop(first, last, one, 0)
        return carry

    lax.fori_loop(0, turns_left - 1, both, 0)
    full_turn = next(i for i in range(turns_left) if min(most * (i + 1), i + 1 + ready + count) > jobs - 3)
    if jobs - 2 > full_turn + ready + count:
        prepare(jobs - 2)
    work(jobs - 2)

    def partly(i, carry):
        there = pl.ds(pl.multiple_of(i * strip, strip), strip)
        gate = acc[0, there, :]
        up = acc[1, there, :]
        sig = 1.0 / (1.0 + jnp.exp(-gate))
        silu = gate * sig
        acc[0, there, :] = up * sig * (1.0 + gate * (1.0 - sig))
        acc[1, there, :] = silu
        act[2, there, :] = (silu * up).astype(jnp.bfloat16)
        return carry

    lax.fori_loop(0, seq // strip, partly, 0)
    service(count * (n - 1) - 1)
    prepare(jobs - 1)
    work(jobs - 1)

    def complete(i, carry):
        there = pl.ds(pl.multiple_of(i * strip, strip), strip)
        d_act = acc[2, there, :]
        act[0, there, :] = (d_act * acc[0, there, :]).astype(jnp.bfloat16)
        act[1, there, :] = (d_act * acc[1, there, :]).astype(jnp.bfloat16)
        return carry

    lax.fori_loop(0, seq // strip, complete, 0)

    def drain(step, carry):
        for side in range(2):
            for message in [small(sub, side) for sub in range(2)] + [large(w, side) for w in range(count)]:
                hop(message, side, step).wait_send()
                hand(message, side, step, core).wait_send()
        tile_hop(step, owner_of(0, step)).wait_send()
        tile_hand(step, core).wait_send()
        return carry

    lax.fori_loop(1, n, drain, 0)
    for side in range(2):
        for message in [small(sub, side) for sub in range(2)] + [large(w, side) for w in range(count)]:
            hand(message, side, 0, core).wait_send()
    tile_hand(0, core).wait_send()
    for swap in (*swaps, send_two):
        swap.wait_send()


def forward_block(shards, tokens, cot, frequency, seg_row, shares, q_heads, kv_heads, dp):
    n = dp // 2
    rows, width = shards[-2].shape
    count = 3
    half, model = tokens.shape
    seq = 2 * half
    q_wide = (q_heads + 2 * kv_heads) * HD
    low, full, dma, vmem, hbm = jnp.bfloat16, jnp.float32, pltpu.SemaphoreType.DMA, pltpu.VMEM, pltpu.HBM
    shape = jax.ShapeDtypeStruct
    place = lambda kind: pl.BlockSpec(memory_space=kind)
    return pl.pallas_call(
        functools.partial(forward_kernel, n, (q_heads, kv_heads, seq, seq // 2)),
        out_shape=[
            shape(((count + 1) * model, width), low),
            shape((seq, q_wide), full),
            shape((seq, q_heads * HD), low),
            shape((half, model), full),
            shape((3, model, seq), low),
            shape((count, seq, width), low),
            shape((1, model), full),
            shape((1, model), full),
            shape((2, HD), full),
            shape((2, seq, HD), full),
            shape((seq, 1), jnp.int32),
        ],
        in_specs=[place(vmem)] * 14,
        out_specs=[place(k) for k in (hbm, hbm, vmem, vmem, hbm, *[vmem] * 6)],
        scratch_shapes=[
            vmem((seq, model), low),
            vmem((seq, model), low),
            vmem((seq, model), low),
            vmem((model, width - q_wide), low),
            vmem((2, model, 256), low),
            vmem((dp, 8, 128), full),
            vmem((2, seq, HD), low),
            vmem((half, model), low),
            vmem((half, model), low),
            vmem((count, seq, width), full),
            vmem((2, 2, 2 * rows, width // 2), low),
            vmem((2, 256, seq), low),
            dma((count + 2, 2)),
            dma((count + 2, 2, n)),
            dma((count + 2, 2, n)),
            dma((count + 2, 2, n)),
            dma((count + 2, 2, n)),
            dma((4, 2)),
            dma((2, 2)),
            dma((2,)),
            dma((2,)),
            dma((4, n)),
            vmem((rows, width), low),
        ],
        compiler_params=pltpu.CompilerParams(
            collective_id=1, has_side_effects=True, vmem_limit_bytes=67043328
        ),
    )(*shards, tokens, cot, frequency, seg_row, *shares)


SLOTS = 3


def undo(incoming, hat, inverse, gain, cosine, sine):
    turned = incoming * cosine - turn(incoming) * sine
    total = jnp.sum(turned * hat, axis=0, keepdims=True)
    scaled = turned * gain
    raw = inverse * (scaled - hat * jnp.mean(scaled * hat, axis=-1, keepdims=True))
    return total, raw.astype(jnp.bfloat16)


def attend_back(group, dims, heads, tab, seg_col, seg_row, gains, d_attn, d_proj, sums, kept):
    q_heads, kv_heads, seq, block = dims
    per_group = q_heads // kv_heads
    low = jnp.bfloat16
    scale = HD ** (-0.5)
    cosine, sine = tab[0], tab[1]
    keys = prepared(heads[per_group], gains[1:2, :], cosine, sine)[2]
    values = heads[per_group + 1].astype(low)
    for r in range(per_group):
        head = group * per_group + r
        q_inverse, q_hat, query = prepared(heads[r], gains[0:1, :], cosine, sine)
        for first in range(0, seq, block):
            width = first + block
            exps = exp_block(query[first:width], keys[:width], seg_col, seg_row, first)
            probs = exps / jnp.sum(exps, axis=-1, keepdims=True)
            incoming = d_attn[first:width, head_at(r)]
            d_probs = tail_product(incoming, values[:width])
            delta = jnp.sum(probs * d_probs, axis=-1, keepdims=True)
            d_scores = (probs * (d_probs - delta)).astype(low)
            kept[0, first:width, :] = product(d_scores, keys[:width]) * scale
            d_keys = lead_product(d_scores, query[first:width])
            d_values = lead_product(probs.astype(low), incoming)
            if r == 0 and first == 0:
                kept[1] = jnp.zeros_like(kept[1])
                kept[2] = jnp.zeros_like(kept[2])
            kept[1, :width, :] += d_keys
            kept[2, :width, :] += d_values
        total, raw = undo(kept[0], q_hat, q_inverse, gains[0:1, :], cosine, sine)
        sums[0:1, :] += total
        d_proj[0, :, head_at(head)] = raw
    k_inverse, k_hat, _ = prepared(heads[per_group], gains[1:2, :], cosine, sine)
    total, raw = undo(kept[1] * scale, k_hat, k_inverse, gains[1:2, :], cosine, sine)
    sums[1:2, :] += total
    d_proj[1, :, head_at(group)] = raw
    d_proj[1, :, head_at(kv_heads + group)] = kept[2].astype(low)


def reducer(n, pos, core, nexts, mate, rights, outs, fetch_left, scratch, stage_of):
    lefts, mine, term, give, take, ship, land, give_sem, take_sem, ship_sem, land_sem, free_sem, out_sem = scratch
    before, sends_before, sends_total = stage_of
    count = rights.shape[0]
    wide = rights.shape[2] // 2
    rows = outs[0].shape[0]
    span = pl.ds(0, wide)

    def owner_of(side, step):
        if side == 0:
            return (pos - 1 - step + 2 * n) % n
        return (pos + 1 + step) % n

    def given(m, side, step):
        slot = (before + step) % 2
        return remote(
            give.at[m, side, :, span], take.at[m, side, slot, :, span],
            give_sem.at[m, side], take_sem.at[m, side, slot], mate,
        )

    def shipped(m, side, step):
        slot = (sends_before + step) % SLOTS
        return remote(
            ship.at[m, side, :, span], land.at[m, side, slot, :, span],
            ship_sem.at[m, side], land_sem.at[m, side, slot], nexts[side],
        )

    def fetch(m, step):
        for side in range(2):
            start = pl.multiple_of(chip_at(owner_of(side, step), n) * 2 * rows, 2 * rows)
            fetch_left(m, side, pl.ds(start, 2 * rows))

    def early(m, step):
        for side in range(2):
            fetch_left(m, side, None)
        for side in range(2):
            tile = min(512, wide)

            def one(i, carry):
                there = pl.multiple_of(i * tile, tile)
                term[:, pl.ds(there, tile)] = product(
                    lefts[side], rights[m, :, pl.ds(pl.multiple_of(side * wide + there, tile), tile)]
                )
                return carry

            lax.fori_loop(0, wide // tile, one, 0)

            @pl.when(step >= 1)
            def _():
                given(m, side, step - 1).wait_send()

            other = term[pl.ds(pl.multiple_of((1 - core) * rows, rows), rows), span]
            give[m, side, :, span] = other.astype(jnp.bfloat16)
            given(m, side, step).start()
            mine[m, side, :, span] = term[pl.ds(pl.multiple_of(core * rows, rows), rows), span]

    def event(e):
        step, m = e // count, e % count

        @pl.when(step < n - 1)
        def _():
            fetch(m, step + 1)

        for side in range(2):
            given(m, side, step).wait_recv()
            near = take[m, side, (before + step) % 2, :, span].astype(jnp.float32)

            @pl.when(step == 0)
            def _():
                mine[m, side, :, span] += near

            @pl.when(step > 0)
            def _():
                shipped(m, side, step - 1).wait_recv()
                far = land[m, side, (sends_before + step - 1) % SLOTS, :, span].astype(jnp.float32)
                mine[m, side, :, span] += near + far

                @pl.when(sends_before + step - 1 + SLOTS < sends_total)
                def _():
                    pl.semaphore_signal(
                        free_sem.at[m, side], inc=1, device_id=nexts[1 - side], device_id_type=MESH
                    )

                shipped(m, side, step - 1).wait_send()

            @pl.when(step < n - 1)
            def _():
                @pl.when(sends_before + step >= SLOTS)
                def _():
                    pl.semaphore_wait(free_sem.at[m, side], 1)

                ship[m, side, :, span] = mine[m, side, :, span].astype(jnp.bfloat16)
                shipped(m, side, step).start()

            @pl.when(step == n - 1)
            def _():
                for i in range(count):
                    @pl.when(m == i)
                    def _():
                        written(m, side, i).start()

        @pl.when(step < n - 1)
        def _():
            early(m, step + 1)

    def written(m, side, i):
        return pltpu.make_async_copy(
            mine.at[m, side, :, span], outs[i].at[:, pl.ds(side * wide, wide)], out_sem.at[m, side]
        )

    def begin(m):
        fetch(m, 0)
        early(m, 0)

    def finish(m):
        for side in range(2):
            given(m, side, n - 1).wait_send()
            written(m, side, 0).wait()

    return begin, event, finish


def backward_kernel(n, dims, *refs):
    (
        flipped, act, weights, qkv, attn, cot, tokens, resid, tab, seg_col, seg_row, gains, attn_gain, mlp_gain,
        grad_gate, grad_up, grad_down, grad_query, grad_pair, grad_out, result, input_grad, gain_out, d_flip,
        d_proj, d_full, d_resid, blocks, columns, own, part, peer, d_attn, heads, kept, stage,
        attn_sum, mlp_sum, qk_sum, table, others, inbox,
        swap_sem, load_sem, head_sem, attn_sem, stage_sem, column_sem, trade_sem, post_sem, mail_sem, left_sem,
        *scratch,
    ) = refs
    q_heads, kv_heads, seq, block = dims
    pos, core = ring_place(n)
    me = lax.axis_index("dp")
    lane = lax.axis_index("tensor")
    nexts = (at((pos + 1) % n, core, n), at((pos + n - 1) % n, core, n))
    mate = at(pos, 1 - core, n)
    twin = (me, 1 - lane)
    fetch_attn = pltpu.make_async_copy(attn, d_proj.at[2], attn_sem.at[0])
    fetch_attn.start()
    barrier = pltpu.get_barrier_semaphore()

    def greet(o, carry):
        pl.semaphore_signal(barrier, inc=1, device_id=at((pos + o) % n, core, n), device_id_type=MESH)
        return carry

    lax.fori_loop(1, n, greet, 0)
    for other in (mate, twin):
        pl.semaphore_signal(barrier, inc=1, device_id=other, device_id_type=MESH)
    pl.semaphore_wait(barrier, n + 1)
    count, _, hidden = act.shape
    half, model = resid.shape
    q_wide = qkv.shape[1]
    per_group = q_heads // kv_heads
    lefts = scratch[0]

    def from_flipped(first):
        def fetch_left(m, side, there):
            if there is None:
                pltpu.make_async_copy(
                    flipped.at[0, pl.ds(0, lefts.shape[1])], lefts.at[side], left_sem.at[side]
                ).wait()
            elif first == 0:
                pltpu.make_async_copy(flipped.at[m // 2, there], lefts.at[side], left_sem.at[side]).start()
            else:
                @pl.when(m < 2)
                def _():
                    pltpu.make_async_copy(flipped.at[2, there], lefts.at[side], left_sem.at[side]).start()

                @pl.when(m == 2)
                def _():
                    pltpu.make_async_copy(d_flip.at[there], lefts.at[side], left_sem.at[side]).start()

        return fetch_left

    links = (n, pos, core, nexts, mate)
    begin, event, finish = reducer(
        *links, act, (grad_gate, grad_up, grad_down), from_flipped(0), scratch, (0, 0, 2 * (n - 1))
    )
    late_begin, late_event, late_finish = reducer(
        *links, d_proj, (grad_query, grad_pair, grad_out), from_flipped(2), scratch, (n, n - 1, 2 * (n - 1))
    )
    deep = blocks.shape[1]
    turns = model // deep

    def fetch(which, i, slot, width):
        start = which * model + i * deep
        return pltpu.make_async_copy(
            weights.at[pl.ds(pl.multiple_of(start, deep), deep), pl.ds(0, width)],
            blocks.at[slot, :, pl.ds(0, width)], load_sem.at[slot],
        )

    def first_m(m, carry):
        begin(m)
        return carry

    lax.fori_loop(0, count, first_m, 0)
    fetch(1, 0, 0, hidden).start()
    fetch(2, 0, 1, hidden).start()
    def run(first, last):
        def one(e, carry):
            event(e)
            return carry

        lax.fori_loop(first, last, one, 0)

    run(0, count)
    theirs = pl.ds(pl.multiple_of((1 - lane) * half, half), half)
    ours = pl.ds(pl.multiple_of(lane * half, half), half)
    done = count

    def events(number):
        nonlocal done
        run(done, done + number)
        done = done + number

    def send_part(slot, target, i):
        return remote(part.at[slot], target, swap_sem.at[i, 0], swap_sem.at[i, 1], twin)

    def dn_two(i, carry):
        there = pl.ds(pl.multiple_of(i * deep, deep), deep)
        for which in range(2):
            fetch(which + 1, i, which, hidden).wait()
            other = tail_product(act[which, theirs, :], blocks[which])
            same = tail_product(act[which, ours, :], blocks[which])
            if which == 0:
                own[:, there] = same
                d_resid[:, there] = other
            else:
                own[:, there] += same
                part[0, :, there] = (d_resid[:, there] + other).astype(jnp.bfloat16)

            @pl.when(i < turns - 1)
            def _():
                fetch(which + 1, i + 1, which, hidden).start()

        @pl.when(i % 4 == 3)
        def _():
            event(count + i // 4)

        return carry

    lax.fori_loop(0, turns, dn_two, 0)
    done = done + turns // 4
    sends = [send_part(0, peer.at[0], 0)]
    sends[0].start()
    fetch(3, 0, 0, hidden).start()
    events(4)
    sends[0].wait_recv()
    sends[0].wait_send()
    strip = 32

    def over_strips(body):
        lax.fori_loop(0, half // strip, body, 0)

    def gather_sum(target, i, total):
        @pl.when(i == 0)
        def _():
            target[...] = total

        @pl.when(i > 0)
        def _():
            target[...] += total

    def norm_two(i, carry):
        there = pl.ds(pl.multiple_of(i * strip, strip), strip)
        incoming = own[there, :] + peer[0, there, :].astype(jnp.float32)
        values = resid[there, :]
        inverse = row_scale(values)
        normed = values * inverse
        scaled = incoming * mlp_gain[...]
        change = cot[there, :].astype(jnp.float32) + inverse * (
            scaled - normed * jnp.mean(scaled * normed, axis=-1, keepdims=True)
        )
        d_resid[there, :] = change
        part[0, there, :] = change.astype(jnp.bfloat16)
        gather_sum(mlp_sum, i, jnp.sum(incoming * normed, axis=0, keepdims=True))
        return carry

    over_strips(norm_two)
    sends.append(send_part(0, d_full.at[ours], 1))
    sends[1].start()
    d_full[ours, :] = part[0]

    def narrow(which, width, slot, base, every, rows_of):
        def one(i, carry):
            @pl.when(i < turns - 1)
            def _():
                fetch(which, i + 1, (i + 1) % 2, width).start()

            fetch(which, i, i % 2, width).wait()
            there = pl.ds(pl.multiple_of(i * deep, deep), deep)
            for rows, mine in ((theirs, False), (ours, True)):
                total = None
                for left, start in rows_of(rows):
                    gained = tail_product(left, blocks[i % 2, :, pl.ds(start, left.shape[1])])
                    total = gained if total is None else total + gained
                if mine:
                    own[:, there] = total
                else:
                    part[slot, :, there] = total.astype(jnp.bfloat16)

            @pl.when(i % every == every - 1)
            def _():
                event(base + i // every)

            return carry

        lax.fori_loop(0, turns, one, 0)

    narrow(3, hidden, 1, done, 4, lambda rows: [(act[2, rows, :], 0)])
    done = done + turns // 4
    sends.append(send_part(1, peer.at[1], 2))
    sends[2].start()
    group_wide = per_group * HD

    def fetch_columns(g):
        return pltpu.make_async_copy(
            weights.at[pl.ds(0, model), pl.ds(pl.multiple_of(q_wide + g * group_wide, group_wide), group_wide)],
            columns.at[g % 2], column_sem.at[g % 2],
        )

    fetch_columns(0).start()
    events(1)
    remote(part.at[0], d_full.at[theirs], swap_sem.at[1, 0], swap_sem.at[1, 1], twin).wait_recv()
    flip_into(d_full, d_flip, stage, stage_sem)
    qk_sum[...] = jnp.zeros_like(qk_sum)
    fetch_attn.wait()

    def group_step(group, carry):
        places = [group * per_group + r for r in range(per_group)]
        places += [q_heads + group, q_heads + kv_heads + group]
        copies = [
            pltpu.make_async_copy(qkv.at[:, head_at(place)], heads.at[i], head_sem.at[i])
            for i, place in enumerate(places)
        ]
        for copy in copies:
            copy.start()

        @pl.when(group < kv_heads - 1)
        def _():
            fetch_columns(group + 1).start()

        fetch_columns(group).wait()
        d_attn[...] = product(d_full[...], columns[group % 2]).astype(jnp.bfloat16)
        for copy in copies:
            copy.wait()
        attend_back(group, dims, heads, tab, seg_col, seg_row, gains, d_attn, d_proj, qk_sum, kept)
        event(done + group)
        return carry

    lax.fori_loop(0, kv_heads, group_step, 0)
    done = done + kv_heads
    sends[2].wait_recv()

    def last_strip(i, carry):
        there = pl.ds(pl.multiple_of(i * strip, strip), strip)
        result[there, :] = (
            resid[there, :] + (own[there, :] + peer[1, there, :].astype(jnp.float32))
        ).astype(jnp.bfloat16)
        return carry

    over_strips(last_strip)
    fetch(0, 0, 0, q_wide).start()
    sends[1].wait_send()
    events(1)
    width = d_proj.shape[2]
    narrow(0, q_wide, 0, done, 8, lambda rows: [(d_proj[0, rows, :], 0), (d_proj[1, rows, :], width)])
    done = done + turns // 8
    sends.append(send_part(0, peer.at[0], 3))
    sends[3].start()
    events(3)
    sends[3].wait_recv()

    def norm_one(i, carry):
        there = pl.ds(pl.multiple_of(i * strip, strip), strip)
        incoming = own[there, :] + peer[0, there, :].astype(jnp.float32)
        values = tokens[there, :].astype(jnp.float32)
        inverse = row_scale(values)
        normed = values * inverse
        scaled = incoming * attn_gain[...]
        change = d_resid[there, :] + inverse * (
            scaled - normed * jnp.mean(scaled * normed, axis=-1, keepdims=True)
        )
        input_grad[there, :] = change.astype(jnp.bfloat16)
        gather_sum(attn_sum, i, jnp.sum(incoming * normed, axis=0, keepdims=True))
        return carry

    over_strips(norm_one)
    dp = 2 * n
    share, head_share = model // dp, 2 * HD // dp
    table[...] = jnp.zeros_like(table)
    for d in range(dp):
        start = d * share // 128 * 128
        row = d * head_share // HD
        table[d, 0:1, :] = attn_sum[:, start : start + 128]
        table[d, 1:2, :] = mlp_sum[:, start : start + 128]
        table[d, 2:3, :] = qk_sum[row : row + 1, :]
    def trade(i, carry):
        partner = ((1 - i) * me + i * mate[0], (1 - i) * twin[1] + i * lane)
        swap = remote(table, others.at[i], trade_sem.at[i, 0], trade_sem.at[i, 1], partner)
        swap.start()
        swap.wait()
        table[...] += others[i]
        return carry

    lax.fori_loop(0, 2, trade, 0)

    def mail(o, target):
        return remote(table.at[target], inbox.at[o], post_sem.at[o], mail_sem.at[o], at((pos + o) % n, core, n))

    def post(o, carry):
        mail(o, chip_at((pos + o) % n, n) * 2 + core).start()
        return carry

    lax.fori_loop(1, n, post, 0)

    last = count * (n - 1)
    run(done, last)

    def hand_over(m, carry):
        event(last + m)
        finish(m)
        late_begin(m)
        late_event(m)
        return carry

    lax.fori_loop(0, count, hand_over, 0)
    gain_out[...] = table[me]

    def collect(o, carry):
        mail(o, 0).wait_recv()
        gain_out[...] += inbox[o]
        return carry

    lax.fori_loop(1, n, collect, 0)

    def late_rest(e, carry):
        late_event(e)
        return carry

    lax.fori_loop(count, count * n, late_rest, 0)
    for m in range(count):
        late_finish(m)
    sends[2].wait_send()
    sends[3].wait_send()

    def sent(o, carry):
        mail(o, 0).wait_send()
        return carry

    lax.fori_loop(1, n, sent, 0)


def backward_block(
    flipped, act, weights, qkv, attn, cot, tokens, resid, tab, seg_col, seg_row, gains, attn_gain, mlp_gain,
    q_heads, kv_heads, dp,
):
    n = dp // 2
    count, seq, hidden = act.shape
    half, model = resid.shape
    rows = model // dp
    wide = hidden // 2
    width = q_heads * HD
    low, full, dma, vmem, hbm = jnp.bfloat16, jnp.float32, pltpu.SemaphoreType.DMA, pltpu.VMEM, pltpu.HBM
    shape = jax.ShapeDtypeStruct
    place = lambda kind: pl.BlockSpec(memory_space=kind)
    per_group = q_heads // kv_heads
    return pl.pallas_call(
        functools.partial(backward_kernel, n, (q_heads, kv_heads, seq, seq // 2)),
        out_shape=[
            *[shape((rows, hidden), full)] * 3,
            *[shape((rows, width), full)] * 3,
            shape((half, model), low),
            shape((half, model), low),
            shape((8, 128), full),
            shape((model, seq), low),
        ],
        in_specs=[place(k) for k in (hbm, vmem, hbm, hbm, hbm, *[vmem] * 9)],
        out_specs=[place(k) for k in (*[hbm] * 6, vmem, vmem, vmem, hbm)],
        scratch_shapes=[
            vmem((3, seq, width), low),
            vmem((seq, model), low),
            vmem((half, model), full),
            vmem((2, 256, hidden), low),
            vmem((2, model, per_group * HD), low),
            vmem((half, model), full),
            vmem((2, half, model), low),
            vmem((2, half, model), low),
            vmem((seq, per_group * HD), low),
            vmem((per_group + 2, seq, HD), full),
            vmem((3, seq, HD), full),
            vmem((2, 256, seq), low),
            vmem((1, model), full),
            vmem((1, model), full),
            vmem((8, HD), full),
            vmem((dp, 8, 128), full),
            vmem((2, dp, 8, 128), full),
            vmem((n, 8, 128), full),
            dma((4, 2)),
            dma((2,)),
            dma((per_group + 2,)),
            dma((1,)),
            dma((2,)),
            dma((2,)),
            dma((2, 2)),
            dma((n,)),
            dma((n,)),
            dma((2,)),
            vmem((2, 2 * rows, seq), low),
            vmem((count, 2, rows, wide), full),
            vmem((2 * rows, wide), full),
            vmem((count, 2, rows, wide), low),
            vmem((count, 2, 2, rows, wide), low),
            vmem((count, 2, rows, wide), low),
            vmem((count, 2, SLOTS, rows, wide), low),
            dma((count, 2)),
            dma((count, 2, 2)),
            dma((count, 2)),
            dma((count, 2, SLOTS)),
            pltpu.SemaphoreType.REGULAR((count, 2)),
            dma((count, 2)),
        ],
        compiler_params=pltpu.CompilerParams(
            collective_id=2, has_side_effects=True, vmem_limit_bytes=67043328
        ),
    )(
        flipped, act, weights, qkv, attn, cot, tokens, resid, tab, seg_col, seg_row, gains, attn_gain, mlp_gain,
    )


def finishing_kernel(dp, *refs):
    gains = refs[0]
    sources, outs = refs[1:9], refs[9:21]
    bufs, turned, in_sem, out_sem = refs[21:29], refs[29:31], refs[31], refs[32]
    loads = [pltpu.make_async_copy(source, buf, in_sem.at[i]) for i, (source, buf) in enumerate(zip(sources, bufs))]
    for i in (2, 6, 7, 5, 3, 4, 0, 1):
        loads[i].start()
    half = outs[3].shape[1]
    stores = [None] * 9

    def store(i, buf, out):
        stores[i] = pltpu.make_async_copy(buf, out, out_sem.at[i])
        stores[i].start()

    def turn_over(i, which, out):
        loads[which].wait()
        turned[i][...] = bufs[which][...].T
        store(7 + i, turned[i], outs[out])

    turn_over(0, 2, 8)
    for i, (which, out) in enumerate(((6, 0), (7, 1))):
        loads[which].wait()
        store(i, bufs[which], outs[out])
    turn_over(1, 5, 5)
    for i, (which, out) in enumerate(((3, 2), (0, 6), (1, 7))):
        loads[which].wait()
        store(2 + i, bufs[which], outs[out])
    loads[4].wait()
    store(5, bufs[4].at[:, pl.ds(0, half)], outs[3])
    store(6, bufs[4].at[:, pl.ds(half, half)], outs[4])
    me = lax.axis_index("dp")
    for row in range(3):
        target = outs[9 + row]
        size = target.shape[1]
        line = gains[row : row + 1, :]
        if size % 128:
            line = pltpu.roll(line, (128 - me * size % 128) % 128, 1)
        target[...] = line[:, :size]
    for copy in stores:
        copy.wait()


def finishing_block(gains, arrays, shapes, dp):
    full, dma, vmem, hbm = jnp.float32, pltpu.SemaphoreType.DMA, pltpu.VMEM, pltpu.HBM
    place = lambda kind: pl.BlockSpec(memory_space=kind)
    return pl.pallas_call(
        functools.partial(finishing_kernel, dp),
        out_shape=shapes,
        in_specs=[place(vmem)] + [place(hbm)] * 8,
        out_specs=[place(hbm)] * 9 + [place(vmem)] * 3,
        scratch_shapes=[
            *[vmem(a.shape, a.dtype) for a in arrays],
            vmem(arrays[2].shape[::-1], full),
            vmem(arrays[5].shape[::-1], full),
            dma((8,)),
            dma((9,)),
        ],
        compiler_params=pltpu.CompilerParams(vmem_limit_bytes=67043328),
    )(gains, *arrays)


def on_device(
    tokens,
    seg_ids,
    w_query,
    w_key,
    w_value,
    w_output,
    w_gate,
    w_up,
    w_down,
    gain_attn,
    gain_mlp,
    gain_qk,
    cotangent,
):
    dp = lax.axis_size("dp")
    q_heads = w_query.shape[1] // HD
    kv_heads = w_key.shape[1] // HD
    places = np.arange(HD) % (HD // 2) * 2
    frequency = jnp.asarray((rope_base ** (-places / HD)).astype(np.float32)[None, :])
    (
        weights, projected, attn_rows, resid, flipped, act, attn_gain, mlp_gain, pair, rope_tab, seg_col,
    ) = forward_block(
        (w_query, w_key, w_value, w_output.T, w_gate, w_up, w_down),
        tokens,
        cotangent,
        frequency,
        seg_ids,
        [g[None, :] for g in (gain_attn, gain_mlp, gain_qk)],
        q_heads,
        kv_heads,
        dp,
    )
    (
        grad_gate, grad_up, grad_down, grad_query, grad_pair, grad_out, result_rows, input_grad, gain_sums, _,
    ) = backward_block(
        flipped,
        act,
        weights,
        projected,
        attn_rows,
        cotangent,
        tokens,
        resid,
        rope_tab,
        seg_col,
        seg_ids,
        pair,
        attn_gain,
        mlp_gain,
        q_heads,
        kv_heads,
        dp,
    )
    full = jnp.float32
    shapes = [jax.ShapeDtypeStruct(tokens.shape, jnp.bfloat16)] * 2
    shapes += [
        jax.ShapeDtypeStruct(w.shape, full)
        for w in (w_query, w_key, w_value, w_output, w_gate, w_up, w_down)
    ]
    shapes += [jax.ShapeDtypeStruct((1, g.shape[0]), full) for g in (gain_attn, gain_mlp, gain_qk)]
    outs = finishing_block(
        gain_sums,
        [grad_gate, grad_up, grad_down, grad_query, grad_pair, grad_out, result_rows, input_grad],
        shapes,
        dp,
    )
    return (*outs[:9], *(g.reshape(-1) for g in outs[9:]))


def solution(mesh):
    return jax.shard_map(
        on_device,
        mesh=mesh,
        in_specs=(
            P(("dp", "tensor"), None),
            P("dp", None),
            P("dp", "tensor"),
            P("dp", "tensor"),
            P("dp", "tensor"),
            P("tensor", "dp"),
            P("dp", "tensor"),
            P("dp", "tensor"),
            P("tensor", "dp"),
            P("dp"),
            P("dp"),
            P("dp"),
            P(("dp", "tensor"), None),
        ),
        out_specs=(
            P(("dp", "tensor"), None),
            P(("dp", "tensor"), None),
            P("dp", "tensor"),
            P("dp", "tensor"),
            P("dp", "tensor"),
            P("tensor", "dp"),
            P("dp", "tensor"),
            P("dp", "tensor"),
            P("tensor", "dp"),
            P("dp"),
            P("dp"),
            P("dp"),
        ),
        check_vma=False,
    )
```

```python
import functools
import jax
import jax.numpy as jnp
import numpy as np
from jax import lax
from jax.experimental import pallas as pl
from jax.experimental.pallas import tpu as pltpu

from jax.sharding import PartitionSpec as P

MESH = pl.DeviceIdType.MESH
HD = 128
epsilon = 1e-06
rope_base = 1000000.0


def ring_place(n):
    me = lax.axis_index("dp")
    chip = me // 2
    core = me % 2
    odd = chip % 2
    pos = (1 - odd) * (chip // 2) + odd * (n - 1 - chip // 2)
    return pos, core


def chip_at(pos, n):
    high = pos // (n // 2)
    return (1 - high) * (2 * pos) + high * (2 * (n - 1 - pos) + 1)


def at(pos, core, n):
    return (chip_at(pos, n) * 2 + core, lax.axis_index("tensor"))


def meet(peers):
    barrier = pltpu.get_barrier_semaphore()
    for peer in peers:
        pl.semaphore_signal(barrier, inc=1, device_id=peer, device_id_type=MESH)
    pl.semaphore_wait(barrier, len(peers))


def remote(src, dst, send, recv, peer):
    return pltpu.make_async_remote_copy(
        src_ref=src, dst_ref=dst, send_sem=send, recv_sem=recv, device_id=peer, device_id_type=MESH
    )


def product(left, right):
    return jnp.dot(left, right, preferred_element_type=jnp.float32)


def lead_product(left, right):
    return lax.dot_general(
        left, right, (((0,), (0,)), ((), ())), preferred_element_type=jnp.float32
    )


def tail_product(left, right):
    return lax.dot_general(
        left, right, (((1,), (1,)), ((), ())), preferred_element_type=jnp.float32
    )


def turn(values):
    return pltpu.roll(values, values.shape[-1] // 2, 1)


def row_scale(values):
    return lax.rsqrt(jnp.mean(values * values, axis=-1, keepdims=True) + epsilon)


def head_at(index):
    return pl.ds(pl.multiple_of(index * HD, HD), HD)


def prepared(raw, gain, cosine, sine):
    inverse = row_scale(raw)
    hat = raw * inverse
    scaled = hat * gain
    return inverse, hat, (scaled * cosine + turn(scaled) * sine).astype(jnp.bfloat16)


def exp_block(query, keys, seg_col, seg_row, first):
    width = keys.shape[0]
    scores = tail_product(query, keys) * HD ** (-0.5)
    rows = lax.broadcasted_iota(jnp.int32, scores.shape, 0) + first
    columns = lax.broadcasted_iota(jnp.int32, scores.shape, 1)
    allowed = (seg_col[first : first + scores.shape[0], :] == seg_row[:, :width]) & (
        columns <= rows
    )
    return jnp.where(allowed, jnp.exp(scores), 0.0)


def attend_group(group, dims, qkv, tab, seg_col, seg_row, gains, attn, kept):
    q_heads, kv_heads, seq, block = dims
    per_group = q_heads // kv_heads
    cosine, sine = tab[0], tab[1]
    raw = qkv[:, head_at(q_heads + group)]
    kept[0] = prepared(raw, gains[1:2, :], cosine, sine)[2]
    kept[1] = qkv[:, head_at(q_heads + kv_heads + group)].astype(jnp.bfloat16)
    for r in range(per_group):
        head = group * per_group + r
        raw = qkv[:, head_at(head)]
        query = prepared(raw, gains[0:1, :], cosine, sine)[2]
        for first in range(0, seq, block):
            width = first + block
            exps = exp_block(query[first:width], kept[0, :width, :], seg_col, seg_row, first)
            probs = (exps / jnp.sum(exps, axis=-1, keepdims=True)).astype(jnp.bfloat16)
            attn[first:width, head_at(head)] = product(probs, kept[1, :width, :]).astype(jnp.bfloat16)


def block_columns(ref, index, width):
    if width % 128 == 0:
        return ref[:, pl.ds(pl.multiple_of(index * width, width), width)]
    fold = 128 // width
    tile = ref[:, pl.ds(pl.multiple_of((index // fold) * 128, 128), 128)]
    picked = tile[:, :width]
    for i in range(1, fold):
        picked = jnp.where(index % fold == i, tile[:, i * width : (i + 1) * width], picked)
    return picked


HALFWAY = 6
READY = 9


def flip_into(source, target, stage, stage_sem):
    deep = stage.shape[1]
    turns = source.shape[1] // deep

    def put(i):
        return pltpu.make_async_copy(
            stage.at[i % 2], target.at[pl.ds(pl.multiple_of(i * deep, deep), deep)], stage_sem.at[i % 2]
        )

    def one(i, carry):
        @pl.when(i >= 2)
        def _():
            put(i - 2).wait()

        stage[i % 2] = source[:, pl.ds(pl.multiple_of(i * deep, deep), deep)].T
        put(i).start()
        return carry

    lax.fori_loop(0, turns, one, 0)
    put(turns - 2).wait()
    put(turns - 1).wait()


def forward_kernel(n, dims, *refs):
    (
        query_shard, key_shard, value_shard, out_shard, gate_shard, up_shard, down_given,
        tokens, cot, frequency, seg_row, attn_share, mlp_share, qk_share,
        weights, qkv_out, attn, resid, flipped, act, attn_gain, mlp_gain, gains, tab, seg_col,
        full_rows, cot_full, full_two, out_weight, columns, box, kept, part, peer, acc, blocks, stage,
        own_sem, send_sem, recv_sem, give_sem, take_sem, swap_sem, load_sem, stage_sem, column_sem, tile_sem, down_shard,
    ) = refs
    q_heads, kv_heads, seq, block = dims
    pos, core = ring_place(n)
    me = lax.axis_index("dp")
    lane = lax.axis_index("tensor")
    nexts = (at((pos + 1) % n, core, n), at((pos + n - 1) % n, core, n))
    mate = at(pos, 1 - core, n)
    twin = (me, 1 - lane)
    ffn_shards = (gate_shard, up_shard, down_shard)
    count = len(ffn_shards)
    rows, width = gate_shard.shape
    wide = width // 2
    q_span, kv_span = query_shard.shape[1], key_shard.shape[1]
    model = 2 * n * rows
    half = seq // 2
    theirs = pl.ds(pl.multiple_of((1 - lane) * half, half), half)
    ours = pl.ds(pl.multiple_of(lane * half, half), half)
    tile = box.at[me]
    tile[...] = jnp.zeros(tile.shape, jnp.float32)
    for i, gain in enumerate((attn_share, mlp_share, qk_share)):
        size = gain.shape[1]
        tile[i : i + 1, 0:size] = gain[...].astype(jnp.float32)
        if size % 128:
            tile[i : i + 1, :] = pltpu.roll(tile[i : i + 1, :], me * size % 128, 1)
    meet((*nexts, mate, twin))

    def owner_of(side, step):
        if side == 0:
            return (pos - step + 2 * n) % n
        return (pos + step) % n

    def small(sub, side):
        start, source = (
            ((0, query_shard), (q_span + 2 * kv_span, out_shard)),
            ((q_span, key_shard), (q_span + kv_span, value_shard)),
        )[sub][side]
        return (sub, 0, pl.ds(start, source.shape[1]), source)

    def large(w, side):
        columns = pl.ds(side * wide, wide)
        source = ffn_shards[w].at[:, columns] if isinstance(w, int) else None
        return (w + 2, (w + 1) * model, columns, source)

    def spot(message, chip, who):
        start = message[1] + (chip * 2 + who) * rows
        return weights.at[pl.ds(pl.multiple_of(start, rows), rows), message[2]]

    def hop(message, side, step):
        k = message[0]
        here = spot(message, chip_at(owner_of(side, step - 1), n), core)
        return remote(here, here, send_sem.at[k, side, step], recv_sem.at[k, side, step], nexts[side])

    def arrived(message, side, step):
        k = message[0]
        here = spot(message, chip_at(owner_of(side, step), n), core)
        return remote(here, here, send_sem.at[k, side, step], recv_sem.at[k, side, step], nexts[side])

    def hand(message, side, step, who):
        k = message[0]
        here = spot(message, chip_at(owner_of(side, step), n), who)
        return remote(here, here, give_sem.at[k, side, step], take_sem.at[k, side, step], mate)

    def begin(message, side):
        k = message[0]
        source = message[3]
        here = spot(message, chip_at(pos, n), core)
        remote(source, here, send_sem.at[k, side, 1], recv_sem.at[k, side, 1], nexts[side]).start()
        remote(source, here, give_sem.at[k, side, 0], take_sem.at[k, side, 0], mate).start()
        pltpu.make_async_copy(source, here, own_sem.at[k, side]).start()

    def keep_own(message, side):
        here = spot(message, chip_at(pos, n), core)
        return pltpu.make_async_copy(here, here, own_sem.at[message[0], side])

    def tile_hop(step, owner):
        place = chip_at(owner, n) * 2 + core
        return remote(box.at[place], box.at[place], tile_sem.at[0, step], tile_sem.at[1, step], nexts[0])

    def tile_hand(step, who):
        place = chip_at(owner_of(0, step), n) * 2 + who
        return remote(box.at[place], box.at[place], tile_sem.at[2, step], tile_sem.at[3, step], mate)

    swaps = [
        remote(source, target.at[ours], swap_sem.at[i, 0], swap_sem.at[i, 1], twin)
        for i, (source, target) in enumerate(((tokens, full_rows), (cot, cot_full)))
    ]
    remote(tile, box.at[me], tile_sem.at[0, 1], tile_sem.at[1, 1], nexts[0]).start()
    remote(tile, box.at[me], tile_sem.at[2, 0], tile_sem.at[3, 0], mate).start()
    for side in range(2):
        begin(small(0, side), side)
    for swap in swaps:
        swap.start()
    full_rows[ours, :] = tokens[...]
    cot_full[ours, :] = cot[...]

    def pass_on(message, side, step):
        arrived(message, side, step).wait_recv()

        @pl.when(step < n - 1)
        def _():
            hop(message, side, step + 1).start()

        hand(message, side, step, core).start()

    def pass_tile(step):
        tile_hop(step, owner_of(0, step)).wait_recv()

        @pl.when(step < n - 1)
        def _():
            tile_hop(step + 1, owner_of(0, step)).start()

        tile_hand(step, core).start()

    def mixed_step(step, carry):
        pass_tile(step)
        for sub in range(2):
            for side in range(2):
                pass_on(small(sub, side), side, step)
        return carry

    def mixed_steps(first, last):
        lax.fori_loop(first, last, mixed_step, 0)

    row = lax.broadcasted_iota(jnp.int32, (seq, seq), 0)
    column = lax.broadcasted_iota(jnp.int32, (seq, seq), 1)
    ids = jnp.broadcast_to(seg_row[...], (seq, seq)).astype(jnp.float32)
    own_id = jnp.sum(jnp.where(row == column, ids, 0.0), axis=1, keepdims=True)
    doc_start = jnp.sum(jnp.where(ids < own_id, 1.0, 0.0), axis=1, keepdims=True)
    place = lax.broadcasted_iota(jnp.int32, (seq, 1), 0).astype(jnp.float32)
    seg_col[...] = own_id.astype(jnp.int32)
    for i in range(0, width, 512):
        down_shard[:, i : i + 512] = down_given[i : i + 512, :].T
    angles = (place - doc_start) * frequency[...]
    tab[0] = jnp.cos(angles)
    sign = jnp.where(lax.broadcasted_iota(jnp.int32, angles.shape, 1) < HD // 2, -1.0, 1.0)
    tab[1] = jnp.sin(angles) * sign
    for side in range(2):
        begin(small(1, side), side)
    mixed_steps(1, n - 1)
    pass_tile(n - 1)
    for side in range(2):
        pass_on(small(0, side), side, n - 1)
    for side in range(2):
        begin(large(0, side), side)
    for side in range(2):
        pass_on(small(1, side), side, n - 1)

    def service(event):
        step, w = event // count + 1, event % count
        for side in range(2):
            pass_on(large(w, side), side, step)

    def services(first, last):
        def one(event, carry):
            service(event)
            return carry

        lax.fori_loop(first, last, one, 0)

    def gathered(step, carry):
        for sub in range(2):
            for side in range(2):
                hand(small(sub, side), side, step, 1 - core).wait_recv()
        tile_hand(step, 1 - core).wait_recv()
        return carry

    lax.fori_loop(0, n, gathered, 0)
    for sub in range(2):
        for side in range(2):
            keep_own(small(sub, side), side).wait()
    q_wide = (q_heads + 2 * kv_heads) * HD
    fetch_out = pltpu.make_async_copy(
        weights.at[pl.ds(0, model), pl.ds(q_wide, width - q_wide)], out_weight, load_sem.at[0, 0]
    )
    turns = q_wide // columns.shape[2]
    deep = columns.shape[2]

    def fetch_columns(i):
        return pltpu.make_async_copy(
            weights.at[pl.ds(0, model), pl.ds(pl.multiple_of(i * deep, deep), deep)],
            columns.at[i % 2], column_sem.at[i % 2],
        )

    fetch_columns(0).start()
    fetch_out.start()
    dp = 2 * n
    share, head_share = model // dp, 2 * HD // dp
    for first, target, per in ((0, attn_gain, share), (1, mlp_gain, share)):
        for s in range(model // 128):
            owners = [d for d in range(dp) if d * per // 128 == s]
            total = box[owners[0], first : first + 1, :]
            for d in owners[1:]:
                total = total + box[d, first : first + 1, :]
            target[:, s * 128 : (s + 1) * 128] = total
    for s in range(2):
        owners = [d for d in range(dp) if d * head_share // HD == s]
        total = box[owners[0], 2:3, :]
        for d in owners[1:]:
            total = total + box[d, 2:3, :]
        gains[s : s + 1, :] = total
    swaps[0].wait_recv()
    strip = 32

    def norm_strip(i, carry):
        there = pl.ds(pl.multiple_of(i * strip, strip), strip)
        values = full_rows[there, :].astype(jnp.float32)
        full_two[there, :] = (values * row_scale(values) * attn_gain[...]).astype(jnp.bfloat16)
        return carry

    lax.fori_loop(0, seq // strip, norm_strip, 0)
    for side in range(2):
        begin(large(1, side), side)
    qkv = acc.at[count - 1]

    def project(i, carry):
        @pl.when(i < turns - 1)
        def _():
            fetch_columns(i + 1).start()

        fetch_columns(i).wait()
        qkv[:, pl.ds(pl.multiple_of(i * deep, deep), deep)] = product(full_two[...], columns[i % 2])
        return carry

    lax.fori_loop(0, turns, project, 0)
    save_qkv = pltpu.make_async_copy(qkv.at[:, pl.ds(0, q_wide)], qkv_out, load_sem.at[0, 1])
    save_qkv.start()
    for side in range(2):
        begin(large(2, side), side)
    service(0)

    def load(job, side):
        step, w = job // count, job % count
        start = (w + 1) * model + chip_at(owner_of(side, step), n) * 2 * rows
        return pltpu.make_async_copy(
            weights.at[pl.ds(pl.multiple_of(start, 2 * rows), 2 * rows), pl.ds(side * wide, wide)],
            blocks.at[job % 2, side], load_sem.at[job % 2, side],
        )

    def prepare(job):
        step, w = job // count, job % count
        for side in range(2):
            hand(large(w, side), side, step, 1 - core).wait_recv()

            @pl.when(step == 0)
            def _():
                keep_own(large(w, side), side).wait()

            load(job, side).start()

    def work(job):
        step, w = job // count, job % count
        for side in range(2):
            load(job, side).wait()
            chip = chip_at(owner_of(side, step), n)

            def with_left(left):
                tile_width = wide // 3

                def one(i, carry):
                    there = pl.ds(pl.multiple_of(side * wide + i * tile_width, tile_width), tile_width)
                    gained = product(
                        left, blocks[job % 2, side, :, pl.ds(pl.multiple_of(i * tile_width, tile_width), tile_width)]
                    )

                    @pl.when(step == 0)
                    def _():
                        acc[w, :, there] = gained

                    @pl.when(step > 0)
                    def _():
                        acc[w, :, there] += gained

                    return carry

                lax.fori_loop(0, 3, one, 0)

            @pl.when(w < count - 1)
            def _():
                with_left(block_columns(full_two, chip, 2 * rows))

            @pl.when(w == count - 1)
            def _():
                with_left(block_columns(cot_full, chip, 2 * rows))

    def flip(source, target):
        flip_into(source, flipped.at[target], stage, stage_sem)

    groups = (qkv, tab, seg_col, seg_row, gains, attn, kept)

    def attend():
        def one(group, carry):
            attend_group(group, dims, *groups)

            @pl.when(group % (kv_heads // 2) == kv_heads // 2 - 1)
            def _():
                service(1 + group // (kv_heads // 2))

            return carry

        lax.fori_loop(0, kv_heads, one, 0)

    flip(full_two, 2)
    attend()
    fetch_out.wait()
    part[...] = tail_product(attn[theirs, :], out_weight[...]).astype(jnp.bfloat16)
    swaps[1].wait_recv()
    send_part = remote(part, peer, swap_sem.at[2, 0], swap_sem.at[2, 1], twin)
    send_part.start()
    resid[...] = tokens[...].astype(jnp.float32) + tail_product(attn[ours, :], out_weight[...])
    services(3, 5)
    flip(cot_full, 1)
    services(5, HALFWAY)
    send_part.wait_recv()
    summed = resid[...] + peer[...].astype(jnp.float32)
    resid[...] = summed
    send_part.wait_send()
    part[...] = (summed * row_scale(summed) * mlp_gain[...]).astype(jnp.bfloat16)
    send_two = remote(part, full_two.at[ours], swap_sem.at[3, 0], swap_sem.at[3, 1], twin)
    send_two.start()
    full_two[ours, :] = part[...]
    ready = READY
    services(HALFWAY, ready)
    remote(part, full_two.at[theirs], swap_sem.at[3, 0], swap_sem.at[3, 1], twin).wait_recv()
    flip(full_two, 0)
    save_qkv.wait()

    jobs, turns_left = count * n, count * (n - 1) - ready
    most = 2 if 2 * (turns_left - 1) >= jobs - 2 else 3

    def done_before(i):
        return jnp.minimum(jnp.minimum(most * i, i + ready + count), jobs - 2)

    def both(i, carry):
        service(ready + i)
        first, last = done_before(i), done_before(i + 1)

        def one(job, carry):
            @pl.when((job == first) & ((i == 0) | (job == i + ready + count)))
            def _():
                prepare(job)

            @pl.when(job + 1 <= i + ready + count)
            def _():
                prepare(job + 1)

            work(job)
            return carry

        lax.fori_loop(first, last, one, 0)
        return carry

    lax.fori_loop(0, turns_left - 1, both, 0)
    full_turn = next(i for i in range(turns_left) if min(most * (i + 1), i + 1 + ready + count) > jobs - 3)
    if jobs - 2 > full_turn + ready + count:
        prepare(jobs - 2)
    work(jobs - 2)

    def partly(i, carry):
        there = pl.ds(pl.multiple_of(i * strip, strip), strip)
        gate = acc[0, there, :]
        up = acc[1, there, :]
        sig = 1.0 / (1.0 + jnp.exp(-gate))
        silu = gate * sig
        acc[0, there, :] = up * sig * (1.0 + gate * (1.0 - sig))
        acc[1, there, :] = silu
        act[2, there, :] = (silu * up).astype(jnp.bfloat16)
        return carry

    lax.fori_loop(0, seq // strip, partly, 0)
    service(count * (n - 1) - 1)
    prepare(jobs - 1)
    work(jobs - 1)

    def complete(i, carry):
        there = pl.ds(pl.multiple_of(i * strip, strip), strip)
        d_act = acc[2, there, :]
        act[0, there, :] = (d_act * acc[0, there, :]).astype(jnp.bfloat16)
        act[1, there, :] = (d_act * acc[1, there, :]).astype(jnp.bfloat16)
        return carry

    lax.fori_loop(0, seq // strip, complete, 0)

    def drain(step, carry):
        for side in range(2):
            for message in [small(sub, side) for sub in range(2)] + [large(w, side) for w in range(count)]:
                hop(message, side, step).wait_send()
                hand(message, side, step, core).wait_send()
        tile_hop(step, owner_of(0, step)).wait_send()
        tile_hand(step, core).wait_send()
        return carry

    lax.fori_loop(1, n, drain, 0)
    for side in range(2):
        for message in [small(sub, side) for sub in range(2)] + [large(w, side) for w in range(count)]:
            hand(message, side, 0, core).wait_send()
    tile_hand(0, core).wait_send()
    for swap in (*swaps, send_two):
        swap.wait_send()


def forward_block(shards, tokens, cot, frequency, seg_row, shares, q_heads, kv_heads, dp):
    n = dp // 2
    rows, width = shards[-2].shape
    count = 3
    half, model = tokens.shape
    seq = 2 * half
    q_wide = (q_heads + 2 * kv_heads) * HD
    low, full, dma, vmem, hbm = jnp.bfloat16, jnp.float32, pltpu.SemaphoreType.DMA, pltpu.VMEM, pltpu.HBM
    shape = jax.ShapeDtypeStruct
    place = lambda kind: pl.BlockSpec(memory_space=kind)
    return pl.pallas_call(
        functools.partial(forward_kernel, n, (q_heads, kv_heads, seq, seq // 2)),
        out_shape=[
            shape(((count + 1) * model, width), low),
            shape((seq, q_wide), full),
            shape((seq, q_heads * HD), low),
            shape((half, model), full),
            shape((3, model, seq), low),
            shape((count, seq, width), low),
            shape((1, model), full),
            shape((1, model), full),
            shape((2, HD), full),
            shape((2, seq, HD), full),
            shape((seq, 1), jnp.int32),
        ],
        in_specs=[place(vmem)] * 14,
        out_specs=[place(k) for k in (hbm, hbm, vmem, vmem, hbm, *[vmem] * 6)],
        scratch_shapes=[
            vmem((seq, model), low),
            vmem((seq, model), low),
            vmem((seq, model), low),
            vmem((model, width - q_wide), low),
            vmem((2, model, 256), low),
            vmem((dp, 8, 128), full),
            vmem((2, seq, HD), low),
            vmem((half, model), low),
            vmem((half, model), low),
            vmem((count, seq, width), full),
            vmem((2, 2, 2 * rows, width // 2), low),
            vmem((2, 256, seq), low),
            dma((count + 2, 2)),
            dma((count + 2, 2, n)),
            dma((count + 2, 2, n)),
            dma((count + 2, 2, n)),
            dma((count + 2, 2, n)),
            dma((4, 2)),
            dma((2, 2)),
            dma((2,)),
            dma((2,)),
            dma((4, n)),
            vmem((rows, width), low),
        ],
        compiler_params=pltpu.CompilerParams(
            collective_id=1, has_side_effects=True, vmem_limit_bytes=67043328
        ),
    )(*shards, tokens, cot, frequency, seg_row, *shares)


SLOTS = 3


def undo(incoming, hat, inverse, gain, cosine, sine):
    turned = incoming * cosine - turn(incoming) * sine
    total = jnp.sum(turned * hat, axis=0, keepdims=True)
    scaled = turned * gain
    raw = inverse * (scaled - hat * jnp.mean(scaled * hat, axis=-1, keepdims=True))
    return total, raw.astype(jnp.bfloat16)


def attend_back(group, dims, heads, tab, seg_col, seg_row, gains, d_attn, d_proj, sums, kept):
    q_heads, kv_heads, seq, block = dims
    per_group = q_heads // kv_heads
    low = jnp.bfloat16
    scale = HD ** (-0.5)
    cosine, sine = tab[0], tab[1]
    keys = prepared(heads[per_group], gains[1:2, :], cosine, sine)[2]
    values = heads[per_group + 1].astype(low)
    for r in range(per_group):
        head = group * per_group + r
        q_inverse, q_hat, query = prepared(heads[r], gains[0:1, :], cosine, sine)
        for first in range(0, seq, block):
            width = first + block
            exps = exp_block(query[first:width], keys[:width], seg_col, seg_row, first)
            probs = exps / jnp.sum(exps, axis=-1, keepdims=True)
            incoming = d_attn[first:width, head_at(r)]
            d_probs = tail_product(incoming, values[:width])
            delta = jnp.sum(probs * d_probs, axis=-1, keepdims=True)
            d_scores = (probs * (d_probs - delta)).astype(low)
            kept[0, first:width, :] = product(d_scores, keys[:width]) * scale
            d_keys = lead_product(d_scores, query[first:width])
            d_values = lead_product(probs.astype(low), incoming)
            if r == 0 and first == 0:
                kept[1] = jnp.zeros_like(kept[1])
                kept[2] = jnp.zeros_like(kept[2])
            kept[1, :width, :] += d_keys
            kept[2, :width, :] += d_values
        total, raw = undo(kept[0], q_hat, q_inverse, gains[0:1, :], cosine, sine)
        sums[0:1, :] += total
        d_proj[0, :, head_at(head)] = raw
    k_inverse, k_hat, _ = prepared(heads[per_group], gains[1:2, :], cosine, sine)
    total, raw = undo(kept[1] * scale, k_hat, k_inverse, gains[1:2, :], cosine, sine)
    sums[1:2, :] += total
    d_proj[1, :, head_at(group)] = raw
    d_proj[1, :, head_at(kv_heads + group)] = kept[2].astype(low)


def reducer(n, pos, core, nexts, mate, rights, outs, fetch_left, scratch, stage_of):
    lefts, mine, term, give, take, ship, land, give_sem, take_sem, ship_sem, land_sem, free_sem, out_sem = scratch
    before, sends_before, sends_total = stage_of
    count = rights.shape[0]
    wide = rights.shape[2] // 2
    rows = outs[0].shape[0]
    span = pl.ds(0, wide)

    def owner_of(side, step):
        if side == 0:
            return (pos - 1 - step + 2 * n) % n
        return (pos + 1 + step) % n

    def given(m, side, step):
        slot = (before + step) % 2
        return remote(
            give.at[m, side, :, span], take.at[m, side, slot, :, span],
            give_sem.at[m, side], take_sem.at[m, side, slot], mate,
        )

    def shipped(m, side, step):
        slot = (sends_before + step) % SLOTS
        return remote(
            ship.at[m, side, :, span], land.at[m, side, slot, :, span],
            ship_sem.at[m, side], land_sem.at[m, side, slot], nexts[side],
        )

    def fetch(m, step):
        for side in range(2):
            start = pl.multiple_of(chip_at(owner_of(side, step), n) * 2 * rows, 2 * rows)
            fetch_left(m, side, pl.ds(start, 2 * rows))

    def early(m, step):
        for side in range(2):
            fetch_left(m, side, None)
        for side in range(2):
            tile = min(512, wide)

            def one(i, carry):
                there = pl.multiple_of(i * tile, tile)
                term[:, pl.ds(there, tile)] = product(
                    lefts[side], rights[m, :, pl.ds(pl.multiple_of(side * wide + there, tile), tile)]
                )
                return carry

            lax.fori_loop(0, wide // tile, one, 0)

            @pl.when(step >= 1)
            def _():
                given(m, side, step - 1).wait_send()

            other = term[pl.ds(pl.multiple_of((1 - core) * rows, rows), rows), span]
            give[m, side, :, span] = other.astype(jnp.bfloat16)
            given(m, side, step).start()
            mine[m, side, :, span] = term[pl.ds(pl.multiple_of(core * rows, rows), rows), span]

    def event(e):
        step, m = e // count, e % count

        @pl.when(step < n - 1)
        def _():
            fetch(m, step + 1)

        for side in range(2):
            given(m, side, step).wait_recv()
            near = take[m, side, (before + step) % 2, :, span].astype(jnp.float32)

            @pl.when(step == 0)
            def _():
                mine[m, side, :, span] += near

            @pl.when(step > 0)
            def _():
                shipped(m, side, step - 1).wait_recv()
                far = land[m, side, (sends_before + step - 1) % SLOTS, :, span].astype(jnp.float32)
                mine[m, side, :, span] += near + far

                @pl.when(sends_before + step - 1 + SLOTS < sends_total)
                def _():
                    pl.semaphore_signal(
                        free_sem.at[m, side], inc=1, device_id=nexts[1 - side], device_id_type=MESH
                    )

                shipped(m, side, step - 1).wait_send()

            @pl.when(step < n - 1)
            def _():
                @pl.when(sends_before + step >= SLOTS)
                def _():
                    pl.semaphore_wait(free_sem.at[m, side], 1)

                ship[m, side, :, span] = mine[m, side, :, span].astype(jnp.bfloat16)
                shipped(m, side, step).start()

            @pl.when(step == n - 1)
            def _():
                for i in range(count):
                    @pl.when(m == i)
                    def _():
                        written(m, side, i).start()

        @pl.when(step < n - 1)
        def _():
            early(m, step + 1)

    def written(m, side, i):
        return pltpu.make_async_copy(
            mine.at[m, side, :, span], outs[i].at[:, pl.ds(side * wide, wide)], out_sem.at[m, side]
        )

    def begin(m):
        fetch(m, 0)
        early(m, 0)

    def finish(m):
        for side in range(2):
            given(m, side, n - 1).wait_send()
            written(m, side, 0).wait()

    return begin, event, finish


def backward_kernel(n, dims, *refs):
    (
        flipped, act, weights, qkv, attn, cot, tokens, resid, tab, seg_col, seg_row, gains, attn_gain, mlp_gain,
        grad_gate, grad_up, grad_down, grad_query, grad_pair, grad_out, result, input_grad, gain_out, d_flip,
        d_proj, d_full, d_resid, blocks, columns, own, part, peer, d_attn, heads, kept, stage,
        attn_sum, mlp_sum, qk_sum, table, others, inbox,
        swap_sem, load_sem, head_sem, attn_sem, stage_sem, column_sem, trade_sem, post_sem, mail_sem, left_sem,
        *scratch,
    ) = refs
    q_heads, kv_heads, seq, block = dims
    pos, core = ring_place(n)
    me = lax.axis_index("dp")
    lane = lax.axis_index("tensor")
    nexts = (at((pos + 1) % n, core, n), at((pos + n - 1) % n, core, n))
    mate = at(pos, 1 - core, n)
    twin = (me, 1 - lane)
    fetch_attn = pltpu.make_async_copy(attn, d_proj.at[2], attn_sem.at[0])
    fetch_attn.start()
    barrier = pltpu.get_barrier_semaphore()

    def greet(o, carry):
        pl.semaphore_signal(barrier, inc=1, device_id=at((pos + o) % n, core, n), device_id_type=MESH)
        return carry

    lax.fori_loop(1, n, greet, 0)
    for other in (mate, twin):
        pl.semaphore_signal(barrier, inc=1, device_id=other, device_id_type=MESH)
    pl.semaphore_wait(barrier, n + 1)
    count, _, hidden = act.shape
    half, model = resid.shape
    q_wide = qkv.shape[1]
    per_group = q_heads // kv_heads
    lefts = scratch[0]

    def from_flipped(first):
        def fetch_left(m, side, there):
            if there is None:
                pltpu.make_async_copy(
                    flipped.at[0, pl.ds(0, lefts.shape[1])], lefts.at[side], left_sem.at[side]
                ).wait()
            elif first == 0:
                pltpu.make_async_copy(flipped.at[m // 2, there], lefts.at[side], left_sem.at[side]).start()
            else:
                @pl.when(m < 2)
                def _():
                    pltpu.make_async_copy(flipped.at[2, there], lefts.at[side], left_sem.at[side]).start()

                @pl.when(m == 2)
                def _():
                    pltpu.make_async_copy(d_flip.at[there], lefts.at[side], left_sem.at[side]).start()

        return fetch_left

    links = (n, pos, core, nexts, mate)
    begin, event, finish = reducer(
        *links, act, (grad_gate, grad_up, grad_down), from_flipped(0), scratch, (0, 0, 2 * (n - 1))
    )
    late_begin, late_event, late_finish = reducer(
        *links, d_proj, (grad_query, grad_pair, grad_out), from_flipped(2), scratch, (n, n - 1, 2 * (n - 1))
    )
    deep = blocks.shape[1]
    turns = model // deep

    def fetch(which, i, slot, width):
        start = which * model + i * deep
        return pltpu.make_async_copy(
            weights.at[pl.ds(pl.multiple_of(start, deep), deep), pl.ds(0, width)],
            blocks.at[slot, :, pl.ds(0, width)], load_sem.at[slot],
        )

    def first_m(m, carry):
        begin(m)
        return carry

    lax.fori_loop(0, count, first_m, 0)
    fetch(1, 0, 0, hidden).start()
    fetch(2, 0, 1, hidden).start()
    def run(first, last):
        def one(e, carry):
            event(e)
            return carry

        lax.fori_loop(first, last, one, 0)

    run(0, count)
    theirs = pl.ds(pl.multiple_of((1 - lane) * half, half), half)
    ours = pl.ds(pl.multiple_of(lane * half, half), half)
    done = count

    def events(number):
        nonlocal done
        run(done, done + number)
        done = done + number

    def send_part(slot, target, i):
        return remote(part.at[slot], target, swap_sem.at[i, 0], swap_sem.at[i, 1], twin)

    def dn_two(i, carry):
        there = pl.ds(pl.multiple_of(i * deep, deep), deep)
        for which in range(2):
            fetch(which + 1, i, which, hidden).wait()
            other = tail_product(act[which, theirs, :], blocks[which])
            same = tail_product(act[which, ours, :], blocks[which])
            if which == 0:
                own[:, there] = same
                d_resid[:, there] = other
            else:
                own[:, there] += same
                part[0, :, there] = (d_resid[:, there] + other).astype(jnp.bfloat16)

            @pl.when(i < turns - 1)
            def _():
                fetch(which + 1, i + 1, which, hidden).start()

        @pl.when(i % 4 == 3)
        def _():
            event(count + i // 4)

        return carry

    lax.fori_loop(0, turns, dn_two, 0)
    done = done + turns // 4
    sends = [send_part(0, peer.at[0], 0)]
    sends[0].start()
    fetch(3, 0, 0, hidden).start()
    events(3)
    sends[0].wait_recv()
    sends[0].wait_send()
    strip = 32

    def over_strips(body):
        lax.fori_loop(0, half // strip, body, 0)

    def gather_sum(target, i, total):
        @pl.when(i == 0)
        def _():
            target[...] = total

        @pl.when(i > 0)
        def _():
            target[...] += total

    def norm_two(i, carry):
        there = pl.ds(pl.multiple_of(i * strip, strip), strip)
        incoming = own[there, :] + peer[0, there, :].astype(jnp.float32)
        values = resid[there, :]
        inverse = row_scale(values)
        normed = values * inverse
        scaled = incoming * mlp_gain[...]
        change = cot[there, :].astype(jnp.float32) + inverse * (
            scaled - normed * jnp.mean(scaled * normed, axis=-1, keepdims=True)
        )
        d_resid[there, :] = change
        part[0, there, :] = change.astype(jnp.bfloat16)
        gather_sum(mlp_sum, i, jnp.sum(incoming * normed, axis=0, keepdims=True))
        return carry

    over_strips(norm_two)
    sends.append(send_part(0, d_full.at[ours], 1))
    sends[1].start()
    d_full[ours, :] = part[0]

    def narrow(which, width, slot, base, every, rows_of):
        def one(i, carry):
            @pl.when(i < turns - 1)
            def _():
                fetch(which, i + 1, (i + 1) % 2, width).start()

            fetch(which, i, i % 2, width).wait()
            there = pl.ds(pl.multiple_of(i * deep, deep), deep)
            for rows, mine in ((theirs, False), (ours, True)):
                total = None
                for left, start in rows_of(rows):
                    gained = tail_product(left, blocks[i % 2, :, pl.ds(start, left.shape[1])])
                    total = gained if total is None else total + gained
                if mine:
                    own[:, there] = total
                else:
                    part[slot, :, there] = total.astype(jnp.bfloat16)

            @pl.when(i % every == every - 1)
            def _():
                event(base + i // every)

            return carry

        lax.fori_loop(0, turns, one, 0)

    narrow(3, hidden, 1, done, 4, lambda rows: [(act[2, rows, :], 0)])
    done = done + turns // 4
    sends.append(send_part(1, peer.at[1], 2))
    sends[2].start()
    group_wide = per_group * HD

    def fetch_columns(g):
        return pltpu.make_async_copy(
            weights.at[pl.ds(0, model), pl.ds(pl.multiple_of(q_wide + g * group_wide, group_wide), group_wide)],
            columns.at[g % 2], column_sem.at[g % 2],
        )

    fetch_columns(0).start()
    events(2)
    remote(part.at[0], d_full.at[theirs], swap_sem.at[1, 0], swap_sem.at[1, 1], twin).wait_recv()
    flip_into(d_full, d_flip, stage, stage_sem)
    qk_sum[...] = jnp.zeros_like(qk_sum)
    fetch_attn.wait()

    def group_step(group, carry):
        places = [group * per_group + r for r in range(per_group)]
        places += [q_heads + group, q_heads + kv_heads + group]
        copies = [
            pltpu.make_async_copy(qkv.at[:, head_at(place)], heads.at[i], head_sem.at[i])
            for i, place in enumerate(places)
        ]
        for copy in copies:
            copy.start()

        @pl.when(group < kv_heads - 1)
        def _():
            fetch_columns(group + 1).start()

        fetch_columns(group).wait()
        d_attn[...] = product(d_full[...], columns[group % 2]).astype(jnp.bfloat16)
        for copy in copies:
            copy.wait()
        attend_back(group, dims, heads, tab, seg_col, seg_row, gains, d_attn, d_proj, qk_sum, kept)
        event(done + group)
        return carry

    lax.fori_loop(0, kv_heads, group_step, 0)
    done = done + kv_heads
    sends[2].wait_recv()

    def last_strip(i, carry):
        there = pl.ds(pl.multiple_of(i * strip, strip), strip)
        result[there, :] = (
            resid[there, :] + (own[there, :] + peer[1, there, :].astype(jnp.float32))
        ).astype(jnp.bfloat16)
        return carry

    over_strips(last_strip)
    fetch(0, 0, 0, q_wide).start()
    sends[1].wait_send()
    events(1)
    width = d_proj.shape[2]
    narrow(0, q_wide, 0, done, 8, lambda rows: [(d_proj[0, rows, :], 0), (d_proj[1, rows, :], width)])
    done = done + turns // 8
    sends.append(send_part(0, peer.at[0], 3))
    sends[3].start()
    events(3)
    sends[3].wait_recv()

    def norm_one(i, carry):
        there = pl.ds(pl.multiple_of(i * strip, strip), strip)
        incoming = own[there, :] + peer[0, there, :].astype(jnp.float32)
        values = tokens[there, :].astype(jnp.float32)
        inverse = row_scale(values)
        normed = values * inverse
        scaled = incoming * attn_gain[...]
        change = d_resid[there, :] + inverse * (
            scaled - normed * jnp.mean(scaled * normed, axis=-1, keepdims=True)
        )
        input_grad[there, :] = change.astype(jnp.bfloat16)
        gather_sum(attn_sum, i, jnp.sum(incoming * normed, axis=0, keepdims=True))
        return carry

    over_strips(norm_one)
    dp = 2 * n
    share, head_share = model // dp, 2 * HD // dp
    table[...] = jnp.zeros_like(table)
    for d in range(dp):
        start = d * share // 128 * 128
        row = d * head_share // HD
        table[d, 0:1, :] = attn_sum[:, start : start + 128]
        table[d, 1:2, :] = mlp_sum[:, start : start + 128]
        table[d, 2:3, :] = qk_sum[row : row + 1, :]
    def trade(i, carry):
        partner = ((1 - i) * me + i * mate[0], (1 - i) * twin[1] + i * lane)
        swap = remote(table, others.at[i], trade_sem.at[i, 0], trade_sem.at[i, 1], partner)
        swap.start()
        swap.wait()
        table[...] += others[i]
        return carry

    lax.fori_loop(0, 2, trade, 0)

    def mail(o, target):
        return remote(table.at[target], inbox.at[o], post_sem.at[o], mail_sem.at[o], at((pos + o) % n, core, n))

    def post(o, carry):
        mail(o, chip_at((pos + o) % n, n) * 2 + core).start()
        return carry

    lax.fori_loop(1, n, post, 0)

    last = count * (n - 1)
    run(done, last)

    def hand_over(m, carry):
        event(last + m)
        finish(m)
        late_begin(m)
        late_event(m)
        return carry

    lax.fori_loop(0, count, hand_over, 0)
    gain_out[...] = table[me]

    def collect(o, carry):
        mail(o, 0).wait_recv()
        gain_out[...] += inbox[o]
        return carry

    lax.fori_loop(1, n, collect, 0)

    def late_rest(e, carry):
        late_event(e)
        return carry

    lax.fori_loop(count, count * n, late_rest, 0)
    for m in range(count):
        late_finish(m)
    sends[2].wait_send()
    sends[3].wait_send()

    def sent(o, carry):
        mail(o, 0).wait_send()
        return carry

    lax.fori_loop(1, n, sent, 0)


def backward_block(
    flipped, act, weights, qkv, attn, cot, tokens, resid, tab, seg_col, seg_row, gains, attn_gain, mlp_gain,
    q_heads, kv_heads, dp,
):
    n = dp // 2
    count, seq, hidden = act.shape
    half, model = resid.shape
    rows = model // dp
    wide = hidden // 2
    width = q_heads * HD
    low, full, dma, vmem, hbm = jnp.bfloat16, jnp.float32, pltpu.SemaphoreType.DMA, pltpu.VMEM, pltpu.HBM
    shape = jax.ShapeDtypeStruct
    place = lambda kind: pl.BlockSpec(memory_space=kind)
    per_group = q_heads // kv_heads
    return pl.pallas_call(
        functools.partial(backward_kernel, n, (q_heads, kv_heads, seq, seq // 2)),
        out_shape=[
            *[shape((rows, hidden), full)] * 3,
            *[shape((rows, width), full)] * 3,
            shape((half, model), low),
            shape((half, model), low),
            shape((8, 128), full),
            shape((model, seq), low),
        ],
        in_specs=[place(k) for k in (hbm, vmem, hbm, hbm, hbm, *[vmem] * 9)],
        out_specs=[place(k) for k in (*[hbm] * 6, vmem, vmem, vmem, hbm)],
        scratch_shapes=[
            vmem((3, seq, width), low),
            vmem((seq, model), low),
            vmem((half, model), full),
            vmem((2, 256, hidden), low),
            vmem((2, model, per_group * HD), low),
            vmem((half, model), full),
            vmem((2, half, model), low),
            vmem((2, half, model), low),
            vmem((seq, per_group * HD), low),
            vmem((per_group + 2, seq, HD), full),
            vmem((3, seq, HD), full),
            vmem((2, 256, seq), low),
            vmem((1, model), full),
            vmem((1, model), full),
            vmem((8, HD), full),
            vmem((dp, 8, 128), full),
            vmem((2, dp, 8, 128), full),
            vmem((n, 8, 128), full),
            dma((4, 2)),
            dma((2,)),
            dma((per_group + 2,)),
            dma((1,)),
            dma((2,)),
            dma((2,)),
            dma((2, 2)),
            dma((n,)),
            dma((n,)),
            dma((2,)),
            vmem((2, 2 * rows, seq), low),
            vmem((count, 2, rows, wide), full),
            vmem((2 * rows, wide), full),
            vmem((count, 2, rows, wide), low),
            vmem((count, 2, 2, rows, wide), low),
            vmem((count, 2, rows, wide), low),
            vmem((count, 2, SLOTS, rows, wide), low),
            dma((count, 2)),
            dma((count, 2, 2)),
            dma((count, 2)),
            dma((count, 2, SLOTS)),
            pltpu.SemaphoreType.REGULAR((count, 2)),
            dma((count, 2)),
        ],
        compiler_params=pltpu.CompilerParams(
            collective_id=2, has_side_effects=True, vmem_limit_bytes=67043328
        ),
    )(
        flipped, act, weights, qkv, attn, cot, tokens, resid, tab, seg_col, seg_row, gains, attn_gain, mlp_gain,
    )


def finishing_kernel(dp, *refs):
    gains = refs[0]
    sources, outs = refs[1:9], refs[9:21]
    bufs, turned, in_sem, out_sem = refs[21:29], refs[29:31], refs[31], refs[32]
    loads = [pltpu.make_async_copy(source, buf, in_sem.at[i]) for i, (source, buf) in enumerate(zip(sources, bufs))]
    for i in (2, 6, 7, 5, 3, 4, 0, 1):
        loads[i].start()
    half = outs[3].shape[1]
    stores = [None] * 9

    def store(i, buf, out):
        stores[i] = pltpu.make_async_copy(buf, out, out_sem.at[i])
        stores[i].start()

    def turn_over(i, which, out):
        loads[which].wait()
        turned[i][...] = bufs[which][...].T
        store(7 + i, turned[i], outs[out])

    turn_over(0, 2, 8)
    for i, (which, out) in enumerate(((6, 0), (7, 1))):
        loads[which].wait()
        store(i, bufs[which], outs[out])
    turn_over(1, 5, 5)
    for i, (which, out) in enumerate(((3, 2), (0, 6), (1, 7))):
        loads[which].wait()
        store(2 + i, bufs[which], outs[out])
    loads[4].wait()
    store(5, bufs[4].at[:, pl.ds(0, half)], outs[3])
    store(6, bufs[4].at[:, pl.ds(half, half)], outs[4])
    me = lax.axis_index("dp")
    for row in range(3):
        target = outs[9 + row]
        size = target.shape[1]
        line = gains[row : row + 1, :]
        if size % 128:
            line = pltpu.roll(line, (128 - me * size % 128) % 128, 1)
        target[...] = line[:, :size]
    for copy in stores:
        copy.wait()


def finishing_block(gains, arrays, shapes, dp):
    full, dma, vmem, hbm = jnp.float32, pltpu.SemaphoreType.DMA, pltpu.VMEM, pltpu.HBM
    place = lambda kind: pl.BlockSpec(memory_space=kind)
    return pl.pallas_call(
        functools.partial(finishing_kernel, dp),
        out_shape=shapes,
        in_specs=[place(vmem)] + [place(hbm)] * 8,
        out_specs=[place(hbm)] * 9 + [place(vmem)] * 3,
        scratch_shapes=[
            *[vmem(a.shape, a.dtype) for a in arrays],
            vmem(arrays[2].shape[::-1], full),
            vmem(arrays[5].shape[::-1], full),
            dma((8,)),
            dma((9,)),
        ],
        compiler_params=pltpu.CompilerParams(vmem_limit_bytes=67043328),
    )(gains, *arrays)


def on_device(
    tokens,
    seg_ids,
    w_query,
    w_key,
    w_value,
    w_output,
    w_gate,
    w_up,
    w_down,
    gain_attn,
    gain_mlp,
    gain_qk,
    cotangent,
):
    dp = lax.axis_size("dp")
    q_heads = w_query.shape[1] // HD
    kv_heads = w_key.shape[1] // HD
    places = np.arange(HD) % (HD // 2) * 2
    frequency = jnp.asarray((rope_base ** (-places / HD)).astype(np.float32)[None, :])
    (
        weights, projected, attn_rows, resid, flipped, act, attn_gain, mlp_gain, pair, rope_tab, seg_col,
    ) = forward_block(
        (w_query, w_key, w_value, w_output.T, w_gate, w_up, w_down),
        tokens,
        cotangent,
        frequency,
        seg_ids,
        [g[None, :] for g in (gain_attn, gain_mlp, gain_qk)],
        q_heads,
        kv_heads,
        dp,
    )
    (
        grad_gate, grad_up, grad_down, grad_query, grad_pair, grad_out, result_rows, input_grad, gain_sums, _,
    ) = backward_block(
        flipped,
        act,
        weights,
        projected,
        attn_rows,
        cotangent,
        tokens,
        resid,
        rope_tab,
        seg_col,
        seg_ids,
        pair,
        attn_gain,
        mlp_gain,
        q_heads,
        kv_heads,
        dp,
    )
    full = jnp.float32
    shapes = [jax.ShapeDtypeStruct(tokens.shape, jnp.bfloat16)] * 2
    shapes += [
        jax.ShapeDtypeStruct(w.shape, full)
        for w in (w_query, w_key, w_value, w_output, w_gate, w_up, w_down)
    ]
    shapes += [jax.ShapeDtypeStruct((1, g.shape[0]), full) for g in (gain_attn, gain_mlp, gain_qk)]
    outs = finishing_block(
        gain_sums,
        [grad_gate, grad_up, grad_down, grad_query, grad_pair, grad_out, result_rows, input_grad],
        shapes,
        dp,
    )
    return (*outs[:9], *(g.reshape(-1) for g in outs[9:]))


def solution(mesh):
    return jax.shard_map(
        on_device,
        mesh=mesh,
        in_specs=(
            P(("dp", "tensor"), None),
            P("dp", None),
            P("dp", "tensor"),
            P("dp", "tensor"),
            P("dp", "tensor"),
            P("tensor", "dp"),
            P("dp", "tensor"),
            P("dp", "tensor"),
            P("tensor", "dp"),
            P("dp"),
            P("dp"),
            P("dp"),
            P(("dp", "tensor"), None),
        ),
        out_specs=(
            P(("dp", "tensor"), None),
            P(("dp", "tensor"), None),
            P("dp", "tensor"),
            P("dp", "tensor"),
            P("dp", "tensor"),
            P("tensor", "dp"),
            P("dp", "tensor"),
            P("dp", "tensor"),
            P("tensor", "dp"),
            P("dp"),
            P("dp"),
            P("dp"),
        ),
        check_vma=False,
    )
```
